16 devices in a mesh: tp: 2 (over z), ep: 8 (over y, x, core).
Axes of the slice: x: 2, y: 2, z: 2, core: 2. Of those that a mesh axis runs over, the one named last changes fastest.
Arguments:
- act_in: bfloat16 [4096, 1536], P('ep')
- w_router: float32 [1536, 64], replicated
- choice_one: int32 [4096], P('ep')
- choice_two: int32 [4096], P('ep')
- w_gelu: bfloat16 [64, 1536, 512], P('ep', None, 'tp')
- w_lin: bfloat16 [64, 1536, 512], P('ep', None, 'tp')
- w_out: bfloat16 [64, 512, 1536], P('ep', 'tp')
- grad_out: bfloat16 [4096, 1536], P('ep')
Outputs:
- output 1: bfloat16 [4096, 1536], P('ep')
- output 2: bfloat16 [4096, 1536], P('ep')
- output 3: float32 [64, 1536, 512], P('ep', None, 'tp')
- output 4: float32 [64, 1536, 512], P('ep', None, 'tp')
- output 5: float32 [64, 512, 1536], P('ep', 'tp')
- output 6: float32 [1536, 64], replicated
All inputs are finite; a program needn't handle non-finite values.
Results may differ from the reference program's by a relative error of at most 0.00999651.
Values are sent between devices in bfloat16 or wider.
A program may use at most 1 GiB of HBM per device.

```python
import jax
import jax.numpy as jnp
from jax import lax

D = 1536
FF = 512
EXPERTS = 64
TOKENS = 512
EP_SIZE = 8
TP_SIZE = 2
ALL_TOKENS = EP_SIZE * TOKENS
SLOT_CAP = 2 * TOKENS // EXPERTS
PIECE_W = FF // TP_SIZE
EXP_ROWS = EP_SIZE * SLOT_CAP
ALL_SLOTS = EXPERTS * SLOT_CAP
GELU_COEF = 0.7978845608028654


def gelu_parts(pre_act):
    inner_arg = GELU_COEF * (pre_act + 0.044715 * pre_act * pre_act * pre_act)
    tanh_val = jnp.tanh(inner_arg)
    gelu_val = 0.5 * pre_act * (1.0 + tanh_val)
    gelu_slope = 0.5 * (1.0 + tanh_val) + 0.5 * pre_act * (1.0 - tanh_val * tanh_val) * GELU_COEF * (1.0 + 0.134145 * pre_act * pre_act)
    return gelu_val, gelu_slope


def draw_choices(base_key):
    key_a, key_b, key_c, key_d = jax.random.split(base_key, 4)
    draws_a = jax.random.randint(key_a, (ALL_TOKENS,), 0, EXPERTS, dtype=jnp.int32)
    draws_b = jax.random.randint(key_b, (ALL_TOKENS,), 0, EXPERTS, dtype=jnp.int32)
    skewed = ((draws_a + 1) * (draws_b + 1) - 1) // EXPERTS
    shifts = jax.random.randint(key_c, (EP_SIZE, 1), 0, EXPERTS, dtype=jnp.int32)
    first_ids = ((skewed.reshape(EP_SIZE, TOKENS) + shifts) % EXPERTS).reshape(ALL_TOKENS)
    first_ids = jnp.concatenate([jnp.arange(EXPERTS, dtype=jnp.int32), first_ids[EXPERTS:]])
    hop_ids = jax.random.randint(key_d, (ALL_TOKENS,), 1, EXPERTS, dtype=jnp.int32)
    second_ids = (first_ids + hop_ids) % EXPERTS
    return first_ids.astype(jnp.int32), second_ids.astype(jnp.int32)


def setup_inputs(seed: int = 0) -> dict:
    key_list = jax.random.split(jax.random.key(seed), 7)
    in_scale = D ** -0.5
    out_scale = FF ** -0.5
    act_in = jax.random.normal(key_list[0], (ALL_TOKENS, D), jnp.float32).astype(jnp.bfloat16)
    w_router = 0.5 * in_scale * jax.random.normal(key_list[1], (D, EXPERTS), jnp.float32)
    choice_one, choice_two = draw_choices(key_list[2])
    w_gelu = (in_scale * jax.random.normal(key_list[3], (EXPERTS, D, FF), jnp.float32)).astype(jnp.bfloat16)
    w_lin = (in_scale * jax.random.normal(key_list[4], (EXPERTS, D, FF), jnp.float32)).astype(jnp.bfloat16)
    w_out = (out_scale * jax.random.normal(key_list[5], (EXPERTS, FF, D), jnp.float32)).astype(jnp.bfloat16)
    grad_out = jax.random.normal(key_list[6], (ALL_TOKENS, D), jnp.float32).astype(jnp.bfloat16)
    return {"act_in": act_in, "w_router": w_router, "choice_one": choice_one, "choice_two": choice_two, "w_gelu": w_gelu, "w_lin": w_lin, "w_out": w_out, "grad_out": grad_out}


def route_shard(x_rows, w_router, first_ids, second_ids):
    logits = jnp.dot(x_rows.astype(jnp.float32), w_router)
    router_prob = jax.nn.softmax(logits, axis=-1)
    expert_ids = jnp.arange(EXPERTS, dtype=jnp.int32)
    hot_one = (first_ids[:, None] == expert_ids[None, :]).astype(jnp.int32)
    hot_two = (second_ids[:, None] == expert_ids[None, :]).astype(jnp.int32)
    prob_one = jnp.sum(router_prob * hot_one, axis=-1)
    prob_two = jnp.sum(router_prob * hot_two, axis=-1)
    fill_one = jnp.sum(hot_one, axis=0)
    pos_one = jnp.sum((jnp.cumsum(hot_one, axis=0) - hot_one) * hot_one, axis=-1)
    pos_two = jnp.sum((jnp.cumsum(hot_two, axis=0) - hot_two + fill_one[None, :]) * hot_two, axis=-1)
    slot_one = jnp.where(pos_one < SLOT_CAP, first_ids * SLOT_CAP + pos_one, ALL_SLOTS)
    slot_two = jnp.where(pos_two < SLOT_CAP, second_ids * SLOT_CAP + pos_two, ALL_SLOTS)
    gate_sum = prob_one + prob_two
    return (router_prob, hot_one, hot_two, prob_one, prob_two, prob_one / gate_sum, prob_two / gate_sum, slot_one, slot_two)


def fill_slots(slot_one, slot_two, gate_one, gate_two):
    token_rows = jnp.arange(TOKENS, dtype=jnp.int32)
    source = jnp.full((ALL_SLOTS,), TOKENS, jnp.int32).at[slot_one].set(token_rows, mode="drop").at[slot_two].set(token_rows, mode="drop")
    weight = jnp.zeros((ALL_SLOTS,), jnp.float32).at[slot_one].set(gate_one, mode="drop").at[slot_two].set(gate_two, mode="drop")
    return source, weight


def dispatch_shard(shard_args, w_router):
    x_rows, first_ids, second_ids, dy_rows = shard_args
    routed = route_shard(x_rows, w_router, first_ids, second_ids)
    source, weight = fill_slots(routed[7], routed[8], routed[5], routed[6])
    disp_rows = jnp.take(x_rows, source, axis=0, mode="fill", fill_value=0)
    dout_rows = (weight[:, None] * jnp.take(dy_rows, source, axis=0, mode="fill", fill_value=0).astype(jnp.float32)).astype(jnp.bfloat16)
    return disp_rows.reshape(EXPERTS, SLOT_CAP, D), dout_rows.reshape(EXPERTS, SLOT_CAP, D)


def expert_pass(expert_args):
    disp_rows, dout_rows, w_a, w_b, w_c = expert_args
    pre_a = jnp.dot(disp_rows, w_a, preferred_element_type=jnp.float32)
    pre_b = jnp.dot(disp_rows, w_b, preferred_element_type=jnp.float32)
    gelu_val, gelu_slope = gelu_parts(pre_a)
    hidden = (gelu_val * pre_b).astype(jnp.bfloat16)
    part_out = jnp.einsum("rkf,kfd->krd", hidden.reshape(EXP_ROWS, TP_SIZE, PIECE_W).astype(jnp.float32), w_c.reshape(TP_SIZE, PIECE_W, D).astype(jnp.float32))
    merged = jnp.sum(part_out.astype(jnp.bfloat16).astype(jnp.float32), axis=0).astype(jnp.bfloat16)
    grad_hidden = jnp.dot(dout_rows, w_c.T, preferred_element_type=jnp.float32)
    grad_a = (grad_hidden * pre_b * gelu_slope).astype(jnp.bfloat16)
    grad_b = (grad_hidden * gelu_val).astype(jnp.bfloat16)
    grad_wc = jnp.dot(hidden.T, dout_rows, preferred_element_type=jnp.float32)
    grad_wa = jnp.dot(disp_rows.T, grad_a, preferred_element_type=jnp.float32)
    grad_wb = jnp.dot(disp_rows.T, grad_b, preferred_element_type=jnp.float32)
    part_in = jnp.einsum("rkf,dkf->krd", grad_a.reshape(EXP_ROWS, TP_SIZE, PIECE_W).astype(jnp.float32), w_a.reshape(D, TP_SIZE, PIECE_W).astype(jnp.float32)) + jnp.einsum("rkf,dkf->krd", grad_b.reshape(EXP_ROWS, TP_SIZE, PIECE_W).astype(jnp.float32), w_b.reshape(D, TP_SIZE, PIECE_W).astype(jnp.float32))
    grad_disp = jnp.sum(part_in.astype(jnp.bfloat16).astype(jnp.float32), axis=0).astype(jnp.bfloat16)
    return merged, grad_disp, grad_wa, grad_wb, grad_wc


def combine_shard(shard_args, w_router):
    x_rows, first_ids, second_ids, dy_rows, merged_rows, grad_rows = shard_args
    (router_prob, hot_one, hot_two, prob_one, prob_two, gate_one, gate_two, slot_one, slot_two) = route_shard(x_rows, w_router, first_ids, second_ids)
    out_one = jnp.take(merged_rows, slot_one, axis=0, mode="fill", fill_value=0).astype(jnp.float32)
    out_two = jnp.take(merged_rows, slot_two, axis=0, mode="fill", fill_value=0).astype(jnp.float32)
    act_out = (gate_one[:, None] * out_one + gate_two[:, None] * out_two).astype(jnp.bfloat16)
    dy_f32 = dy_rows.astype(jnp.float32)
    dgate_one = jnp.sum(dy_f32 * out_one, axis=-1)
    dgate_two = jnp.sum(dy_f32 * out_two, axis=-1)
    shared = dgate_one * gate_one + dgate_two * gate_two
    gate_sum = prob_one + prob_two
    dprob_one = (dgate_one - shared) / gate_sum
    dprob_two = (dgate_two - shared) / gate_sum
    centre = dprob_one * prob_one + dprob_two * prob_two
    grad_logits = router_prob * (dprob_one[:, None] * hot_one + dprob_two[:, None] * hot_two - centre[:, None])
    back_one = jnp.take(grad_rows, slot_one, axis=0, mode="fill", fill_value=0).astype(jnp.float32)
    back_two = jnp.take(grad_rows, slot_two, axis=0, mode="fill", fill_value=0).astype(jnp.float32)
    grad_in = (back_one + back_two + jnp.dot(grad_logits, w_router.T)).astype(jnp.bfloat16)
    return act_out, grad_in, grad_logits


def reference(act_in, w_router, choice_one, choice_two, w_gelu, w_lin, w_out, grad_out):
    x_shards = act_in.reshape(EP_SIZE, TOKENS, D)
    dy_shards = grad_out.reshape(EP_SIZE, TOKENS, D)
    first_sh = choice_one.reshape(EP_SIZE, TOKENS)
    second_sh = choice_two.reshape(EP_SIZE, TOKENS)

    def dispatch_step(shard_args):
        return dispatch_shard(shard_args, w_router)

    def combine_step(shard_args):
        return combine_shard(shard_args, w_router)

    disp_all, dout_all = lax.map(dispatch_step, (x_shards, first_sh, second_sh, dy_shards))
    disp_exp = disp_all.transpose(1, 0, 2, 3).reshape(EXPERTS, EXP_ROWS, D)
    dout_exp = dout_all.transpose(1, 0, 2, 3).reshape(EXPERTS, EXP_ROWS, D)
    merged, grad_disp, grad_gelu, grad_lin, grad_wout = lax.map(expert_pass, (disp_exp, dout_exp, w_gelu, w_lin, w_out))
    merged_tok = merged.reshape(EXPERTS, EP_SIZE, SLOT_CAP, D).transpose(1, 0, 2, 3).reshape(EP_SIZE, ALL_SLOTS, D)
    grad_tok = grad_disp.reshape(EXPERTS, EP_SIZE, SLOT_CAP, D).transpose(1, 0, 2, 3).reshape(EP_SIZE, ALL_SLOTS, D)
    act_out, grad_in, grad_logits = lax.map(combine_step, (x_shards, first_sh, second_sh, dy_shards, merged_tok, grad_tok))
    grad_router = jnp.einsum("td,te->de", act_in.astype(jnp.float32), grad_logits.reshape(ALL_TOKENS, EXPERTS))
    return (act_out.reshape(ALL_TOKENS, D), grad_in.reshape(ALL_TOKENS, D), grad_gelu, grad_lin, grad_wout, grad_router)
```

```python
import functools

import jax
import jax.numpy as jnp
from jax import lax
from jax.experimental import pallas as pl
from jax.experimental.pallas import tpu as pltpu
from jax.sharding import PartitionSpec as P

BF = jnp.bfloat16
F32 = jnp.float32
I32 = jnp.int32
MESH = pl.DeviceIdType.MESH
GELU_COEF = 0.7978845608028654
NN = (((1,), (0,)), ((), ()))
NT = (((1,), (1,)), ((), ()))
TN = (((0,), (0,)), ((), ()))


def dot(a, b, dims=NN):
    return lax.dot_general(a, b, dims, preferred_element_type=F32)


def split3(v):
    hi = v.astype(BF)
    rest = v - hi.astype(F32)
    mid = rest.astype(BF)
    low = (rest - mid.astype(F32)).astype(BF)
    return hi, mid, low


def moe_kernel(
    tp_size, ep_size, cap,
    ids1_ref, ids2_ref, x_hbm, dy_hbm, wr_hbm, wa_hbm, wb_hbm, wc_hbm,
    y_out, dx_out, dwr_out, xe_out, de_out, h_out, da_out, db_out,
    x_v, dy_v, wr_v, wa_v, wb_v, wc_v,
    xs, ds, xr, dr, h_v, da_v, db_v, bs_v, gv_v,
    ps, pr, pdr, orr, dxr, y_v, dx_v,
    s1r, s2r, g1r, g2r, s1c, s2c, g1c, g2c, q1c, q2c, i1c, i2c, prob_v, dl_v,
    dwp, dwi, dwf,
    in_sem, w_sem, out_sem,
    xs_sem, xr_sem, ds_sem, dr_sem,
    ps_sem, pr_sem, pds_sem, pdr_sem,
    os_sem, or_sem, dxs_sem, dxr_sem,
    ys_sem, yr_sem, dys_sem, dyr_sem,
    rs_sem, rr_sem, fs_sem, fr_sem,
):
    k = lax.axis_index("tp")
    r = lax.axis_index("ep")
    n_loc = wa_v.shape[0]
    n_tok, width = x_v.shape
    hid = wa_v.shape[2]
    n_exp = n_loc * ep_size
    blk = ep_size * cap
    half = ep_size // tp_size
    my_place = (r % tp_size) * half + r // tp_size
    owner = (r % tp_size) == k
    other = 1 - k

    ins = [
        pltpu.make_async_copy(x_hbm, x_v, in_sem.at[0]),
        pltpu.make_async_copy(dy_hbm, dy_v, in_sem.at[1]),
        pltpu.make_async_copy(wr_hbm, wr_v, in_sem.at[2]),
    ]
    ins[0].start()
    ins[1].start()
    ins[2].start()

    def weight_copies(j):
        return [
            pltpu.make_async_copy(wa_hbm.at[j], wa_v.at[j], w_sem.at[0, j]),
            pltpu.make_async_copy(wb_hbm.at[j], wb_v.at[j], w_sem.at[1, j]),
            pltpu.make_async_copy(wc_hbm.at[j], wc_v.at[j], w_sem.at[2, j]),
        ]

    @pl.loop(0, n_loc)
    def _(j):
        for c in weight_copies(j):
            c.start()

    n_dev = tp_size * ep_size
    barrier = pltpu.get_barrier_semaphore()
    for d in range(1, n_dev):
        flat = (k * ep_size + r + d) % n_dev
        pl.semaphore_signal(barrier, inc=1, device_id=(flat // ep_size, flat % ep_size), device_id_type=MESH)

    ids1 = ids1_ref[...]
    ids2 = ids2_ref[...]
    e_iota = lax.broadcasted_iota(I32, (n_exp, n_tok), 0)
    hot1 = jnp.where(ids1 == e_iota, 1.0, 0.0).astype(F32)
    hot2 = jnp.where(ids2 == e_iota, 1.0, 0.0).astype(F32)
    before = jnp.where(
        lax.broadcasted_iota(I32, (n_tok, n_tok), 0) < lax.broadcasted_iota(I32, (n_tok, n_tok), 1), 1.0, 0.0
    ).astype(BF)
    cum1 = dot(hot1.astype(BF), before)
    cum2 = dot(hot2.astype(BF), before)
    fill1 = jnp.sum(hot1, axis=1, keepdims=True)
    pos1 = jnp.sum(cum1 * hot1, axis=0, keepdims=True)
    pos2 = jnp.sum((cum2 + fill1) * hot2, axis=0, keepdims=True)

    def place(ids, pos):
        spot = (ids & (n_loc - 1)) * blk + (ids // n_loc) * cap
        return jnp.where(pos < cap, spot.astype(F32) + pos, float(n_exp * cap))

    s1r[...] = place(ids1, pos1)
    s2r[...] = place(ids2, pos2)

    def masks(j):
        spot = (lax.broadcasted_iota(I32, (blk, n_tok), 0) + j * blk).astype(F32)
        return s1r[...] == spot, s2r[...] == spot

    def send_rows(src, dst, send_sem, recv_sem, j):
        for d in range(1, ep_size):
            q = (r + d) % ep_size
            pltpu.make_async_remote_copy(
                src_ref=src.at[j, q], dst_ref=dst.at[j, my_place],
                send_sem=send_sem, recv_sem=recv_sem.at[j],
                device_id=(k, q), device_id_type=MESH,
            ).start()

    def wait_recv(view, sem):
        pltpu.make_async_remote_copy(
            src_ref=view, dst_ref=view, send_sem=sem, recv_sem=sem, device_id=(k, r), device_id_type=MESH
        ).wait_recv()

    def wait_send(view, sem):
        pltpu.make_async_remote_copy(
            src_ref=view, dst_ref=view, send_sem=sem, recv_sem=sem, device_id=(k, r), device_id_type=MESH
        ).wait_send()

    ins[0].wait()
    pl.semaphore_wait(barrier, n_dev - 1)

    @pl.loop(0, n_loc)
    def _(j):
        m1, m2 = masks(j)
        pick = jnp.where(m1 | m2, 1.0, 0.0).astype(BF)
        for c in range(0, width, 512):
            rows = dot(pick, x_v[:, c:c + 512]).astype(BF)
            xs[j, :, :, c:c + 512] = rows.reshape(ep_size, cap, 512)
        send_rows(xs, xr, xs_sem, xr_sem, j)
        xr[j, my_place] = xs[j, r]

    def column(row):
        return jnp.transpose(jnp.broadcast_to(row, (128, n_tok)))

    s1c[...] = column(s1r[...])
    s2c[...] = column(s2r[...])
    i1c[...] = column(ids1.astype(F32))
    i2c[...] = column(ids2.astype(F32))
    ins[2].wait()
    wr_hi, wr_mid, wr_low = split3(wr_v[...])
    xv = x_v[...]
    logits = dot(xv, wr_hi, NT) + (dot(xv, wr_mid, NT) + dot(xv, wr_low, NT))
    ex = jnp.exp(logits - jnp.max(logits, axis=1, keepdims=True))
    prob = ex / jnp.sum(ex, axis=1, keepdims=True)
    prob_v[...] = prob
    lane = lax.broadcasted_iota(I32, (n_tok, n_exp), 1).astype(F32)
    q1 = jnp.sum(jnp.where(i1c[:, :n_exp] == lane, prob, 0.0), axis=1, keepdims=True)
    q2 = jnp.sum(jnp.where(i2c[:, :n_exp] == lane, prob, 0.0), axis=1, keepdims=True)
    g1 = jnp.broadcast_to(q1 / (q1 + q2), (n_tok, 128))
    g2 = jnp.broadcast_to(q2 / (q1 + q2), (n_tok, 128))
    g1c[...] = g1
    g2c[...] = g2
    q1c[...] = jnp.broadcast_to(q1, (n_tok, 128))
    q2c[...] = jnp.broadcast_to(q2, (n_tok, 128))
    g1r[...] = jnp.transpose(g1)[0:1, :]
    g2r[...] = jnp.transpose(g2)[0:1, :]
    ins[1].wait()

    @pl.loop(0, n_loc)
    def _(j):
        m1, m2 = masks(j)
        pick = jnp.where(m1 | m2, 1.0, 0.0).astype(BF)
        gate = jnp.sum(jnp.where(m1, g1r[...], 0.0) + jnp.where(m2, g2r[...], 0.0), axis=1, keepdims=True)
        for c in range(0, width, 512):
            rows = (gate * dot(pick, dy_v[:, c:c + 512])).astype(BF)
            ds[j, :, :, c:c + 512] = rows.reshape(ep_size, cap, 512)
        send_rows(ds, dr, ds_sem, dr_sem, j)
        dr[j, my_place] = ds[j, r]

    def send_half(src, dst, send_sem, recv_sem, j):
        pltpu.make_async_remote_copy(
            src_ref=src.at[j, pl.ds(other * half, half)], dst_ref=dst.at[j],
            send_sem=send_sem, recv_sem=recv_sem.at[j],
            device_id=(other, r), device_id_type=MESH,
        ).start()

    def merge_and_return(src, got, got_sem, dst, send_sem, recv_sem, j):
        wait_recv(got.at[j], got_sem.at[j])
        mine = pl.ds(k * half, half)
        src[j, mine] = (src[j, mine].astype(F32) + got[j].astype(F32)).astype(BF)
        for d in range(half):
            c = (r // tp_size + d) % half
            q = tp_size * c + k

            @pl.when(q != r)
            def _():
                pltpu.make_async_remote_copy(
                    src_ref=src.at[j, k * half + c], dst_ref=dst.at[j, r],
                    send_sem=send_sem, recv_sem=recv_sem.at[j],
                    device_id=(k, q), device_id_type=MESH,
                ).start()

            @pl.when(q == r)
            def _():
                dst[j, r] = src[j, k * half + c]

    @pl.loop(0, n_loc)
    def _(j):
        for c in weight_copies(j):
            c.wait()
        wait_recv(xr.at[j, pl.ds(0, ep_size - 1)], xr_sem.at[j])
        rows = xr[j].reshape(blk, width)
        pa = dot(rows, wa_v[j])
        pb = dot(rows, wb_v[j])
        th = jnp.tanh(GELU_COEF * (pa + 0.044715 * pa * pa * pa))
        gv = 0.5 * pa * (1.0 + th)
        slope = 0.5 * (1.0 + th) + 0.5 * pa * (1.0 - th * th) * GELU_COEF * (1.0 + 0.134145 * pa * pa)
        gv_v[j] = gv
        bs_v[j] = pb * slope
        hidden = (gv * pb).astype(BF)
        h_v[j] = hidden
        for c in range(0, width, 512):
            ps[j, :, :, c:c + 512] = dot(hidden, wc_v[j, :, c:c + 512]).astype(BF).reshape(ep_size, cap, 512)
        send_half(ps, pr, ps_sem, pr_sem, j)

        @pl.when(j > 0)
        def _():
            merge_and_return(ps, pr, pr_sem, orr, os_sem, or_sem, j - 1)

    merge_and_return(ps, pr, pr_sem, orr, os_sem, or_sem, n_loc - 1)

    wait_send(xs.at[:, pl.ds(0, ep_size - 1)], xs_sem)

    @pl.loop(0, n_loc)
    def _(j):
        wait_recv(dr.at[j, pl.ds(0, ep_size - 1)], dr_sem.at[j])
        rows = dr[j].reshape(blk, width)
        dh = dot(rows, wc_v[j], NT)
        da = (dh * bs_v[j]).astype(BF)
        db = (dh * gv_v[j]).astype(BF)
        da_v[j] = da
        db_v[j] = db
        for c in range(0, width, 512):
            part = dot(da, wa_v[j, c:c + 512, :], NT) + dot(db, wb_v[j, c:c + 512, :], NT)
            xs[j, :, :, c:c + 512] = part.astype(BF).reshape(ep_size, cap, 512)
        send_half(xs, pdr, pds_sem, pdr_sem, j)

        @pl.when(j > 0)
        def _():
            merge_and_return(xs, pdr, pdr_sem, dxr, dxs_sem, dxr_sem, j - 1)

    merge_and_return(xs, pdr, pdr_sem, dxr, dxs_sem, dxr_sem, n_loc - 1)

    outs = [
        pltpu.make_async_copy(xr, xe_out, out_sem.at[0]),
        pltpu.make_async_copy(dr, de_out, out_sem.at[1]),
        pltpu.make_async_copy(h_v, h_out, out_sem.at[2]),
        pltpu.make_async_copy(da_v, da_out, out_sem.at[3]),
        pltpu.make_async_copy(db_v, db_out, out_sem.at[4]),
    ]
    for c in outs:
        c.start()

    tb = 128
    n_tb = n_tok // tb

    def spots(col, toks):
        lanes = lax.broadcasted_iota(I32, (tb, 128), 1).astype(F32)
        base = col[toks, :]
        return jnp.concatenate([base == lanes + float(u * 128) for u in range(n_exp * cap // 128)], axis=1)

    def ship(buf, toks, send_sem, recv_sem):
        pltpu.make_async_remote_copy(
            src_ref=buf.at[toks], dst_ref=buf.at[toks], send_sem=send_sem, recv_sem=recv_sem,
            device_id=(other, r), device_id_type=MESH,
        ).start()

    @pl.when(owner)
    def _():
        @pl.loop(0, n_loc)
        def _(j):
            wait_recv(orr.at[j, pl.ds(0, ep_size - 1)], or_sem.at[j])

        @pl.loop(0, n_tb)
        def _(t):
            toks = pl.ds(pl.multiple_of(t * tb, tb), tb)
            pick1 = jnp.where(spots(s1c, toks), 1.0, 0.0).astype(BF)
            pick2 = jnp.where(spots(s2c, toks), 1.0, 0.0).astype(BF)
            dg1 = jnp.zeros((tb, 1), F32)
            dg2 = jnp.zeros((tb, 1), F32)
            ga = g1c[toks, 0:1]
            gb = g2c[toks, 0:1]
            for c in range(0, width, 512):
                rows = orr[:, :, :, c:c + 512].reshape(n_exp * cap, 512)
                o1 = dot(pick1, rows)
                o2 = dot(pick2, rows)
                y_v[toks, c:c + 512] = (ga * o1 + gb * o2).astype(BF)
                dyf = dy_v[toks, c:c + 512].astype(F32)
                dg1 = dg1 + jnp.sum(dyf * o1, axis=1, keepdims=True)
                dg2 = dg2 + jnp.sum(dyf * o2, axis=1, keepdims=True)
            ship(y_v, toks, ys_sem, yr_sem)
            qa = q1c[toks, 0:1]
            qb = q2c[toks, 0:1]
            shared = dg1 * ga + dg2 * gb
            dq1 = (dg1 - shared) / (qa + qb)
            dq2 = (dg2 - shared) / (qa + qb)
            centre = dq1 * qa + dq2 * qb
            lanes = lax.broadcasted_iota(I32, (tb, n_exp), 1).astype(F32)
            pull = jnp.where(i1c[toks, :n_exp] == lanes, dq1, 0.0) + jnp.where(i2c[toks, :n_exp] == lanes, dq2, 0.0)
            dl_v[toks, :] = prob_v[toks, :] * (pull - centre)

        d_hi, d_mid, d_low = split3(dl_v[...])
        for c in range(0, width, 512):
            xc = x_v[:, c:c + 512]
            piece = dot(d_hi, xc, TN) + (dot(d_mid, xc, TN) + dot(d_low, xc, TN))
            dwp[:, :, c:c + 512] = piece.reshape(ep_size, n_loc, 512)
        for d in range(1, ep_size):
            q = (r + d) % ep_size
            pltpu.make_async_remote_copy(
                src_ref=dwp.at[q], dst_ref=dwi.at[r], send_sem=rs_sem, recv_sem=rr_sem,
                device_id=(q % tp_size, q), device_id_type=MESH,
            ).start()
        dwi[r] = dwp[r]

        @pl.loop(0, n_loc)
        def _(j):
            wait_recv(dxr.at[j, pl.ds(0, ep_size - 1)], dxr_sem.at[j])

        @pl.loop(0, n_tb)
        def _(t):
            toks = pl.ds(pl.multiple_of(t * tb, tb), tb)
            pick = jnp.where(spots(s1c, toks) | spots(s2c, toks), 1.0, 0.0).astype(BF)
            dl = dl_v[toks, :]
            for c in range(0, width, 512):
                rows = dxr[:, :, :, c:c + 512].reshape(n_exp * cap, 512)
                back = dot(pick, rows)
                router = lax.dot_general(
                    dl, wr_v[:, c:c + 512], NN, precision=lax.Precision.HIGHEST, preferred_element_type=F32
                )
                dx_v[toks, c:c + 512] = (back + router).astype(BF)
            ship(dx_v, toks, dys_sem, dyr_sem)

        wait_recv(dwi.at[pl.ds(0, ep_size - 1)], rr_sem)
        total = dwi[0]
        for q in range(1, ep_size):
            total = total + dwi[q]
        dwf[r] = total
        for d in range(1, n_dev):
            flat = (k * ep_size + r + d) % n_dev
            pltpu.make_async_remote_copy(
                src_ref=dwf.at[r], dst_ref=dwf.at[r], send_sem=fs_sem, recv_sem=fr_sem,
                device_id=(flat // ep_size, flat % ep_size), device_id_type=MESH,
            ).start()
        wait_recv(dwf.at[pl.ds(0, ep_size - 1)], fr_sem)
        wait_send(dwp.at[pl.ds(0, ep_size - 1)], rs_sem)
        for half_sends in range(n_dev - 1):
            wait_send(dwf.at[r], fs_sem)
        wait_send(y_v, ys_sem)
        wait_send(dx_v, dys_sem)
        wait_send(orr.at[:, pl.ds(0, half - 1)], os_sem)
        wait_send(dxr.at[:, pl.ds(0, half - 1)], dxs_sem)

    @pl.when(jnp.logical_not(owner))
    def _():
        wait_recv(y_v, yr_sem)
        wait_recv(dx_v, dyr_sem)
        wait_recv(dwf, fr_sem)
        wait_send(orr.at[:, pl.ds(0, half)], os_sem)
        wait_send(dxr.at[:, pl.ds(0, half)], dxs_sem)

    finals = [
        pltpu.make_async_copy(y_v, y_out, in_sem.at[0]),
        pltpu.make_async_copy(dx_v, dx_out, in_sem.at[1]),
        pltpu.make_async_copy(dwf, dwr_out, in_sem.at[2]),
    ]
    for c in finals:
        c.start()
    wait_send(ds.at[:, pl.ds(0, ep_size - 1)], ds_sem)
    wait_send(ps.at[:, pl.ds(0, half)], ps_sem)
    wait_send(xs.at[:, pl.ds(0, half)], pds_sem)
    for c in outs + finals:
        c.wait()


def weight_kernel(xe, de, h, da, db, ga_out, gb_out, gc_out):
    rows = xe[0]
    ga_out[0] = dot(rows, da[0], TN)
    gb_out[0] = dot(rows, db[0], TN)
    gc_out[0] = dot(h[0], de[0], TN)


def solution(mesh):
    tp_size = mesh.shape["tp"]
    ep_size = mesh.shape["ep"]

    def local_step(x_rows, w_router, first_ids, second_ids, w_gelu, w_lin, w_out, dy_rows):
        n_tok, width = x_rows.shape
        n_exp = w_router.shape[1]
        n_loc, _, hid = w_gelu.shape
        cap = 2 * n_tok // n_exp
        blk = ep_size * cap
        half = ep_size // tp_size
        dma = pltpu.SemaphoreType.DMA
        any_spec = pl.BlockSpec(memory_space=pl.ANY)
        vmem_spec = pl.BlockSpec(memory_space=pltpu.VMEM)
        sds = jax.ShapeDtypeStruct
        rows_shape = (n_loc, ep_size, cap, width)
        half_shape = (n_loc, half, cap, width)
        hid_shape = (n_loc, blk, hid)
        col = pltpu.VMEM((n_tok, 128), F32)
        row = pltpu.VMEM((1, n_tok), F32)
        outs = pl.pallas_call(
            functools.partial(moe_kernel, tp_size, ep_size, cap),
            name="moe",
            in_specs=[vmem_spec] * 2 + [any_spec] * 6,
            out_specs=[any_spec] * 8,
            out_shape=[
                sds((n_tok, width), BF), sds((n_tok, width), BF), sds((ep_size, n_loc, width), F32),
                sds(rows_shape, BF), sds(rows_shape, BF), sds(hid_shape, BF), sds(hid_shape, BF), sds(hid_shape, BF),
            ],
            scratch_shapes=[
                pltpu.VMEM((n_tok, width), BF), pltpu.VMEM((n_tok, width), BF), pltpu.VMEM((n_exp, width), F32),
                pltpu.VMEM((n_loc, width, hid), BF), pltpu.VMEM((n_loc, width, hid), BF), pltpu.VMEM((n_loc, hid, width), BF),
                pltpu.VMEM(rows_shape, BF), pltpu.VMEM(rows_shape, BF), pltpu.VMEM(rows_shape, BF), pltpu.VMEM(rows_shape, BF),
                pltpu.VMEM(hid_shape, BF), pltpu.VMEM(hid_shape, BF), pltpu.VMEM(hid_shape, BF),
                pltpu.VMEM(hid_shape, F32), pltpu.VMEM(hid_shape, F32),
                pltpu.VMEM(rows_shape, BF), pltpu.VMEM(half_shape, BF), pltpu.VMEM(half_shape, BF),
                pltpu.VMEM(rows_shape, BF), pltpu.VMEM(rows_shape, BF),
                pltpu.VMEM((n_tok, width), BF), pltpu.VMEM((n_tok, width), BF),
                row, row, row, row, col, col, col, col, col, col, col, col,
                pltpu.VMEM((n_tok, n_exp), F32), pltpu.VMEM((n_tok, n_exp), F32),
                pltpu.VMEM((ep_size, n_loc, width), F32), pltpu.VMEM((ep_size, n_loc, width), F32),
                pltpu.VMEM((ep_size, n_loc, width), F32),
                dma((3,)), dma((3, n_loc)), dma((5,)),
                dma(()), dma((n_loc,)), dma(()), dma((n_loc,)),
                dma(()), dma((n_loc,)), dma(()), dma((n_loc,)),
                dma(()), dma((n_loc,)), dma(()), dma((n_loc,)),
                dma(()), dma(()), dma(()), dma(()),
                dma(()), dma(()), dma(()), dma(()),
            ],
            compiler_params=pltpu.CompilerParams(
                collective_id=0, has_side_effects=True, vmem_limit_bytes=67043328
            ),
        )(
            first_ids.reshape(1, n_tok), second_ids.reshape(1, n_tok), x_rows, dy_rows, w_router.T,
            w_gelu, w_lin, w_out,
        )
        act_out, grad_in, grad_router, xe, de, h, da, db = outs
        xe = xe.reshape(n_loc, blk, width)
        de = de.reshape(n_loc, blk, width)

        def spec(*shape):
            return pl.BlockSpec((1,) + shape, lambda e: (e, 0, 0))

        grad_wa, grad_wb, grad_wc = pl.pallas_call(
            weight_kernel,
            name="weight_grads",
            grid=(n_loc,),
            in_specs=[spec(blk, width), spec(blk, width), spec(blk, hid), spec(blk, hid), spec(blk, hid)],
            out_specs=[spec(width, hid), spec(width, hid), spec(hid, width)],
            out_shape=[
                sds((n_loc, width, hid), F32), sds((n_loc, width, hid), F32), sds((n_loc, hid, width), F32),
            ],
            compiler_params=pltpu.CompilerParams(
                dimension_semantics=("arbitrary",), vmem_limit_bytes=40 * 1024 * 1024
            ),
        )(xe, de, h, da, db)
        return act_out, grad_in, grad_wa, grad_wb, grad_wc, grad_router.reshape(n_exp, width).T

    return jax.shard_map(
        local_step,
        mesh=mesh,
        in_specs=(P("ep", None), P(), P("ep"), P("ep"), P("ep", None, "tp"), P("ep", None, "tp"), P("ep", "tp", None), P("ep", None)),
        out_specs=(P("ep", None), P("ep", None), P("ep", None, "tp"), P("ep", None, "tp"), P("ep", "tp", None), P()),
        check_vma=False,
    )
```

```python
import functools

import jax
import jax.numpy as jnp
from jax import lax
from jax.experimental import pallas as pl
from jax.experimental.pallas import tpu as pltpu
from jax.sharding import PartitionSpec as P

BF = jnp.bfloat16
F32 = jnp.float32
I32 = jnp.int32
MESH = pl.DeviceIdType.MESH
GELU_COEF = 0.7978845608028654
NN = (((1,), (0,)), ((), ()))
NT = (((1,), (1,)), ((), ()))
TN = (((0,), (0,)), ((), ()))


def dot(a, b, dims=NN):
    return lax.dot_general(a, b, dims, preferred_element_type=F32)


def split3(v):
    hi = v.astype(BF)
    rest = v - hi.astype(F32)
    mid = rest.astype(BF)
    low = (rest - mid.astype(F32)).astype(BF)
    return hi, mid, low


def moe_kernel(
    tp_size, ep_size, cap,
    ids1_ref, ids2_ref, x_hbm, dy_hbm, wr_hbm, wa_hbm, wb_hbm, wc_hbm,
    y_out, dx_out, dwr_out, xe_out, de_out, h_out, da_out, db_out,
    x_v, dy_v, wr_v, wa_v, wb_v, wc_v,
    xs, ds, xr, dr, h_v, da_v, db_v, bs_v, gv_v,
    ps, pr, pdr, orr, dxr, y_v, dx_v,
    s1r, s2r, g1r, g2r, s1c, s2c, g1c, g2c, q1c, q2c, i1c, i2c, prob_v, dl_v,
    dwp, dwi, dwf,
    in_sem, w_sem, out_sem,
    xs_sem, xr_sem, ds_sem, dr_sem,
    ps_sem, pr_sem, pds_sem, pdr_sem,
    os_sem, or_sem, dxs_sem, dxr_sem,
    ys_sem, yr_sem,
    rs_sem, rr_sem, fs_sem, fr_sem,
):
    k = lax.axis_index("tp")
    r = lax.axis_index("ep")
    n_loc = wa_v.shape[0]
    n_tok, width = x_v.shape
    hid = wa_v.shape[2]
    n_exp = n_loc * ep_size
    blk = ep_size * cap
    half = ep_size // tp_size
    my_place = (r % tp_size) * half + r // tp_size
    owner = (r % tp_size) == k
    other = 1 - k

    ins = [
        pltpu.make_async_copy(x_hbm, x_v, in_sem.at[0]),
        pltpu.make_async_copy(dy_hbm, dy_v, in_sem.at[1]),
        pltpu.make_async_copy(wr_hbm, wr_v, in_sem.at[2]),
    ]
    ins[0].start()
    ins[1].start()
    ins[2].start()

    def weight_copies(j):
        return [
            pltpu.make_async_copy(wa_hbm.at[j], wa_v.at[j], w_sem.at[0, j]),
            pltpu.make_async_copy(wb_hbm.at[j], wb_v.at[j], w_sem.at[1, j]),
            pltpu.make_async_copy(wc_hbm.at[j], wc_v.at[j], w_sem.at[2, j]),
        ]

    @pl.loop(0, n_loc)
    def _(j):
        for c in weight_copies(j):
            c.start()

    n_dev = tp_size * ep_size
    barrier = pltpu.get_barrier_semaphore()
    for d in range(1, n_dev):
        flat = (k * ep_size + r + d) % n_dev
        pl.semaphore_signal(barrier, inc=1, device_id=(flat // ep_size, flat % ep_size), device_id_type=MESH)

    ids1 = ids1_ref[...]
    ids2 = ids2_ref[...]
    e_iota = lax.broadcasted_iota(I32, (n_exp, n_tok), 0)
    hot1 = jnp.where(ids1 == e_iota, 1.0, 0.0).astype(F32)
    hot2 = jnp.where(ids2 == e_iota, 1.0, 0.0).astype(F32)
    before = jnp.where(
        lax.broadcasted_iota(I32, (n_tok, n_tok), 0) < lax.broadcasted_iota(I32, (n_tok, n_tok), 1), 1.0, 0.0
    ).astype(BF)
    cum1 = dot(hot1.astype(BF), before)
    cum2 = dot(hot2.astype(BF), before)
    fill1 = jnp.sum(hot1, axis=1, keepdims=True)
    pos1 = jnp.sum(cum1 * hot1, axis=0, keepdims=True)
    pos2 = jnp.sum((cum2 + fill1) * hot2, axis=0, keepdims=True)

    def place(ids, pos):
        spot = (ids & (n_loc - 1)) * blk + (ids // n_loc) * cap
        return jnp.where(pos < cap, spot.astype(F32) + pos, float(n_exp * cap))

    s1r[...] = place(ids1, pos1)
    s2r[...] = place(ids2, pos2)

    def masks(j):
        spot = (lax.broadcasted_iota(I32, (blk, n_tok), 0) + j * blk).astype(F32)
        return s1r[...] == spot, s2r[...] == spot

    def send_rows(src, dst, send_sem, recv_sem, j):
        for d in range(1, ep_size):
            q = (r + d) % ep_size
            pltpu.make_async_remote_copy(
                src_ref=src.at[j, q], dst_ref=dst.at[j, my_place],
                send_sem=send_sem, recv_sem=recv_sem.at[j],
                device_id=(k, q), device_id_type=MESH,
            ).start()

    def wait_recv(view, sem):
        pltpu.make_async_remote_copy(
            src_ref=view, dst_ref=view, send_sem=sem, recv_sem=sem, device_id=(k, r), device_id_type=MESH
        ).wait_recv()

    def wait_send(view, sem):
        pltpu.make_async_remote_copy(
            src_ref=view, dst_ref=view, send_sem=sem, recv_sem=sem, device_id=(k, r), device_id_type=MESH
        ).wait_send()

    ins[0].wait()
    pl.semaphore_wait(barrier, n_dev - 1)

    @pl.loop(0, n_loc)
    def _(j):
        m1, m2 = masks(j)
        pick = jnp.where(m1 | m2, 1.0, 0.0).astype(BF)
        for c in range(0, width, 512):
            rows = dot(pick, x_v[:, c:c + 512]).astype(BF)
            xs[j, :, :, c:c + 512] = rows.reshape(ep_size, cap, 512)
        send_rows(xs, xr, xs_sem, xr_sem, j)
        xr[j, my_place] = xs[j, r]

    def column(row):
        return jnp.transpose(jnp.broadcast_to(row, (128, n_tok)))

    s1c[...] = column(s1r[...])
    s2c[...] = column(s2r[...])
    i1c[...] = column(ids1.astype(F32))
    i2c[...] = column(ids2.astype(F32))
    ins[2].wait()
    wr_hi, wr_mid, wr_low = split3(wr_v[...])
    xv = x_v[...]
    logits = dot(xv, wr_hi, NT) + (dot(xv, wr_mid, NT) + dot(xv, wr_low, NT))
    ex = jnp.exp(logits - jnp.max(logits, axis=1, keepdims=True))
    prob = ex / jnp.sum(ex, axis=1, keepdims=True)
    prob_v[...] = prob
    lane = lax.broadcasted_iota(I32, (n_tok, n_exp), 1).astype(F32)
    q1 = jnp.sum(jnp.where(i1c[:, :n_exp] == lane, prob, 0.0), axis=1, keepdims=True)
    q2 = jnp.sum(jnp.where(i2c[:, :n_exp] == lane, prob, 0.0), axis=1, keepdims=True)
    g1 = jnp.broadcast_to(q1 / (q1 + q2), (n_tok, 128))
    g2 = jnp.broadcast_to(q2 / (q1 + q2), (n_tok, 128))
    g1c[...] = g1
    g2c[...] = g2
    q1c[...] = jnp.broadcast_to(q1, (n_tok, 128))
    q2c[...] = jnp.broadcast_to(q2, (n_tok, 128))
    g1r[...] = jnp.transpose(g1)[0:1, :]
    g2r[...] = jnp.transpose(g2)[0:1, :]
    ins[1].wait()

    @pl.loop(0, n_loc)
    def _(j):
        m1, m2 = masks(j)
        pick = jnp.where(m1 | m2, 1.0, 0.0).astype(BF)
        gate = jnp.sum(jnp.where(m1, g1r[...], 0.0) + jnp.where(m2, g2r[...], 0.0), axis=1, keepdims=True)
        for c in range(0, width, 512):
            rows = (gate * dot(pick, dy_v[:, c:c + 512])).astype(BF)
            ds[j, :, :, c:c + 512] = rows.reshape(ep_size, cap, 512)
        send_rows(ds, dr, ds_sem, dr_sem, j)
        dr[j, my_place] = ds[j, r]

    def send_half(src, dst, send_sem, recv_sem, j):
        pltpu.make_async_remote_copy(
            src_ref=src.at[j, pl.ds(other * half, half)], dst_ref=dst.at[j],
            send_sem=send_sem, recv_sem=recv_sem.at[j],
            device_id=(other, r), device_id_type=MESH,
        ).start()

    def merge_and_return(src, got, got_sem, dst, send_sem, recv_sem, j):
        wait_recv(got.at[j], got_sem.at[j])
        mine = pl.ds(k * half, half)
        src[j, mine] = (src[j, mine].astype(F32) + got[j].astype(F32)).astype(BF)
        for d in range(half):
            c = (r // tp_size + d) % half
            q = tp_size * c + k

            @pl.when(q != r)
            def _():
                pltpu.make_async_remote_copy(
                    src_ref=src.at[j, k * half + c], dst_ref=dst.at[j, r],
                    send_sem=send_sem, recv_sem=recv_sem.at[j],
                    device_id=(k, q), device_id_type=MESH,
                ).start()

            @pl.when(q == r)
            def _():
                dst[j, r] = src[j, k * half + c]

    @pl.loop(0, n_loc)
    def _(j):
        for c in weight_copies(j):
            c.wait()
        wait_recv(xr.at[j, pl.ds(0, ep_size - 1)], xr_sem.at[j])
        rows = xr[j].reshape(blk, width)
        pa = dot(rows, wa_v[j])
        pb = dot(rows, wb_v[j])
        th = jnp.tanh(GELU_COEF * (pa + 0.044715 * pa * pa * pa))
        gv = 0.5 * pa * (1.0 + th)
        slope = 0.5 * (1.0 + th) + 0.5 * pa * (1.0 - th * th) * GELU_COEF * (1.0 + 0.134145 * pa * pa)
        gv_v[j] = gv
        bs_v[j] = pb * slope
        hidden = (gv * pb).astype(BF)
        h_v[j] = hidden
        for c in range(0, width, 512):
            ps[j, :, :, c:c + 512] = dot(hidden, wc_v[j, :, c:c + 512]).astype(BF).reshape(ep_size, cap, 512)
        send_half(ps, pr, ps_sem, pr_sem, j)

        @pl.when(j > 0)
        def _():
            merge_and_return(ps, pr, pr_sem, orr, os_sem, or_sem, j - 1)

    merge_and_return(ps, pr, pr_sem, orr, os_sem, or_sem, n_loc - 1)

    wait_send(xs.at[:, pl.ds(0, ep_size - 1)], xs_sem)

    @pl.loop(0, n_loc)
    def _(j):
        wait_recv(dr.at[j, pl.ds(0, ep_size - 1)], dr_sem.at[j])
        rows = dr[j].reshape(blk, width)
        dh = dot(rows, wc_v[j], NT)
        da = (dh * bs_v[j]).astype(BF)
        db = (dh * gv_v[j]).astype(BF)
        da_v[j] = da
        db_v[j] = db
        for c in range(0, width, 512):
            part = dot(da, wa_v[j, c:c + 512, :], NT) + dot(db, wb_v[j, c:c + 512, :], NT)
            xs[j, :, :, c:c + 512] = part.astype(BF).reshape(ep_size, cap, 512)
        send_half(xs, pdr, pds_sem, pdr_sem, j)

        @pl.when(j > 0)
        def _():
            merge_and_return(xs, pdr, pdr_sem, dxr, dxs_sem, dxr_sem, j - 1)

    merge_and_return(xs, pdr, pdr_sem, dxr, dxs_sem, dxr_sem, n_loc - 1)

    outs = [
        pltpu.make_async_copy(xr, xe_out, out_sem.at[0]),
        pltpu.make_async_copy(dr, de_out, out_sem.at[1]),
        pltpu.make_async_copy(h_v, h_out, out_sem.at[2]),
        pltpu.make_async_copy(da_v, da_out, out_sem.at[3]),
        pltpu.make_async_copy(db_v, db_out, out_sem.at[4]),
    ]
    for c in outs:
        c.start()

    tb = 128
    n_tb = n_tok // tb

    def spots(col, toks):
        lanes = lax.broadcasted_iota(I32, (tb, 128), 1).astype(F32)
        base = col[toks, :]
        return jnp.concatenate([base == lanes + float(u * 128) for u in range(n_exp * cap // 128)], axis=1)

    def ship(buf, toks, send_sem, recv_sem):
        pltpu.make_async_remote_copy(
            src_ref=buf.at[toks], dst_ref=buf.at[toks], send_sem=send_sem, recv_sem=recv_sem,
            device_id=(other, r), device_id_type=MESH,
        ).start()

    @pl.when(owner)
    def _():
        @pl.loop(0, n_loc)
        def _(j):
            wait_recv(orr.at[j, pl.ds(0, ep_size - 1)], or_sem.at[j])

        @pl.loop(0, n_tb)
        def _(t):
            toks = pl.ds(pl.multiple_of(t * tb, tb), tb)
            pick1 = jnp.where(spots(s1c, toks), 1.0, 0.0).astype(BF)
            pick2 = jnp.where(spots(s2c, toks), 1.0, 0.0).astype(BF)
            dg1 = jnp.zeros((tb, 1), F32)
            dg2 = jnp.zeros((tb, 1), F32)
            ga = g1c[toks, 0:1]
            gb = g2c[toks, 0:1]
            for c in range(0, width, 512):
                rows = orr[:, :, :, c:c + 512].reshape(n_exp * cap, 512)
                o1 = dot(pick1, rows)
                o2 = dot(pick2, rows)
                y_v[toks, c:c + 512] = (ga * o1 + gb * o2).astype(BF)
                dyf = dy_v[toks, c:c + 512].astype(F32)
                dg1 = dg1 + jnp.sum(dyf * o1, axis=1, keepdims=True)
                dg2 = dg2 + jnp.sum(dyf * o2, axis=1, keepdims=True)
            ship(y_v, toks, ys_sem, yr_sem)
            qa = q1c[toks, 0:1]
            qb = q2c[toks, 0:1]
            shared = dg1 * ga + dg2 * gb
            dq1 = (dg1 - shared) / (qa + qb)
            dq2 = (dg2 - shared) / (qa + qb)
            centre = dq1 * qa + dq2 * qb
            lanes = lax.broadcasted_iota(I32, (tb, n_exp), 1).astype(F32)
            pull = jnp.where(i1c[toks, :n_exp] == lanes, dq1, 0.0) + jnp.where(i2c[toks, :n_exp] == lanes, dq2, 0.0)
            dl_v[toks, :] = prob_v[toks, :] * (pull - centre)

        d_hi, d_mid, d_low = split3(dl_v[...])
        for c in range(0, width, 512):
            xc = x_v[:, c:c + 512]
            piece = dot(d_hi, xc, TN) + (dot(d_mid, xc, TN) + dot(d_low, xc, TN))
            dwp[:, :, c:c + 512] = piece.reshape(ep_size, n_loc, 512)
        for d in range(1, ep_size):
            q = (r + d) % ep_size
            pltpu.make_async_remote_copy(
                src_ref=dwp.at[q], dst_ref=dwi.at[r], send_sem=rs_sem, recv_sem=rr_sem,
                device_id=(q % tp_size, q), device_id_type=MESH,
            ).start()
        dwi[r] = dwp[r]

        @pl.loop(0, n_loc)
        def _(j):
            wait_recv(dxr.at[j, pl.ds(0, ep_size - 1)], dxr_sem.at[j])

        wait_recv(dwi.at[pl.ds(0, ep_size - 1)], rr_sem)
        total = dwi[0]
        for q in range(1, ep_size):
            total = total + dwi[q]
        dwf[r] = total
        for d in range(1, n_dev):
            flat = (k * ep_size + r + d) % n_dev
            pltpu.make_async_remote_copy(
                src_ref=dwf.at[r], dst_ref=dwf.at[r], send_sem=fs_sem, recv_sem=fr_sem,
                device_id=(flat // ep_size, flat % ep_size), device_id_type=MESH,
            ).start()
        @pl.loop(0, n_tb)
        def _(t):
            toks = pl.ds(pl.multiple_of(t * tb, tb), tb)
            pick = jnp.where(spots(s1c, toks) | spots(s2c, toks), 1.0, 0.0).astype(BF)
            dl = dl_v[toks, :]
            for c in range(0, width, 512):
                rows = dxr[:, :, :, c:c + 512].reshape(n_exp * cap, 512)
                back = dot(pick, rows)
                router = lax.dot_general(
                    dl, wr_v[:, c:c + 512], NN, precision=lax.Precision.HIGHEST, preferred_element_type=F32
                )
                dx_v[toks, c:c + 512] = (back + router).astype(BF)
            pltpu.make_async_copy(dx_v.at[toks], dx_out.at[toks], in_sem.at[1]).start()

        wait_recv(dwf.at[pl.ds(0, ep_size - 1)], fr_sem)
        wait_send(dwp.at[pl.ds(0, ep_size - 1)], rs_sem)
        for half_sends in range(n_dev - 1):
            wait_send(dwf.at[r], fs_sem)
        wait_send(y_v, ys_sem)
        wait_send(orr.at[:, pl.ds(0, half - 1)], os_sem)
        wait_send(dxr.at[:, pl.ds(0, half - 1)], dxs_sem)

    @pl.when(jnp.logical_not(owner))
    def _():
        dx_v[...] = jnp.zeros_like(dx_v)
        pltpu.make_async_copy(dx_v, dx_out, in_sem.at[1]).start()
        wait_recv(y_v, yr_sem)
        wait_recv(dwf, fr_sem)
        wait_send(orr.at[:, pl.ds(0, half)], os_sem)
        wait_send(dxr.at[:, pl.ds(0, half)], dxs_sem)

    finals = [
        pltpu.make_async_copy(y_v, y_out, in_sem.at[0]),
        pltpu.make_async_copy(dwf, dwr_out, in_sem.at[2]),
    ]
    for c in finals:
        c.start()
    finals.append(pltpu.make_async_copy(dx_v, dx_out, in_sem.at[1]))
    wait_send(ds.at[:, pl.ds(0, ep_size - 1)], ds_sem)
    wait_send(ps.at[:, pl.ds(0, half)], ps_sem)
    wait_send(xs.at[:, pl.ds(0, half)], pds_sem)
    for c in outs + finals:
        c.wait()


def weight_kernel(xe, de, h, da, db, ga_out, gb_out, gc_out):
    rows = xe[0]
    ga_out[0] = dot(rows, da[0], TN)
    gb_out[0] = dot(rows, db[0], TN)
    gc_out[0] = dot(h[0], de[0], TN)


def solution(mesh):
    tp_size = mesh.shape["tp"]
    ep_size = mesh.shape["ep"]

    def local_step(x_rows, w_router, first_ids, second_ids, w_gelu, w_lin, w_out, dy_rows):
        n_tok, width = x_rows.shape
        n_exp = w_router.shape[1]
        n_loc, _, hid = w_gelu.shape
        cap = 2 * n_tok // n_exp
        blk = ep_size * cap
        half = ep_size // tp_size
        dma = pltpu.SemaphoreType.DMA
        any_spec = pl.BlockSpec(memory_space=pl.ANY)
        vmem_spec = pl.BlockSpec(memory_space=pltpu.VMEM)
        sds = jax.ShapeDtypeStruct
        rows_shape = (n_loc, ep_size, cap, width)
        half_shape = (n_loc, half, cap, width)
        hid_shape = (n_loc, blk, hid)
        col = pltpu.VMEM((n_tok, 128), F32)
        row = pltpu.VMEM((1, n_tok), F32)
        outs = pl.pallas_call(
            functools.partial(moe_kernel, tp_size, ep_size, cap),
            name="moe",
            in_specs=[vmem_spec] * 2 + [any_spec] * 6,
            out_specs=[any_spec] * 8,
            out_shape=[
                sds((n_tok, width), BF), sds((n_tok, width), BF), sds((ep_size, n_loc, width), F32),
                sds(rows_shape, BF), sds(rows_shape, BF), sds(hid_shape, BF), sds(hid_shape, BF), sds(hid_shape, BF),
            ],
            scratch_shapes=[
                pltpu.VMEM((n_tok, width), BF), pltpu.VMEM((n_tok, width), BF), pltpu.VMEM((n_exp, width), F32),
                pltpu.VMEM((n_loc, width, hid), BF), pltpu.VMEM((n_loc, width, hid), BF), pltpu.VMEM((n_loc, hid, width), BF),
                pltpu.VMEM(rows_shape, BF), pltpu.VMEM(rows_shape, BF), pltpu.VMEM(rows_shape, BF), pltpu.VMEM(rows_shape, BF),
                pltpu.VMEM(hid_shape, BF), pltpu.VMEM(hid_shape, BF), pltpu.VMEM(hid_shape, BF),
                pltpu.VMEM(hid_shape, F32), pltpu.VMEM(hid_shape, F32),
                pltpu.VMEM(rows_shape, BF), pltpu.VMEM(half_shape, BF), pltpu.VMEM(half_shape, BF),
                pltpu.VMEM(rows_shape, BF), pltpu.VMEM(rows_shape, BF),
                pltpu.VMEM((n_tok, width), BF), pltpu.VMEM((n_tok, width), BF),
                row, row, row, row, col, col, col, col, col, col, col, col,
                pltpu.VMEM((n_tok, n_exp), F32), pltpu.VMEM((n_tok, n_exp), F32),
                pltpu.VMEM((ep_size, n_loc, width), F32), pltpu.VMEM((ep_size, n_loc, width), F32),
                pltpu.VMEM((ep_size, n_loc, width), F32),
                dma((3,)), dma((3, n_loc)), dma((5,)),
                dma(()), dma((n_loc,)), dma(()), dma((n_loc,)),
                dma(()), dma((n_loc,)), dma(()), dma((n_loc,)),
                dma(()), dma((n_loc,)), dma(()), dma((n_loc,)),
                dma(()), dma(()),
                dma(()), dma(()), dma(()), dma(()),
            ],
            compiler_params=pltpu.CompilerParams(
                collective_id=0, has_side_effects=True, vmem_limit_bytes=67043328
            ),
        )(
            first_ids.reshape(1, n_tok), second_ids.reshape(1, n_tok), x_rows, dy_rows, w_router.T,
            w_gelu, w_lin, w_out,
        )
        act_out, grad_in, grad_router, xe, de, h, da, db = outs
        partners = [
            ((q % tp_size) * ep_size + q, (1 - q % tp_size) * ep_size + q) for q in range(ep_size)
        ]
        passed = lax.ppermute(grad_in, ("tp", "ep"), partners)
        owner = lax.axis_index("ep") % tp_size == lax.axis_index("tp")
        grad_in = jnp.where(owner, grad_in, passed)
        xe = xe.reshape(n_loc, blk, width)
        de = de.reshape(n_loc, blk, width)

        def spec(*shape):
            return pl.BlockSpec((1,) + shape, lambda e: (e, 0, 0))

        grad_wa, grad_wb, grad_wc = pl.pallas_call(
            weight_kernel,
            name="weight_grads",
            grid=(n_loc,),
            in_specs=[spec(blk, width), spec(blk, width), spec(blk, hid), spec(blk, hid), spec(blk, hid)],
            out_specs=[spec(width, hid), spec(width, hid), spec(hid, width)],
            out_shape=[
                sds((n_loc, width, hid), F32), sds((n_loc, width, hid), F32), sds((n_loc, hid, width), F32),
            ],
            compiler_params=pltpu.CompilerParams(
                dimension_semantics=("arbitrary",), vmem_limit_bytes=67043328
            ),
            cost_estimate=pl.CostEstimate(
                flops=6 * n_loc * blk * width * hid, transcendentals=0,
                bytes_accessed=12 * n_loc * width * hid + 4 * n_loc * blk * width + 6 * n_loc * blk * hid,
            ),
        )(xe, de, h, da, db)
        return act_out, grad_in, grad_wa, grad_wb, grad_wc, grad_router.reshape(n_exp, width).T

    return jax.shard_map(
        local_step,
        mesh=mesh,
        in_specs=(P("ep", None), P(), P("ep"), P("ep"), P("ep", None, "tp"), P("ep", None, "tp"), P("ep", "tp", None), P("ep", None)),
        out_specs=(P("ep", None), P("ep", None), P("ep", None, "tp"), P("ep", None, "tp"), P("ep", "tp", None), P()),
        check_vma=False,
    )
```

```python
import functools

import jax
import jax.numpy as jnp
from jax import lax
from jax.experimental import pallas as pl
from jax.experimental.pallas import tpu as pltpu
from jax.sharding import PartitionSpec as P

BF = jnp.bfloat16
F32 = jnp.float32
I32 = jnp.int32
MESH = pl.DeviceIdType.MESH
GELU_COEF = 0.7978845608028654
NN = (((1,), (0,)), ((), ()))
NT = (((1,), (1,)), ((), ()))
TN = (((0,), (0,)), ((), ()))


def dot(a, b, dims=NN):
    return lax.dot_general(a, b, dims, preferred_element_type=F32)


def split3(v):
    hi = v.astype(BF)
    rest = v - hi.astype(F32)
    mid = rest.astype(BF)
    low = (rest - mid.astype(F32)).astype(BF)
    return hi, mid, low


def moe_kernel(
    tp_size, ep_size, cap,
    ids1_ref, ids2_ref, x_hbm, dy_hbm, wr_hbm, wa_hbm, wb_hbm, wc_hbm,
    y_out, dx_out, dwr_out, xe_out, de_out, h_out, da_out, db_out,
    x_v, dy_v, wr_v, wa_v, wb_v, wc_v,
    xs, ds, xr, dr, h_v, da_v, db_v, bs_v, gv_v,
    ps, pr, pdr, orr, dxr, y_v, dx_v,
    s1r, s2r, g1r, g2r, s1c, s2c, g1c, g2c, q1c, q2c, i1c, i2c, prob_v, dl_v,
    dwp, dwi, dwf,
    in_sem, w_sem, out_sem,
    xs_sem, xr_sem, xd_sem, xf_sem, xfs_sem, ds_sem, dr_sem,
    ps_sem, pr_sem, pds_sem, pdr_sem,
    os_sem, or_sem, dxs_sem, dxr_sem,
    ys_sem, yr_sem,
    rs_sem, rr_sem, fs_sem, fr_sem,
):
    k = lax.axis_index("tp")
    r = lax.axis_index("ep")
    n_loc = wa_v.shape[0]
    n_tok, width = x_v.shape
    hid = wa_v.shape[2]
    n_exp = n_loc * ep_size
    blk = ep_size * cap
    half = ep_size // tp_size
    my_place = (r % tp_size) * half + r // tp_size
    owner = (r % tp_size) == k
    other = 1 - k

    ins = [
        pltpu.make_async_copy(x_hbm, x_v, in_sem.at[0]),
        pltpu.make_async_copy(dy_hbm, dy_v, in_sem.at[1]),
        pltpu.make_async_copy(wr_hbm, wr_v, in_sem.at[2]),
    ]
    ins[0].start()
    ins[1].start()
    ins[2].start()

    def weight_copies(j):
        return [
            pltpu.make_async_copy(wa_hbm.at[j], wa_v.at[j], w_sem.at[0, j]),
            pltpu.make_async_copy(wb_hbm.at[j], wb_v.at[j], w_sem.at[1, j]),
            pltpu.make_async_copy(wc_hbm.at[j], wc_v.at[j], w_sem.at[2, j]),
        ]

    @pl.loop(0, n_loc)
    def _(j):
        for c in weight_copies(j):
            c.start()

    n_dev = tp_size * ep_size
    barrier = pltpu.get_barrier_semaphore()
    for d in range(1, n_dev):
        flat = (k * ep_size + r + d) % n_dev
        pl.semaphore_signal(barrier, inc=1, device_id=(flat // ep_size, flat % ep_size), device_id_type=MESH)

    ids1 = ids1_ref[...]
    ids2 = ids2_ref[...]
    e_iota = lax.broadcasted_iota(I32, (n_exp, n_tok), 0)
    hot1 = jnp.where(ids1 == e_iota, 1.0, 0.0).astype(F32)
    hot2 = jnp.where(ids2 == e_iota, 1.0, 0.0).astype(F32)
    before = jnp.where(
        lax.broadcasted_iota(I32, (n_tok, n_tok), 0) < lax.broadcasted_iota(I32, (n_tok, n_tok), 1), 1.0, 0.0
    ).astype(BF)
    cum1 = dot(hot1.astype(BF), before)
    cum2 = dot(hot2.astype(BF), before)
    fill1 = jnp.sum(hot1, axis=1, keepdims=True)
    pos1 = jnp.sum(cum1 * hot1, axis=0, keepdims=True)
    pos2 = jnp.sum((cum2 + fill1) * hot2, axis=0, keepdims=True)

    def place(ids, pos):
        spot = (ids & (n_loc - 1)) * blk + (ids // n_loc) * cap
        return jnp.where(pos < cap, spot.astype(F32) + pos, float(n_exp * cap))

    s1r[...] = place(ids1, pos1)
    s2r[...] = place(ids2, pos2)

    def masks(j):
        spot = (lax.broadcasted_iota(I32, (blk, n_tok), 0) + j * blk).astype(F32)
        return s1r[...] == spot, s2r[...] == spot

    chip = r // 2
    chip_x = chip + 1 - 2 * (chip % 2)
    chip_y = (chip + 2) % 4
    chip_d = 3 - chip
    core = r % 2
    diag = 2 * chip_d + (k + r) % 2
    near = [2 * chip_x + core, 2 * chip_y + core, 2 * chip_x + 1 - core, 2 * chip_y + 1 - core, 2 * chip + 1 - core]
    far = [2 * chip_d + core, 2 * chip_d + 1 - core]

    def place_of(q):
        return (q % tp_size) * half + q // tp_size

    def send_row(src, dst, send_sem, recv_sem, j, q):
        pltpu.make_async_remote_copy(
            src_ref=src.at[j, q], dst_ref=dst.at[j, my_place],
            send_sem=send_sem, recv_sem=recv_sem.at[j],
            device_id=(k, q), device_id_type=MESH,
        ).start()

    def wait_recv(view, sem):
        pltpu.make_async_remote_copy(
            src_ref=view, dst_ref=view, send_sem=sem, recv_sem=sem, device_id=(k, r), device_id_type=MESH
        ).wait_recv()

    def wait_send(view, sem):
        pltpu.make_async_remote_copy(
            src_ref=view, dst_ref=view, send_sem=sem, recv_sem=sem, device_id=(k, r), device_id_type=MESH
        ).wait_send()

    ins[0].wait()
    pl.semaphore_wait(barrier, n_dev - 1)

    @pl.loop(0, n_loc)
    def _(j):
        m1, m2 = masks(j)
        pick = jnp.where(m1 | m2, 1.0, 0.0).astype(BF)
        for c in range(0, width, 512):
            rows = dot(pick, x_v[:, c:c + 512]).astype(BF)
            xs[j, :, :, c:c + 512] = rows.reshape(ep_size, cap, 512)
        send_row(xs, xr, xs_sem, xd_sem, j, diag)
        for q in near:
            send_row(xs, xr, xs_sem, xr_sem, j, q)
        xr[j, my_place] = xs[j, r]

    def column(row):
        return jnp.transpose(jnp.broadcast_to(row, (128, n_tok)))

    s1c[...] = column(s1r[...])
    s2c[...] = column(s2r[...])
    i1c[...] = column(ids1.astype(F32))
    i2c[...] = column(ids2.astype(F32))
    ins[2].wait()
    wr_hi, wr_mid, wr_low = split3(wr_v[...])
    xv = x_v[...]
    logits = dot(xv, wr_hi, NT) + (dot(xv, wr_mid, NT) + dot(xv, wr_low, NT))
    ex = jnp.exp(logits - jnp.max(logits, axis=1, keepdims=True))
    prob = ex / jnp.sum(ex, axis=1, keepdims=True)
    prob_v[...] = prob
    lane = lax.broadcasted_iota(I32, (n_tok, n_exp), 1).astype(F32)
    q1 = jnp.sum(jnp.where(i1c[:, :n_exp] == lane, prob, 0.0), axis=1, keepdims=True)
    q2 = jnp.sum(jnp.where(i2c[:, :n_exp] == lane, prob, 0.0), axis=1, keepdims=True)
    g1 = jnp.broadcast_to(q1 / (q1 + q2), (n_tok, 128))
    g2 = jnp.broadcast_to(q2 / (q1 + q2), (n_tok, 128))
    g1c[...] = g1
    g2c[...] = g2
    q1c[...] = jnp.broadcast_to(q1, (n_tok, 128))
    q2c[...] = jnp.broadcast_to(q2, (n_tok, 128))
    g1r[...] = jnp.transpose(g1)[0:1, :]
    g2r[...] = jnp.transpose(g2)[0:1, :]
    ins[1].wait()

    @pl.loop(0, n_loc)
    def _(j):
        m1, m2 = masks(j)
        pick = jnp.where(m1 | m2, 1.0, 0.0).astype(BF)
        gate = jnp.sum(jnp.where(m1, g1r[...], 0.0) + jnp.where(m2, g2r[...], 0.0), axis=1, keepdims=True)
        for c in range(0, width, 512):
            rows = (gate * dot(pick, dy_v[:, c:c + 512])).astype(BF)
            ds[j, :, :, c:c + 512] = rows.reshape(ep_size, cap, 512)
        for q in far + near:
            send_row(ds, dr, ds_sem, dr_sem, j, q)
        dr[j, my_place] = ds[j, r]

    def send_half(src, dst, send_sem, recv_sem, j):
        pltpu.make_async_remote_copy(
            src_ref=src.at[j, pl.ds(other * half, half)], dst_ref=dst.at[j],
            send_sem=send_sem, recv_sem=recv_sem.at[j],
            device_id=(other, r), device_id_type=MESH,
        ).start()

    def merge_and_return(src, got, got_sem, dst, send_sem, recv_sem, j):
        wait_recv(got.at[j], got_sem.at[j])
        mine = pl.ds(k * half, half)
        src[j, mine] = (src[j, mine].astype(F32) + got[j].astype(F32)).astype(BF)
        for d in range(half):
            c = (r // tp_size + d) % half
            q = tp_size * c + k

            @pl.when(q != r)
            def _():
                pltpu.make_async_remote_copy(
                    src_ref=src.at[j, k * half + c], dst_ref=dst.at[j, r],
                    send_sem=send_sem, recv_sem=recv_sem.at[j],
                    device_id=(k, q), device_id_type=MESH,
                ).start()

            @pl.when(q == r)
            def _():
                dst[j, r] = src[j, k * half + c]

    n_near = len(near)
    diag_place = place_of(diag)

    def forward_diag(j):
        wait_recv(xr.at[j, 0], xd_sem.at[j])
        pltpu.make_async_remote_copy(
            src_ref=xr.at[j, diag_place], dst_ref=xr.at[j, diag_place],
            send_sem=xfs_sem, recv_sem=xf_sem.at[j],
            device_id=(other, r), device_id_type=MESH,
        ).start()

    forward_diag(0)

    @pl.loop(0, n_loc)
    def _(j):
        @pl.when(j + 1 < n_loc)
        def _():
            forward_diag(j + 1)

        for c in weight_copies(j):
            c.wait()
        wait_recv(xr.at[j, pl.ds(0, n_near)], xr_sem.at[j])
        wait_recv(xr.at[j, 0], xf_sem.at[j])
        rows = xr[j].reshape(blk, width)
        pa = dot(rows, wa_v[j])
        pb = dot(rows, wb_v[j])
        th = jnp.tanh(GELU_COEF * (pa + 0.044715 * pa * pa * pa))
        gv = 0.5 * pa * (1.0 + th)
        slope = 0.5 * (1.0 + th) + 0.5 * pa * (1.0 - th * th) * GELU_COEF * (1.0 + 0.134145 * pa * pa)
        gv_v[j] = gv
        bs_v[j] = pb * slope
        hidden = (gv * pb).astype(BF)
        h_v[j] = hidden
        for c in range(0, width, 512):
            ps[j, :, :, c:c + 512] = dot(hidden, wc_v[j, :, c:c + 512]).astype(BF).reshape(ep_size, cap, 512)
        send_half(ps, pr, ps_sem, pr_sem, j)

        @pl.when(j > 0)
        def _():
            merge_and_return(ps, pr, pr_sem, orr, os_sem, or_sem, j - 1)

    merge_and_return(ps, pr, pr_sem, orr, os_sem, or_sem, n_loc - 1)

    wait_send(xs.at[:, pl.ds(0, n_near + 1)], xs_sem)

    @pl.loop(0, n_loc)
    def _(j):
        wait_recv(dr.at[j, pl.ds(0, ep_size - 1)], dr_sem.at[j])
        rows = dr[j].reshape(blk, width)
        dh = dot(rows, wc_v[j], NT)
        da = (dh * bs_v[j]).astype(BF)
        db = (dh * gv_v[j]).astype(BF)
        da_v[j] = da
        db_v[j] = db
        for c in range(0, width, 512):
            part = dot(da, wa_v[j, c:c + 512, :], NT) + dot(db, wb_v[j, c:c + 512, :], NT)
            xs[j, :, :, c:c + 512] = part.astype(BF).reshape(ep_size, cap, 512)
        send_half(xs, pdr, pds_sem, pdr_sem, j)

        @pl.when(j > 0)
        def _():
            merge_and_return(xs, pdr, pdr_sem, dxr, dxs_sem, dxr_sem, j - 1)

    merge_and_return(xs, pdr, pdr_sem, dxr, dxs_sem, dxr_sem, n_loc - 1)

    outs = [
        pltpu.make_async_copy(xr, xe_out, out_sem.at[0]),
        pltpu.make_async_copy(dr, de_out, out_sem.at[1]),
        pltpu.make_async_copy(h_v, h_out, out_sem.at[2]),
        pltpu.make_async_copy(da_v, da_out, out_sem.at[3]),
        pltpu.make_async_copy(db_v, db_out, out_sem.at[4]),
    ]
    for c in outs:
        c.start()

    tb = 128
    n_tb = n_tok // tb

    def spots(col, toks):
        lanes = lax.broadcasted_iota(I32, (tb, 128), 1).astype(F32)
        base = col[toks, :]
        return jnp.concatenate([base == lanes + float(u * 128) for u in range(n_exp * cap // 128)], axis=1)

    def ship(buf, toks, send_sem, recv_sem):
        pltpu.make_async_remote_copy(
            src_ref=buf.at[toks], dst_ref=buf.at[toks], send_sem=send_sem, recv_sem=recv_sem,
            device_id=(other, r), device_id_type=MESH,
        ).start()

    @pl.when(owner)
    def _():
        @pl.loop(0, n_loc)
        def _(j):
            wait_recv(orr.at[j, pl.ds(0, ep_size - 1)], or_sem.at[j])

        @pl.loop(0, n_tb)
        def _(t):
            toks = pl.ds(pl.multiple_of(t * tb, tb), tb)
            pick1 = jnp.where(spots(s1c, toks), 1.0, 0.0).astype(BF)
            pick2 = jnp.where(spots(s2c, toks), 1.0, 0.0).astype(BF)
            dg1 = jnp.zeros((tb, 1), F32)
            dg2 = jnp.zeros((tb, 1), F32)
            ga = g1c[toks, 0:1]
            gb = g2c[toks, 0:1]
            for c in range(0, width, 512):
                rows = orr[:, :, :, c:c + 512].reshape(n_exp * cap, 512)
                o1 = dot(pick1, rows)
                o2 = dot(pick2, rows)
                y_v[toks, c:c + 512] = (ga * o1 + gb * o2).astype(BF)
                dyf = dy_v[toks, c:c + 512].astype(F32)
                dg1 = dg1 + jnp.sum(dyf * o1, axis=1, keepdims=True)
                dg2 = dg2 + jnp.sum(dyf * o2, axis=1, keepdims=True)
            ship(y_v, toks, ys_sem, yr_sem)
            qa = q1c[toks, 0:1]
            qb = q2c[toks, 0:1]
            shared = dg1 * ga + dg2 * gb
            dq1 = (dg1 - shared) / (qa + qb)
            dq2 = (dg2 - shared) / (qa + qb)
            centre = dq1 * qa + dq2 * qb
            lanes = lax.broadcasted_iota(I32, (tb, n_exp), 1).astype(F32)
            pull = jnp.where(i1c[toks, :n_exp] == lanes, dq1, 0.0) + jnp.where(i2c[toks, :n_exp] == lanes, dq2, 0.0)
            dl_v[toks, :] = prob_v[toks, :] * (pull - centre)

        d_hi, d_mid, d_low = split3(dl_v[...])
        for c in range(0, width, 512):
            xc = x_v[:, c:c + 512]
            piece = dot(d_hi, xc, TN) + (dot(d_mid, xc, TN) + dot(d_low, xc, TN))
            dwp[:, :, c:c + 512] = piece.reshape(ep_size, n_loc, 512)
        for d in range(1, ep_size):
            q = (r + d) % ep_size
            pltpu.make_async_remote_copy(
                src_ref=dwp.at[q], dst_ref=dwi.at[r], send_sem=rs_sem, recv_sem=rr_sem,
                device_id=(q % tp_size, q), device_id_type=MESH,
            ).start()
        dwi[r] = dwp[r]

        @pl.loop(0, n_loc)
        def _(j):
            wait_recv(dxr.at[j, pl.ds(0, ep_size - 1)], dxr_sem.at[j])

        wait_recv(dwi.at[pl.ds(0, ep_size - 1)], rr_sem)
        total = dwi[0]
        for q in range(1, ep_size):
            total = total + dwi[q]
        dwf[r] = total
        for d in range(1, n_dev):
            flat = (k * ep_size + r + d) % n_dev
            pltpu.make_async_remote_copy(
                src_ref=dwf.at[r], dst_ref=dwf.at[r], send_sem=fs_sem, recv_sem=fr_sem,
                device_id=(flat // ep_size, flat % ep_size), device_id_type=MESH,
            ).start()
        @pl.loop(0, n_tb)
        def _(t):
            toks = pl.ds(pl.multiple_of(t * tb, tb), tb)
            pick = jnp.where(spots(s1c, toks) | spots(s2c, toks), 1.0, 0.0).astype(BF)
            dl = dl_v[toks, :]
            for c in range(0, width, 512):
                rows = dxr[:, :, :, c:c + 512].reshape(n_exp * cap, 512)
                back = dot(pick, rows)
                router = lax.dot_general(
                    dl, wr_v[:, c:c + 512], NN, precision=lax.Precision.HIGHEST, preferred_element_type=F32
                )
                dx_v[toks, c:c + 512] = (back + router).astype(BF)
            pltpu.make_async_copy(dx_v.at[toks], dx_out.at[toks], in_sem.at[1]).start()

        wait_recv(dwf.at[pl.ds(0, ep_size - 1)], fr_sem)
        wait_send(dwp.at[pl.ds(0, ep_size - 1)], rs_sem)
        for half_sends in range(n_dev - 1):
            wait_send(dwf.at[r], fs_sem)
        wait_send(y_v, ys_sem)
        wait_send(orr.at[:, pl.ds(0, half - 1)], os_sem)
        wait_send(dxr.at[:, pl.ds(0, half - 1)], dxs_sem)

    @pl.when(jnp.logical_not(owner))
    def _():
        dx_v[...] = jnp.zeros_like(dx_v)
        pltpu.make_async_copy(dx_v, dx_out, in_sem.at[1]).start()
        wait_recv(y_v, yr_sem)
        wait_recv(dwf, fr_sem)
        wait_send(orr.at[:, pl.ds(0, half)], os_sem)
        wait_send(dxr.at[:, pl.ds(0, half)], dxs_sem)

    finals = [
        pltpu.make_async_copy(y_v, y_out, in_sem.at[0]),
        pltpu.make_async_copy(dwf, dwr_out, in_sem.at[2]),
    ]
    for c in finals:
        c.start()
    finals.append(pltpu.make_async_copy(dx_v, dx_out, in_sem.at[1]))
    wait_send(ds.at[:, pl.ds(0, ep_size - 1)], ds_sem)
    wait_send(xr.at[:, 0], xfs_sem)
    wait_send(ps.at[:, pl.ds(0, half)], ps_sem)
    wait_send(xs.at[:, pl.ds(0, half)], pds_sem)
    for c in outs + finals:
        c.wait()


def weight_kernel(xe, de, h, da, db, y, dwr, ga_out, gb_out, gc_out, y_out, dwr_out):
    y_out[...] = y[...]
    dwr_out[...] = dwr[...]
    rows = xe[0]
    ga_out[0] = dot(rows, da[0], TN)
    gb_out[0] = dot(rows, db[0], TN)
    gc_out[0] = dot(h[0], de[0], TN)


def solution(mesh):
    tp_size = mesh.shape["tp"]
    ep_size = mesh.shape["ep"]

    def local_step(x_rows, w_router, first_ids, second_ids, w_gelu, w_lin, w_out, dy_rows):
        n_tok, width = x_rows.shape
        n_exp = w_router.shape[1]
        n_loc, _, hid = w_gelu.shape
        cap = 2 * n_tok // n_exp
        blk = ep_size * cap
        half = ep_size // tp_size
        dma = pltpu.SemaphoreType.DMA
        any_spec = pl.BlockSpec(memory_space=pl.ANY)
        vmem_spec = pl.BlockSpec(memory_space=pltpu.VMEM)
        sds = jax.ShapeDtypeStruct
        rows_shape = (n_loc, ep_size, cap, width)
        half_shape = (n_loc, half, cap, width)
        hid_shape = (n_loc, blk, hid)
        col = pltpu.VMEM((n_tok, 128), F32)
        row = pltpu.VMEM((1, n_tok), F32)
        outs = pl.pallas_call(
            functools.partial(moe_kernel, tp_size, ep_size, cap),
            name="moe",
            in_specs=[vmem_spec] * 2 + [any_spec] * 6,
            out_specs=[any_spec] * 8,
            out_shape=[
                sds((n_tok, width), BF), sds((n_tok, width), BF), sds((ep_size, n_loc, width), F32),
                sds(rows_shape, BF), sds(rows_shape, BF), sds(hid_shape, BF), sds(hid_shape, BF), sds(hid_shape, BF),
            ],
            scratch_shapes=[
                pltpu.VMEM((n_tok, width), BF), pltpu.VMEM((n_tok, width), BF), pltpu.VMEM((n_exp, width), F32),
                pltpu.VMEM((n_loc, width, hid), BF), pltpu.VMEM((n_loc, width, hid), BF), pltpu.VMEM((n_loc, hid, width), BF),
                pltpu.VMEM(rows_shape, BF), pltpu.VMEM(rows_shape, BF), pltpu.VMEM(rows_shape, BF), pltpu.VMEM(rows_shape, BF),
                pltpu.VMEM(hid_shape, BF), pltpu.VMEM(hid_shape, BF), pltpu.VMEM(hid_shape, BF),
                pltpu.VMEM(hid_shape, F32), pltpu.VMEM(hid_shape, F32),
                pltpu.VMEM(rows_shape, BF), pltpu.VMEM(half_shape, BF), pltpu.VMEM(half_shape, BF),
                pltpu.VMEM(rows_shape, BF), pltpu.VMEM(rows_shape, BF),
                pltpu.VMEM((n_tok, width), BF), pltpu.VMEM((n_tok, width), BF),
                row, row, row, row, col, col, col, col, col, col, col, col,
                pltpu.VMEM((n_tok, n_exp), F32), pltpu.VMEM((n_tok, n_exp), F32),
                pltpu.VMEM((ep_size, n_loc, width), F32), pltpu.VMEM((ep_size, n_loc, width), F32),
                pltpu.VMEM((ep_size, n_loc, width), F32),
                dma((3,)), dma((3, n_loc)), dma((5,)),
                dma(()), dma((n_loc,)), dma((n_loc,)), dma((n_loc,)), dma(()), dma(()), dma((n_loc,)),
                dma(()), dma((n_loc,)), dma(()), dma((n_loc,)),
                dma(()), dma((n_loc,)), dma(()), dma((n_loc,)),
                dma(()), dma(()),
                dma(()), dma(()), dma(()), dma(()),
            ],
            compiler_params=pltpu.CompilerParams(
                collective_id=0, has_side_effects=True, vmem_limit_bytes=67043328
            ),
        )(
            first_ids.reshape(1, n_tok), second_ids.reshape(1, n_tok), x_rows, dy_rows, w_router.T,
            w_gelu, w_lin, w_out,
        )
        act_out, grad_in, grad_router, xe, de, h, da, db = outs
        partners = [
            ((q % tp_size) * ep_size + q, (1 - q % tp_size) * ep_size + q) for q in range(ep_size)
        ]
        passed = lax.ppermute(grad_in, ("tp", "ep"), partners)
        owner = lax.axis_index("ep") % tp_size == lax.axis_index("tp")
        grad_in = jnp.where(owner, grad_in, passed)
        xe = xe.reshape(n_loc, blk, width)
        de = de.reshape(n_loc, blk, width)

        y_spec = pl.BlockSpec((n_tok // n_loc, width), lambda e: (e, 0))

        def spec(*shape):
            return pl.BlockSpec((1,) + shape, lambda e: (e, 0, 0))

        grad_wa, grad_wb, grad_wc, act_out, grad_router = pl.pallas_call(
            weight_kernel,
            name="weight_grads",
            grid=(n_loc,),
            in_specs=[spec(blk, width), spec(blk, width), spec(blk, hid), spec(blk, hid), spec(blk, hid), y_spec, spec(n_exp // n_loc, width)],
            out_specs=[spec(width, hid), spec(width, hid), spec(hid, width), y_spec, spec(n_exp // n_loc, width)],
            out_shape=[
                sds((n_loc, width, hid), F32), sds((n_loc, width, hid), F32), sds((n_loc, hid, width), F32),
                sds((n_tok, width), BF), sds((n_loc, n_exp // n_loc, width), F32),
            ],
            compiler_params=pltpu.CompilerParams(
                dimension_semantics=("arbitrary",), vmem_limit_bytes=67043328
            ),
            cost_estimate=pl.CostEstimate(
                flops=6 * n_loc * blk * width * hid, transcendentals=0,
                bytes_accessed=12 * n_loc * width * hid + 4 * n_loc * blk * width + 6 * n_loc * blk * hid,
            ),
        )(xe, de, h, da, db, act_out, grad_router.reshape(n_loc, n_exp // n_loc, width))
        return act_out, grad_in, grad_wa, grad_wb, grad_wc, grad_router.reshape(n_exp, width).T

    return jax.shard_map(
        local_step,
        mesh=mesh,
        in_specs=(P("ep", None), P(), P("ep"), P("ep"), P("ep", None, "tp"), P("ep", None, "tp"), P("ep", "tp", None), P("ep", None)),
        out_specs=(P("ep", None), P("ep", None), P("ep", None, "tp"), P("ep", None, "tp"), P("ep", "tp", None), P()),
        check_vma=False,
    )
```

```python
import functools

import jax
import jax.numpy as jnp
from jax import lax
from jax.experimental import pallas as pl
from jax.experimental.pallas import tpu as pltpu
from jax.sharding import PartitionSpec as P

BF = jnp.bfloat16
F32 = jnp.float32
I32 = jnp.int32
MESH = pl.DeviceIdType.MESH
GELU_COEF = 0.7978845608028654
AHEAD = 3
Y_STEP = 3
NN = (((1,), (0,)), ((), ()))
NT = (((1,), (1,)), ((), ()))
TN = (((0,), (0,)), ((), ()))


def dot(a, b, dims=NN):
    return lax.dot_general(a, b, dims, preferred_element_type=F32)


def split3(v):
    hi = v.astype(BF)
    rest = v - hi.astype(F32)
    mid = rest.astype(BF)
    low = (rest - mid.astype(F32)).astype(BF)
    return hi, mid, low


def moe_kernel(
    tp_size, ep_size, cap,
    ids1_ref, ids2_ref, x_hbm, dy_hbm, wr_hbm, wa_hbm, wb_hbm, wc_hbm,
    y_out, dx_out, dwr_out, xe_out, de_out, h_out, da_out, db_out,
    x_v, dy_v, wr_v, wa_v, wb_v, wc_v,
    xs, ds, xr, dr, h_v, da_v, db_v, bs_v, gv_v,
    ps, pr, pdr, orr, dxr, y_v, dx_v,
    s1r, s2r, g1r, g2r, s1c, s2c, g1c, g2c, q1c, q2c, i1c, i2c, prob_v, dl_v,
    dwp, dwi, dwf,
    in_sem, w_sem, out_sem,
    xs_sem, xr_sem, xd_sem, xf_sem, xfs_sem, ds_sem, dr_sem,
    ps_sem, pr_sem, pds_sem, pdr_sem,
    os_sem, or_sem, dxs_sem, dxr_sem,
    ys_sem, yr_sem,
    rs_sem, rr_sem, fs_sem, fr_sem,
):
    k = lax.axis_index("tp")
    r = lax.axis_index("ep")
    n_loc = wa_v.shape[0]
    n_tok, width = x_v.shape
    hid = wa_v.shape[2]
    n_exp = n_loc * ep_size
    blk = ep_size * cap
    half = ep_size // tp_size
    my_place = (r % tp_size) * half + r // tp_size
    owner = (r % tp_size) == k
    other = 1 - k

    ins = [
        pltpu.make_async_copy(x_hbm, x_v, in_sem.at[0]),
        pltpu.make_async_copy(dy_hbm, dy_v, in_sem.at[1]),
        pltpu.make_async_copy(wr_hbm, wr_v, in_sem.at[2]),
    ]
    ins[0].start()

    def weight_copies(j):
        return [
            pltpu.make_async_copy(wa_hbm.at[j], wa_v.at[j], w_sem.at[0, j]),
            pltpu.make_async_copy(wb_hbm.at[j], wb_v.at[j], w_sem.at[1, j]),
            pltpu.make_async_copy(wc_hbm.at[j], wc_v.at[j], w_sem.at[2, j]),
        ]

    n_dev = tp_size * ep_size
    barrier = pltpu.get_barrier_semaphore()
    for d in range(1, n_dev):
        flat = (k * ep_size + r + d) % n_dev
        pl.semaphore_signal(barrier, inc=1, device_id=(flat // ep_size, flat % ep_size), device_id_type=MESH)

    ids1 = ids1_ref[...]
    ids2 = ids2_ref[...]
    e_iota = lax.broadcasted_iota(I32, (n_exp, n_tok), 0)
    hot1 = jnp.where(ids1 == e_iota, 1.0, 0.0).astype(F32)
    hot2 = jnp.where(ids2 == e_iota, 1.0, 0.0).astype(F32)
    before = jnp.where(
        lax.broadcasted_iota(I32, (n_tok, n_tok), 0) < lax.broadcasted_iota(I32, (n_tok, n_tok), 1), 1.0, 0.0
    ).astype(BF)
    cum1 = dot(hot1.astype(BF), before)
    cum2 = dot(hot2.astype(BF), before)
    fill1 = jnp.sum(hot1, axis=1, keepdims=True)
    pos1 = jnp.sum(cum1 * hot1, axis=0, keepdims=True)
    pos2 = jnp.sum((cum2 + fill1) * hot2, axis=0, keepdims=True)

    def place(ids, pos):
        spot = (ids & (n_loc - 1)) * blk + (ids // n_loc) * cap
        return jnp.where(pos < cap, spot.astype(F32) + pos, float(n_exp * cap))

    s1r[...] = place(ids1, pos1)
    s2r[...] = place(ids2, pos2)

    def masks(j):
        spot = (lax.broadcasted_iota(I32, (blk, n_tok), 0) + j * blk).astype(F32)
        return s1r[...] == spot, s2r[...] == spot

    chip = r // 2
    chip_x = chip + 1 - 2 * (chip % 2)
    chip_y = (chip + 2) % 4
    chip_d = 3 - chip
    core = r % 2
    diag = 2 * chip_d + (k + r) % 2
    near = [2 * chip_x + core, 2 * chip_y + core, 2 * chip_x + 1 - core, 2 * chip_y + 1 - core, 2 * chip + 1 - core]
    far = [2 * chip_d + core, 2 * chip_d + 1 - core]

    def place_of(q):
        return (q % tp_size) * half + q // tp_size

    def send_row(src, dst, send_sem, recv_sem, j, q):
        pltpu.make_async_remote_copy(
            src_ref=src.at[j, q], dst_ref=dst.at[j, my_place],
            send_sem=send_sem, recv_sem=recv_sem.at[j],
            device_id=(k, q), device_id_type=MESH,
        ).start()

    def wait_recv(view, sem):
        pltpu.make_async_remote_copy(
            src_ref=view, dst_ref=view, send_sem=sem, recv_sem=sem, device_id=(k, r), device_id_type=MESH
        ).wait_recv()

    def wait_send(view, sem):
        pltpu.make_async_remote_copy(
            src_ref=view, dst_ref=view, send_sem=sem, recv_sem=sem, device_id=(k, r), device_id_type=MESH
        ).wait_send()

    def build_x(j):
        m1, m2 = masks(j)
        pick = jnp.where(m1 | m2, 1.0, 0.0).astype(BF)
        for c in range(0, width, 512):
            rows = dot(pick, x_v[:, c:c + 512]).astype(BF)
            xs[j, :, :, c:c + 512] = rows.reshape(ep_size, cap, 512)
        send_row(xs, xr, xs_sem, xd_sem, j, diag)
        for q in near:
            send_row(xs, xr, xs_sem, xr_sem, j, q)
        xr[j, my_place] = xs[j, r]

    ins[0].wait()
    ins[2].start()
    ins[1].start()

    @pl.loop(0, n_loc)
    def _(j):
        for c in weight_copies(j):
            c.start()

    pl.semaphore_wait(barrier, n_dev - 1)

    @pl.loop(0, AHEAD)
    def _(j):
        build_x(j)

    def column(row):
        return jnp.transpose(jnp.broadcast_to(row, (128, n_tok)))

    s1c[...] = column(s1r[...])
    s2c[...] = column(s2r[...])
    i1c[...] = column(ids1.astype(F32))
    i2c[...] = column(ids2.astype(F32))
    ins[2].wait()
    wr_hi, wr_mid, wr_low = split3(wr_v[...])
    xv = x_v[...]
    logits = dot(xv, wr_hi, NT) + (dot(xv, wr_mid, NT) + dot(xv, wr_low, NT))
    ex = jnp.exp(logits - jnp.max(logits, axis=1, keepdims=True))
    prob = ex / jnp.sum(ex, axis=1, keepdims=True)
    prob_v[...] = prob
    lane = lax.broadcasted_iota(I32, (n_tok, n_exp), 1).astype(F32)
    q1 = jnp.sum(jnp.where(i1c[:, :n_exp] == lane, prob, 0.0), axis=1, keepdims=True)
    q2 = jnp.sum(jnp.where(i2c[:, :n_exp] == lane, prob, 0.0), axis=1, keepdims=True)
    g1 = jnp.broadcast_to(q1 / (q1 + q2), (n_tok, 128))
    g2 = jnp.broadcast_to(q2 / (q1 + q2), (n_tok, 128))
    g1c[...] = g1
    g2c[...] = g2
    q1c[...] = jnp.broadcast_to(q1, (n_tok, 128))
    q2c[...] = jnp.broadcast_to(q2, (n_tok, 128))
    g1r[...] = jnp.transpose(g1)[0:1, :]
    g2r[...] = jnp.transpose(g2)[0:1, :]
    ins[1].wait()

    def build_d(j):
        m1, m2 = masks(j)
        pick = jnp.where(m1 | m2, 1.0, 0.0).astype(BF)
        gate = jnp.sum(jnp.where(m1, g1r[...], 0.0) + jnp.where(m2, g2r[...], 0.0), axis=1, keepdims=True)
        for c in range(0, width, 512):
            rows = (gate * dot(pick, dy_v[:, c:c + 512])).astype(BF)
            ds[j, :, :, c:c + 512] = rows.reshape(ep_size, cap, 512)
        for q in far + near:
            send_row(ds, dr, ds_sem, dr_sem, j, q)
        dr[j, my_place] = ds[j, r]

    def send_half(src, dst, send_sem, recv_sem, j):
        pltpu.make_async_remote_copy(
            src_ref=src.at[j, pl.ds(other * half, half)], dst_ref=dst.at[j],
            send_sem=send_sem, recv_sem=recv_sem.at[j],
            device_id=(other, r), device_id_type=MESH,
        ).start()

    def merge_and_return(src, got, got_sem, dst, send_sem, recv_sem, j):
        wait_recv(got.at[j], got_sem.at[j])
        mine = pl.ds(k * half, half)
        src[j, mine] = (src[j, mine].astype(F32) + got[j].astype(F32)).astype(BF)
        for d in range(half):
            c = (r // tp_size + d) % half
            q = tp_size * c + k

            @pl.when(q != r)
            def _():
                pltpu.make_async_remote_copy(
                    src_ref=src.at[j, k * half + c], dst_ref=dst.at[j, r],
                    send_sem=send_sem, recv_sem=recv_sem.at[j],
                    device_id=(k, q), device_id_type=MESH,
                ).start()

            @pl.when(q == r)
            def _():
                dst[j, r] = src[j, k * half + c]

    n_near = len(near)
    diag_place = place_of(diag)

    def forward_diag(j):
        wait_recv(xr.at[j, 0], xd_sem.at[j])
        pltpu.make_async_remote_copy(
            src_ref=xr.at[j, diag_place], dst_ref=xr.at[j, diag_place],
            send_sem=xfs_sem, recv_sem=xf_sem.at[j],
            device_id=(other, r), device_id_type=MESH,
        ).start()

    forward_diag(0)

    @pl.loop(0, n_loc)
    def _(j):
        @pl.when(j + AHEAD < n_loc)
        def _():
            build_x(j + AHEAD)

        @pl.when(j + AHEAD >= n_loc)
        def _():
            build_d(j + AHEAD - n_loc)

        @pl.when(j + 1 < n_loc)
        def _():
            forward_diag(j + 1)

        for c in weight_copies(j):
            c.wait()
        wait_recv(xr.at[j, pl.ds(0, n_near)], xr_sem.at[j])
        wait_recv(xr.at[j, 0], xf_sem.at[j])
        rows = xr[j].reshape(blk, width)
        pa = dot(rows, wa_v[j])
        pb = dot(rows, wb_v[j])
        th = jnp.tanh(GELU_COEF * (pa + 0.044715 * pa * pa * pa))
        gv = 0.5 * pa * (1.0 + th)
        slope = 0.5 * (1.0 + th) + 0.5 * pa * (1.0 - th * th) * GELU_COEF * (1.0 + 0.134145 * pa * pa)
        gv_v[j] = gv
        bs_v[j] = pb * slope
        hidden = (gv * pb).astype(BF)
        h_v[j] = hidden
        for c in range(0, width, 512):
            ps[j, :, :, c:c + 512] = dot(hidden, wc_v[j, :, c:c + 512]).astype(BF).reshape(ep_size, cap, 512)
        send_half(ps, pr, ps_sem, pr_sem, j)

        @pl.when(j > 0)
        def _():
            merge_and_return(ps, pr, pr_sem, orr, os_sem, or_sem, j - 1)

    tb = 128
    n_tb = n_tok // tb

    def spots(col, toks):
        lanes = lax.broadcasted_iota(I32, (tb, 128), 1).astype(F32)
        base = col[toks, :]
        return jnp.concatenate([base == lanes + float(u * 128) for u in range(n_exp * cap // 128)], axis=1)

    def ship(buf, toks, send_sem, recv_sem):
        pltpu.make_async_remote_copy(
            src_ref=buf.at[toks], dst_ref=buf.at[toks], send_sem=send_sem, recv_sem=recv_sem,
            device_id=(other, r), device_id_type=MESH,
        ).start()

    def combine_y(t):
        toks = pl.ds(pl.multiple_of(t * tb, tb), tb)
        pick1 = jnp.where(spots(s1c, toks), 1.0, 0.0).astype(BF)
        pick2 = jnp.where(spots(s2c, toks), 1.0, 0.0).astype(BF)
        dg1 = jnp.zeros((tb, 1), F32)
        dg2 = jnp.zeros((tb, 1), F32)
        ga = g1c[toks, 0:1]
        gb = g2c[toks, 0:1]
        for c in range(0, width, 512):
            rows = orr[:, :, :, c:c + 512].reshape(n_exp * cap, 512)
            o1 = dot(pick1, rows)
            o2 = dot(pick2, rows)
            y_v[toks, c:c + 512] = (ga * o1 + gb * o2).astype(BF)
            dyf = dy_v[toks, c:c + 512].astype(F32)
            dg1 = dg1 + jnp.sum(dyf * o1, axis=1, keepdims=True)
            dg2 = dg2 + jnp.sum(dyf * o2, axis=1, keepdims=True)
        ship(y_v, toks, ys_sem, yr_sem)
        qa = q1c[toks, 0:1]
        qb = q2c[toks, 0:1]
        shared = dg1 * ga + dg2 * gb
        dq1 = (dg1 - shared) / (qa + qb)
        dq2 = (dg2 - shared) / (qa + qb)
        centre = dq1 * qa + dq2 * qb
        lanes = lax.broadcasted_iota(I32, (tb, n_exp), 1).astype(F32)
        pull = jnp.where(i1c[toks, :n_exp] == lanes, dq1, 0.0) + jnp.where(i2c[toks, :n_exp] == lanes, dq2, 0.0)
        dl_v[toks, :] = prob_v[toks, :] * (pull - centre)

    wait_send(xs.at[:, pl.ds(0, n_near + 1)], xs_sem)

    @pl.loop(0, n_loc)
    def _(j):
        @pl.when(j + AHEAD < n_loc)
        def _():
            build_d(j + AHEAD)

        wait_recv(dr.at[j, pl.ds(0, ep_size - 1)], dr_sem.at[j])
        rows = dr[j].reshape(blk, width)
        dh = dot(rows, wc_v[j], NT)
        da = (dh * bs_v[j]).astype(BF)
        db = (dh * gv_v[j]).astype(BF)
        da_v[j] = da
        db_v[j] = db
        for c in range(0, width, 512):
            part = dot(da, wa_v[j, c:c + 512, :], NT) + dot(db, wb_v[j, c:c + 512, :], NT)
            xs[j, :, :, c:c + 512] = part.astype(BF).reshape(ep_size, cap, 512)
        send_half(xs, pdr, pds_sem, pdr_sem, j)

        @pl.when(j == 0)
        def _():
            merge_and_return(ps, pr, pr_sem, orr, os_sem, or_sem, n_loc - 1)

        @pl.when(j > 0)
        def _():
            merge_and_return(xs, pdr, pdr_sem, dxr, dxs_sem, dxr_sem, j - 1)

        @pl.when(owner & (j == Y_STEP))
        def _():
            @pl.loop(0, n_loc)
            def _(i):
                wait_recv(orr.at[i, pl.ds(0, ep_size - 1)], or_sem.at[i])

        @pl.when(owner & (j >= Y_STEP) & (j < Y_STEP + n_tb))
        def _():
            combine_y(j - Y_STEP)

    merge_and_return(xs, pdr, pdr_sem, dxr, dxs_sem, dxr_sem, n_loc - 1)

    outs = [
        pltpu.make_async_copy(xr, xe_out, out_sem.at[0]),
        pltpu.make_async_copy(dr, de_out, out_sem.at[1]),
        pltpu.make_async_copy(h_v, h_out, out_sem.at[2]),
        pltpu.make_async_copy(da_v, da_out, out_sem.at[3]),
        pltpu.make_async_copy(db_v, db_out, out_sem.at[4]),
    ]
    for c in outs:
        c.start()

    @pl.when(owner)
    def _():
        d_hi, d_mid, d_low = split3(dl_v[...])
        for c in range(0, width, 512):
            xc = x_v[:, c:c + 512]
            piece = dot(d_hi, xc, TN) + (dot(d_mid, xc, TN) + dot(d_low, xc, TN))
            dwp[:, :, c:c + 512] = piece.reshape(ep_size, n_loc, 512)
        for d in range(1, ep_size):
            q = (r + d) % ep_size
            pltpu.make_async_remote_copy(
                src_ref=dwp.at[q], dst_ref=dwi.at[r], send_sem=rs_sem, recv_sem=rr_sem,
                device_id=(q % tp_size, q), device_id_type=MESH,
            ).start()
        dwi[r] = dwp[r]

        @pl.loop(0, n_loc)
        def _(j):
            wait_recv(dxr.at[j, pl.ds(0, ep_size - 1)], dxr_sem.at[j])

        wait_recv(dwi.at[pl.ds(0, ep_size - 1)], rr_sem)
        total = dwi[0]
        for q in range(1, ep_size):
            total = total + dwi[q]
        dwf[r] = total
        for d in range(1, n_dev):
            flat = (k * ep_size + r + d) % n_dev
            pltpu.make_async_remote_copy(
                src_ref=dwf.at[r], dst_ref=dwf.at[r], send_sem=fs_sem, recv_sem=fr_sem,
                device_id=(flat // ep_size, flat % ep_size), device_id_type=MESH,
            ).start()
        @pl.loop(0, n_tb)
        def _(t):
            toks = pl.ds(pl.multiple_of(t * tb, tb), tb)
            pick = jnp.where(spots(s1c, toks) | spots(s2c, toks), 1.0, 0.0).astype(BF)
            dl = dl_v[toks, :]
            for c in range(0, width, 512):
                rows = dxr[:, :, :, c:c + 512].reshape(n_exp * cap, 512)
                back = dot(pick, rows)
                router = lax.dot_general(
                    dl, wr_v[:, c:c + 512], NN, precision=lax.Precision.HIGHEST, preferred_element_type=F32
                )
                dx_v[toks, c:c + 512] = (back + router).astype(BF)
            pltpu.make_async_copy(dx_v.at[toks], dx_out.at[toks], in_sem.at[1]).start()

        wait_recv(dwf.at[pl.ds(0, ep_size - 1)], fr_sem)
        wait_send(dwp.at[pl.ds(0, ep_size - 1)], rs_sem)
        for half_sends in range(n_dev - 1):
            wait_send(dwf.at[r], fs_sem)
        wait_send(y_v, ys_sem)
        wait_send(orr.at[:, pl.ds(0, half - 1)], os_sem)
        wait_send(dxr.at[:, pl.ds(0, half - 1)], dxs_sem)

    @pl.when(jnp.logical_not(owner))
    def _():
        dx_v[...] = jnp.zeros_like(dx_v)
        pltpu.make_async_copy(dx_v, dx_out, in_sem.at[1]).start()
        wait_recv(y_v, yr_sem)
        wait_recv(dwf, fr_sem)
        wait_send(orr.at[:, pl.ds(0, half)], os_sem)
        wait_send(dxr.at[:, pl.ds(0, half)], dxs_sem)

    finals = [
        pltpu.make_async_copy(y_v, y_out, in_sem.at[0]),
        pltpu.make_async_copy(dwf, dwr_out, in_sem.at[2]),
    ]
    for c in finals:
        c.start()
    finals.append(pltpu.make_async_copy(dx_v, dx_out, in_sem.at[1]))
    wait_send(ds.at[:, pl.ds(0, ep_size - 1)], ds_sem)
    wait_send(xr.at[:, 0], xfs_sem)
    wait_send(ps.at[:, pl.ds(0, half)], ps_sem)
    wait_send(xs.at[:, pl.ds(0, half)], pds_sem)
    for c in outs + finals:
        c.wait()


def weight_kernel(xe, de, h, da, db, y, dwr, ga_out, gb_out, gc_out, y_out, dwr_out):
    y_out[...] = y[...]
    dwr_out[...] = dwr[...]
    rows = xe[0]
    ga_out[0] = dot(rows, da[0], TN)
    gb_out[0] = dot(rows, db[0], TN)
    gc_out[0] = dot(h[0], de[0], TN)


def solution(mesh):
    tp_size = mesh.shape["tp"]
    ep_size = mesh.shape["ep"]

    def local_step(x_rows, w_router, first_ids, second_ids, w_gelu, w_lin, w_out, dy_rows):
        n_tok, width = x_rows.shape
        n_exp = w_router.shape[1]
        n_loc, _, hid = w_gelu.shape
        cap = 2 * n_tok // n_exp
        blk = ep_size * cap
        half = ep_size // tp_size
        dma = pltpu.SemaphoreType.DMA
        any_spec = pl.BlockSpec(memory_space=pl.ANY)
        vmem_spec = pl.BlockSpec(memory_space=pltpu.VMEM)
        sds = jax.ShapeDtypeStruct
        rows_shape = (n_loc, ep_size, cap, width)
        half_shape = (n_loc, half, cap, width)
        hid_shape = (n_loc, blk, hid)
        col = pltpu.VMEM((n_tok, 128), F32)
        row = pltpu.VMEM((1, n_tok), F32)
        outs = pl.pallas_call(
            functools.partial(moe_kernel, tp_size, ep_size, cap),
            name="moe",
            in_specs=[vmem_spec] * 2 + [any_spec] * 6,
            out_specs=[any_spec] * 8,
            out_shape=[
                sds((n_tok, width), BF), sds((n_tok, width), BF), sds((ep_size, n_loc, width), F32),
                sds(rows_shape, BF), sds(rows_shape, BF), sds(hid_shape, BF), sds(hid_shape, BF), sds(hid_shape, BF),
            ],
            scratch_shapes=[
                pltpu.VMEM((n_tok, width), BF), pltpu.VMEM((n_tok, width), BF), pltpu.VMEM((n_exp, width), F32),
                pltpu.VMEM((n_loc, width, hid), BF), pltpu.VMEM((n_loc, width, hid), BF), pltpu.VMEM((n_loc, hid, width), BF),
                pltpu.VMEM(rows_shape, BF), pltpu.VMEM(rows_shape, BF), pltpu.VMEM(rows_shape, BF), pltpu.VMEM(rows_shape, BF),
                pltpu.VMEM(hid_shape, BF), pltpu.VMEM(hid_shape, BF), pltpu.VMEM(hid_shape, BF),
                pltpu.VMEM(hid_shape, F32), pltpu.VMEM(hid_shape, F32),
                pltpu.VMEM(rows_shape, BF), pltpu.VMEM(half_shape, BF), pltpu.VMEM(half_shape, BF),
                pltpu.VMEM(rows_shape, BF), pltpu.VMEM(rows_shape, BF),
                pltpu.VMEM((n_tok, width), BF), pltpu.VMEM((n_tok, width), BF),
                row, row, row, row, col, col, col, col, col, col, col, col,
                pltpu.VMEM((n_tok, n_exp), F32), pltpu.VMEM((n_tok, n_exp), F32),
                pltpu.VMEM((ep_size, n_loc, width), F32), pltpu.VMEM((ep_size, n_loc, width), F32),
                pltpu.VMEM((ep_size, n_loc, width), F32),
                dma((3,)), dma((3, n_loc)), dma((5,)),
                dma(()), dma((n_loc,)), dma((n_loc,)), dma((n_loc,)), dma(()), dma(()), dma((n_loc,)),
                dma(()), dma((n_loc,)), dma(()), dma((n_loc,)),
                dma(()), dma((n_loc,)), dma(()), dma((n_loc,)),
                dma(()), dma(()),
                dma(()), dma(()), dma(()), dma(()),
            ],
            compiler_params=pltpu.CompilerParams(
                collective_id=0, has_side_effects=True, vmem_limit_bytes=67043328
            ),
        )(
            first_ids.reshape(1, n_tok), second_ids.reshape(1, n_tok), x_rows, dy_rows, w_router.T,
            w_gelu, w_lin, w_out,
        )
        act_out, grad_in, grad_router, xe, de, h, da, db = outs
        partners = [
            ((q % tp_size) * ep_size + q, (1 - q % tp_size) * ep_size + q) for q in range(ep_size)
        ]
        passed = lax.ppermute(grad_in, ("tp", "ep"), partners)
        owner = lax.axis_index("ep") % tp_size == lax.axis_index("tp")
        grad_in = jnp.where(owner, grad_in, passed)
        xe = xe.reshape(n_loc, blk, width)
        de = de.reshape(n_loc, blk, width)

        y_spec = pl.BlockSpec((n_tok // n_loc, width), lambda e: (e, 0))

        def spec(*shape):
            return pl.BlockSpec((1,) + shape, lambda e: (e, 0, 0))

        grad_wa, grad_wb, grad_wc, act_out, grad_router = pl.pallas_call(
            weight_kernel,
            name="weight_grads",
            grid=(n_loc,),
            in_specs=[spec(blk, width), spec(blk, width), spec(blk, hid), spec(blk, hid), spec(blk, hid), y_spec, spec(n_exp // n_loc, width)],
            out_specs=[spec(width, hid), spec(width, hid), spec(hid, width), y_spec, spec(n_exp // n_loc, width)],
            out_shape=[
                sds((n_loc, width, hid), F32), sds((n_loc, width, hid), F32), sds((n_loc, hid, width), F32),
                sds((n_tok, width), BF), sds((n_loc, n_exp // n_loc, width), F32),
            ],
            compiler_params=pltpu.CompilerParams(
                dimension_semantics=("arbitrary",), vmem_limit_bytes=67043328
            ),
            cost_estimate=pl.CostEstimate(
                flops=6 * n_loc * blk * width * hid, transcendentals=0,
                bytes_accessed=12 * n_loc * width * hid + 4 * n_loc * blk * width + 6 * n_loc * blk * hid,
            ),
        )(xe, de, h, da, db, act_out, grad_router.reshape(n_loc, n_exp // n_loc, width))
        return act_out, grad_in, grad_wa, grad_wb, grad_wc, grad_router.reshape(n_exp, width).T

    return jax.shard_map(
        local_step,
        mesh=mesh,
        in_specs=(P("ep", None), P(), P("ep"), P("ep"), P("ep", None, "tp"), P("ep", None, "tp"), P("ep", "tp", None), P("ep", None)),
        out_specs=(P("ep", None), P("ep", None), P("ep", None, "tp"), P("ep", None, "tp"), P("ep", "tp", None), P()),
        check_vma=False,
    )
```

```python
import functools

import jax
import jax.numpy as jnp
from jax import lax
from jax.experimental import pallas as pl
from jax.experimental.pallas import tpu as pltpu
from jax.sharding import PartitionSpec as P

BF = jnp.bfloat16
F32 = jnp.float32
I32 = jnp.int32
MESH = pl.DeviceIdType.MESH
GELU_COEF = 0.7978845608028654
AHEAD = 3
Y_STEP = 3
Y_INNER = 2
NN = (((1,), (0,)), ((), ()))
NT = (((1,), (1,)), ((), ()))
TN = (((0,), (0,)), ((), ()))


def dot(a, b, dims=NN):
    return lax.dot_general(a, b, dims, preferred_element_type=F32)


def split3(v):
    hi = v.astype(BF)
    rest = v - hi.astype(F32)
    mid = rest.astype(BF)
    low = (rest - mid.astype(F32)).astype(BF)
    return hi, mid, low


def moe_kernel(
    tp_size, ep_size, cap,
    ids1_ref, ids2_ref, x_hbm, dy_hbm, wr_hbm, wa_hbm, wb_hbm, wc_hbm,
    y_out, dx_out, dwr_out, xe_out, de_out, h_out, da_out, db_out,
    x_v, dy_v, wr_v, wa_v, wb_v, wc_v,
    xs, ds, xr, dr, h_v, da_v, db_v, bs_v, gv_v,
    ps, pr, pdr, orr, dxr, y_v, dx_v,
    s1r, s2r, g1r, g2r, s1c, s2c, g1c, g2c, q1c, q2c, i1c, i2c, prob_v, dl_v,
    dwp, dwi, dwf, acc_v,
    in_sem, w_sem, out_sem,
    xs_sem, xr_sem, xd_sem, xf_sem, xfs_sem, ds_sem, dr_sem,
    ps_sem, pr_sem, pds_sem, pdr_sem,
    os_sem, or_sem, dxs_sem, dxr_sem,
    ys_sem, yr_sem,
    rs_sem, rr_sem, fs_sem, fr_sem,
):
    k = lax.axis_index("tp")
    r = lax.axis_index("ep")
    n_loc = wa_v.shape[0]
    n_tok, width = x_v.shape
    hid = wa_v.shape[2]
    n_exp = n_loc * ep_size
    blk = ep_size * cap
    half = ep_size // tp_size
    my_place = (r % tp_size) * half + r // tp_size
    owner = (r % tp_size) == k
    other = 1 - k

    ins = [
        pltpu.make_async_copy(x_hbm, x_v, in_sem.at[0]),
        pltpu.make_async_copy(dy_hbm, dy_v, in_sem.at[1]),
        pltpu.make_async_copy(wr_hbm, wr_v, in_sem.at[2]),
    ]
    ins[0].start()

    def weight_copies(j):
        return [
            pltpu.make_async_copy(wa_hbm.at[j], wa_v.at[j], w_sem.at[0, j]),
            pltpu.make_async_copy(wb_hbm.at[j], wb_v.at[j], w_sem.at[1, j]),
            pltpu.make_async_copy(wc_hbm.at[j], wc_v.at[j], w_sem.at[2, j]),
        ]

    n_dev = tp_size * ep_size
    barrier = pltpu.get_barrier_semaphore()
    for d in range(1, n_dev):
        flat = (k * ep_size + r + d) % n_dev
        pl.semaphore_signal(barrier, inc=1, device_id=(flat // ep_size, flat % ep_size), device_id_type=MESH)

    ids1 = ids1_ref[...]
    ids2 = ids2_ref[...]
    e_iota = lax.broadcasted_iota(I32, (n_exp, n_tok), 0)
    hot1 = jnp.where(ids1 == e_iota, 1.0, 0.0).astype(F32)
    hot2 = jnp.where(ids2 == e_iota, 1.0, 0.0).astype(F32)
    before = jnp.where(
        lax.broadcasted_iota(I32, (n_tok, n_tok), 0) < lax.broadcasted_iota(I32, (n_tok, n_tok), 1), 1.0, 0.0
    ).astype(BF)
    cum1 = dot(hot1.astype(BF), before)
    cum2 = dot(hot2.astype(BF), before)
    fill1 = jnp.sum(hot1, axis=1, keepdims=True)
    pos1 = jnp.sum(cum1 * hot1, axis=0, keepdims=True)
    pos2 = jnp.sum((cum2 + fill1) * hot2, axis=0, keepdims=True)

    def place(ids, pos):
        spot = (ids & (n_loc - 1)) * blk + (ids // n_loc) * cap
        return jnp.where(pos < cap, spot.astype(F32) + pos, float(n_exp * cap))

    s1r[...] = place(ids1, pos1)
    s2r[...] = place(ids2, pos2)

    def masks(j):
        spot = (lax.broadcasted_iota(I32, (blk, n_tok), 0) + j * blk).astype(F32)
        return s1r[...] == spot, s2r[...] == spot

    chip = r // 2
    chip_x = chip + 1 - 2 * (chip % 2)
    chip_y = (chip + 2) % 4
    chip_d = 3 - chip
    core = r % 2
    diag = 2 * chip_d + (k + r) % 2
    near = [2 * chip_x + core, 2 * chip_y + core, 2 * chip_x + 1 - core, 2 * chip_y + 1 - core, 2 * chip + 1 - core]
    far = [2 * chip_d + core, 2 * chip_d + 1 - core]

    def place_of(q):
        return (q % tp_size) * half + q // tp_size

    def send_row(src, dst, send_sem, recv_sem, j, q):
        pltpu.make_async_remote_copy(
            src_ref=src.at[j, q], dst_ref=dst.at[j, my_place],
            send_sem=send_sem, recv_sem=recv_sem.at[j],
            device_id=(k, q), device_id_type=MESH,
        ).start()

    def wait_recv(view, sem):
        pltpu.make_async_remote_copy(
            src_ref=view, dst_ref=view, send_sem=sem, recv_sem=sem, device_id=(k, r), device_id_type=MESH
        ).wait_recv()

    def wait_send(view, sem):
        pltpu.make_async_remote_copy(
            src_ref=view, dst_ref=view, send_sem=sem, recv_sem=sem, device_id=(k, r), device_id_type=MESH
        ).wait_send()

    def build_x(j):
        m1, m2 = masks(j)
        pick = jnp.where(m1 | m2, 1.0, 0.0).astype(BF)
        for c in range(0, width, 512):
            rows = dot(pick, x_v[:, c:c + 512]).astype(BF)
            xs[j, :, :, c:c + 512] = rows.reshape(ep_size, cap, 512)
        send_row(xs, xr, xs_sem, xd_sem, j, diag)
        for q in near:
            send_row(xs, xr, xs_sem, xr_sem, j, q)
        xr[j, my_place] = xs[j, r]

    ins[0].wait()
    ins[2].start()
    ins[1].start()

    @pl.loop(0, n_loc)
    def _(j):
        for c in weight_copies(j):
            c.start()

    pl.semaphore_wait(barrier, n_dev - 1)

    @pl.loop(0, AHEAD)
    def _(j):
        build_x(j)

    def column(row):
        return jnp.transpose(jnp.broadcast_to(row, (128, n_tok)))

    s1c[...] = column(s1r[...])
    s2c[...] = column(s2r[...])
    i1c[...] = column(ids1.astype(F32))
    i2c[...] = column(ids2.astype(F32))
    ins[2].wait()
    wr_hi, wr_mid, wr_low = split3(wr_v[...])
    xv = x_v[...]
    logits = dot(xv, wr_hi, NT) + (dot(xv, wr_mid, NT) + dot(xv, wr_low, NT))
    ex = jnp.exp(logits - jnp.max(logits, axis=1, keepdims=True))
    prob = ex / jnp.sum(ex, axis=1, keepdims=True)
    prob_v[...] = prob
    lane = lax.broadcasted_iota(I32, (n_tok, n_exp), 1).astype(F32)
    q1 = jnp.sum(jnp.where(i1c[:, :n_exp] == lane, prob, 0.0), axis=1, keepdims=True)
    q2 = jnp.sum(jnp.where(i2c[:, :n_exp] == lane, prob, 0.0), axis=1, keepdims=True)
    g1 = jnp.broadcast_to(q1 / (q1 + q2), (n_tok, 128))
    g2 = jnp.broadcast_to(q2 / (q1 + q2), (n_tok, 128))
    g1c[...] = g1
    g2c[...] = g2
    q1c[...] = jnp.broadcast_to(q1, (n_tok, 128))
    q2c[...] = jnp.broadcast_to(q2, (n_tok, 128))
    g1r[...] = jnp.transpose(g1)[0:1, :]
    g2r[...] = jnp.transpose(g2)[0:1, :]
    ins[1].wait()

    def build_d(j):
        m1, m2 = masks(j)
        pick = jnp.where(m1 | m2, 1.0, 0.0).astype(BF)
        gate = jnp.sum(jnp.where(m1, g1r[...], 0.0) + jnp.where(m2, g2r[...], 0.0), axis=1, keepdims=True)
        for c in range(0, width, 512):
            rows = (gate * dot(pick, dy_v[:, c:c + 512])).astype(BF)
            ds[j, :, :, c:c + 512] = rows.reshape(ep_size, cap, 512)
        for q in far + near:
            send_row(ds, dr, ds_sem, dr_sem, j, q)
        dr[j, my_place] = ds[j, r]

    def send_half(src, dst, send_sem, recv_sem, j):
        pltpu.make_async_remote_copy(
            src_ref=src.at[j, pl.ds(other * half, half)], dst_ref=dst.at[j],
            send_sem=send_sem, recv_sem=recv_sem.at[j],
            device_id=(other, r), device_id_type=MESH,
        ).start()

    def merge_and_return(src, got, got_sem, dst, send_sem, recv_sem, j):
        wait_recv(got.at[j], got_sem.at[j])
        mine = pl.ds(k * half, half)
        src[j, mine] = (src[j, mine].astype(F32) + got[j].astype(F32)).astype(BF)
        for d in range(half):
            c = (r // tp_size + d) % half
            q = tp_size * c + k

            @pl.when(q != r)
            def _():
                pltpu.make_async_remote_copy(
                    src_ref=src.at[j, k * half + c], dst_ref=dst.at[j, r],
                    send_sem=send_sem, recv_sem=recv_sem.at[j],
                    device_id=(k, q), device_id_type=MESH,
                ).start()

            @pl.when(q == r)
            def _():
                dst[j, r] = src[j, k * half + c]

    n_near = len(near)
    diag_place = place_of(diag)

    def forward_diag(j):
        wait_recv(xr.at[j, 0], xd_sem.at[j])
        pltpu.make_async_remote_copy(
            src_ref=xr.at[j, diag_place], dst_ref=xr.at[j, diag_place],
            send_sem=xfs_sem, recv_sem=xf_sem.at[j],
            device_id=(other, r), device_id_type=MESH,
        ).start()

    forward_diag(0)

    @pl.loop(0, n_loc)
    def _(j):
        @pl.when(j + AHEAD < n_loc)
        def _():
            build_x(j + AHEAD)

        @pl.when(j + AHEAD >= n_loc)
        def _():
            build_d(j + AHEAD - n_loc)

        @pl.when(j > 0)
        def _():
            merge_and_return(ps, pr, pr_sem, orr, os_sem, or_sem, j - 1)

        @pl.when(j + 1 < n_loc)
        def _():
            forward_diag(j + 1)

        for c in weight_copies(j):
            c.wait()
        wait_recv(xr.at[j, pl.ds(0, n_near)], xr_sem.at[j])
        wait_recv(xr.at[j, 0], xf_sem.at[j])
        rows = xr[j].reshape(blk, width)
        pa = dot(rows, wa_v[j])
        pb = dot(rows, wb_v[j])
        th = jnp.tanh(GELU_COEF * (pa + 0.044715 * pa * pa * pa))
        gv = 0.5 * pa * (1.0 + th)
        slope = 0.5 * (1.0 + th) + 0.5 * pa * (1.0 - th * th) * GELU_COEF * (1.0 + 0.134145 * pa * pa)
        gv_v[j] = gv
        bs_v[j] = pb * slope
        hidden = (gv * pb).astype(BF)
        h_v[j] = hidden
        for c in range(0, width, 512):
            ps[j, :, :, c:c + 512] = dot(hidden, wc_v[j, :, c:c + 512]).astype(BF).reshape(ep_size, cap, 512)
        send_half(ps, pr, ps_sem, pr_sem, j)

    tb = 128
    n_tb = n_tok // tb

    def spots(col, toks):
        lanes = lax.broadcasted_iota(I32, (tb, 128), 1).astype(F32)
        base = col[toks, :]
        return jnp.concatenate([base == lanes + float(u * 128) for u in range(n_exp * cap // 128)], axis=1)

    def ship(buf, toks, send_sem, recv_sem):
        pltpu.make_async_remote_copy(
            src_ref=buf.at[toks], dst_ref=buf.at[toks], send_sem=send_sem, recv_sem=recv_sem,
            device_id=(other, r), device_id_type=MESH,
        ).start()

    def combine_y(t):
        toks = pl.ds(pl.multiple_of(t * tb, tb), tb)
        pick1 = jnp.where(spots(s1c, toks), 1.0, 0.0).astype(BF)
        pick2 = jnp.where(spots(s2c, toks), 1.0, 0.0).astype(BF)
        dg1 = jnp.zeros((tb, 1), F32)
        dg2 = jnp.zeros((tb, 1), F32)
        ga = g1c[toks, 0:1]
        gb = g2c[toks, 0:1]
        for c in range(0, width, 512):
            rows = orr[:, :, :, c:c + 512].reshape(n_exp * cap, 512)
            o1 = dot(pick1, rows)
            o2 = dot(pick2, rows)
            y_v[toks, c:c + 512] = (ga * o1 + gb * o2).astype(BF)
            dyf = dy_v[toks, c:c + 512].astype(F32)
            dg1 = dg1 + jnp.sum(dyf * o1, axis=1, keepdims=True)
            dg2 = dg2 + jnp.sum(dyf * o2, axis=1, keepdims=True)
        ship(y_v, toks, ys_sem, yr_sem)
        qa = q1c[toks, 0:1]
        qb = q2c[toks, 0:1]
        shared = dg1 * ga + dg2 * gb
        dq1 = (dg1 - shared) / (qa + qb)
        dq2 = (dg2 - shared) / (qa + qb)
        centre = dq1 * qa + dq2 * qb
        lanes = lax.broadcasted_iota(I32, (tb, n_exp), 1).astype(F32)
        pull = jnp.where(i1c[toks, :n_exp] == lanes, dq1, 0.0) + jnp.where(i2c[toks, :n_exp] == lanes, dq2, 0.0)
        dl_v[toks, :] = prob_v[toks, :] * (pull - centre)

    wait_send(xs.at[:, pl.ds(0, n_near + 1)], xs_sem)
    merge_and_return(ps, pr, pr_sem, orr, os_sem, or_sem, n_loc - 1)

    @pl.loop(0, n_loc)
    def _(j):
        @pl.when(j + AHEAD < n_loc)
        def _():
            build_d(j + AHEAD)

        @pl.when(j > 0)
        def _():
            merge_and_return(xs, pdr, pdr_sem, dxr, dxs_sem, dxr_sem, j - 1)

        wait_recv(dr.at[j, pl.ds(0, ep_size - 1)], dr_sem.at[j])
        rows = dr[j].reshape(blk, width)
        dh = dot(rows, wc_v[j], NT)
        da = (dh * bs_v[j]).astype(BF)
        db = (dh * gv_v[j]).astype(BF)
        da_v[j] = da
        db_v[j] = db
        for c in range(0, width, 512):
            part = dot(da, wa_v[j, c:c + 512, :], NT) + dot(db, wb_v[j, c:c + 512, :], NT)
            xs[j, :, :, c:c + 512] = part.astype(BF).reshape(ep_size, cap, 512)
        send_half(xs, pdr, pds_sem, pdr_sem, j)

        @pl.when(owner & (j == Y_STEP))
        def _():
            @pl.loop(0, n_loc)
            def _(i):
                wait_recv(orr.at[i, pl.ds(0, ep_size - 1)], or_sem.at[i])

        @pl.when(owner & (j >= Y_STEP) & (j < Y_STEP + Y_INNER))
        def _():
            combine_y(j - Y_STEP)

    outs = [
        pltpu.make_async_copy(xr, xe_out, out_sem.at[0]),
        pltpu.make_async_copy(dr, de_out, out_sem.at[1]),
        pltpu.make_async_copy(h_v, h_out, out_sem.at[2]),
        pltpu.make_async_copy(da_v, da_out, out_sem.at[3]),
        pltpu.make_async_copy(db_v, db_out, out_sem.at[4]),
    ]
    for c in outs[:3]:
        c.start()

    split = n_loc - 2

    def pick_both(t):
        toks = pl.ds(pl.multiple_of(t * tb, tb), tb)
        return toks, jnp.where(spots(s1c, toks) | spots(s2c, toks), 1.0, 0.0).astype(BF)

    def sum_first(t):
        toks, pick = pick_both(t)
        dl = dl_v[toks, :]
        for c in range(0, width, 512):
            rows = dxr[0:split, :, :, c:c + 512].reshape(split * blk, 512)
            router = lax.dot_general(
                dl, wr_v[:, c:c + 512], NN, precision=lax.Precision.HIGHEST, preferred_element_type=F32
            )
            acc_v[toks, c:c + 512] = dot(pick[:, :split * blk], rows) + router

    def sum_last(t):
        toks, pick = pick_both(t)
        for c in range(0, width, 512):
            rows = dxr[split:n_loc, :, :, c:c + 512].reshape((n_loc - split) * blk, 512)
            dx_v[toks, c:c + 512] = (acc_v[toks, c:c + 512] + dot(pick[:, split * blk:], rows)).astype(BF)
        pltpu.make_async_copy(dx_v.at[toks], dx_out.at[toks], in_sem.at[1]).start()

    @pl.when(owner)
    def _():
        @pl.loop(Y_INNER, n_tb)
        def _(t):
            combine_y(t)

        d_hi, d_mid, d_low = split3(dl_v[...])
        for c in range(0, width, 512):
            xc = x_v[:, c:c + 512]
            piece = dot(d_hi, xc, TN) + (dot(d_mid, xc, TN) + dot(d_low, xc, TN))
            dwp[:, :, c:c + 512] = piece.reshape(ep_size, n_loc, 512)
        for d in range(1, ep_size):
            q = (r + d) % ep_size
            pltpu.make_async_remote_copy(
                src_ref=dwp.at[q], dst_ref=dwi.at[r], send_sem=rs_sem, recv_sem=rr_sem,
                device_id=(q % tp_size, q), device_id_type=MESH,
            ).start()
        dwi[r] = dwp[r]

    merge_and_return(xs, pdr, pdr_sem, dxr, dxs_sem, dxr_sem, n_loc - 1)
    for c in outs[3:]:
        c.start()

    @pl.when(owner)
    def _():
        @pl.loop(0, split)
        def _(j):
            wait_recv(dxr.at[j, pl.ds(0, ep_size - 1)], dxr_sem.at[j])

        @pl.loop(0, n_tb)
        def _(t):
            sum_first(t)

        wait_recv(dwi.at[pl.ds(0, ep_size - 1)], rr_sem)
        total = dwi[0]
        for q in range(1, ep_size):
            total = total + dwi[q]
        dwf[r] = total
        for d in range(1, n_dev):
            flat = (k * ep_size + r + d) % n_dev
            pltpu.make_async_remote_copy(
                src_ref=dwf.at[r], dst_ref=dwf.at[r], send_sem=fs_sem, recv_sem=fr_sem,
                device_id=(flat // ep_size, flat % ep_size), device_id_type=MESH,
            ).start()

        @pl.loop(split, n_loc)
        def _(j):
            wait_recv(dxr.at[j, pl.ds(0, ep_size - 1)], dxr_sem.at[j])

        @pl.loop(0, n_tb)
        def _(t):
            sum_last(t)

        wait_recv(dwf.at[pl.ds(0, ep_size - 1)], fr_sem)
        wait_send(dwp.at[pl.ds(0, ep_size - 1)], rs_sem)
        for half_sends in range(n_dev - 1):
            wait_send(dwf.at[r], fs_sem)
        wait_send(y_v, ys_sem)
        wait_send(orr.at[:, pl.ds(0, half - 1)], os_sem)
        wait_send(dxr.at[:, pl.ds(0, half - 1)], dxs_sem)

    @pl.when(jnp.logical_not(owner))
    def _():
        dx_v[...] = jnp.zeros_like(dx_v)
        pltpu.make_async_copy(dx_v, dx_out, in_sem.at[1]).start()
        wait_recv(y_v, yr_sem)
        wait_recv(dwf, fr_sem)
        wait_send(orr.at[:, pl.ds(0, half)], os_sem)
        wait_send(dxr.at[:, pl.ds(0, half)], dxs_sem)

    finals = [
        pltpu.make_async_copy(y_v, y_out, in_sem.at[0]),
        pltpu.make_async_copy(dwf, dwr_out, in_sem.at[2]),
    ]
    for c in finals:
        c.start()
    finals.append(pltpu.make_async_copy(dx_v, dx_out, in_sem.at[1]))
    wait_send(ds.at[:, pl.ds(0, ep_size - 1)], ds_sem)
    wait_send(xr.at[:, 0], xfs_sem)
    wait_send(ps.at[:, pl.ds(0, half)], ps_sem)
    wait_send(xs.at[:, pl.ds(0, half)], pds_sem)
    for c in outs + finals:
        c.wait()


def weight_kernel(xe, de, h, da, db, y, dwr, ga_out, gb_out, gc_out, y_out, dwr_out):
    y_out[...] = y[...]
    dwr_out[...] = dwr[...]
    rows = xe[0]
    ga_out[0] = dot(rows, da[0], TN)
    gb_out[0] = dot(rows, db[0], TN)
    gc_out[0] = dot(h[0], de[0], TN)


def settle_kernel(tp_size, pieces, mine, passed, out, buf, in_sem, out_sem):
    n = buf.shape[0] // pieces

    @pl.when(lax.axis_index("ep") % tp_size == lax.axis_index("tp"))
    def _():
        loads = [pltpu.make_async_copy(mine.at[pl.ds(i * n, n)], buf.at[pl.ds(i * n, n)], in_sem.at[i]) for i in range(pieces)]
        stores = [pltpu.make_async_copy(buf.at[pl.ds(i * n, n)], out.at[pl.ds(i * n, n)], out_sem.at[i]) for i in range(pieces)]
        for c in loads:
            c.start()
        for i in range(pieces):
            loads[i].wait()
            stores[i].start()
        for c in stores:
            c.wait()


def solution(mesh):
    tp_size = mesh.shape["tp"]
    ep_size = mesh.shape["ep"]

    def local_step(x_rows, w_router, first_ids, second_ids, w_gelu, w_lin, w_out, dy_rows):
        n_tok, width = x_rows.shape
        n_exp = w_router.shape[1]
        n_loc, _, hid = w_gelu.shape
        cap = 2 * n_tok // n_exp
        blk = ep_size * cap
        half = ep_size // tp_size
        dma = pltpu.SemaphoreType.DMA
        any_spec = pl.BlockSpec(memory_space=pl.ANY)
        vmem_spec = pl.BlockSpec(memory_space=pltpu.VMEM)
        sds = jax.ShapeDtypeStruct
        rows_shape = (n_loc, ep_size, cap, width)
        half_shape = (n_loc, half, cap, width)
        hid_shape = (n_loc, blk, hid)
        col = pltpu.VMEM((n_tok, 128), F32)
        row = pltpu.VMEM((1, n_tok), F32)
        outs = pl.pallas_call(
            functools.partial(moe_kernel, tp_size, ep_size, cap),
            name="moe",
            in_specs=[vmem_spec] * 2 + [any_spec] * 6,
            out_specs=[any_spec] * 8,
            out_shape=[
                sds((n_tok, width), BF), sds((n_tok, width), BF), sds((ep_size, n_loc, width), F32),
                sds(rows_shape, BF), sds(rows_shape, BF), sds(hid_shape, BF), sds(hid_shape, BF), sds(hid_shape, BF),
            ],
            scratch_shapes=[
                pltpu.VMEM((n_tok, width), BF), pltpu.VMEM((n_tok, width), BF), pltpu.VMEM((n_exp, width), F32),
                pltpu.VMEM((n_loc, width, hid), BF), pltpu.VMEM((n_loc, width, hid), BF), pltpu.VMEM((n_loc, hid, width), BF),
                pltpu.VMEM(rows_shape, BF), pltpu.VMEM(rows_shape, BF), pltpu.VMEM(rows_shape, BF), pltpu.VMEM(rows_shape, BF),
                pltpu.VMEM(hid_shape, BF), pltpu.VMEM(hid_shape, BF), pltpu.VMEM(hid_shape, BF),
                pltpu.VMEM(hid_shape, F32), pltpu.VMEM(hid_shape, F32),
                pltpu.VMEM(rows_shape, BF), pltpu.VMEM(half_shape, BF), pltpu.VMEM(half_shape, BF),
                pltpu.VMEM(rows_shape, BF), pltpu.VMEM(rows_shape, BF),
                pltpu.VMEM((n_tok, width), BF), pltpu.VMEM((n_tok, width), BF),
                row, row, row, row, col, col, col, col, col, col, col, col,
                pltpu.VMEM((n_tok, n_exp), F32), pltpu.VMEM((n_tok, n_exp), F32),
                pltpu.VMEM((ep_size, n_loc, width), F32), pltpu.VMEM((ep_size, n_loc, width), F32),
                pltpu.VMEM((ep_size, n_loc, width), F32), pltpu.VMEM((n_tok, width), F32),
                dma((3,)), dma((3, n_loc)), dma((5,)),
                dma(()), dma((n_loc,)), dma((n_loc,)), dma((n_loc,)), dma(()), dma(()), dma((n_loc,)),
                dma(()), dma((n_loc,)), dma(()), dma((n_loc,)),
                dma(()), dma((n_loc,)), dma(()), dma((n_loc,)),
                dma(()), dma(()),
                dma(()), dma(()), dma(()), dma(()),
            ],
            compiler_params=pltpu.CompilerParams(
                collective_id=0, has_side_effects=True, vmem_limit_bytes=67043328
            ),
        )(
            first_ids.reshape(1, n_tok), second_ids.reshape(1, n_tok), x_rows, dy_rows, w_router.T,
            w_gelu, w_lin, w_out,
        )
        act_out, grad_in, grad_router, xe, de, h, da, db = outs
        partners = [
            ((q % tp_size) * ep_size + q, (1 - q % tp_size) * ep_size + q) for q in range(ep_size)
        ]
        passed = lax.ppermute(grad_in, ("tp", "ep"), partners)
        xe = xe.reshape(n_loc, blk, width)
        de = de.reshape(n_loc, blk, width)

        y_spec = pl.BlockSpec((n_tok // n_loc, width), lambda e: (e, 0))

        def spec(*shape):
            return pl.BlockSpec((1,) + shape, lambda e: (e, 0, 0))

        grad_wa, grad_wb, grad_wc, act_out, grad_router = pl.pallas_call(
            weight_kernel,
            name="weight_grads",
            grid=(n_loc,),
            in_specs=[spec(blk, width), spec(blk, width), spec(blk, hid), spec(blk, hid), spec(blk, hid), y_spec, spec(n_exp // n_loc, width)],
            out_specs=[spec(width, hid), spec(width, hid), spec(hid, width), y_spec, spec(n_exp // n_loc, width)],
            out_shape=[
                sds((n_loc, width, hid), F32), sds((n_loc, width, hid), F32), sds((n_loc, hid, width), F32),
                sds((n_tok, width), BF), sds((n_loc, n_exp // n_loc, width), F32),
            ],
            compiler_params=pltpu.CompilerParams(
                dimension_semantics=("arbitrary",), vmem_limit_bytes=67043328
            ),
            cost_estimate=pl.CostEstimate(
                flops=6 * n_loc * blk * width * hid, transcendentals=0,
                bytes_accessed=12 * n_loc * width * hid + 4 * n_loc * blk * width + 6 * n_loc * blk * hid,
            ),
        )(xe, de, h, da, db, act_out, grad_router.reshape(n_loc, n_exp // n_loc, width))
        pieces = n_loc
        grad_in = pl.pallas_call(
            functools.partial(settle_kernel, tp_size, pieces),
            name="settle",
            in_specs=[any_spec, any_spec],
            out_specs=any_spec,
            out_shape=sds((n_tok, width), BF),
            scratch_shapes=[pltpu.VMEM((n_tok, width), BF), dma((pieces,)), dma((pieces,))],
            input_output_aliases={1: 0},
        )(grad_in, passed)
        return act_out, grad_in, grad_wa, grad_wb, grad_wc, grad_router.reshape(n_exp, width).T

    return jax.shard_map(
        local_step,
        mesh=mesh,
        in_specs=(P("ep", None), P(), P("ep"), P("ep"), P("ep", None, "tp"), P("ep", None, "tp"), P("ep", "tp", None), P("ep", None)),
        out_specs=(P("ep", None), P("ep", None), P("ep", None, "tp"), P("ep", None, "tp"), P("ep", "tp", None), P()),
        check_vma=False,
    )
```

```python
import functools

import jax
import jax.numpy as jnp
from jax import lax
from jax.experimental import pallas as pl
from jax.experimental.pallas import tpu as pltpu
from jax.sharding import PartitionSpec as P

BF = jnp.bfloat16
F32 = jnp.float32
I32 = jnp.int32
MESH = pl.DeviceIdType.MESH
GELU_COEF = 0.7978845608028654
AHEAD = 3
LAG = 2
Y_STEP = 4
Y_INNER = 2
NN = (((1,), (0,)), ((), ()))
NT = (((1,), (1,)), ((), ()))
TN = (((0,), (0,)), ((), ()))


def dot(a, b, dims=NN):
    return lax.dot_general(a, b, dims, preferred_element_type=F32)


def split3(v):
    hi = v.astype(BF)
    rest = v - hi.astype(F32)
    mid = rest.astype(BF)
    low = (rest - mid.astype(F32)).astype(BF)
    return hi, mid, low


def moe_kernel(
    tp_size, ep_size, cap,
    ids1_ref, ids2_ref, x_hbm, dy_hbm, wr_hbm, wa_hbm, wb_hbm, wc_hbm,
    y_out, dx_out, dwr_out, xe_out, de_out, h_out, da_out, db_out,
    x_v, dy_v, wr_v, wa_v, wb_v, wc_v,
    xs, ds, xr, dr, h_v, da_v, db_v, bs_v, gv_v,
    ps, pr, pdr, orr, dxr, y_v, dx_v,
    s1r, s2r, g1r, g2r, s1c, s2c, g1c, g2c, q1c, q2c, i1c, i2c, prob_v, dl_v,
    dwp, dwi, dwf, acc_v,
    in_sem, w_sem, out_sem,
    xs_sem, xr_sem, xd_sem, xf_sem, xfs_sem, ds_sem, dr_sem,
    ps_sem, pr_sem, pds_sem, pdr_sem,
    os_sem, or_sem, dxs_sem, dxr_sem,
    ys_sem, yr_sem,
    rs_sem, rr_sem, fs_sem, fr_sem,
):
    k = lax.axis_index("tp")
    r = lax.axis_index("ep")
    n_loc = wa_v.shape[0]
    n_tok, width = x_v.shape
    hid = wa_v.shape[2]
    n_exp = n_loc * ep_size
    blk = ep_size * cap
    half = ep_size // tp_size
    my_place = (r % tp_size) * half + r // tp_size
    owner = (r % tp_size) == k
    other = 1 - k

    ins = [
        pltpu.make_async_copy(x_hbm, x_v, in_sem.at[0]),
        pltpu.make_async_copy(dy_hbm, dy_v, in_sem.at[1]),
        pltpu.make_async_copy(wr_hbm, wr_v, in_sem.at[2]),
    ]
    ins[0].start()

    def weight_copies(j):
        return [
            pltpu.make_async_copy(wa_hbm.at[j], wa_v.at[j], w_sem.at[0, j]),
            pltpu.make_async_copy(wb_hbm.at[j], wb_v.at[j], w_sem.at[1, j]),
            pltpu.make_async_copy(wc_hbm.at[j], wc_v.at[j], w_sem.at[2, j]),
        ]

    n_dev = tp_size * ep_size
    barrier = pltpu.get_barrier_semaphore()
    for d in range(1, n_dev):
        flat = (k * ep_size + r + d) % n_dev
        pl.semaphore_signal(barrier, inc=1, device_id=(flat // ep_size, flat % ep_size), device_id_type=MESH)

    ids1 = ids1_ref[...]
    ids2 = ids2_ref[...]
    e_iota = lax.broadcasted_iota(I32, (n_exp, n_tok), 0)
    hot1 = jnp.where(ids1 == e_iota, 1.0, 0.0).astype(F32)
    hot2 = jnp.where(ids2 == e_iota, 1.0, 0.0).astype(F32)
    before = jnp.where(
        lax.broadcasted_iota(I32, (n_tok, n_tok), 0) < lax.broadcasted_iota(I32, (n_tok, n_tok), 1), 1.0, 0.0
    ).astype(BF)
    cum1 = dot(hot1.astype(BF), before)
    cum2 = dot(hot2.astype(BF), before)
    fill1 = jnp.sum(hot1, axis=1, keepdims=True)
    pos1 = jnp.sum(cum1 * hot1, axis=0, keepdims=True)
    pos2 = jnp.sum((cum2 + fill1) * hot2, axis=0, keepdims=True)

    def place(ids, pos):
        spot = (ids & (n_loc - 1)) * blk + (ids // n_loc) * cap
        return jnp.where(pos < cap, spot.astype(F32) + pos, float(n_exp * cap))

    s1r[...] = place(ids1, pos1)
    s2r[...] = place(ids2, pos2)

    def masks(j):
        spot = (lax.broadcasted_iota(I32, (blk, n_tok), 0) + j * blk).astype(F32)
        return s1r[...] == spot, s2r[...] == spot

    chip = r // 2
    chip_x = chip + 1 - 2 * (chip % 2)
    chip_y = (chip + 2) % 4
    chip_d = 3 - chip
    core = r % 2
    diag = 2 * chip_d + (k + r) % 2
    near = [2 * chip_x + core, 2 * chip_y + core, 2 * chip_x + 1 - core, 2 * chip_y + 1 - core, 2 * chip + 1 - core]
    far = [2 * chip_d + core, 2 * chip_d + 1 - core]

    def place_of(q):
        return (q % tp_size) * half + q // tp_size

    def send_row(src, dst, send_sem, recv_sem, j, q):
        pltpu.make_async_remote_copy(
            src_ref=src.at[j, q], dst_ref=dst.at[j, my_place],
            send_sem=send_sem, recv_sem=recv_sem.at[j],
            device_id=(k, q), device_id_type=MESH,
        ).start()

    def wait_recv(view, sem):
        pltpu.make_async_remote_copy(
            src_ref=view, dst_ref=view, send_sem=sem, recv_sem=sem, device_id=(k, r), device_id_type=MESH
        ).wait_recv()

    def wait_send(view, sem):
        pltpu.make_async_remote_copy(
            src_ref=view, dst_ref=view, send_sem=sem, recv_sem=sem, device_id=(k, r), device_id_type=MESH
        ).wait_send()

    def build_x(j):
        m1, m2 = masks(j)
        pick = jnp.where(m1 | m2, 1.0, 0.0).astype(BF)
        for c in range(0, width, 512):
            rows = dot(pick, x_v[:, c:c + 512]).astype(BF)
            xs[j, :, :, c:c + 512] = rows.reshape(ep_size, cap, 512)
        send_row(xs, xr, xs_sem, xd_sem, j, diag)
        for q in near:
            send_row(xs, xr, xs_sem, xr_sem, j, q)
        xr[j, my_place] = xs[j, r]

    ins[0].wait()
    ins[2].start()
    ins[1].start()

    @pl.loop(0, n_loc)
    def _(j):
        for c in weight_copies(j):
            c.start()

    pl.semaphore_wait(barrier, n_dev - 1)

    @pl.loop(0, AHEAD)
    def _(j):
        build_x(j)

    def column(row):
        return jnp.transpose(jnp.broadcast_to(row, (128, n_tok)))

    s1c[...] = column(s1r[...])
    s2c[...] = column(s2r[...])
    i1c[...] = column(ids1.astype(F32))
    i2c[...] = column(ids2.astype(F32))
    ins[2].wait()
    wr_hi, wr_mid, wr_low = split3(wr_v[...])
    xv = x_v[...]
    logits = dot(xv, wr_hi, NT) + (dot(xv, wr_mid, NT) + dot(xv, wr_low, NT))
    ex = jnp.exp(logits - jnp.max(logits, axis=1, keepdims=True))
    prob = ex / jnp.sum(ex, axis=1, keepdims=True)
    prob_v[...] = prob
    lane = lax.broadcasted_iota(I32, (n_tok, n_exp), 1).astype(F32)
    q1 = jnp.sum(jnp.where(i1c[:, :n_exp] == lane, prob, 0.0), axis=1, keepdims=True)
    q2 = jnp.sum(jnp.where(i2c[:, :n_exp] == lane, prob, 0.0), axis=1, keepdims=True)
    g1 = jnp.broadcast_to(q1 / (q1 + q2), (n_tok, 128))
    g2 = jnp.broadcast_to(q2 / (q1 + q2), (n_tok, 128))
    g1c[...] = g1
    g2c[...] = g2
    q1c[...] = jnp.broadcast_to(q1, (n_tok, 128))
    q2c[...] = jnp.broadcast_to(q2, (n_tok, 128))
    g1r[...] = jnp.transpose(g1)[0:1, :]
    g2r[...] = jnp.transpose(g2)[0:1, :]
    ins[1].wait()

    def build_d(j):
        m1, m2 = masks(j)
        pick = jnp.where(m1 | m2, 1.0, 0.0).astype(BF)
        gate = jnp.sum(jnp.where(m1, g1r[...], 0.0) + jnp.where(m2, g2r[...], 0.0), axis=1, keepdims=True)
        for c in range(0, width, 512):
            rows = (gate * dot(pick, dy_v[:, c:c + 512])).astype(BF)
            ds[j, :, :, c:c + 512] = rows.reshape(ep_size, cap, 512)
        for q in far + near:
            send_row(ds, dr, ds_sem, dr_sem, j, q)
        dr[j, my_place] = ds[j, r]

    def send_half(src, dst, send_sem, recv_sem, j):
        pltpu.make_async_remote_copy(
            src_ref=src.at[j, pl.ds(other * half, half)], dst_ref=dst.at[j],
            send_sem=send_sem, recv_sem=recv_sem.at[j],
            device_id=(other, r), device_id_type=MESH,
        ).start()

    def merge_and_return(src, got, got_sem, dst, send_sem, recv_sem, j):
        wait_recv(got.at[j], got_sem.at[j])
        mine = pl.ds(k * half, half)
        src[j, mine] = (src[j, mine].astype(F32) + got[j].astype(F32)).astype(BF)
        for d in range(half):
            c = (r // tp_size + d) % half
            q = tp_size * c + k

            @pl.when(q != r)
            def _():
                pltpu.make_async_remote_copy(
                    src_ref=src.at[j, k * half + c], dst_ref=dst.at[j, r],
                    send_sem=send_sem, recv_sem=recv_sem.at[j],
                    device_id=(k, q), device_id_type=MESH,
                ).start()

            @pl.when(q == r)
            def _():
                dst[j, r] = src[j, k * half + c]

    n_near = len(near)
    diag_place = place_of(diag)

    def forward_diag(j):
        wait_recv(xr.at[j, 0], xd_sem.at[j])
        pltpu.make_async_remote_copy(
            src_ref=xr.at[j, diag_place], dst_ref=xr.at[j, diag_place],
            send_sem=xfs_sem, recv_sem=xf_sem.at[j],
            device_id=(other, r), device_id_type=MESH,
        ).start()

    forward_diag(0)

    @pl.loop(0, n_loc)
    def _(j):
        @pl.when(j + AHEAD < n_loc)
        def _():
            build_x(j + AHEAD)

        @pl.when(j + AHEAD >= n_loc)
        def _():
            build_d(j + AHEAD - n_loc)

        @pl.when(j + 1 < n_loc)
        def _():
            forward_diag(j + 1)

        for c in weight_copies(j):
            c.wait()
        wait_recv(xr.at[j, pl.ds(0, n_near)], xr_sem.at[j])
        wait_recv(xr.at[j, 0], xf_sem.at[j])
        rows = xr[j].reshape(blk, width)
        pa = dot(rows, wa_v[j])
        pb = dot(rows, wb_v[j])
        th = jnp.tanh(GELU_COEF * (pa + 0.044715 * pa * pa * pa))
        gv = 0.5 * pa * (1.0 + th)
        slope = 0.5 * (1.0 + th) + 0.5 * pa * (1.0 - th * th) * GELU_COEF * (1.0 + 0.134145 * pa * pa)
        gv_v[j] = gv
        bs_v[j] = pb * slope
        hidden = (gv * pb).astype(BF)
        h_v[j] = hidden
        for c in range(0, width, 512):
            ps[j, :, :, c:c + 512] = dot(hidden, wc_v[j, :, c:c + 512]).astype(BF).reshape(ep_size, cap, 512)
        send_half(ps, pr, ps_sem, pr_sem, j)

        @pl.when(j >= LAG)
        def _():
            merge_and_return(ps, pr, pr_sem, orr, os_sem, or_sem, j - LAG)

    tb = 128
    n_tb = n_tok // tb

    def spots(col, toks):
        lanes = lax.broadcasted_iota(I32, (tb, 128), 1).astype(F32)
        base = col[toks, :]
        return jnp.concatenate([base == lanes + float(u * 128) for u in range(n_exp * cap // 128)], axis=1)

    def ship(buf, toks, send_sem, recv_sem):
        pltpu.make_async_remote_copy(
            src_ref=buf.at[toks], dst_ref=buf.at[toks], send_sem=send_sem, recv_sem=recv_sem,
            device_id=(other, r), device_id_type=MESH,
        ).start()

    def combine_y(t):
        toks = pl.ds(pl.multiple_of(t * tb, tb), tb)
        pick1 = jnp.where(spots(s1c, toks), 1.0, 0.0).astype(BF)
        pick2 = jnp.where(spots(s2c, toks), 1.0, 0.0).astype(BF)
        dg1 = jnp.zeros((tb, 1), F32)
        dg2 = jnp.zeros((tb, 1), F32)
        ga = g1c[toks, 0:1]
        gb = g2c[toks, 0:1]
        for c in range(0, width, 512):
            rows = orr[:, :, :, c:c + 512].reshape(n_exp * cap, 512)
            o1 = dot(pick1, rows)
            o2 = dot(pick2, rows)
            y_v[toks, c:c + 512] = (ga * o1 + gb * o2).astype(BF)
            dyf = dy_v[toks, c:c + 512].astype(F32)
            dg1 = dg1 + jnp.sum(dyf * o1, axis=1, keepdims=True)
            dg2 = dg2 + jnp.sum(dyf * o2, axis=1, keepdims=True)
        ship(y_v, toks, ys_sem, yr_sem)
        qa = q1c[toks, 0:1]
        qb = q2c[toks, 0:1]
        shared = dg1 * ga + dg2 * gb
        dq1 = (dg1 - shared) / (qa + qb)
        dq2 = (dg2 - shared) / (qa + qb)
        centre = dq1 * qa + dq2 * qb
        lanes = lax.broadcasted_iota(I32, (tb, n_exp), 1).astype(F32)
        pull = jnp.where(i1c[toks, :n_exp] == lanes, dq1, 0.0) + jnp.where(i2c[toks, :n_exp] == lanes, dq2, 0.0)
        dl_v[toks, :] = prob_v[toks, :] * (pull - centre)

    wait_send(xs.at[:, pl.ds(0, n_near + 1)], xs_sem)
    @pl.loop(0, n_loc)
    def _(j):
        @pl.when(j + AHEAD < n_loc)
        def _():
            build_d(j + AHEAD)

        wait_recv(dr.at[j, pl.ds(0, ep_size - 1)], dr_sem.at[j])
        rows = dr[j].reshape(blk, width)
        dh = dot(rows, wc_v[j], NT)
        da = (dh * bs_v[j]).astype(BF)
        db = (dh * gv_v[j]).astype(BF)
        da_v[j] = da
        db_v[j] = db
        for c in range(0, width, 512):
            part = dot(da, wa_v[j, c:c + 512, :], NT) + dot(db, wb_v[j, c:c + 512, :], NT)
            xs[j, :, :, c:c + 512] = part.astype(BF).reshape(ep_size, cap, 512)
        send_half(xs, pdr, pds_sem, pdr_sem, j)

        @pl.when(j == 0)
        def _():
            for i in range(LAG):
                merge_and_return(ps, pr, pr_sem, orr, os_sem, or_sem, n_loc - LAG + i)

        @pl.when(j >= LAG)
        def _():
            merge_and_return(xs, pdr, pdr_sem, dxr, dxs_sem, dxr_sem, j - LAG)

        @pl.when(owner & (j == Y_STEP))
        def _():
            @pl.loop(0, n_loc)
            def _(i):
                wait_recv(orr.at[i, pl.ds(0, ep_size - 1)], or_sem.at[i])

        @pl.when(owner & (j >= Y_STEP) & (j < Y_STEP + Y_INNER))
        def _():
            combine_y(j - Y_STEP)

    outs = [
        pltpu.make_async_copy(xr, xe_out, out_sem.at[0]),
        pltpu.make_async_copy(dr, de_out, out_sem.at[1]),
        pltpu.make_async_copy(h_v, h_out, out_sem.at[2]),
        pltpu.make_async_copy(da_v, da_out, out_sem.at[3]),
        pltpu.make_async_copy(db_v, db_out, out_sem.at[4]),
    ]
    for c in outs[:3]:
        c.start()

    split = n_loc - 2

    def pick_both(t):
        toks = pl.ds(pl.multiple_of(t * tb, tb), tb)
        return toks, jnp.where(spots(s1c, toks) | spots(s2c, toks), 1.0, 0.0).astype(BF)

    def sum_first(t):
        toks, pick = pick_both(t)
        dl = dl_v[toks, :]
        for c in range(0, width, 512):
            rows = dxr[0:split, :, :, c:c + 512].reshape(split * blk, 512)
            router = lax.dot_general(
                dl, wr_v[:, c:c + 512], NN, precision=lax.Precision.HIGHEST, preferred_element_type=F32
            )
            acc_v[toks, c:c + 512] = dot(pick[:, :split * blk], rows) + router

    def sum_last(t):
        toks, pick = pick_both(t)
        for c in range(0, width, 512):
            rows = dxr[split:n_loc, :, :, c:c + 512].reshape((n_loc - split) * blk, 512)
            dx_v[toks, c:c + 512] = (acc_v[toks, c:c + 512] + dot(pick[:, split * blk:], rows)).astype(BF)
        pltpu.make_async_copy(dx_v.at[toks], dx_out.at[toks], in_sem.at[1]).start()

    for i in range(LAG - 1):
        merge_and_return(xs, pdr, pdr_sem, dxr, dxs_sem, dxr_sem, n_loc - LAG + i)

    @pl.when(owner)
    def _():
        @pl.loop(Y_INNER, n_tb)
        def _(t):
            combine_y(t)

        d_hi, d_mid, d_low = split3(dl_v[...])
        for c in range(0, width, 512):
            xc = x_v[:, c:c + 512]
            piece = dot(d_hi, xc, TN) + (dot(d_mid, xc, TN) + dot(d_low, xc, TN))
            dwp[:, :, c:c + 512] = piece.reshape(ep_size, n_loc, 512)
        for d in range(1, ep_size):
            q = (r + d) % ep_size
            pltpu.make_async_remote_copy(
                src_ref=dwp.at[q], dst_ref=dwi.at[r], send_sem=rs_sem, recv_sem=rr_sem,
                device_id=(q % tp_size, q), device_id_type=MESH,
            ).start()
        dwi[r] = dwp[r]

    merge_and_return(xs, pdr, pdr_sem, dxr, dxs_sem, dxr_sem, n_loc - 1)
    for c in outs[3:]:
        c.start()

    @pl.when(owner)
    def _():
        @pl.loop(0, split)
        def _(j):
            wait_recv(dxr.at[j, pl.ds(0, ep_size - 1)], dxr_sem.at[j])

        @pl.loop(0, n_tb)
        def _(t):
            sum_first(t)

        wait_recv(dwi.at[pl.ds(0, ep_size - 1)], rr_sem)
        total = dwi[0]
        for q in range(1, ep_size):
            total = total + dwi[q]
        dwf[r] = total
        for d in range(1, n_dev):
            flat = (k * ep_size + r + d) % n_dev
            pltpu.make_async_remote_copy(
                src_ref=dwf.at[r], dst_ref=dwf.at[r], send_sem=fs_sem, recv_sem=fr_sem,
                device_id=(flat // ep_size, flat % ep_size), device_id_type=MESH,
            ).start()

        @pl.loop(split, n_loc)
        def _(j):
            wait_recv(dxr.at[j, pl.ds(0, ep_size - 1)], dxr_sem.at[j])

        @pl.loop(0, n_tb)
        def _(t):
            sum_last(t)

        wait_recv(dwf.at[pl.ds(0, ep_size - 1)], fr_sem)
        wait_send(dwp.at[pl.ds(0, ep_size - 1)], rs_sem)
        for half_sends in range(n_dev - 1):
            wait_send(dwf.at[r], fs_sem)
        wait_send(y_v, ys_sem)
        wait_send(orr.at[:, pl.ds(0, half - 1)], os_sem)
        wait_send(dxr.at[:, pl.ds(0, half - 1)], dxs_sem)

    @pl.when(jnp.logical_not(owner))
    def _():
        dx_v[...] = jnp.zeros_like(dx_v)
        pltpu.make_async_copy(dx_v, dx_out, in_sem.at[1]).start()
        wait_recv(y_v, yr_sem)
        wait_recv(dwf, fr_sem)
        wait_send(orr.at[:, pl.ds(0, half)], os_sem)
        wait_send(dxr.at[:, pl.ds(0, half)], dxs_sem)

    finals = [
        pltpu.make_async_copy(y_v, y_out, in_sem.at[0]),
        pltpu.make_async_copy(dwf, dwr_out, in_sem.at[2]),
    ]
    for c in finals:
        c.start()
    finals.append(pltpu.make_async_copy(dx_v, dx_out, in_sem.at[1]))
    wait_send(ds.at[:, pl.ds(0, ep_size - 1)], ds_sem)
    wait_send(xr.at[:, 0], xfs_sem)
    wait_send(ps.at[:, pl.ds(0, half)], ps_sem)
    wait_send(xs.at[:, pl.ds(0, half)], pds_sem)
    for c in outs + finals:
        c.wait()


def weight_kernel(xe, de, h, da, db, y, dwr, ga_out, gb_out, gc_out, y_out, dwr_out):
    y_out[...] = y[...]
    dwr_out[...] = dwr[...]
    rows = xe[0]
    ga_out[0] = dot(rows, da[0], TN)
    gb_out[0] = dot(rows, db[0], TN)
    gc_out[0] = dot(h[0], de[0], TN)


def solution(mesh):
    tp_size = mesh.shape["tp"]
    ep_size = mesh.shape["ep"]

    def local_step(x_rows, w_router, first_ids, second_ids, w_gelu, w_lin, w_out, dy_rows):
        n_tok, width = x_rows.shape
        n_exp = w_router.shape[1]
        n_loc, _, hid = w_gelu.shape
        cap = 2 * n_tok // n_exp
        blk = ep_size * cap
        half = ep_size // tp_size
        dma = pltpu.SemaphoreType.DMA
        any_spec = pl.BlockSpec(memory_space=pl.ANY)
        vmem_spec = pl.BlockSpec(memory_space=pltpu.VMEM)
        sds = jax.ShapeDtypeStruct
        rows_shape = (n_loc, ep_size, cap, width)
        half_shape = (n_loc, half, cap, width)
        hid_shape = (n_loc, blk, hid)
        col = pltpu.VMEM((n_tok, 128), F32)
        row = pltpu.VMEM((1, n_tok), F32)
        outs = pl.pallas_call(
            functools.partial(moe_kernel, tp_size, ep_size, cap),
            name="moe",
            in_specs=[vmem_spec] * 2 + [any_spec] * 6,
            out_specs=[any_spec] * 8,
            out_shape=[
                sds((n_tok, width), BF), sds((n_tok, width), BF), sds((ep_size, n_loc, width), F32),
                sds(rows_shape, BF), sds(rows_shape, BF), sds(hid_shape, BF), sds(hid_shape, BF), sds(hid_shape, BF),
            ],
            scratch_shapes=[
                pltpu.VMEM((n_tok, width), BF), pltpu.VMEM((n_tok, width), BF), pltpu.VMEM((n_exp, width), F32),
                pltpu.VMEM((n_loc, width, hid), BF), pltpu.VMEM((n_loc, width, hid), BF), pltpu.VMEM((n_loc, hid, width), BF),
                pltpu.VMEM(rows_shape, BF), pltpu.VMEM(rows_shape, BF), pltpu.VMEM(rows_shape, BF), pltpu.VMEM(rows_shape, BF),
                pltpu.VMEM(hid_shape, BF), pltpu.VMEM(hid_shape, BF), pltpu.VMEM(hid_shape, BF),
                pltpu.VMEM(hid_shape, F32), pltpu.VMEM(hid_shape, F32),
                pltpu.VMEM(rows_shape, BF), pltpu.VMEM(half_shape, BF), pltpu.VMEM(half_shape, BF),
                pltpu.VMEM(rows_shape, BF), pltpu.VMEM(rows_shape, BF),
                pltpu.VMEM((n_tok, width), BF), pltpu.VMEM((n_tok, width), BF),
                row, row, row, row, col, col, col, col, col, col, col, col,
                pltpu.VMEM((n_tok, n_exp), F32), pltpu.VMEM((n_tok, n_exp), F32),
                pltpu.VMEM((ep_size, n_loc, width), F32), pltpu.VMEM((ep_size, n_loc, width), F32),
                pltpu.VMEM((ep_size, n_loc, width), F32), pltpu.VMEM((n_tok, width), F32),
                dma((3,)), dma((3, n_loc)), dma((5,)),
                dma(()), dma((n_loc,)), dma((n_loc,)), dma((n_loc,)), dma(()), dma(()), dma((n_loc,)),
                dma(()), dma((n_loc,)), dma(()), dma((n_loc,)),
                dma(()), dma((n_loc,)), dma(()), dma((n_loc,)),
                dma(()), dma(()),
                dma(()), dma(()), dma(()), dma(()),
            ],
            compiler_params=pltpu.CompilerParams(
                collective_id=0, has_side_effects=True, vmem_limit_bytes=67043328
            ),
        )(
            first_ids.reshape(1, n_tok), second_ids.reshape(1, n_tok), x_rows, dy_rows, w_router.T,
            w_gelu, w_lin, w_out,
        )
        act_out, grad_in, grad_router, xe, de, h, da, db = outs
        partners = [
            ((q % tp_size) * ep_size + q, (1 - q % tp_size) * ep_size + q) for q in range(ep_size)
        ]
        passed = lax.ppermute(grad_in, ("tp", "ep"), partners)
        owner = lax.axis_index("ep") % tp_size == lax.axis_index("tp")
        grad_in = jnp.where(owner, grad_in, passed)
        xe = xe.reshape(n_loc, blk, width)
        de = de.reshape(n_loc, blk, width)

        y_spec = pl.BlockSpec((n_tok // n_loc, width), lambda e: (e, 0))

        def spec(*shape):
            return pl.BlockSpec((1,) + shape, lambda e: (e, 0, 0))

        grad_wa, grad_wb, grad_wc, act_out, grad_router = pl.pallas_call(
            weight_kernel,
            name="weight_grads",
            grid=(n_loc,),
            in_specs=[spec(blk, width), spec(blk, width), spec(blk, hid), spec(blk, hid), spec(blk, hid), y_spec, spec(n_exp // n_loc, width)],
            out_specs=[spec(width, hid), spec(width, hid), spec(hid, width), y_spec, spec(n_exp // n_loc, width)],
            out_shape=[
                sds((n_loc, width, hid), F32), sds((n_loc, width, hid), F32), sds((n_loc, hid, width), F32),
                sds((n_tok, width), BF), sds((n_loc, n_exp // n_loc, width), F32),
            ],
            compiler_params=pltpu.CompilerParams(
                dimension_semantics=("arbitrary",), vmem_limit_bytes=67043328
            ),
            cost_estimate=pl.CostEstimate(
                flops=6 * n_loc * blk * width * hid, transcendentals=0,
                bytes_accessed=12 * n_loc * width * hid + 4 * n_loc * blk * width + 6 * n_loc * blk * hid,
            ),
        )(xe, de, h, da, db, act_out, grad_router.reshape(n_loc, n_exp // n_loc, width))
        return act_out, grad_in, grad_wa, grad_wb, grad_wc, grad_router.reshape(n_exp, width).T

    return jax.shard_map(
        local_step,
        mesh=mesh,
        in_specs=(P("ep", None), P(), P("ep"), P("ep"), P("ep", None, "tp"), P("ep", None, "tp"), P("ep", "tp", None), P("ep", None)),
        out_specs=(P("ep", None), P("ep", None), P("ep", None, "tp"), P("ep", None, "tp"), P("ep", "tp", None), P()),
        check_vma=False,
    )
```

```python
import functools

import jax
import jax.numpy as jnp
from jax import lax
from jax.experimental import pallas as pl
from jax.experimental.pallas import tpu as pltpu
from jax.sharding import PartitionSpec as P

BF = jnp.bfloat16
F32 = jnp.float32
I32 = jnp.int32
MESH = pl.DeviceIdType.MESH
GELU_COEF = 0.7978845608028654
AHEAD = 8
LAG = 3
Y_STEP = 8
Y_INNER = 0
NN = (((1,), (0,)), ((), ()))
NT = (((1,), (1,)), ((), ()))
TN = (((0,), (0,)), ((), ()))


def dot(a, b, dims=NN):
    return lax.dot_general(a, b, dims, preferred_element_type=F32)


def split3(v):
    hi = v.astype(BF)
    rest = v - hi.astype(F32)
    mid = rest.astype(BF)
    low = (rest - mid.astype(F32)).astype(BF)
    return hi, mid, low


def moe_kernel(
    tp_size, ep_size, cap,
    ids1_hbm, ids2_hbm, x_hbm, dy_hbm, wr_hbm, wa_hbm, wb_hbm, wc_hbm,
    y_out, dx_out, dwr_out, xe_out, de_out, h_out, da_out, db_out,
    x_v, dy_v, wr_v, wa_v, wb_v, wc_v,
    xs, ds, xr, dr, h_v, da_v, db_v, bs_v, gv_v,
    ps, pr, pdr, orr, dxr, y_v, dx_v,
    s1r, s2r, g1r, g2r, s1c, s2c, g1c, g2c, q1c, q2c, i1c, i2c, prob_v, dl_v,
    dwp, dwi, dwf, acc_v, ids1_ref, ids2_ref,
    in_sem, w_sem, out_sem, id_sem,
    xs_sem, xr_sem, xd_sem, xf_sem, xfs_sem, ds_sem, dr_sem,
    ps_sem, pr_sem, pds_sem, pdr_sem,
    os_sem, or_sem, dxs_sem, dxr_sem,
    ys_sem, yr_sem,
    rs_sem, rr_sem, fs_sem, fr_sem,
):
    k = lax.axis_index("tp")
    r = lax.axis_index("ep")
    n_loc = wa_v.shape[0]
    n_tok, width = x_v.shape
    hid = wa_v.shape[2]
    n_exp = n_loc * ep_size
    blk = ep_size * cap
    half = ep_size // tp_size
    my_place = (r % tp_size) * half + r // tp_size
    owner = (r % tp_size) == k
    other = 1 - k

    ins = [
        pltpu.make_async_copy(x_hbm, x_v, in_sem.at[0]),
        pltpu.make_async_copy(dy_hbm, dy_v, in_sem.at[1]),
        pltpu.make_async_copy(wr_hbm, wr_v, in_sem.at[2]),
    ]
    id_loads = [pltpu.make_async_copy(ids1_hbm, ids1_ref, id_sem.at[0]), pltpu.make_async_copy(ids2_hbm, ids2_ref, id_sem.at[1])]
    for c in id_loads:
        c.start()
    ins[0].start()

    def weight_copies(j):
        return [
            pltpu.make_async_copy(wa_hbm.at[j], wa_v.at[j], w_sem.at[0, j]),
            pltpu.make_async_copy(wb_hbm.at[j], wb_v.at[j], w_sem.at[1, j]),
            pltpu.make_async_copy(wc_hbm.at[j], wc_v.at[j], w_sem.at[2, j]),
        ]

    n_dev = tp_size * ep_size
    barrier = pltpu.get_barrier_semaphore()
    for d in range(1, n_dev):
        flat = (k * ep_size + r + d) % n_dev
        pl.semaphore_signal(barrier, inc=1, device_id=(flat // ep_size, flat % ep_size), device_id_type=MESH)

    for c in id_loads:
        c.wait()
    ids1 = ids1_ref[...]
    ids2 = ids2_ref[...]
    e_iota = lax.broadcasted_iota(I32, (n_exp, n_tok), 0)
    hot1 = jnp.where(ids1 == e_iota, 1.0, 0.0).astype(F32)
    hot2 = jnp.where(ids2 == e_iota, 1.0, 0.0).astype(F32)
    before = jnp.where(
        lax.broadcasted_iota(I32, (n_tok, n_tok), 0) < lax.broadcasted_iota(I32, (n_tok, n_tok), 1), 1.0, 0.0
    ).astype(BF)
    cum1 = dot(hot1.astype(BF), before)
    cum2 = dot(hot2.astype(BF), before)
    fill1 = jnp.sum(hot1, axis=1, keepdims=True)
    pos1 = jnp.sum(cum1 * hot1, axis=0, keepdims=True)
    pos2 = jnp.sum((cum2 + fill1) * hot2, axis=0, keepdims=True)

    def place(ids, pos):
        spot = (ids & (n_loc - 1)) * blk + (ids // n_loc) * cap
        return jnp.where(pos < cap, spot.astype(F32) + pos, float(n_exp * cap))

    s1r[...] = place(ids1, pos1)
    s2r[...] = place(ids2, pos2)

    def masks(j):
        spot = (lax.broadcasted_iota(I32, (blk, n_tok), 0) + j * blk).astype(F32)
        return s1r[...] == spot, s2r[...] == spot

    chip = r // 2
    chip_x = chip + 1 - 2 * (chip % 2)
    chip_y = (chip + 2) % 4
    chip_d = 3 - chip
    core = r % 2
    diag = 2 * chip_d + (k + r) % 2
    near = [2 * chip_x + core, 2 * chip_y + core, 2 * chip_x + 1 - core, 2 * chip_y + 1 - core, 2 * chip + 1 - core]
    far = [2 * chip_d + core, 2 * chip_d + 1 - core]

    def place_of(q):
        return (q % tp_size) * half + q // tp_size

    def send_row(src, dst, send_sem, recv_sem, j, q):
        pltpu.make_async_remote_copy(
            src_ref=src.at[j, q], dst_ref=dst.at[j, my_place],
            send_sem=send_sem, recv_sem=recv_sem.at[j],
            device_id=(k, q), device_id_type=MESH,
        ).start()

    def wait_recv(view, sem):
        pltpu.make_async_remote_copy(
            src_ref=view, dst_ref=view, send_sem=sem, recv_sem=sem, device_id=(k, r), device_id_type=MESH
        ).wait_recv()

    def wait_send(view, sem):
        pltpu.make_async_remote_copy(
            src_ref=view, dst_ref=view, send_sem=sem, recv_sem=sem, device_id=(k, r), device_id_type=MESH
        ).wait_send()

    def build_x(j):
        m1, m2 = masks(j)
        pick = jnp.where(m1 | m2, 1.0, 0.0).astype(BF)
        for c in range(0, width, 512):
            rows = dot(pick, x_v[:, c:c + 512]).astype(BF)
            xs[j, :, :, c:c + 512] = rows.reshape(ep_size, cap, 512)
        send_row(xs, xr, xs_sem, xd_sem, j, diag)
        for q in near:
            send_row(xs, xr, xs_sem, xr_sem, j, q)
        xr[j, my_place] = xs[j, r]

    ins[0].wait()
    ins[2].start()
    ins[1].start()

    @pl.loop(0, n_loc)
    def _(j):
        for c in weight_copies(j):
            c.start()

    pl.semaphore_wait(barrier, n_dev - 1)

    @pl.loop(0, AHEAD)
    def _(j):
        build_x(j)

    def column(row):
        return jnp.transpose(jnp.broadcast_to(row, (128, n_tok)))

    s1c[...] = column(s1r[...])
    s2c[...] = column(s2r[...])
    i1c[...] = column(ids1.astype(F32))
    i2c[...] = column(ids2.astype(F32))
    ins[2].wait()
    wr_hi, wr_mid, wr_low = split3(wr_v[...])
    xv = x_v[...]
    logits = dot(xv, wr_hi, NT) + (dot(xv, wr_mid, NT) + dot(xv, wr_low, NT))
    ex = jnp.exp(logits - jnp.max(logits, axis=1, keepdims=True))
    prob = ex / jnp.sum(ex, axis=1, keepdims=True)
    prob_v[...] = prob
    lane = lax.broadcasted_iota(I32, (n_tok, n_exp), 1).astype(F32)
    q1 = jnp.sum(jnp.where(i1c[:, :n_exp] == lane, prob, 0.0), axis=1, keepdims=True)
    q2 = jnp.sum(jnp.where(i2c[:, :n_exp] == lane, prob, 0.0), axis=1, keepdims=True)
    g1 = jnp.broadcast_to(q1 / (q1 + q2), (n_tok, 128))
    g2 = jnp.broadcast_to(q2 / (q1 + q2), (n_tok, 128))
    g1c[...] = g1
    g2c[...] = g2
    q1c[...] = jnp.broadcast_to(q1, (n_tok, 128))
    q2c[...] = jnp.broadcast_to(q2, (n_tok, 128))
    g1r[...] = jnp.transpose(g1)[0:1, :]
    g2r[...] = jnp.transpose(g2)[0:1, :]
    ins[1].wait()

    def build_d(j):
        m1, m2 = masks(j)
        pick = jnp.where(m1 | m2, 1.0, 0.0).astype(BF)
        gate = jnp.sum(jnp.where(m1, g1r[...], 0.0) + jnp.where(m2, g2r[...], 0.0), axis=1, keepdims=True)
        for c in range(0, width, 512):
            rows = (gate * dot(pick, dy_v[:, c:c + 512])).astype(BF)
            ds[j, :, :, c:c + 512] = rows.reshape(ep_size, cap, 512)
        for q in far + near:
            send_row(ds, dr, ds_sem, dr_sem, j, q)
        dr[j, my_place] = ds[j, r]

    def send_half(src, dst, send_sem, recv_sem, j):
        pltpu.make_async_remote_copy(
            src_ref=src.at[j, pl.ds(other * half, half)], dst_ref=dst.at[j],
            send_sem=send_sem, recv_sem=recv_sem.at[j],
            device_id=(other, r), device_id_type=MESH,
        ).start()

    def merge_and_return(src, got, got_sem, dst, send_sem, recv_sem, j):
        wait_recv(got.at[j], got_sem.at[j])
        mine = pl.ds(k * half, half)
        src[j, mine] = (src[j, mine].astype(F32) + got[j].astype(F32)).astype(BF)
        for d in range(half):
            c = (r // tp_size + d) % half
            q = tp_size * c + k

            @pl.when(q != r)
            def _():
                pltpu.make_async_remote_copy(
                    src_ref=src.at[j, k * half + c], dst_ref=dst.at[j, r],
                    send_sem=send_sem, recv_sem=recv_sem.at[j],
                    device_id=(k, q), device_id_type=MESH,
                ).start()

            @pl.when(q == r)
            def _():
                dst[j, r] = src[j, k * half + c]

    n_near = len(near)
    diag_place = place_of(diag)

    def forward_diag(j):
        wait_recv(xr.at[j, 0], xd_sem.at[j])
        pltpu.make_async_remote_copy(
            src_ref=xr.at[j, diag_place], dst_ref=xr.at[j, diag_place],
            send_sem=xfs_sem, recv_sem=xf_sem.at[j],
            device_id=(other, r), device_id_type=MESH,
        ).start()

    forward_diag(0)

    @pl.loop(0, n_loc)
    def _(j):
        if AHEAD < n_loc:
            @pl.when(j + AHEAD < n_loc)
            def _():
                build_x(j + AHEAD)

            @pl.when(j + AHEAD >= n_loc)
            def _():
                build_d(j + AHEAD - n_loc)
        else:
            build_d(j)

        @pl.when(j + 1 < n_loc)
        def _():
            forward_diag(j + 1)

        for c in weight_copies(j):
            c.wait()
        wait_recv(xr.at[j, pl.ds(0, n_near)], xr_sem.at[j])
        wait_recv(xr.at[j, 0], xf_sem.at[j])
        rows = xr[j].reshape(blk, width)
        pa = dot(rows, wa_v[j])
        pb = dot(rows, wb_v[j])
        th = jnp.tanh(GELU_COEF * (pa + 0.044715 * pa * pa * pa))
        gv = 0.5 * pa * (1.0 + th)
        slope = 0.5 * (1.0 + th) + 0.5 * pa * (1.0 - th * th) * GELU_COEF * (1.0 + 0.134145 * pa * pa)
        gv_v[j] = gv
        bs_v[j] = pb * slope
        hidden = (gv * pb).astype(BF)
        h_v[j] = hidden
        for c in range(0, width, 512):
            ps[j, :, :, c:c + 512] = dot(hidden, wc_v[j, :, c:c + 512]).astype(BF).reshape(ep_size, cap, 512)
        send_half(ps, pr, ps_sem, pr_sem, j)

        @pl.when(j >= LAG)
        def _():
            merge_and_return(ps, pr, pr_sem, orr, os_sem, or_sem, j - LAG)

    tb = 128
    n_tb = n_tok // tb

    def spots(col, toks):
        lanes = lax.broadcasted_iota(I32, (tb, 128), 1).astype(F32)
        base = col[toks, :]
        return jnp.concatenate([base == lanes + float(u * 128) for u in range(n_exp * cap // 128)], axis=1)

    def ship(buf, toks, send_sem, recv_sem):
        pltpu.make_async_remote_copy(
            src_ref=buf.at[toks], dst_ref=buf.at[toks], send_sem=send_sem, recv_sem=recv_sem,
            device_id=(other, r), device_id_type=MESH,
        ).start()

    def wait_returned():
        @pl.loop(0, n_loc)
        def _(i):
            wait_recv(orr.at[i, pl.ds(0, ep_size - 1)], or_sem.at[i])

    def combine_y(t):
        toks = pl.ds(pl.multiple_of(t * tb, tb), tb)
        pick1 = jnp.where(spots(s1c, toks), 1.0, 0.0).astype(BF)
        pick2 = jnp.where(spots(s2c, toks), 1.0, 0.0).astype(BF)
        dg1 = jnp.zeros((tb, 1), F32)
        dg2 = jnp.zeros((tb, 1), F32)
        ga = g1c[toks, 0:1]
        gb = g2c[toks, 0:1]
        for c in range(0, width, 512):
            rows = orr[:, :, :, c:c + 512].reshape(n_exp * cap, 512)
            o1 = dot(pick1, rows)
            o2 = dot(pick2, rows)
            y_v[toks, c:c + 512] = (ga * o1 + gb * o2).astype(BF)
            dyf = dy_v[toks, c:c + 512].astype(F32)
            dg1 = dg1 + jnp.sum(dyf * o1, axis=1, keepdims=True)
            dg2 = dg2 + jnp.sum(dyf * o2, axis=1, keepdims=True)
        ship(y_v, toks, ys_sem, yr_sem)
        qa = q1c[toks, 0:1]
        qb = q2c[toks, 0:1]
        shared = dg1 * ga + dg2 * gb
        dq1 = (dg1 - shared) / (qa + qb)
        dq2 = (dg2 - shared) / (qa + qb)
        centre = dq1 * qa + dq2 * qb
        lanes = lax.broadcasted_iota(I32, (tb, n_exp), 1).astype(F32)
        pull = jnp.where(i1c[toks, :n_exp] == lanes, dq1, 0.0) + jnp.where(i2c[toks, :n_exp] == lanes, dq2, 0.0)
        dl_v[toks, :] = prob_v[toks, :] * (pull - centre)

    wait_send(xs.at[:, pl.ds(0, n_near + 1)], xs_sem)
    @pl.loop(0, n_loc)
    def _(j):
        if AHEAD < n_loc:
            @pl.when(j + AHEAD < n_loc)
            def _():
                build_d(j + AHEAD)

        wait_recv(dr.at[j, pl.ds(0, ep_size - 1)], dr_sem.at[j])
        rows = dr[j].reshape(blk, width)
        dh = dot(rows, wc_v[j], NT)
        da = (dh * bs_v[j]).astype(BF)
        db = (dh * gv_v[j]).astype(BF)
        da_v[j] = da
        db_v[j] = db
        for c in range(0, width, 512):
            part = dot(da, wa_v[j, c:c + 512, :], NT) + dot(db, wb_v[j, c:c + 512, :], NT)
            xs[j, :, :, c:c + 512] = part.astype(BF).reshape(ep_size, cap, 512)
        send_half(xs, pdr, pds_sem, pdr_sem, j)

        @pl.when(j == 0)
        def _():
            for i in range(LAG):
                merge_and_return(ps, pr, pr_sem, orr, os_sem, or_sem, n_loc - LAG + i)

        @pl.when(j >= LAG)
        def _():
            merge_and_return(xs, pdr, pdr_sem, dxr, dxs_sem, dxr_sem, j - LAG)

        if Y_INNER > 0:
            @pl.when(owner & (j == Y_STEP))
            def _():
                wait_returned()

            @pl.when(owner & (j >= Y_STEP) & (j < Y_STEP + Y_INNER))
            def _():
                combine_y(j - Y_STEP)

    outs = [
        pltpu.make_async_copy(xr, xe_out, out_sem.at[0]),
        pltpu.make_async_copy(dr, de_out, out_sem.at[1]),
        pltpu.make_async_copy(h_v, h_out, out_sem.at[2]),
        pltpu.make_async_copy(da_v, da_out, out_sem.at[3]),
        pltpu.make_async_copy(db_v, db_out, out_sem.at[4]),
    ]
    for c in outs[:3]:
        c.start()

    split = n_loc - 2

    def pick_both(t):
        toks = pl.ds(pl.multiple_of(t * tb, tb), tb)
        return toks, jnp.where(spots(s1c, toks) | spots(s2c, toks), 1.0, 0.0).astype(BF)

    def sum_first(t):
        toks, pick = pick_both(t)
        dl = dl_v[toks, :]
        for c in range(0, width, 512):
            rows = dxr[0:split, :, :, c:c + 512].reshape(split * blk, 512)
            router = lax.dot_general(
                dl, wr_v[:, c:c + 512], NN, precision=lax.Precision.HIGHEST, preferred_element_type=F32
            )
            acc_v[toks, c:c + 512] = dot(pick[:, :split * blk], rows) + router

    def sum_last(t):
        toks, pick = pick_both(t)
        for c in range(0, width, 512):
            rows = dxr[split:n_loc, :, :, c:c + 512].reshape((n_loc - split) * blk, 512)
            dx_v[toks, c:c + 512] = (acc_v[toks, c:c + 512] + dot(pick[:, split * blk:], rows)).astype(BF)
        pltpu.make_async_copy(dx_v.at[toks], dx_out.at[toks], in_sem.at[1]).start()

    @pl.when(owner)
    def _():
        if Y_INNER == 0:
            wait_returned()

        @pl.loop(Y_INNER, n_tb)
        def _(t):
            combine_y(t)

        d_hi, d_mid, d_low = split3(dl_v[...])
        for c in range(0, width, 512):
            xc = x_v[:, c:c + 512]
            piece = dot(d_hi, xc, TN) + (dot(d_mid, xc, TN) + dot(d_low, xc, TN))
            dwp[:, :, c:c + 512] = piece.reshape(ep_size, n_loc, 512)
        for d in range(1, ep_size):
            q = (r + d) % ep_size
            pltpu.make_async_remote_copy(
                src_ref=dwp.at[q], dst_ref=dwi.at[r], send_sem=rs_sem, recv_sem=rr_sem,
                device_id=(q % tp_size, q), device_id_type=MESH,
            ).start()
        dwi[r] = dwp[r]

    for i in range(LAG):
        merge_and_return(xs, pdr, pdr_sem, dxr, dxs_sem, dxr_sem, n_loc - LAG + i)

    for c in outs[3:]:
        c.start()

    @pl.when(owner)
    def _():
        @pl.loop(0, split)
        def _(j):
            wait_recv(dxr.at[j, pl.ds(0, ep_size - 1)], dxr_sem.at[j])

        @pl.loop(0, n_tb)
        def _(t):
            sum_first(t)

        wait_recv(dwi.at[pl.ds(0, ep_size - 1)], rr_sem)
        total = dwi[0]
        for q in range(1, ep_size):
            total = total + dwi[q]
        dwf[r] = total
        for d in range(1, n_dev):
            flat = (k * ep_size + r + d) % n_dev
            pltpu.make_async_remote_copy(
                src_ref=dwf.at[r], dst_ref=dwf.at[r], send_sem=fs_sem, recv_sem=fr_sem,
                device_id=(flat // ep_size, flat % ep_size), device_id_type=MESH,
            ).start()

        @pl.loop(split, n_loc)
        def _(j):
            wait_recv(dxr.at[j, pl.ds(0, ep_size - 1)], dxr_sem.at[j])

        @pl.loop(0, n_tb)
        def _(t):
            sum_last(t)

        wait_recv(dwf.at[pl.ds(0, ep_size - 1)], fr_sem)
        wait_send(dwp.at[pl.ds(0, ep_size - 1)], rs_sem)
        for half_sends in range(n_dev - 1):
            wait_send(dwf.at[r], fs_sem)
        wait_send(y_v, ys_sem)
        wait_send(orr.at[:, pl.ds(0, half - 1)], os_sem)
        wait_send(dxr.at[:, pl.ds(0, half - 1)], dxs_sem)

    @pl.when(jnp.logical_not(owner))
    def _():
        dx_v[...] = jnp.zeros_like(dx_v)
        pltpu.make_async_copy(dx_v, dx_out, in_sem.at[1]).start()
        wait_recv(y_v, yr_sem)
        wait_recv(dwf, fr_sem)
        wait_send(orr.at[:, pl.ds(0, half)], os_sem)
        wait_send(dxr.at[:, pl.ds(0, half)], dxs_sem)

    finals = [
        pltpu.make_async_copy(y_v, y_out, in_sem.at[0]),
        pltpu.make_async_copy(dwf, dwr_out, in_sem.at[2]),
    ]
    for c in finals:
        c.start()
    finals.append(pltpu.make_async_copy(dx_v, dx_out, in_sem.at[1]))
    wait_send(ds.at[:, pl.ds(0, ep_size - 1)], ds_sem)
    wait_send(xr.at[:, 0], xfs_sem)
    wait_send(ps.at[:, pl.ds(0, half)], ps_sem)
    wait_send(xs.at[:, pl.ds(0, half)], pds_sem)
    for c in outs + finals:
        c.wait()


def weight_kernel(xe, de, h, da, db, y, dwr, ga_out, gb_out, gc_out, y_out, dwr_out):
    y_out[...] = y[...]
    dwr_out[...] = dwr[...]
    rows = xe[0]
    ga_out[0] = dot(rows, da[0], TN)
    gb_out[0] = dot(rows, db[0], TN)
    gc_out[0] = dot(h[0], de[0], TN)


def solution(mesh):
    tp_size = mesh.shape["tp"]
    ep_size = mesh.shape["ep"]

    def local_step(x_rows, w_router, first_ids, second_ids, w_gelu, w_lin, w_out, dy_rows):
        n_tok, width = x_rows.shape
        n_exp = w_router.shape[1]
        n_loc, _, hid = w_gelu.shape
        cap = 2 * n_tok // n_exp
        blk = ep_size * cap
        half = ep_size // tp_size
        dma = pltpu.SemaphoreType.DMA
        any_spec = pl.BlockSpec(memory_space=pl.ANY)
        sds = jax.ShapeDtypeStruct
        rows_shape = (n_loc, ep_size, cap, width)
        half_shape = (n_loc, half, cap, width)
        hid_shape = (n_loc, blk, hid)
        col = pltpu.VMEM((n_tok, 128), F32)
        row = pltpu.VMEM((1, n_tok), F32)
        outs = pl.pallas_call(
            functools.partial(moe_kernel, tp_size, ep_size, cap),
            name="moe",
            in_specs=[any_spec] * 8,
            out_specs=[any_spec] * 8,
            out_shape=[
                sds((n_tok, width), BF), sds((n_tok, width), BF), sds((ep_size, n_loc, width), F32),
                sds(rows_shape, BF), sds(rows_shape, BF), sds(hid_shape, BF), sds(hid_shape, BF), sds(hid_shape, BF),
            ],
            scratch_shapes=[
                pltpu.VMEM((n_tok, width), BF), pltpu.VMEM((n_tok, width), BF), pltpu.VMEM((n_exp, width), F32),
                pltpu.VMEM((n_loc, width, hid), BF), pltpu.VMEM((n_loc, width, hid), BF), pltpu.VMEM((n_loc, hid, width), BF),
                pltpu.VMEM(rows_shape, BF), pltpu.VMEM(rows_shape, BF), pltpu.VMEM(rows_shape, BF), pltpu.VMEM(rows_shape, BF),
                pltpu.VMEM(hid_shape, BF), pltpu.VMEM(hid_shape, BF), pltpu.VMEM(hid_shape, BF),
                pltpu.VMEM(hid_shape, F32), pltpu.VMEM(hid_shape, F32),
                pltpu.VMEM(rows_shape, BF), pltpu.VMEM(half_shape, BF), pltpu.VMEM(half_shape, BF),
                pltpu.VMEM(rows_shape, BF), pltpu.VMEM(rows_shape, BF),
                pltpu.VMEM((n_tok, width), BF), pltpu.VMEM((n_tok, width), BF),
                row, row, row, row, col, col, col, col, col, col, col, col,
                pltpu.VMEM((n_tok, n_exp), F32), pltpu.VMEM((n_tok, n_exp), F32),
                pltpu.VMEM((ep_size, n_loc, width), F32), pltpu.VMEM((ep_size, n_loc, width), F32),
                pltpu.VMEM((ep_size, n_loc, width), F32), pltpu.VMEM((n_tok, width), F32),
                pltpu.VMEM((1, n_tok), I32), pltpu.VMEM((1, n_tok), I32),
                dma((3,)), dma((3, n_loc)), dma((5,)), dma((2,)),
                dma(()), dma((n_loc,)), dma((n_loc,)), dma((n_loc,)), dma(()), dma(()), dma((n_loc,)),
                dma(()), dma((n_loc,)), dma(()), dma((n_loc,)),
                dma(()), dma((n_loc,)), dma(()), dma((n_loc,)),
                dma(()), dma(()),
                dma(()), dma(()), dma(()), dma(()),
            ],
            compiler_params=pltpu.CompilerParams(
                collective_id=0, has_side_effects=True, vmem_limit_bytes=67043328
            ),
        )(
            first_ids.reshape(1, n_tok), second_ids.reshape(1, n_tok), x_rows, dy_rows, w_router.T,
            w_gelu, w_lin, w_out,
        )
        act_out, grad_in, grad_router, xe, de, h, da, db = outs
        partners = [
            ((q % tp_size) * ep_size + q, (1 - q % tp_size) * ep_size + q) for q in range(ep_size)
        ]
        passed = lax.ppermute(grad_in, ("tp", "ep"), partners)
        owner = lax.axis_index("ep") % tp_size == lax.axis_index("tp")
        grad_in = jnp.where(owner, grad_in, passed)
        xe = xe.reshape(n_loc, blk, width)
        de = de.reshape(n_loc, blk, width)

        y_spec = pl.BlockSpec((n_tok // n_loc, width), lambda e: (e, 0))

        def spec(*shape):
            return pl.BlockSpec((1,) + shape, lambda e: (e, 0, 0))

        grad_wa, grad_wb, grad_wc, act_out, grad_router = pl.pallas_call(
            weight_kernel,
            name="weight_grads",
            grid=(n_loc,),
            in_specs=[spec(blk, width), spec(blk, width), spec(blk, hid), spec(blk, hid), spec(blk, hid), y_spec, spec(n_exp // n_loc, width)],
            out_specs=[spec(width, hid), spec(width, hid), spec(hid, width), y_spec, spec(n_exp // n_loc, width)],
            out_shape=[
                sds((n_loc, width, hid), F32), sds((n_loc, width, hid), F32), sds((n_loc, hid, width), F32),
                sds((n_tok, width), BF), sds((n_loc, n_exp // n_loc, width), F32),
            ],
            compiler_params=pltpu.CompilerParams(
                dimension_semantics=("arbitrary",), vmem_limit_bytes=67043328
            ),
            cost_estimate=pl.CostEstimate(
                flops=6 * n_loc * blk * width * hid, transcendentals=0,
                bytes_accessed=12 * n_loc * width * hid + 4 * n_loc * blk * width + 6 * n_loc * blk * hid,
            ),
        )(xe, de, h, da, db, act_out, grad_router.reshape(n_loc, n_exp // n_loc, width))
        return act_out, grad_in, grad_wa, grad_wb, grad_wc, grad_router.reshape(n_exp, width).T

    return jax.shard_map(
        local_step,
        mesh=mesh,
        in_specs=(P("ep", None), P(), P("ep"), P("ep"), P("ep", None, "tp"), P("ep", None, "tp"), P("ep", "tp", None), P("ep", None)),
        out_specs=(P("ep", None), P("ep", None), P("ep", None, "tp"), P("ep", None, "tp"), P("ep", "tp", None), P()),
        check_vma=False,
    )
```

```python
import functools

import jax
import jax.numpy as jnp
from jax import lax
from jax.experimental import pallas as pl
from jax.experimental.pallas import tpu as pltpu
from jax.sharding import PartitionSpec as P

BF = jnp.bfloat16
F32 = jnp.float32
I32 = jnp.int32
MESH = pl.DeviceIdType.MESH
GELU_COEF = 0.7978845608028654
AHEAD = 5
LAG = 3
Y_STEP = 5
FORWARD = 2
NN = (((1,), (0,)), ((), ()))
NT = (((1,), (1,)), ((), ()))
TN = (((0,), (0,)), ((), ()))


def dot(a, b, dims=NN):
    return lax.dot_general(a, b, dims, preferred_element_type=F32)


def split3(v):
    hi = v.astype(BF)
    rest = v - hi.astype(F32)
    mid = rest.astype(BF)
    low = (rest - mid.astype(F32)).astype(BF)
    return hi, mid, low


def moe_kernel(
    tp_size, ep_size, cap,
    ids1_hbm, ids2_hbm, x_hbm, dy_hbm, wr_hbm, wa_hbm, wb_hbm, wc_hbm,
    y_out, dx_out, dwr_out, xe_out, de_out, h_out, da_out, db_out,
    x_v, dy_v, wr_v, wa_v, wb_v, wc_v,
    xs, ds, xr, dr, h_v, da_v, db_v, bs_v, gv_v,
    ps, pr, pdr, orr, dxr, y_v, dx_v,
    s1r, s2r, g1r, g2r, s1c, s2c, g1c, g2c, q1c, q2c, i1c, i2c, prob_v, dl_v,
    dwp, dwi, dwf, acc_v, ids1_ref, ids2_ref,
    in_sem, w_sem, out_sem, id_sem,
    xs_sem, xr_sem, xd_sem, xf_sem, xfs_sem, ds_sem, dr_sem,
    ps_sem, pr_sem, pds_sem, pdr_sem,
    os_sem, or_sem, dxs_sem, dxr_sem,
    ys_sem, yr_sem,
    rs_sem, rr_sem, fs_sem, fr_sem, gs_sem, gr_sem,
):
    k = lax.axis_index("tp")
    r = lax.axis_index("ep")
    n_loc = wa_v.shape[0]
    n_tok, width = x_v.shape
    hid = wa_v.shape[2]
    n_exp = n_loc * ep_size
    blk = ep_size * cap
    half = ep_size // tp_size
    my_place = (r % tp_size) * half + r // tp_size
    owner = (r % tp_size) == k
    other = 1 - k

    ins = [
        pltpu.make_async_copy(x_hbm, x_v, in_sem.at[0]),
        pltpu.make_async_copy(dy_hbm, dy_v, in_sem.at[1]),
        pltpu.make_async_copy(wr_hbm, wr_v, in_sem.at[2]),
    ]
    id_loads = [pltpu.make_async_copy(ids1_hbm, ids1_ref, id_sem.at[0]), pltpu.make_async_copy(ids2_hbm, ids2_ref, id_sem.at[1])]
    for c in id_loads:
        c.start()
    ins[0].start()

    def weight_copies(j):
        return [
            pltpu.make_async_copy(wa_hbm.at[j], wa_v.at[j], w_sem.at[0, j]),
            pltpu.make_async_copy(wb_hbm.at[j], wb_v.at[j], w_sem.at[1, j]),
            pltpu.make_async_copy(wc_hbm.at[j], wc_v.at[j], w_sem.at[2, j]),
        ]

    n_dev = tp_size * ep_size
    barrier = pltpu.get_barrier_semaphore()
    for d in range(1, n_dev):
        flat = (k * ep_size + r + d) % n_dev
        pl.semaphore_signal(barrier, inc=1, device_id=(flat // ep_size, flat % ep_size), device_id_type=MESH)

    for c in id_loads:
        c.wait()
    ids1 = ids1_ref[...]
    ids2 = ids2_ref[...]
    e_iota = lax.broadcasted_iota(I32, (n_exp, n_tok), 0)
    hot1 = jnp.where(ids1 == e_iota, 1.0, 0.0).astype(F32)
    hot2 = jnp.where(ids2 == e_iota, 1.0, 0.0).astype(F32)
    before = jnp.where(
        lax.broadcasted_iota(I32, (n_tok, n_tok), 0) < lax.broadcasted_iota(I32, (n_tok, n_tok), 1), 1.0, 0.0
    ).astype(BF)
    cum1 = dot(hot1.astype(BF), before)
    cum2 = dot(hot2.astype(BF), before)
    fill1 = jnp.sum(hot1, axis=1, keepdims=True)
    pos1 = jnp.sum(cum1 * hot1, axis=0, keepdims=True)
    pos2 = jnp.sum((cum2 + fill1) * hot2, axis=0, keepdims=True)

    def place(ids, pos):
        spot = (ids & (n_loc - 1)) * blk + (ids // n_loc) * cap
        return jnp.where(pos < cap, spot.astype(F32) + pos, float(n_exp * cap))

    s1r[...] = place(ids1, pos1)
    s2r[...] = place(ids2, pos2)

    def masks(j):
        spot = (lax.broadcasted_iota(I32, (blk, n_tok), 0) + j * blk).astype(F32)
        return s1r[...] == spot, s2r[...] == spot

    chip = r // 2
    chip_x = chip + 1 - 2 * (chip % 2)
    chip_y = (chip + 2) % 4
    chip_d = 3 - chip
    core = r % 2
    diag = 2 * chip_d + (k + r) % 2
    near = [2 * chip_x + core, 2 * chip_y + core, 2 * chip_x + 1 - core, 2 * chip_y + 1 - core, 2 * chip + 1 - core]
    far = [2 * chip_d + core, 2 * chip_d + 1 - core]

    def place_of(q):
        return (q % tp_size) * half + q // tp_size

    def send_row(src, dst, send_sem, recv_sem, j, q):
        pltpu.make_async_remote_copy(
            src_ref=src.at[j, q], dst_ref=dst.at[j, my_place],
            send_sem=send_sem, recv_sem=recv_sem.at[j],
            device_id=(k, q), device_id_type=MESH,
        ).start()

    def wait_recv(view, sem):
        pltpu.make_async_remote_copy(
            src_ref=view, dst_ref=view, send_sem=sem, recv_sem=sem, device_id=(k, r), device_id_type=MESH
        ).wait_recv()

    def wait_send(view, sem):
        pltpu.make_async_remote_copy(
            src_ref=view, dst_ref=view, send_sem=sem, recv_sem=sem, device_id=(k, r), device_id_type=MESH
        ).wait_send()

    def build_x(j):
        m1, m2 = masks(j)
        pick = jnp.where(m1 | m2, 1.0, 0.0).astype(BF)
        for c in range(0, width, 512):
            rows = dot(pick, x_v[:, c:c + 512]).astype(BF)
            xs[j, :, :, c:c + 512] = rows.reshape(ep_size, cap, 512)
        send_row(xs, xr, xs_sem, xd_sem, j, diag)
        for q in near:
            send_row(xs, xr, xs_sem, xr_sem, j, q)
        xr[j, my_place] = xs[j, r]

    ins[0].wait()
    ins[2].start()
    ins[1].start()

    @pl.loop(0, n_loc)
    def _(j):
        for c in weight_copies(j):
            c.start()

    pl.semaphore_wait(barrier, n_dev - 1)

    @pl.loop(0, n_loc)
    def _(j):
        build_x(j)

    def column(row):
        return jnp.transpose(jnp.broadcast_to(row, (128, n_tok)))

    s1c[...] = column(s1r[...])
    s2c[...] = column(s2r[...])
    i1c[...] = column(ids1.astype(F32))
    i2c[...] = column(ids2.astype(F32))
    ins[2].wait()
    wr_hi, wr_mid, wr_low = split3(wr_v[...])
    xv = x_v[...]
    logits = dot(xv, wr_hi, NT) + (dot(xv, wr_mid, NT) + dot(xv, wr_low, NT))
    ex = jnp.exp(logits - jnp.max(logits, axis=1, keepdims=True))
    prob = ex / jnp.sum(ex, axis=1, keepdims=True)
    prob_v[...] = prob
    lane = lax.broadcasted_iota(I32, (n_tok, n_exp), 1).astype(F32)
    q1 = jnp.sum(jnp.where(i1c[:, :n_exp] == lane, prob, 0.0), axis=1, keepdims=True)
    q2 = jnp.sum(jnp.where(i2c[:, :n_exp] == lane, prob, 0.0), axis=1, keepdims=True)
    g1 = jnp.broadcast_to(q1 / (q1 + q2), (n_tok, 128))
    g2 = jnp.broadcast_to(q2 / (q1 + q2), (n_tok, 128))
    g1c[...] = g1
    g2c[...] = g2
    q1c[...] = jnp.broadcast_to(q1, (n_tok, 128))
    q2c[...] = jnp.broadcast_to(q2, (n_tok, 128))
    g1r[...] = jnp.transpose(g1)[0:1, :]
    g2r[...] = jnp.transpose(g2)[0:1, :]
    ins[1].wait()

    def build_d(j):
        m1, m2 = masks(j)
        pick = jnp.where(m1 | m2, 1.0, 0.0).astype(BF)
        gate = jnp.sum(jnp.where(m1, g1r[...], 0.0) + jnp.where(m2, g2r[...], 0.0), axis=1, keepdims=True)
        for c in range(0, width, 512):
            rows = (gate * dot(pick, dy_v[:, c:c + 512])).astype(BF)
            ds[j, :, :, c:c + 512] = rows.reshape(ep_size, cap, 512)
        for q in far + near:
            send_row(ds, dr, ds_sem, dr_sem, j, q)
        dr[j, my_place] = ds[j, r]

    def send_half(src, dst, send_sem, recv_sem, j):
        pltpu.make_async_remote_copy(
            src_ref=src.at[j, pl.ds(other * half, half)], dst_ref=dst.at[j],
            send_sem=send_sem, recv_sem=recv_sem.at[j],
            device_id=(other, r), device_id_type=MESH,
        ).start()

    def merge_and_return(src, got, got_sem, dst, send_sem, recv_sem, j):
        wait_recv(got.at[j], got_sem.at[j])
        mine = pl.ds(k * half, half)
        src[j, mine] = (src[j, mine].astype(F32) + got[j].astype(F32)).astype(BF)
        for d in range(half):
            c = (r // tp_size + d) % half
            q = tp_size * c + k

            @pl.when(q != r)
            def _():
                pltpu.make_async_remote_copy(
                    src_ref=src.at[j, k * half + c], dst_ref=dst.at[j, r],
                    send_sem=send_sem, recv_sem=recv_sem.at[j],
                    device_id=(k, q), device_id_type=MESH,
                ).start()

            @pl.when(q == r)
            def _():
                dst[j, r] = src[j, k * half + c]

    n_near = len(near)
    diag_place = place_of(diag)

    def forward_diag(j):
        wait_recv(xr.at[j, 0], xd_sem.at[j])
        pltpu.make_async_remote_copy(
            src_ref=xr.at[j, diag_place], dst_ref=xr.at[j, diag_place],
            send_sem=xfs_sem, recv_sem=xf_sem.at[j],
            device_id=(other, r), device_id_type=MESH,
        ).start()

    for i in range(FORWARD):
        forward_diag(i)

    @pl.loop(0, n_loc)
    def _(j):
        @pl.when(j >= n_loc - AHEAD)
        def _():
            build_d(j + AHEAD - n_loc)

        @pl.when(j + FORWARD < n_loc)
        def _():
            forward_diag(j + FORWARD)

        for c in weight_copies(j):
            c.wait()
        wait_recv(xr.at[j, pl.ds(0, n_near)], xr_sem.at[j])
        wait_recv(xr.at[j, 0], xf_sem.at[j])
        rows = xr[j].reshape(blk, width)
        pa = dot(rows, wa_v[j])
        pb = dot(rows, wb_v[j])
        th = jnp.tanh(GELU_COEF * (pa + 0.044715 * pa * pa * pa))
        gv = 0.5 * pa * (1.0 + th)
        slope = 0.5 * (1.0 + th) + 0.5 * pa * (1.0 - th * th) * GELU_COEF * (1.0 + 0.134145 * pa * pa)
        gv_v[j] = gv
        bs_v[j] = pb * slope
        hidden = (gv * pb).astype(BF)
        h_v[j] = hidden
        for c in range(0, width, 512):
            ps[j, :, :, c:c + 512] = dot(hidden, wc_v[j, :, c:c + 512]).astype(BF).reshape(ep_size, cap, 512)
        send_half(ps, pr, ps_sem, pr_sem, j)

        @pl.when(j >= LAG)
        def _():
            merge_and_return(ps, pr, pr_sem, orr, os_sem, or_sem, j - LAG)

    tb = 128
    n_tb = n_tok // tb

    def spots(col, toks):
        lanes = lax.broadcasted_iota(I32, (tb, 128), 1).astype(F32)
        base = col[toks, :]
        return jnp.concatenate([base == lanes + float(u * 128) for u in range(n_exp * cap // 128)], axis=1)

    def ship(buf, t, send_sem, recv_sem):
        toks = pl.ds(pl.multiple_of(t * tb, tb), tb)
        pltpu.make_async_remote_copy(
            src_ref=buf.at[toks], dst_ref=buf.at[toks], send_sem=send_sem, recv_sem=recv_sem,
            device_id=(other, r), device_id_type=MESH,
        ).start()

    def combine_y(t):
        toks = pl.ds(pl.multiple_of(t * tb, tb), tb)
        pick1 = jnp.where(spots(s1c, toks), 1.0, 0.0).astype(BF)
        pick2 = jnp.where(spots(s2c, toks), 1.0, 0.0).astype(BF)
        dg1 = jnp.zeros((tb, 1), F32)
        dg2 = jnp.zeros((tb, 1), F32)
        ga = g1c[toks, 0:1]
        gb = g2c[toks, 0:1]
        for c in range(0, width, 512):
            rows = orr[:, :, :, c:c + 512].reshape(n_exp * cap, 512)
            o1 = dot(pick1, rows)
            o2 = dot(pick2, rows)
            y_v[toks, c:c + 512] = (ga * o1 + gb * o2).astype(BF)
            dyf = dy_v[toks, c:c + 512].astype(F32)
            dg1 = dg1 + jnp.sum(dyf * o1, axis=1, keepdims=True)
            dg2 = dg2 + jnp.sum(dyf * o2, axis=1, keepdims=True)
        qa = q1c[toks, 0:1]
        qb = q2c[toks, 0:1]
        shared = dg1 * ga + dg2 * gb
        dq1 = (dg1 - shared) / (qa + qb)
        dq2 = (dg2 - shared) / (qa + qb)
        centre = dq1 * qa + dq2 * qb
        lanes = lax.broadcasted_iota(I32, (tb, n_exp), 1).astype(F32)
        pull = jnp.where(i1c[toks, :n_exp] == lanes, dq1, 0.0) + jnp.where(i2c[toks, :n_exp] == lanes, dq2, 0.0)
        dl_v[toks, :] = prob_v[toks, :] * (pull - centre)

    def router_parts():
        d_hi, d_mid, d_low = split3(dl_v[...])
        for c in range(0, width, 512):
            xc = x_v[:, c:c + 512]
            piece = dot(d_hi, xc, TN) + (dot(d_mid, xc, TN) + dot(d_low, xc, TN))
            dwp[:, :, c:c + 512] = piece.reshape(ep_size, n_loc, 512)
        for d in range(1, ep_size):
            q = (r + d) % ep_size
            pltpu.make_async_remote_copy(
                src_ref=dwp.at[q], dst_ref=dwi.at[r], send_sem=rs_sem, recv_sem=rr_sem,
                device_id=(q % tp_size, q), device_id_type=MESH,
            ).start()
        dwi[r] = dwp[r]

    wait_send(xs.at[:, pl.ds(0, n_near + 1)], xs_sem)
    @pl.loop(0, n_loc)
    def _(j):
        @pl.when(j + AHEAD < n_loc)
        def _():
            build_d(j + AHEAD)

        wait_recv(dr.at[j, pl.ds(0, ep_size - 1)], dr_sem.at[j])
        rows = dr[j].reshape(blk, width)
        dh = dot(rows, wc_v[j], NT)
        da = (dh * bs_v[j]).astype(BF)
        db = (dh * gv_v[j]).astype(BF)
        da_v[j] = da
        db_v[j] = db
        for c in range(0, width, 512):
            part = dot(da, wa_v[j, c:c + 512, :], NT) + dot(db, wb_v[j, c:c + 512, :], NT)
            xs[j, :, :, c:c + 512] = part.astype(BF).reshape(ep_size, cap, 512)
        send_half(xs, pdr, pds_sem, pdr_sem, j)

        @pl.when(j == 0)
        def _():
            for i in range(LAG):
                merge_and_return(ps, pr, pr_sem, orr, os_sem, or_sem, n_loc - LAG + i)

        @pl.when(j >= LAG)
        def _():
            merge_and_return(xs, pdr, pdr_sem, dxr, dxs_sem, dxr_sem, j - LAG)

        @pl.when(owner & (j == Y_STEP))
        def _():
            @pl.loop(0, n_loc)
            def _(i):
                wait_recv(orr.at[i, pl.ds(0, ep_size - 1)], or_sem.at[i])

        @pl.when(owner & (j >= Y_STEP) & (j < Y_STEP + n_tb // 2))
        def _():
            t0 = 2 * (j - Y_STEP)

            @pl.loop(t0, t0 + 2)
            def _(t):
                combine_y(t)

            ship(y_v, j - Y_STEP, ys_sem, yr_sem)

        @pl.when(owner & (j == Y_STEP + n_tb // 2 - 1))
        def _():
            router_parts()

    outs = [
        pltpu.make_async_copy(xr, xe_out, out_sem.at[0]),
        pltpu.make_async_copy(dr, de_out, out_sem.at[1]),
        pltpu.make_async_copy(h_v, h_out, out_sem.at[2]),
        pltpu.make_async_copy(da_v, da_out, out_sem.at[3]),
        pltpu.make_async_copy(db_v, db_out, out_sem.at[4]),
    ]
    for c in outs[:3]:
        c.start()

    split = n_loc - 2

    def pick_both(t):
        toks = pl.ds(pl.multiple_of(t * tb, tb), tb)
        return toks, jnp.where(spots(s1c, toks) | spots(s2c, toks), 1.0, 0.0).astype(BF)

    def sum_first(t):
        toks, pick = pick_both(t)
        dl = dl_v[toks, :]
        for c in range(0, width, 512):
            rows = dxr[0:split, :, :, c:c + 512].reshape(split * blk, 512)
            router = lax.dot_general(
                dl, wr_v[:, c:c + 512], NN, precision=lax.Precision.HIGHEST, preferred_element_type=F32
            )
            acc_v[toks, c:c + 512] = dot(pick[:, :split * blk], rows) + router

    def sum_last(t):
        toks, pick = pick_both(t)
        for c in range(0, width, 512):
            rows = dxr[split:n_loc, :, :, c:c + 512].reshape((n_loc - split) * blk, 512)
            dx_v[toks, c:c + 512] = (acc_v[toks, c:c + 512] + dot(pick[:, split * blk:], rows)).astype(BF)
        pltpu.make_async_copy(dx_v.at[toks], dx_out.at[toks], in_sem.at[1]).start()

    @pl.when(owner)
    def _():
        @pl.loop(n_tb // 2, n_tb)
        def _(t):
            ship(y_v, t, ys_sem, yr_sem)

    for i in range(LAG):
        merge_and_return(xs, pdr, pdr_sem, dxr, dxs_sem, dxr_sem, n_loc - LAG + i)

    for c in outs[3:]:
        c.start()

    @pl.when(owner)
    def _():
        wait_recv(dwi.at[pl.ds(0, ep_size - 1)], rr_sem)
        total = dwi[0]
        for q in range(1, ep_size):
            total = total + dwi[q]
        dwf[r] = total
        for d in range(1, ep_size):
            q = (r + d) % ep_size
            pltpu.make_async_remote_copy(
                src_ref=dwf.at[r], dst_ref=dwf.at[r], send_sem=fs_sem, recv_sem=fr_sem,
                device_id=(q % tp_size, q), device_id_type=MESH,
            ).start()

        @pl.loop(0, split)
        def _(j):
            wait_recv(dxr.at[j, pl.ds(0, ep_size - 1)], dxr_sem.at[j])

        @pl.loop(0, n_tb)
        def _(t):
            sum_first(t)

        @pl.loop(split, n_loc)
        def _(j):
            wait_recv(dxr.at[j, pl.ds(0, ep_size - 1)], dxr_sem.at[j])

        @pl.loop(0, n_tb)
        def _(t):
            sum_last(t)

        wait_recv(dwf.at[pl.ds(0, ep_size - 1)], fr_sem)
        pltpu.make_async_remote_copy(
            src_ref=dwf, dst_ref=dwf, send_sem=gs_sem, recv_sem=gr_sem,
            device_id=(k, 2 * chip + 1 - core), device_id_type=MESH,
        ).start()
        wait_send(dwp.at[pl.ds(0, ep_size - 1)], rs_sem)
        wait_send(dwf.at[pl.ds(0, ep_size - 1)], fs_sem)
        wait_send(dwf, gs_sem)
        wait_send(y_v, ys_sem)
        wait_send(orr.at[:, pl.ds(0, half - 1)], os_sem)
        wait_send(dxr.at[:, pl.ds(0, half - 1)], dxs_sem)

    @pl.when(jnp.logical_not(owner))
    def _():
        dx_v[...] = jnp.zeros_like(dx_v)
        pltpu.make_async_copy(dx_v, dx_out, in_sem.at[1]).start()
        wait_recv(y_v, yr_sem)
        wait_recv(dwf, gr_sem)
        wait_send(orr.at[:, pl.ds(0, half)], os_sem)
        wait_send(dxr.at[:, pl.ds(0, half)], dxs_sem)

    finals = [
        pltpu.make_async_copy(y_v, y_out, in_sem.at[0]),
        pltpu.make_async_copy(dwf, dwr_out, in_sem.at[2]),
    ]
    for c in finals:
        c.start()
    finals.append(pltpu.make_async_copy(dx_v, dx_out, in_sem.at[1]))
    wait_send(ds.at[:, pl.ds(0, ep_size - 1)], ds_sem)
    wait_send(xr.at[:, 0], xfs_sem)
    wait_send(ps.at[:, pl.ds(0, half)], ps_sem)
    wait_send(xs.at[:, pl.ds(0, half)], pds_sem)
    for c in outs + finals:
        c.wait()


def weight_kernel(xe, de, h, da, db, y, dwr, ga_out, gb_out, gc_out, y_out, dwr_out):
    y_out[...] = y[...]
    dwr_out[...] = dwr[...]
    rows = xe[0]
    ga_out[0] = dot(rows, da[0], TN)
    gb_out[0] = dot(rows, db[0], TN)
    gc_out[0] = dot(h[0], de[0], TN)


def solution(mesh):
    tp_size = mesh.shape["tp"]
    ep_size = mesh.shape["ep"]

    def local_step(x_rows, w_router, first_ids, second_ids, w_gelu, w_lin, w_out, dy_rows):
        n_tok, width = x_rows.shape
        n_exp = w_router.shape[1]
        n_loc, _, hid = w_gelu.shape
        cap = 2 * n_tok // n_exp
        blk = ep_size * cap
        half = ep_size // tp_size
        dma = pltpu.SemaphoreType.DMA
        any_spec = pl.BlockSpec(memory_space=pl.ANY)
        sds = jax.ShapeDtypeStruct
        rows_shape = (n_loc, ep_size, cap, width)
        half_shape = (n_loc, half, cap, width)
        hid_shape = (n_loc, blk, hid)
        col = pltpu.VMEM((n_tok, 128), F32)
        row = pltpu.VMEM((1, n_tok), F32)
        outs = pl.pallas_call(
            functools.partial(moe_kernel, tp_size, ep_size, cap),
            name="moe",
            in_specs=[any_spec] * 8,
            out_specs=[any_spec] * 8,
            out_shape=[
                sds((n_tok, width), BF), sds((n_tok, width), BF), sds((ep_size, n_loc, width), F32),
                sds(rows_shape, BF), sds(rows_shape, BF), sds(hid_shape, BF), sds(hid_shape, BF), sds(hid_shape, BF),
            ],
            scratch_shapes=[
                pltpu.VMEM((n_tok, width), BF), pltpu.VMEM((n_tok, width), BF), pltpu.VMEM((n_exp, width), F32),
                pltpu.VMEM((n_loc, width, hid), BF), pltpu.VMEM((n_loc, width, hid), BF), pltpu.VMEM((n_loc, hid, width), BF),
                pltpu.VMEM(rows_shape, BF), pltpu.VMEM(rows_shape, BF), pltpu.VMEM(rows_shape, BF), pltpu.VMEM(rows_shape, BF),
                pltpu.VMEM(hid_shape, BF), pltpu.VMEM(hid_shape, BF), pltpu.VMEM(hid_shape, BF),
                pltpu.VMEM(hid_shape, F32), pltpu.VMEM(hid_shape, F32),
                pltpu.VMEM(rows_shape, BF), pltpu.VMEM(half_shape, BF), pltpu.VMEM(half_shape, BF),
                pltpu.VMEM(rows_shape, BF), pltpu.VMEM(rows_shape, BF),
                pltpu.VMEM((n_tok, width), BF), pltpu.VMEM((n_tok, width), BF),
                row, row, row, row, col, col, col, col, col, col, col, col,
                pltpu.VMEM((n_tok, n_exp), F32), pltpu.VMEM((n_tok, n_exp), F32),
                pltpu.VMEM((ep_size, n_loc, width), F32), pltpu.VMEM((ep_size, n_loc, width), F32),
                pltpu.VMEM((ep_size, n_loc, width), F32), pltpu.VMEM((n_tok, width), F32),
                pltpu.VMEM((1, n_tok), I32), pltpu.VMEM((1, n_tok), I32),
                dma((3,)), dma((3, n_loc)), dma((5,)), dma((2,)),
                dma(()), dma((n_loc,)), dma((n_loc,)), dma((n_loc,)), dma(()), dma(()), dma((n_loc,)),
                dma(()), dma((n_loc,)), dma(()), dma((n_loc,)),
                dma(()), dma((n_loc,)), dma(()), dma((n_loc,)),
                dma(()), dma(()),
                dma(()), dma(()), dma(()), dma(()), dma(()), dma(()),
            ],
            compiler_params=pltpu.CompilerParams(
                collective_id=0, has_side_effects=True, vmem_limit_bytes=67043328
            ),
        )(
            first_ids.reshape(1, n_tok), second_ids.reshape(1, n_tok), x_rows, dy_rows, w_router.T,
            w_gelu, w_lin, w_out,
        )
        act_out, grad_in, grad_router, xe, de, h, da, db = outs
        partners = [
            ((q % tp_size) * ep_size + q, (1 - q % tp_size) * ep_size + q) for q in range(ep_size)
        ]
        passed = lax.ppermute(grad_in, ("tp", "ep"), partners)
        owner = lax.axis_index("ep") % tp_size == lax.axis_index("tp")
        grad_in = jnp.where(owner, grad_in, passed)
        xe = xe.reshape(n_loc, blk, width)
        de = de.reshape(n_loc, blk, width)

        y_spec = pl.BlockSpec((n_tok // n_loc, width), lambda e: (e, 0))

        def spec(*shape):
            return pl.BlockSpec((1,) + shape, lambda e: (e, 0, 0))

        grad_wa, grad_wb, grad_wc, act_out, grad_router = pl.pallas_call(
            weight_kernel,
            name="weight_grads",
            grid=(n_loc,),
            in_specs=[spec(blk, width), spec(blk, width), spec(blk, hid), spec(blk, hid), spec(blk, hid), y_spec, spec(n_exp // n_loc, width)],
            out_specs=[spec(width, hid), spec(width, hid), spec(hid, width), y_spec, spec(n_exp // n_loc, width)],
            out_shape=[
                sds((n_loc, width, hid), F32), sds((n_loc, width, hid), F32), sds((n_loc, hid, width), F32),
                sds((n_tok, width), BF), sds((n_loc, n_exp // n_loc, width), F32),
            ],
            compiler_params=pltpu.CompilerParams(
                dimension_semantics=("arbitrary",), vmem_limit_bytes=67043328
            ),
            cost_estimate=pl.CostEstimate(
                flops=6 * n_loc * blk * width * hid, transcendentals=0,
                bytes_accessed=12 * n_loc * width * hid + 4 * n_loc * blk * width + 6 * n_loc * blk * hid,
            ),
        )(xe, de, h, da, db, act_out, grad_router.reshape(n_loc, n_exp // n_loc, width))
        return act_out, grad_in, grad_wa, grad_wb, grad_wc, grad_router.reshape(n_exp, width).T

    return jax.shard_map(
        local_step,
        mesh=mesh,
        in_specs=(P("ep", None), P(), P("ep"), P("ep"), P("ep", None, "tp"), P("ep", None, "tp"), P("ep", "tp", None), P("ep", None)),
        out_specs=(P("ep", None), P("ep", None), P("ep", None, "tp"), P("ep", None, "tp"), P("ep", "tp", None), P()),
        check_vma=False,
    )
```

```python
import functools

import jax
import jax.numpy as jnp
from jax import lax
from jax.experimental import pallas as pl
from jax.experimental.pallas import tpu as pltpu
from jax.sharding import PartitionSpec as P

BF = jnp.bfloat16
F32 = jnp.float32
I32 = jnp.int32
MESH = pl.DeviceIdType.MESH
GELU_COEF = 0.7978845608028654
AHEAD = 5
LAG = 3
Y_STEP = 5
FORWARD = 2
VIA_TP = 6
NN = (((1,), (0,)), ((), ()))
NT = (((1,), (1,)), ((), ()))
TN = (((0,), (0,)), ((), ()))


def dot(a, b, dims=NN):
    return lax.dot_general(a, b, dims, preferred_element_type=F32)


def split3(v):
    hi = v.astype(BF)
    rest = v - hi.astype(F32)
    mid = rest.astype(BF)
    low = (rest - mid.astype(F32)).astype(BF)
    return hi, mid, low


def moe_kernel(
    tp_size, ep_size, cap,
    ids1_hbm, ids2_hbm, x_hbm, dy_hbm, wr_hbm, wa_hbm, wb_hbm, wc_hbm,
    y_out, dx_out, dwr_out, xe_out, de_out, h_out, da_out, db_out,
    x_v, dy_v, wr_v, wa_v, wb_v, wc_v,
    xs, ds, xr, dr, h_v, da_v, db_v, bs_v, gv_v,
    ps, pr, pdr, orr, dxr, y_v, dx_v,
    s1r, s2r, g1r, g2r, s1c, s2c, g1c, g2c, q1c, q2c, i1c, i2c, prob_v, dl_v,
    dwp, dwi, dwf, acc_v, ids1_ref, ids2_ref,
    in_sem, w_sem, out_sem, id_sem,
    xs_sem, xr_sem, xd_sem, xf_sem, xfs_sem, ds_sem, dr_sem,
    ps_sem, pr_sem, pds_sem, pdr_sem,
    os_sem, or_sem, dxs_sem, dxr_sem,
    ys_sem, yr_sem,
    rs_sem, rr_sem, fs_sem, fr_sem, gs_sem, gr_sem,
):
    k = lax.axis_index("tp")
    r = lax.axis_index("ep")
    n_loc = wa_v.shape[0]
    n_tok, width = x_v.shape
    hid = wa_v.shape[2]
    n_exp = n_loc * ep_size
    blk = ep_size * cap
    half = ep_size // tp_size
    my_place = (r % tp_size) * half + r // tp_size
    owner = (r % tp_size) == k
    other = 1 - k

    ins = [
        pltpu.make_async_copy(x_hbm, x_v, in_sem.at[0]),
        pltpu.make_async_copy(dy_hbm, dy_v, in_sem.at[1]),
        pltpu.make_async_copy(wr_hbm, wr_v, in_sem.at[2]),
    ]
    id_loads = [pltpu.make_async_copy(ids1_hbm, ids1_ref, id_sem.at[0]), pltpu.make_async_copy(ids2_hbm, ids2_ref, id_sem.at[1])]
    for c in id_loads:
        c.start()
    ins[0].start()

    def weight_copies(j):
        return [
            pltpu.make_async_copy(wa_hbm.at[j], wa_v.at[j], w_sem.at[0, j]),
            pltpu.make_async_copy(wb_hbm.at[j], wb_v.at[j], w_sem.at[1, j]),
            pltpu.make_async_copy(wc_hbm.at[j], wc_v.at[j], w_sem.at[2, j]),
        ]

    n_dev = tp_size * ep_size
    barrier = pltpu.get_barrier_semaphore()
    for d in range(1, n_dev):
        flat = (k * ep_size + r + d) % n_dev
        pl.semaphore_signal(barrier, inc=1, device_id=(flat // ep_size, flat % ep_size), device_id_type=MESH)

    for c in id_loads:
        c.wait()
    ids1 = ids1_ref[...]
    ids2 = ids2_ref[...]
    e_iota = lax.broadcasted_iota(I32, (n_exp, n_tok), 0)
    hot1 = jnp.where(ids1 == e_iota, 1.0, 0.0).astype(F32)
    hot2 = jnp.where(ids2 == e_iota, 1.0, 0.0).astype(F32)
    before = jnp.where(
        lax.broadcasted_iota(I32, (n_tok, n_tok), 0) < lax.broadcasted_iota(I32, (n_tok, n_tok), 1), 1.0, 0.0
    ).astype(BF)
    cum1 = dot(hot1.astype(BF), before)
    cum2 = dot(hot2.astype(BF), before)
    fill1 = jnp.sum(hot1, axis=1, keepdims=True)
    pos1 = jnp.sum(cum1 * hot1, axis=0, keepdims=True)
    pos2 = jnp.sum((cum2 + fill1) * hot2, axis=0, keepdims=True)

    def place(ids, pos):
        spot = (ids & (n_loc - 1)) * blk + (ids // n_loc) * cap
        return jnp.where(pos < cap, spot.astype(F32) + pos, float(n_exp * cap))

    s1r[...] = place(ids1, pos1)
    s2r[...] = place(ids2, pos2)

    def masks(j):
        spot = (lax.broadcasted_iota(I32, (blk, n_tok), 0) + j * blk).astype(F32)
        return s1r[...] == spot, s2r[...] == spot

    chip = r // 2
    chip_x = chip + 1 - 2 * (chip % 2)
    chip_y = (chip + 2) % 4
    chip_d = 3 - chip
    core = r % 2
    diag = 2 * chip_d + (k + r) % 2
    near = [2 * chip_x + core, 2 * chip_y + core, 2 * chip_x + 1 - core, 2 * chip_y + 1 - core, 2 * chip + 1 - core]
    far = [2 * chip_d + core, 2 * chip_d + 1 - core]

    def place_of(q):
        return (q % tp_size) * half + q // tp_size

    def send_row(src, dst, send_sem, recv_sem, j, q):
        pltpu.make_async_remote_copy(
            src_ref=src.at[j, q], dst_ref=dst.at[j, my_place],
            send_sem=send_sem, recv_sem=recv_sem.at[j],
            device_id=(k, q), device_id_type=MESH,
        ).start()

    def wait_recv(view, sem):
        pltpu.make_async_remote_copy(
            src_ref=view, dst_ref=view, send_sem=sem, recv_sem=sem, device_id=(k, r), device_id_type=MESH
        ).wait_recv()

    def wait_send(view, sem):
        pltpu.make_async_remote_copy(
            src_ref=view, dst_ref=view, send_sem=sem, recv_sem=sem, device_id=(k, r), device_id_type=MESH
        ).wait_send()

    def build_x(j, via_tp):
        m1, m2 = masks(j)
        pick = jnp.where(m1 | m2, 1.0, 0.0).astype(BF)
        for c in range(0, width, 512):
            rows = dot(pick, x_v[:, c:c + 512]).astype(BF)
            xs[j, :, :, c:c + 512] = rows.reshape(ep_size, cap, 512)
        if via_tp:
            send_row(xs, xr, xs_sem, xd_sem, j, diag)
        for q in near if via_tp else far + near:
            send_row(xs, xr, xs_sem, xr_sem, j, q)
        xr[j, my_place] = xs[j, r]

    ins[0].wait()
    ins[2].start()
    ins[1].start()

    @pl.loop(0, n_loc)
    def _(j):
        for c in weight_copies(j):
            c.start()

    pl.semaphore_wait(barrier, n_dev - 1)

    @pl.loop(0, VIA_TP)
    def _(j):
        build_x(j, True)

    @pl.loop(VIA_TP, n_loc)
    def _(j):
        build_x(j, False)

    def column(row):
        return jnp.transpose(jnp.broadcast_to(row, (128, n_tok)))

    s1c[...] = column(s1r[...])
    s2c[...] = column(s2r[...])
    i1c[...] = column(ids1.astype(F32))
    i2c[...] = column(ids2.astype(F32))
    ins[2].wait()
    wr_hi, wr_mid, wr_low = split3(wr_v[...])
    xv = x_v[...]
    logits = dot(xv, wr_hi, NT) + (dot(xv, wr_mid, NT) + dot(xv, wr_low, NT))
    ex = jnp.exp(logits - jnp.max(logits, axis=1, keepdims=True))
    prob = ex / jnp.sum(ex, axis=1, keepdims=True)
    prob_v[...] = prob
    lane = lax.broadcasted_iota(I32, (n_tok, n_exp), 1).astype(F32)
    q1 = jnp.sum(jnp.where(i1c[:, :n_exp] == lane, prob, 0.0), axis=1, keepdims=True)
    q2 = jnp.sum(jnp.where(i2c[:, :n_exp] == lane, prob, 0.0), axis=1, keepdims=True)
    g1 = jnp.broadcast_to(q1 / (q1 + q2), (n_tok, 128))
    g2 = jnp.broadcast_to(q2 / (q1 + q2), (n_tok, 128))
    g1c[...] = g1
    g2c[...] = g2
    q1c[...] = jnp.broadcast_to(q1, (n_tok, 128))
    q2c[...] = jnp.broadcast_to(q2, (n_tok, 128))
    g1r[...] = jnp.transpose(g1)[0:1, :]
    g2r[...] = jnp.transpose(g2)[0:1, :]
    ins[1].wait()

    def build_d(j):
        m1, m2 = masks(j)
        pick = jnp.where(m1 | m2, 1.0, 0.0).astype(BF)
        gate = jnp.sum(jnp.where(m1, g1r[...], 0.0) + jnp.where(m2, g2r[...], 0.0), axis=1, keepdims=True)
        for c in range(0, width, 512):
            rows = (gate * dot(pick, dy_v[:, c:c + 512])).astype(BF)
            ds[j, :, :, c:c + 512] = rows.reshape(ep_size, cap, 512)
        for q in far + near:
            send_row(ds, dr, ds_sem, dr_sem, j, q)
        dr[j, my_place] = ds[j, r]

    def send_half(src, dst, send_sem, recv_sem, j):
        pltpu.make_async_remote_copy(
            src_ref=src.at[j, pl.ds(other * half, half)], dst_ref=dst.at[j],
            send_sem=send_sem, recv_sem=recv_sem.at[j],
            device_id=(other, r), device_id_type=MESH,
        ).start()

    def merge_and_return(src, got, got_sem, dst, send_sem, recv_sem, j):
        wait_recv(got.at[j], got_sem.at[j])
        mine = pl.ds(k * half, half)
        src[j, mine] = (src[j, mine].astype(F32) + got[j].astype(F32)).astype(BF)
        for d in range(half):
            c = (r // tp_size + d) % half
            q = tp_size * c + k

            @pl.when(q != r)
            def _():
                pltpu.make_async_remote_copy(
                    src_ref=src.at[j, k * half + c], dst_ref=dst.at[j, r],
                    send_sem=send_sem, recv_sem=recv_sem.at[j],
                    device_id=(k, q), device_id_type=MESH,
                ).start()

            @pl.when(q == r)
            def _():
                dst[j, r] = src[j, k * half + c]

    n_near = len(near)
    diag_place = place_of(diag)

    def forward_diag(j):
        wait_recv(xr.at[j, 0], xd_sem.at[j])
        pltpu.make_async_remote_copy(
            src_ref=xr.at[j, diag_place], dst_ref=xr.at[j, diag_place],
            send_sem=xfs_sem, recv_sem=xf_sem.at[j],
            device_id=(other, r), device_id_type=MESH,
        ).start()

    for i in range(FORWARD):
        forward_diag(i)

    @pl.loop(0, n_loc)
    def _(j):
        @pl.when(j >= n_loc - AHEAD)
        def _():
            build_d(j + AHEAD - n_loc)

        @pl.when(j + FORWARD < VIA_TP)
        def _():
            forward_diag(j + FORWARD)

        for c in weight_copies(j):
            c.wait()

        @pl.when(j < VIA_TP)
        def _():
            wait_recv(xr.at[j, pl.ds(0, n_near)], xr_sem.at[j])
            wait_recv(xr.at[j, 0], xf_sem.at[j])

        @pl.when(j >= VIA_TP)
        def _():
            wait_recv(xr.at[j, pl.ds(0, ep_size - 1)], xr_sem.at[j])

        rows = xr[j].reshape(blk, width)
        pa = dot(rows, wa_v[j])
        pb = dot(rows, wb_v[j])
        th = jnp.tanh(GELU_COEF * (pa + 0.044715 * pa * pa * pa))
        gv = 0.5 * pa * (1.0 + th)
        slope = 0.5 * (1.0 + th) + 0.5 * pa * (1.0 - th * th) * GELU_COEF * (1.0 + 0.134145 * pa * pa)
        gv_v[j] = gv
        bs_v[j] = pb * slope
        hidden = (gv * pb).astype(BF)
        h_v[j] = hidden
        for c in range(0, width, 512):
            ps[j, :, :, c:c + 512] = dot(hidden, wc_v[j, :, c:c + 512]).astype(BF).reshape(ep_size, cap, 512)
        send_half(ps, pr, ps_sem, pr_sem, j)

        @pl.when(j >= LAG)
        def _():
            merge_and_return(ps, pr, pr_sem, orr, os_sem, or_sem, j - LAG)

    tb = 128
    n_tb = n_tok // tb

    def spots(col, toks):
        lanes = lax.broadcasted_iota(I32, (tb, 128), 1).astype(F32)
        base = col[toks, :]
        return jnp.concatenate([base == lanes + float(u * 128) for u in range(n_exp * cap // 128)], axis=1)

    def ship(buf, t, send_sem, recv_sem):
        toks = pl.ds(pl.multiple_of(t * tb, tb), tb)
        pltpu.make_async_remote_copy(
            src_ref=buf.at[toks], dst_ref=buf.at[toks], send_sem=send_sem, recv_sem=recv_sem,
            device_id=(other, r), device_id_type=MESH,
        ).start()

    def combine_y(t):
        toks = pl.ds(pl.multiple_of(t * tb, tb), tb)
        pick1 = jnp.where(spots(s1c, toks), 1.0, 0.0).astype(BF)
        pick2 = jnp.where(spots(s2c, toks), 1.0, 0.0).astype(BF)
        dg1 = jnp.zeros((tb, 1), F32)
        dg2 = jnp.zeros((tb, 1), F32)
        ga = g1c[toks, 0:1]
        gb = g2c[toks, 0:1]
        for c in range(0, width, 512):
            rows = orr[:, :, :, c:c + 512].reshape(n_exp * cap, 512)
            o1 = dot(pick1, rows)
            o2 = dot(pick2, rows)
            y_v[toks, c:c + 512] = (ga * o1 + gb * o2).astype(BF)
            dyf = dy_v[toks, c:c + 512].astype(F32)
            dg1 = dg1 + jnp.sum(dyf * o1, axis=1, keepdims=True)
            dg2 = dg2 + jnp.sum(dyf * o2, axis=1, keepdims=True)
        qa = q1c[toks, 0:1]
        qb = q2c[toks, 0:1]
        shared = dg1 * ga + dg2 * gb
        dq1 = (dg1 - shared) / (qa + qb)
        dq2 = (dg2 - shared) / (qa + qb)
        centre = dq1 * qa + dq2 * qb
        lanes = lax.broadcasted_iota(I32, (tb, n_exp), 1).astype(F32)
        pull = jnp.where(i1c[toks, :n_exp] == lanes, dq1, 0.0) + jnp.where(i2c[toks, :n_exp] == lanes, dq2, 0.0)
        dl_v[toks, :] = prob_v[toks, :] * (pull - centre)

    def router_parts():
        d_hi, d_mid, d_low = split3(dl_v[...])
        for c in range(0, width, 512):
            xc = x_v[:, c:c + 512]
            piece = dot(d_hi, xc, TN) + (dot(d_mid, xc, TN) + dot(d_low, xc, TN))
            dwp[:, :, c:c + 512] = piece.reshape(ep_size, n_loc, 512)
        for d in range(1, ep_size):
            q = (r + d) % ep_size
            pltpu.make_async_remote_copy(
                src_ref=dwp.at[q], dst_ref=dwi.at[r], send_sem=rs_sem, recv_sem=rr_sem,
                device_id=(q % tp_size, q), device_id_type=MESH,
            ).start()
        dwi[r] = dwp[r]

    def router_sum():
        wait_recv(dwi.at[pl.ds(0, ep_size - 1)], rr_sem)
        total = dwi[0]
        for q in range(1, ep_size):
            total = total + dwi[q]
        dwf[r] = total
        for d in range(1, ep_size):
            q = (r + d) % ep_size
            pltpu.make_async_remote_copy(
                src_ref=dwf.at[r], dst_ref=dwf.at[r], send_sem=fs_sem, recv_sem=fr_sem,
                device_id=(q % tp_size, q), device_id_type=MESH,
            ).start()

    wait_send(xs.at[pl.ds(0, VIA_TP), pl.ds(0, n_near + 1)], xs_sem)
    wait_send(xs.at[pl.ds(VIA_TP, n_loc - VIA_TP), pl.ds(0, ep_size - 1)], xs_sem)
    @pl.loop(0, n_loc)
    def _(j):
        @pl.when(j + AHEAD < n_loc)
        def _():
            build_d(j + AHEAD)

        wait_recv(dr.at[j, pl.ds(0, ep_size - 1)], dr_sem.at[j])
        rows = dr[j].reshape(blk, width)
        dh = dot(rows, wc_v[j], NT)
        da = (dh * bs_v[j]).astype(BF)
        db = (dh * gv_v[j]).astype(BF)
        da_v[j] = da
        db_v[j] = db
        for c in range(0, width, 512):
            part = dot(da, wa_v[j, c:c + 512, :], NT) + dot(db, wb_v[j, c:c + 512, :], NT)
            xs[j, :, :, c:c + 512] = part.astype(BF).reshape(ep_size, cap, 512)
        send_half(xs, pdr, pds_sem, pdr_sem, j)

        @pl.when(j == 0)
        def _():
            for i in range(LAG):
                merge_and_return(ps, pr, pr_sem, orr, os_sem, or_sem, n_loc - LAG + i)

        @pl.when(j >= LAG)
        def _():
            merge_and_return(xs, pdr, pdr_sem, dxr, dxs_sem, dxr_sem, j - LAG)

        @pl.when(owner & (j == Y_STEP))
        def _():
            @pl.loop(0, n_loc)
            def _(i):
                wait_recv(orr.at[i, pl.ds(0, ep_size - 1)], or_sem.at[i])

        @pl.when(owner & (j >= Y_STEP) & (j < Y_STEP + n_tb // 2))
        def _():
            t0 = 2 * (j - Y_STEP)

            @pl.loop(t0, t0 + 2)
            def _(t):
                combine_y(t)

            ship(y_v, j - Y_STEP, ys_sem, yr_sem)

        @pl.when(owner & (j == Y_STEP + n_tb // 2 - 1))
        def _():
            router_parts()

    outs = [
        pltpu.make_async_copy(xr, xe_out, out_sem.at[0]),
        pltpu.make_async_copy(dr, de_out, out_sem.at[1]),
        pltpu.make_async_copy(h_v, h_out, out_sem.at[2]),
        pltpu.make_async_copy(da_v, da_out, out_sem.at[3]),
        pltpu.make_async_copy(db_v, db_out, out_sem.at[4]),
    ]
    for c in outs[:3]:
        c.start()

    split = n_loc - 2

    def pick_both(t):
        toks = pl.ds(pl.multiple_of(t * tb, tb), tb)
        return toks, jnp.where(spots(s1c, toks) | spots(s2c, toks), 1.0, 0.0).astype(BF)

    def sum_first(t):
        toks, pick = pick_both(t)
        dl = dl_v[toks, :]
        for c in range(0, width, 512):
            rows = dxr[0:split, :, :, c:c + 512].reshape(split * blk, 512)
            router = lax.dot_general(
                dl, wr_v[:, c:c + 512], NN, precision=lax.Precision.HIGHEST, preferred_element_type=F32
            )
            acc_v[toks, c:c + 512] = dot(pick[:, :split * blk], rows) + router

    def sum_last(t):
        toks, pick = pick_both(t)
        for c in range(0, width, 512):
            rows = dxr[split:n_loc, :, :, c:c + 512].reshape((n_loc - split) * blk, 512)
            dx_v[toks, c:c + 512] = (acc_v[toks, c:c + 512] + dot(pick[:, split * blk:], rows)).astype(BF)
        pltpu.make_async_copy(dx_v.at[toks], dx_out.at[toks], in_sem.at[1]).start()

    for c in outs[3:]:
        c.start()

    @pl.when(owner)
    def _():
        ship(y_v, n_tb - 2, ys_sem, yr_sem)

    for i in range(LAG - 1):
        merge_and_return(xs, pdr, pdr_sem, dxr, dxs_sem, dxr_sem, n_loc - LAG + i)

    @pl.when(owner)
    def _():
        router_sum()
        ship(y_v, n_tb - 1, ys_sem, yr_sem)

    merge_and_return(xs, pdr, pdr_sem, dxr, dxs_sem, dxr_sem, n_loc - 1)

    @pl.when(owner)
    def _():
        @pl.loop(0, split)
        def _(j):
            wait_recv(dxr.at[j, pl.ds(0, ep_size - 1)], dxr_sem.at[j])

        @pl.loop(0, n_tb)
        def _(t):
            sum_first(t)

        @pl.loop(split, n_loc)
        def _(j):
            wait_recv(dxr.at[j, pl.ds(0, ep_size - 1)], dxr_sem.at[j])

        @pl.loop(0, n_tb)
        def _(t):
            sum_last(t)

        wait_recv(dwf.at[pl.ds(0, ep_size - 1)], fr_sem)
        pltpu.make_async_remote_copy(
            src_ref=dwf, dst_ref=dwf, send_sem=gs_sem, recv_sem=gr_sem,
            device_id=(k, 2 * chip + 1 - core), device_id_type=MESH,
        ).start()
        wait_send(dwp.at[pl.ds(0, ep_size - 1)], rs_sem)
        wait_send(dwf.at[pl.ds(0, ep_size - 1)], fs_sem)
        wait_send(dwf, gs_sem)
        wait_send(y_v, ys_sem)
        wait_send(orr.at[:, pl.ds(0, half - 1)], os_sem)
        wait_send(dxr.at[:, pl.ds(0, half - 1)], dxs_sem)

    @pl.when(jnp.logical_not(owner))
    def _():
        dx_v[...] = jnp.zeros_like(dx_v)
        pltpu.make_async_copy(dx_v, dx_out, in_sem.at[1]).start()
        wait_recv(y_v, yr_sem)
        wait_recv(dwf, gr_sem)
        wait_send(orr.at[:, pl.ds(0, half)], os_sem)
        wait_send(dxr.at[:, pl.ds(0, half)], dxs_sem)

    finals = [
        pltpu.make_async_copy(y_v, y_out, in_sem.at[0]),
        pltpu.make_async_copy(dwf, dwr_out, in_sem.at[2]),
    ]
    for c in finals:
        c.start()
    finals.append(pltpu.make_async_copy(dx_v, dx_out, in_sem.at[1]))
    wait_send(ds.at[:, pl.ds(0, ep_size - 1)], ds_sem)
    wait_send(xr.at[pl.ds(0, VIA_TP), 0], xfs_sem)
    wait_send(ps.at[:, pl.ds(0, half)], ps_sem)
    wait_send(xs.at[:, pl.ds(0, half)], pds_sem)
    for c in outs + finals:
        c.wait()


def weight_kernel(xe, de, h, da, db, y, dwr, ga_out, gb_out, gc_out, y_out, dwr_out):
    y_out[...] = y[...]
    dwr_out[...] = dwr[...]
    rows = xe[0]
    ga_out[0] = dot(rows, da[0], TN)
    gb_out[0] = dot(rows, db[0], TN)
    gc_out[0] = dot(h[0], de[0], TN)


def solution(mesh):
    tp_size = mesh.shape["tp"]
    ep_size = mesh.shape["ep"]

    def local_step(x_rows, w_router, first_ids, second_ids, w_gelu, w_lin, w_out, dy_rows):
        n_tok, width = x_rows.shape
        n_exp = w_router.shape[1]
        n_loc, _, hid = w_gelu.shape
        cap = 2 * n_tok // n_exp
        blk = ep_size * cap
        half = ep_size // tp_size
        dma = pltpu.SemaphoreType.DMA
        any_spec = pl.BlockSpec(memory_space=pl.ANY)
        sds = jax.ShapeDtypeStruct
        rows_shape = (n_loc, ep_size, cap, width)
        half_shape = (n_loc, half, cap, width)
        hid_shape = (n_loc, blk, hid)
        col = pltpu.VMEM((n_tok, 128), F32)
        row = pltpu.VMEM((1, n_tok), F32)
        outs = pl.pallas_call(
            functools.partial(moe_kernel, tp_size, ep_size, cap),
            name="moe",
            in_specs=[any_spec] * 8,
            out_specs=[any_spec] * 8,
            out_shape=[
                sds((n_tok, width), BF), sds((n_tok, width), BF), sds((ep_size, n_loc, width), F32),
                sds(rows_shape, BF), sds(rows_shape, BF), sds(hid_shape, BF), sds(hid_shape, BF), sds(hid_shape, BF),
            ],
            scratch_shapes=[
                pltpu.VMEM((n_tok, width), BF), pltpu.VMEM((n_tok, width), BF), pltpu.VMEM((n_exp, width), F32),
                pltpu.VMEM((n_loc, width, hid), BF), pltpu.VMEM((n_loc, width, hid), BF), pltpu.VMEM((n_loc, hid, width), BF),
                pltpu.VMEM(rows_shape, BF), pltpu.VMEM(rows_shape, BF), pltpu.VMEM(rows_shape, BF), pltpu.VMEM(rows_shape, BF),
                pltpu.VMEM(hid_shape, BF), pltpu.VMEM(hid_shape, BF), pltpu.VMEM(hid_shape, BF),
                pltpu.VMEM(hid_shape, F32), pltpu.VMEM(hid_shape, F32),
                pltpu.VMEM(rows_shape, BF), pltpu.VMEM(half_shape, BF), pltpu.VMEM(half_shape, BF),
                pltpu.VMEM(rows_shape, BF), pltpu.VMEM(rows_shape, BF),
                pltpu.VMEM((n_tok, width), BF), pltpu.VMEM((n_tok, width), BF),
                row, row, row, row, col, col, col, col, col, col, col, col,
                pltpu.VMEM((n_tok, n_exp), F32), pltpu.VMEM((n_tok, n_exp), F32),
                pltpu.VMEM((ep_size, n_loc, width), F32), pltpu.VMEM((ep_size, n_loc, width), F32),
                pltpu.VMEM((ep_size, n_loc, width), F32), pltpu.VMEM((n_tok, width), F32),
                pltpu.VMEM((1, n_tok), I32), pltpu.VMEM((1, n_tok), I32),
                dma((3,)), dma((3, n_loc)), dma((5,)), dma((2,)),
                dma(()), dma((n_loc,)), dma((n_loc,)), dma((n_loc,)), dma(()), dma(()), dma((n_loc,)),
                dma(()), dma((n_loc,)), dma(()), dma((n_loc,)),
                dma(()), dma((n_loc,)), dma(()), dma((n_loc,)),
                dma(()), dma(()),
                dma(()), dma(()), dma(()), dma(()), dma(()), dma(()),
            ],
            compiler_params=pltpu.CompilerParams(
                collective_id=0, has_side_effects=True, vmem_limit_bytes=67043328
            ),
        )(
            first_ids.reshape(1, n_tok), second_ids.reshape(1, n_tok), x_rows, dy_rows, w_router.T,
            w_gelu, w_lin, w_out,
        )
        act_out, grad_in, grad_router, xe, de, h, da, db = outs
        partners = [
            ((q % tp_size) * ep_size + q, (1 - q % tp_size) * ep_size + q) for q in range(ep_size)
        ]
        passed = lax.ppermute(grad_in, ("tp", "ep"), partners)
        owner = lax.axis_index("ep") % tp_size == lax.axis_index("tp")
        grad_in = jnp.where(owner, grad_in, passed)
        xe = xe.reshape(n_loc, blk, width)
        de = de.reshape(n_loc, blk, width)

        y_spec = pl.BlockSpec((n_tok // n_loc, width), lambda e: (e, 0))

        def spec(*shape):
            return pl.BlockSpec((1,) + shape, lambda e: (e, 0, 0))

        grad_wa, grad_wb, grad_wc, act_out, grad_router = pl.pallas_call(
            weight_kernel,
            name="weight_grads",
            grid=(n_loc,),
            in_specs=[spec(blk, width), spec(blk, width), spec(blk, hid), spec(blk, hid), spec(blk, hid), y_spec, spec(n_exp // n_loc, width)],
            out_specs=[spec(width, hid), spec(width, hid), spec(hid, width), y_spec, spec(n_exp // n_loc, width)],
            out_shape=[
                sds((n_loc, width, hid), F32), sds((n_loc, width, hid), F32), sds((n_loc, hid, width), F32),
                sds((n_tok, width), BF), sds((n_loc, n_exp // n_loc, width), F32),
            ],
            compiler_params=pltpu.CompilerParams(
                dimension_semantics=("arbitrary",), vmem_limit_bytes=67043328
            ),
            cost_estimate=pl.CostEstimate(
                flops=6 * n_loc * blk * width * hid, transcendentals=0,
                bytes_accessed=12 * n_loc * width * hid + 4 * n_loc * blk * width + 6 * n_loc * blk * hid,
            ),
        )(xe, de, h, da, db, act_out, grad_router.reshape(n_loc, n_exp // n_loc, width))
        return act_out, grad_in, grad_wa, grad_wb, grad_wc, grad_router.reshape(n_exp, width).T

    return jax.shard_map(
        local_step,
        mesh=mesh,
        in_specs=(P("ep", None), P(), P("ep"), P("ep"), P("ep", None, "tp"), P("ep", None, "tp"), P("ep", "tp", None), P("ep", None)),
        out_specs=(P("ep", None), P("ep", None), P("ep", None, "tp"), P("ep", None, "tp"), P("ep", "tp", None), P()),
        check_vma=False,
    )
```

```python
import functools

import jax
import jax.numpy as jnp
from jax import lax
from jax.experimental import pallas as pl
from jax.experimental.pallas import tpu as pltpu
from jax.sharding import PartitionSpec as P

BF = jnp.bfloat16
F32 = jnp.float32
I32 = jnp.int32
MESH = pl.DeviceIdType.MESH
GELU_COEF = 0.7978845608028654
AHEAD = 5
LAG = 3
Y_STEP = 5
FORWARD = 2
VIA_TP = 4
NN = (((1,), (0,)), ((), ()))
NT = (((1,), (1,)), ((), ()))
TN = (((0,), (0,)), ((), ()))


def dot(a, b, dims=NN):
    return lax.dot_general(a, b, dims, preferred_element_type=F32)


def split3(v):
    hi = v.astype(BF)
    rest = v - hi.astype(F32)
    mid = rest.astype(BF)
    low = (rest - mid.astype(F32)).astype(BF)
    return hi, mid, low


def moe_kernel(
    tp_size, ep_size, cap,
    ids1_hbm, ids2_hbm, x_hbm, dy_hbm, wr_hbm, wa_hbm, wb_hbm, wc_hbm,
    y_out, dx_out, dwr_out, xe_out, de_out, h_out, da_out, db_out,
    x_v, dy_v, wr_v, wa_v, wb_v, wc_v,
    xs, ds, xr, dr, h_v, da_v, db_v, bs_v, gv_v,
    ps, pr, pdr, orr, dxr, y_v, dx_v,
    s1r, s2r, g1r, g2r, s1c, s2c, g1c, g2c, q1c, q2c, i1c, i2c, prob_v, dl_v,
    dwp, dwi, dwf, acc_v, ids1_ref, ids2_ref,
    in_sem, w_sem, out_sem, id_sem,
    xs_sem, xr_sem, xd_sem, xf_sem, xfs_sem, ds_sem, dr_sem,
    ps_sem, pr_sem, pds_sem, pdr_sem,
    os_sem, or_sem, dxs_sem, dxr_sem,
    ys_sem, yr_sem,
    rs_sem, rr_sem, fs_sem, fr_sem, gs_sem, gr_sem,
):
    k = lax.axis_index("tp")
    r = lax.axis_index("ep")
    n_loc = wa_v.shape[0]
    n_tok, width = x_v.shape
    hid = wa_v.shape[2]
    n_exp = n_loc * ep_size
    blk = ep_size * cap
    half = ep_size // tp_size
    my_place = (r % tp_size) * half + r // tp_size
    owner = (r % tp_size) == k
    other = 1 - k

    ins = [
        pltpu.make_async_copy(x_hbm, x_v, in_sem.at[0]),
        pltpu.make_async_copy(dy_hbm, dy_v, in_sem.at[1]),
        pltpu.make_async_copy(wr_hbm, wr_v, in_sem.at[2]),
    ]
    id_loads = [pltpu.make_async_copy(ids1_hbm, ids1_ref, id_sem.at[0]), pltpu.make_async_copy(ids2_hbm, ids2_ref, id_sem.at[1])]
    for c in id_loads:
        c.start()
    ins[0].start()

    def weight_copies(j):
        return [
            pltpu.make_async_copy(wa_hbm.at[j], wa_v.at[j], w_sem.at[0, j]),
            pltpu.make_async_copy(wb_hbm.at[j], wb_v.at[j], w_sem.at[1, j]),
            pltpu.make_async_copy(wc_hbm.at[j], wc_v.at[j], w_sem.at[2, j]),
        ]

    n_dev = tp_size * ep_size
    barrier = pltpu.get_barrier_semaphore()
    for d in range(1, n_dev):
        flat = (k * ep_size + r + d) % n_dev
        pl.semaphore_signal(barrier, inc=1, device_id=(flat // ep_size, flat % ep_size), device_id_type=MESH)

    for c in id_loads:
        c.wait()
    ids1 = ids1_ref[...]
    ids2 = ids2_ref[...]
    e_iota = lax.broadcasted_iota(I32, (n_exp, n_tok), 0)
    hot1 = jnp.where(ids1 == e_iota, 1.0, 0.0).astype(F32)
    hot2 = jnp.where(ids2 == e_iota, 1.0, 0.0).astype(F32)
    before = jnp.where(
        lax.broadcasted_iota(I32, (n_tok, n_tok), 0) < lax.broadcasted_iota(I32, (n_tok, n_tok), 1), 1.0, 0.0
    ).astype(BF)
    cum1 = dot(hot1.astype(BF), before)
    cum2 = dot(hot2.astype(BF), before)
    fill1 = jnp.sum(hot1, axis=1, keepdims=True)
    pos1 = jnp.sum(cum1 * hot1, axis=0, keepdims=True)
    pos2 = jnp.sum((cum2 + fill1) * hot2, axis=0, keepdims=True)

    def place(ids, pos):
        spot = (ids & (n_loc - 1)) * blk + (ids // n_loc) * cap
        return jnp.where(pos < cap, spot.astype(F32) + pos, float(n_exp * cap))

    s1r[...] = place(ids1, pos1)
    s2r[...] = place(ids2, pos2)

    def masks(j):
        spot = (lax.broadcasted_iota(I32, (blk, n_tok), 0) + j * blk).astype(F32)
        return s1r[...] == spot, s2r[...] == spot

    chip = r // 2
    chip_x = chip + 1 - 2 * (chip % 2)
    chip_y = (chip + 2) % 4
    chip_d = 3 - chip
    core = r % 2
    diag = 2 * chip_d + (k + r) % 2
    near = [2 * chip_x + core, 2 * chip_y + core, 2 * chip_x + 1 - core, 2 * chip_y + 1 - core, 2 * chip + 1 - core]
    far = [2 * chip_d + core, 2 * chip_d + 1 - core]

    def place_of(q):
        return (q % tp_size) * half + q // tp_size

    def send_row(src, dst, send_sem, recv_sem, j, q):
        pltpu.make_async_remote_copy(
            src_ref=src.at[j, q], dst_ref=dst.at[j, my_place],
            send_sem=send_sem, recv_sem=recv_sem.at[j],
            device_id=(k, q), device_id_type=MESH,
        ).start()

    def wait_recv(view, sem):
        pltpu.make_async_remote_copy(
            src_ref=view, dst_ref=view, send_sem=sem, recv_sem=sem, device_id=(k, r), device_id_type=MESH
        ).wait_recv()

    def wait_send(view, sem):
        pltpu.make_async_remote_copy(
            src_ref=view, dst_ref=view, send_sem=sem, recv_sem=sem, device_id=(k, r), device_id_type=MESH
        ).wait_send()

    def build_x(j, via_tp):
        m1, m2 = masks(j)
        pick = jnp.where(m1 | m2, 1.0, 0.0).astype(BF)
        for c in range(0, width, 512):
            rows = dot(pick, x_v[:, c:c + 512]).astype(BF)
            xs[j, :, :, c:c + 512] = rows.reshape(ep_size, cap, 512)
        if via_tp:
            send_row(xs, xr, xs_sem, xd_sem, j, diag)
        for q in near if via_tp else far + near:
            send_row(xs, xr, xs_sem, xr_sem, j, q)
        xr[j, my_place] = xs[j, r]

    ins[0].wait()
    ins[2].start()
    ins[1].start()

    @pl.loop(0, n_loc)
    def _(j):
        for c in weight_copies(j):
            c.start()

    pl.semaphore_wait(barrier, n_dev - 1)

    @pl.loop(0, VIA_TP)
    def _(j):
        build_x(j, True)

    @pl.loop(VIA_TP, n_loc)
    def _(j):
        build_x(j, False)

    def column(row):
        return jnp.transpose(jnp.broadcast_to(row, (128, n_tok)))

    s1c[...] = column(s1r[...])
    s2c[...] = column(s2r[...])
    i1c[...] = column(ids1.astype(F32))
    i2c[...] = column(ids2.astype(F32))
    ins[2].wait()
    wr_hi, wr_mid, wr_low = split3(wr_v[...])
    xv = x_v[...]
    logits = dot(xv, wr_hi, NT) + (dot(xv, wr_mid, NT) + dot(xv, wr_low, NT))
    ex = jnp.exp(logits - jnp.max(logits, axis=1, keepdims=True))
    prob = ex / jnp.sum(ex, axis=1, keepdims=True)
    prob_v[...] = prob
    lane = lax.broadcasted_iota(I32, (n_tok, n_exp), 1).astype(F32)
    q1 = jnp.sum(jnp.where(i1c[:, :n_exp] == lane, prob, 0.0), axis=1, keepdims=True)
    q2 = jnp.sum(jnp.where(i2c[:, :n_exp] == lane, prob, 0.0), axis=1, keepdims=True)
    g1 = jnp.broadcast_to(q1 / (q1 + q2), (n_tok, 128))
    g2 = jnp.broadcast_to(q2 / (q1 + q2), (n_tok, 128))
    g1c[...] = g1
    g2c[...] = g2
    q1c[...] = jnp.broadcast_to(q1, (n_tok, 128))
    q2c[...] = jnp.broadcast_to(q2, (n_tok, 128))
    g1r[...] = jnp.transpose(g1)[0:1, :]
    g2r[...] = jnp.transpose(g2)[0:1, :]
    ins[1].wait()

    def build_d(j):
        m1, m2 = masks(j)
        pick = jnp.where(m1 | m2, 1.0, 0.0).astype(BF)
        gate = jnp.sum(jnp.where(m1, g1r[...], 0.0) + jnp.where(m2, g2r[...], 0.0), axis=1, keepdims=True)
        for c in range(0, width, 512):
            rows = (gate * dot(pick, dy_v[:, c:c + 512])).astype(BF)
            ds[j, :, :, c:c + 512] = rows.reshape(ep_size, cap, 512)
        for q in far + near:
            send_row(ds, dr, ds_sem, dr_sem, j, q)
        dr[j, my_place] = ds[j, r]

    def send_half(src, dst, send_sem, recv_sem, j):
        pltpu.make_async_remote_copy(
            src_ref=src.at[j, pl.ds(other * half, half)], dst_ref=dst.at[j],
            send_sem=send_sem, recv_sem=recv_sem.at[j],
            device_id=(other, r), device_id_type=MESH,
        ).start()

    def merge_and_return(src, got, got_sem, dst, send_sem, recv_sem, j):
        wait_recv(got.at[j], got_sem.at[j])
        mine = pl.ds(k * half, half)
        src[j, mine] = (src[j, mine].astype(F32) + got[j].astype(F32)).astype(BF)
        for d in range(half):
            c = (r // tp_size + d) % half
            q = tp_size * c + k

            @pl.when(q != r)
            def _():
                pltpu.make_async_remote_copy(
                    src_ref=src.at[j, k * half + c], dst_ref=dst.at[j, r],
                    send_sem=send_sem, recv_sem=recv_sem.at[j],
                    device_id=(k, q), device_id_type=MESH,
                ).start()

            @pl.when(q == r)
            def _():
                dst[j, r] = src[j, k * half + c]

    n_near = len(near)
    diag_place = place_of(diag)

    def forward_diag(j):
        wait_recv(xr.at[j, 0], xd_sem.at[j])
        pltpu.make_async_remote_copy(
            src_ref=xr.at[j, diag_place], dst_ref=xr.at[j, diag_place],
            send_sem=xfs_sem, recv_sem=xf_sem.at[j],
            device_id=(other, r), device_id_type=MESH,
        ).start()

    for i in range(FORWARD):
        forward_diag(i)

    @pl.loop(0, n_loc)
    def _(j):
        @pl.when(j >= n_loc - AHEAD)
        def _():
            build_d(j + AHEAD - n_loc)

        @pl.when(j + FORWARD < VIA_TP)
        def _():
            forward_diag(j + FORWARD)

        for c in weight_copies(j):
            c.wait()

        @pl.when(j < VIA_TP)
        def _():
            wait_recv(xr.at[j, pl.ds(0, n_near)], xr_sem.at[j])
            wait_recv(xr.at[j, 0], xf_sem.at[j])

        @pl.when(j >= VIA_TP)
        def _():
            wait_recv(xr.at[j, pl.ds(0, ep_size - 1)], xr_sem.at[j])

        rows = xr[j].reshape(blk, width)
        pa = dot(rows, wa_v[j])
        pb = dot(rows, wb_v[j])
        th = jnp.tanh(GELU_COEF * (pa + 0.044715 * pa * pa * pa))
        gv = 0.5 * pa * (1.0 + th)
        slope = 0.5 * (1.0 + th) + 0.5 * pa * (1.0 - th * th) * GELU_COEF * (1.0 + 0.134145 * pa * pa)
        gv_v[j] = gv
        bs_v[j] = pb * slope
        hidden = (gv * pb).astype(BF)
        h_v[j] = hidden
        for c in range(0, width, 512):
            ps[j, :, :, c:c + 512] = dot(hidden, wc_v[j, :, c:c + 512]).astype(BF).reshape(ep_size, cap, 512)
        send_half(ps, pr, ps_sem, pr_sem, j)

        @pl.when(j >= LAG)
        def _():
            merge_and_return(ps, pr, pr_sem, orr, os_sem, or_sem, j - LAG)

    tb = 128
    n_tb = n_tok // tb

    def spots(col, toks):
        lanes = lax.broadcasted_iota(I32, (tb, 128), 1).astype(F32)
        base = col[toks, :]
        return jnp.concatenate([base == lanes + float(u * 128) for u in range(n_exp * cap // 128)], axis=1)

    def ship(buf, t, send_sem, recv_sem):
        toks = pl.ds(pl.multiple_of(t * tb, tb), tb)
        pltpu.make_async_remote_copy(
            src_ref=buf.at[toks], dst_ref=buf.at[toks], send_sem=send_sem, recv_sem=recv_sem.at[t],
            device_id=(other, r), device_id_type=MESH,
        ).start()

    def combine_y(t):
        toks = pl.ds(pl.multiple_of(t * tb, tb), tb)
        pick1 = jnp.where(spots(s1c, toks), 1.0, 0.0).astype(BF)
        pick2 = jnp.where(spots(s2c, toks), 1.0, 0.0).astype(BF)
        dg1 = jnp.zeros((tb, 1), F32)
        dg2 = jnp.zeros((tb, 1), F32)
        ga = g1c[toks, 0:1]
        gb = g2c[toks, 0:1]
        for c in range(0, width, 512):
            rows = orr[:, :, :, c:c + 512].reshape(n_exp * cap, 512)
            o1 = dot(pick1, rows)
            o2 = dot(pick2, rows)
            y_v[toks, c:c + 512] = (ga * o1 + gb * o2).astype(BF)
            dyf = dy_v[toks, c:c + 512].astype(F32)
            dg1 = dg1 + jnp.sum(dyf * o1, axis=1, keepdims=True)
            dg2 = dg2 + jnp.sum(dyf * o2, axis=1, keepdims=True)
        qa = q1c[toks, 0:1]
        qb = q2c[toks, 0:1]
        shared = dg1 * ga + dg2 * gb
        dq1 = (dg1 - shared) / (qa + qb)
        dq2 = (dg2 - shared) / (qa + qb)
        centre = dq1 * qa + dq2 * qb
        lanes = lax.broadcasted_iota(I32, (tb, n_exp), 1).astype(F32)
        pull = jnp.where(i1c[toks, :n_exp] == lanes, dq1, 0.0) + jnp.where(i2c[toks, :n_exp] == lanes, dq2, 0.0)
        dl_v[toks, :] = prob_v[toks, :] * (pull - centre)

    def router_parts():
        d_hi, d_mid, d_low = split3(dl_v[...])
        for c in range(0, width, 512):
            xc = x_v[:, c:c + 512]
            piece = dot(d_hi, xc, TN) + (dot(d_mid, xc, TN) + dot(d_low, xc, TN))
            dwp[:, :, c:c + 512] = piece.reshape(ep_size, n_loc, 512)
        for d in range(1, ep_size):
            q = (r + d) % ep_size
            pltpu.make_async_remote_copy(
                src_ref=dwp.at[q], dst_ref=dwi.at[r], send_sem=rs_sem, recv_sem=rr_sem,
                device_id=(q % tp_size, q), device_id_type=MESH,
            ).start()
        dwi[r] = dwp[r]

    def router_sum():
        wait_recv(dwi.at[pl.ds(0, ep_size - 1)], rr_sem)
        total = dwi[0]
        for q in range(1, ep_size):
            total = total + dwi[q]
        dwf[r] = total
        for d in range(1, ep_size):
            q = (r + d) % ep_size
            pltpu.make_async_remote_copy(
                src_ref=dwf.at[r], dst_ref=dwf.at[r], send_sem=fs_sem, recv_sem=fr_sem,
                device_id=(q % tp_size, q), device_id_type=MESH,
            ).start()

    wait_send(xs.at[pl.ds(0, VIA_TP), pl.ds(0, n_near + 1)], xs_sem)
    wait_send(xs.at[pl.ds(VIA_TP, n_loc - VIA_TP), pl.ds(0, ep_size - 1)], xs_sem)
    @pl.loop(0, n_loc)
    def _(j):
        @pl.when(j + AHEAD < n_loc)
        def _():
            build_d(j + AHEAD)

        wait_recv(dr.at[j, pl.ds(0, ep_size - 1)], dr_sem.at[j])
        rows = dr[j].reshape(blk, width)
        dh = dot(rows, wc_v[j], NT)
        da = (dh * bs_v[j]).astype(BF)
        db = (dh * gv_v[j]).astype(BF)
        da_v[j] = da
        db_v[j] = db
        for c in range(0, width, 512):
            part = dot(da, wa_v[j, c:c + 512, :], NT) + dot(db, wb_v[j, c:c + 512, :], NT)
            xs[j, :, :, c:c + 512] = part.astype(BF).reshape(ep_size, cap, 512)
        send_half(xs, pdr, pds_sem, pdr_sem, j)

        @pl.when(j == 0)
        def _():
            for i in range(LAG):
                merge_and_return(ps, pr, pr_sem, orr, os_sem, or_sem, n_loc - LAG + i)

        @pl.when(j >= LAG)
        def _():
            merge_and_return(xs, pdr, pdr_sem, dxr, dxs_sem, dxr_sem, j - LAG)

        @pl.when(owner & (j == Y_STEP))
        def _():
            @pl.loop(0, n_loc)
            def _(i):
                wait_recv(orr.at[i, pl.ds(0, ep_size - 1)], or_sem.at[i])

        @pl.when(owner & (j >= Y_STEP) & (j < Y_STEP + n_tb // 2))
        def _():
            t0 = 2 * (j - Y_STEP)

            @pl.loop(t0, t0 + 2)
            def _(t):
                combine_y(t)

            ship(y_v, j - Y_STEP, ys_sem, yr_sem)

        @pl.when(owner & (j == Y_STEP + n_tb // 2 - 1))
        def _():
            router_parts()

    outs = [
        pltpu.make_async_copy(xr, xe_out, out_sem.at[0]),
        pltpu.make_async_copy(dr, de_out, out_sem.at[1]),
        pltpu.make_async_copy(h_v, h_out, out_sem.at[2]),
        pltpu.make_async_copy(da_v, da_out, out_sem.at[3]),
        pltpu.make_async_copy(db_v, db_out, out_sem.at[4]),
    ]
    for c in outs[:3]:
        c.start()

    split = n_loc - 2

    def pick_both(t):
        toks = pl.ds(pl.multiple_of(t * tb, tb), tb)
        return toks, jnp.where(spots(s1c, toks) | spots(s2c, toks), 1.0, 0.0).astype(BF)

    def sum_first(t):
        toks, pick = pick_both(t)
        dl = dl_v[toks, :]
        for c in range(0, width, 512):
            rows = dxr[0:split, :, :, c:c + 512].reshape(split * blk, 512)
            router = lax.dot_general(
                dl, wr_v[:, c:c + 512], NN, precision=lax.Precision.HIGHEST, preferred_element_type=F32
            )
            acc_v[toks, c:c + 512] = dot(pick[:, :split * blk], rows) + router

    def sum_last(t):
        toks, pick = pick_both(t)
        for c in range(0, width, 512):
            rows = dxr[split:n_loc, :, :, c:c + 512].reshape((n_loc - split) * blk, 512)
            dx_v[toks, c:c + 512] = (acc_v[toks, c:c + 512] + dot(pick[:, split * blk:], rows)).astype(BF)
        pltpu.make_async_copy(dx_v.at[toks], dx_out.at[toks], in_sem.at[1]).start()

    for c in outs[3:]:
        c.start()

    @pl.when(owner)
    def _():
        ship(y_v, n_tb - 2, ys_sem, yr_sem)

    for i in range(LAG - 1):
        merge_and_return(xs, pdr, pdr_sem, dxr, dxs_sem, dxr_sem, n_loc - LAG + i)

    @pl.when(owner)
    def _():
        router_sum()
        ship(y_v, n_tb - 1, ys_sem, yr_sem)
        pltpu.make_async_copy(y_v, y_out, in_sem.at[0]).start()

    merge_and_return(xs, pdr, pdr_sem, dxr, dxs_sem, dxr_sem, n_loc - 1)

    @pl.when(owner)
    def _():
        @pl.loop(0, split)
        def _(j):
            wait_recv(dxr.at[j, pl.ds(0, ep_size - 1)], dxr_sem.at[j])

        @pl.loop(0, n_tb)
        def _(t):
            sum_first(t)

        wait_recv(dwf.at[pl.ds(0, ep_size - 1)], fr_sem)
        pltpu.make_async_remote_copy(
            src_ref=dwf, dst_ref=dwf, send_sem=gs_sem, recv_sem=gr_sem,
            device_id=(k, 2 * chip + 1 - core), device_id_type=MESH,
        ).start()

        @pl.loop(split, n_loc)
        def _(j):
            wait_recv(dxr.at[j, pl.ds(0, ep_size - 1)], dxr_sem.at[j])

        @pl.loop(0, n_tb)
        def _(t):
            sum_last(t)

        wait_send(dwp.at[pl.ds(0, ep_size - 1)], rs_sem)
        wait_send(dwf.at[pl.ds(0, ep_size - 1)], fs_sem)
        wait_send(dwf, gs_sem)
        wait_send(y_v, ys_sem)
        wait_send(orr.at[:, pl.ds(0, half - 1)], os_sem)
        wait_send(dxr.at[:, pl.ds(0, half - 1)], dxs_sem)

    @pl.when(jnp.logical_not(owner))
    def _():
        dx_v[...] = jnp.zeros_like(dx_v)
        pltpu.make_async_copy(dx_v, dx_out, in_sem.at[1]).start()
        for t in range(n_tb):
            toks = pl.ds(t * tb, tb)
            wait_recv(y_v.at[toks], yr_sem.at[t])
            pltpu.make_async_copy(y_v.at[toks], y_out.at[toks], in_sem.at[0]).start()
        wait_recv(dwf, gr_sem)
        wait_send(orr.at[:, pl.ds(0, half)], os_sem)
        wait_send(dxr.at[:, pl.ds(0, half)], dxs_sem)

    finals = [
        pltpu.make_async_copy(dwf, dwr_out, in_sem.at[2]),
        pltpu.make_async_copy(y_v, y_out, in_sem.at[0]),
        pltpu.make_async_copy(dx_v, dx_out, in_sem.at[1]),
    ]
    finals[0].start()
    wait_send(ds.at[:, pl.ds(0, ep_size - 1)], ds_sem)
    wait_send(xr.at[pl.ds(0, VIA_TP), 0], xfs_sem)
    wait_send(ps.at[:, pl.ds(0, half)], ps_sem)
    wait_send(xs.at[:, pl.ds(0, half)], pds_sem)
    for c in outs + finals:
        c.wait()


def weight_kernel(xe, de, h, da, db, y, dwr, ga_out, gb_out, gc_out, y_out, dwr_out):
    y_out[...] = y[...]
    dwr_out[...] = dwr[...]
    rows = xe[0]
    ga_out[0] = dot(rows, da[0], TN)
    gb_out[0] = dot(rows, db[0], TN)
    gc_out[0] = dot(h[0], de[0], TN)


def solution(mesh):
    tp_size = mesh.shape["tp"]
    ep_size = mesh.shape["ep"]

    def local_step(x_rows, w_router, first_ids, second_ids, w_gelu, w_lin, w_out, dy_rows):
        n_tok, width = x_rows.shape
        n_exp = w_router.shape[1]
        n_loc, _, hid = w_gelu.shape
        cap = 2 * n_tok // n_exp
        blk = ep_size * cap
        half = ep_size // tp_size
        dma = pltpu.SemaphoreType.DMA
        any_spec = pl.BlockSpec(memory_space=pl.ANY)
        sds = jax.ShapeDtypeStruct
        rows_shape = (n_loc, ep_size, cap, width)
        half_shape = (n_loc, half, cap, width)
        hid_shape = (n_loc, blk, hid)
        col = pltpu.VMEM((n_tok, 128), F32)
        row = pltpu.VMEM((1, n_tok), F32)
        outs = pl.pallas_call(
            functools.partial(moe_kernel, tp_size, ep_size, cap),
            name="moe",
            in_specs=[any_spec] * 8,
            out_specs=[any_spec] * 8,
            out_shape=[
                sds((n_tok, width), BF), sds((n_tok, width), BF), sds((ep_size, n_loc, width), F32),
                sds(rows_shape, BF), sds(rows_shape, BF), sds(hid_shape, BF), sds(hid_shape, BF), sds(hid_shape, BF),
            ],
            scratch_shapes=[
                pltpu.VMEM((n_tok, width), BF), pltpu.VMEM((n_tok, width), BF), pltpu.VMEM((n_exp, width), F32),
                pltpu.VMEM((n_loc, width, hid), BF), pltpu.VMEM((n_loc, width, hid), BF), pltpu.VMEM((n_loc, hid, width), BF),
                pltpu.VMEM(rows_shape, BF), pltpu.VMEM(rows_shape, BF), pltpu.VMEM(rows_shape, BF), pltpu.VMEM(rows_shape, BF),
                pltpu.VMEM(hid_shape, BF), pltpu.VMEM(hid_shape, BF), pltpu.VMEM(hid_shape, BF),
                pltpu.VMEM(hid_shape, F32), pltpu.VMEM(hid_shape, F32),
                pltpu.VMEM(rows_shape, BF), pltpu.VMEM(half_shape, BF), pltpu.VMEM(half_shape, BF),
                pltpu.VMEM(rows_shape, BF), pltpu.VMEM(rows_shape, BF),
                pltpu.VMEM((n_tok, width), BF), pltpu.VMEM((n_tok, width), BF),
                row, row, row, row, col, col, col, col, col, col, col, col,
                pltpu.VMEM((n_tok, n_exp), F32), pltpu.VMEM((n_tok, n_exp), F32),
                pltpu.VMEM((ep_size, n_loc, width), F32), pltpu.VMEM((ep_size, n_loc, width), F32),
                pltpu.VMEM((ep_size, n_loc, width), F32), pltpu.VMEM((n_tok, width), F32),
                pltpu.VMEM((1, n_tok), I32), pltpu.VMEM((1, n_tok), I32),
                dma((3,)), dma((3, n_loc)), dma((5,)), dma((2,)),
                dma(()), dma((n_loc,)), dma((n_loc,)), dma((n_loc,)), dma(()), dma(()), dma((n_loc,)),
                dma(()), dma((n_loc,)), dma(()), dma((n_loc,)),
                dma(()), dma((n_loc,)), dma(()), dma((n_loc,)),
                dma(()), dma((n_tok // 128,)),
                dma(()), dma(()), dma(()), dma(()), dma(()), dma(()),
            ],
            compiler_params=pltpu.CompilerParams(
                collective_id=0, has_side_effects=True, vmem_limit_bytes=67043328
            ),
        )(
            first_ids.reshape(1, n_tok), second_ids.reshape(1, n_tok), x_rows, dy_rows, w_router.T,
            w_gelu, w_lin, w_out,
        )
        act_out, grad_in, grad_router, xe, de, h, da, db = outs
        partners = [
            ((q % tp_size) * ep_size + q, (1 - q % tp_size) * ep_size + q) for q in range(ep_size)
        ]
        passed = lax.ppermute(grad_in, ("tp", "ep"), partners)
        owner = lax.axis_index("ep") % tp_size == lax.axis_index("tp")
        grad_in = jnp.where(owner, grad_in, passed)
        xe = xe.reshape(n_loc, blk, width)
        de = de.reshape(n_loc, blk, width)

        y_spec = pl.BlockSpec((n_tok // n_loc, width), lambda e: (e, 0))

        def spec(*shape):
            return pl.BlockSpec((1,) + shape, lambda e: (e, 0, 0))

        grad_wa, grad_wb, grad_wc, act_out, grad_router = pl.pallas_call(
            weight_kernel,
            name="weight_grads",
            grid=(n_loc,),
            in_specs=[spec(blk, width), spec(blk, width), spec(blk, hid), spec(blk, hid), spec(blk, hid), y_spec, spec(n_exp // n_loc, width)],
            out_specs=[spec(width, hid), spec(width, hid), spec(hid, width), y_spec, spec(n_exp // n_loc, width)],
            out_shape=[
                sds((n_loc, width, hid), F32), sds((n_loc, width, hid), F32), sds((n_loc, hid, width), F32),
                sds((n_tok, width), BF), sds((n_loc, n_exp // n_loc, width), F32),
            ],
            compiler_params=pltpu.CompilerParams(
                dimension_semantics=("arbitrary",), vmem_limit_bytes=67043328
            ),
            cost_estimate=pl.CostEstimate(
                flops=6 * n_loc * blk * width * hid, transcendentals=0,
                bytes_accessed=12 * n_loc * width * hid + 4 * n_loc * blk * width + 6 * n_loc * blk * hid,
            ),
        )(xe, de, h, da, db, act_out, grad_router.reshape(n_loc, n_exp // n_loc, width))
        return act_out, grad_in, grad_wa, grad_wb, grad_wc, grad_router.reshape(n_exp, width).T

    return jax.shard_map(
        local_step,
        mesh=mesh,
        in_specs=(P("ep", None), P(), P("ep"), P("ep"), P("ep", None, "tp"), P("ep", None, "tp"), P("ep", "tp", None), P("ep", None)),
        out_specs=(P("ep", None), P("ep", None), P("ep", None, "tp"), P("ep", None, "tp"), P("ep", "tp", None), P()),
        check_vma=False,
    )
```

```python
import functools

import jax
import jax.numpy as jnp
from jax import lax
from jax.experimental import pallas as pl
from jax.experimental.pallas import tpu as pltpu
from jax.sharding import PartitionSpec as P

BF = jnp.bfloat16
F32 = jnp.float32
I32 = jnp.int32
MESH = pl.DeviceIdType.MESH
GELU_COEF = 0.7978845608028654
AHEAD = 5
LAG = 3
Y_STEP = 5
FORWARD = 2
VIA_TP = 7
NN = (((1,), (0,)), ((), ()))
NT = (((1,), (1,)), ((), ()))
TN = (((0,), (0,)), ((), ()))


def dot(a, b, dims=NN):
    return lax.dot_general(a, b, dims, preferred_element_type=F32)


def split3(v):
    hi = v.astype(BF)
    rest = v - hi.astype(F32)
    mid = rest.astype(BF)
    low = (rest - mid.astype(F32)).astype(BF)
    return hi, mid, low


def moe_kernel(
    tp_size, ep_size, cap,
    ids1_hbm, ids2_hbm, x_hbm, dy_hbm, wr_hbm, wa_hbm, wb_hbm, wc_hbm,
    y_out, dx_out, dwr_out, xe_out, de_out, h_out, da_out, db_out,
    x_v, dy_v, wr_v, wa_v, wb_v, wc_v,
    xs, ds, xr, dr, h_v, da_v, db_v, bs_v, gv_v,
    ps, pr, pdr, orr, dxr, y_v, dx_v,
    s1r, s2r, g1r, g2r, s1c, s2c, g1c, g2c, q1c, q2c, i1c, i2c, prob_v, dl_v,
    dwp, dwi, dwf, acc_v, ids1_ref, ids2_ref,
    in_sem, w_sem, out_sem, id_sem,
    xs_sem, xr_sem, xd_sem, xf_sem, xfs_sem, ds_sem, dr_sem,
    ps_sem, pr_sem, pds_sem, pdr_sem,
    os_sem, or_sem, dxs_sem, dxr_sem,
    ys_sem, yr_sem,
    rs_sem, rr_sem, fs_sem, fr_sem, gs_sem, gr_sem,
):
    k = lax.axis_index("tp")
    r = lax.axis_index("ep")
    n_loc = wa_v.shape[0]
    n_tok, width = x_v.shape
    hid = wa_v.shape[2]
    n_exp = n_loc * ep_size
    blk = ep_size * cap
    half = ep_size // tp_size
    my_place = (r % tp_size) * half + r // tp_size
    owner = (r % tp_size) == k
    other = 1 - k

    ins = [
        pltpu.make_async_copy(x_hbm, x_v, in_sem.at[0]),
        pltpu.make_async_copy(dy_hbm, dy_v, in_sem.at[1]),
        pltpu.make_async_copy(wr_hbm, wr_v, in_sem.at[2]),
    ]
    id_loads = [pltpu.make_async_copy(ids1_hbm, ids1_ref, id_sem.at[0]), pltpu.make_async_copy(ids2_hbm, ids2_ref, id_sem.at[1])]
    for c in id_loads:
        c.start()
    ins[0].start()

    def weight_copies(j):
        return [
            pltpu.make_async_copy(wa_hbm.at[j], wa_v.at[j], w_sem.at[0, j]),
            pltpu.make_async_copy(wb_hbm.at[j], wb_v.at[j], w_sem.at[1, j]),
            pltpu.make_async_copy(wc_hbm.at[j], wc_v.at[j], w_sem.at[2, j]),
        ]

    n_dev = tp_size * ep_size
    barrier = pltpu.get_barrier_semaphore()
    for d in range(1, n_dev):
        flat = (k * ep_size + r + d) % n_dev
        pl.semaphore_signal(barrier, inc=1, device_id=(flat // ep_size, flat % ep_size), device_id_type=MESH)

    for c in id_loads:
        c.wait()
    ids1 = ids1_ref[...]
    ids2 = ids2_ref[...]
    e_iota = lax.broadcasted_iota(I32, (n_exp, n_tok), 0)
    hot1 = jnp.where(ids1 == e_iota, 1.0, 0.0).astype(F32)
    hot2 = jnp.where(ids2 == e_iota, 1.0, 0.0).astype(F32)
    before = jnp.where(
        lax.broadcasted_iota(I32, (n_tok, n_tok), 0) < lax.broadcasted_iota(I32, (n_tok, n_tok), 1), 1.0, 0.0
    ).astype(BF)
    cum1 = dot(hot1.astype(BF), before)
    cum2 = dot(hot2.astype(BF), before)
    fill1 = jnp.sum(hot1, axis=1, keepdims=True)
    pos1 = jnp.sum(cum1 * hot1, axis=0, keepdims=True)
    pos2 = jnp.sum((cum2 + fill1) * hot2, axis=0, keepdims=True)

    def place(ids, pos):
        spot = (ids & (n_loc - 1)) * blk + (ids // n_loc) * cap
        return jnp.where(pos < cap, spot.astype(F32) + pos, float(n_exp * cap))

    s1r[...] = place(ids1, pos1)
    s2r[...] = place(ids2, pos2)

    def masks(j):
        spot = (lax.broadcasted_iota(I32, (blk, n_tok), 0) + j * blk).astype(F32)
        return s1r[...] == spot, s2r[...] == spot

    chip = r // 2
    chip_x = chip + 1 - 2 * (chip % 2)
    chip_y = (chip + 2) % 4
    chip_d = 3 - chip
    core = r % 2
    diag = 2 * chip_d + (k + r) % 2
    near = [2 * chip_x + core, 2 * chip_y + core, 2 * chip_x + 1 - core, 2 * chip_y + 1 - core, 2 * chip + 1 - core]
    far = [2 * chip_d + core, 2 * chip_d + 1 - core]

    def place_of(q):
        return (q % tp_size) * half + q // tp_size

    def send_row(src, dst, send_sem, recv_sem, j, q):
        pltpu.make_async_remote_copy(
            src_ref=src.at[j, q], dst_ref=dst.at[j, my_place],
            send_sem=send_sem, recv_sem=recv_sem.at[j],
            device_id=(k, q), device_id_type=MESH,
        ).start()

    def wait_recv(view, sem):
        pltpu.make_async_remote_copy(
            src_ref=view, dst_ref=view, send_sem=sem, recv_sem=sem, device_id=(k, r), device_id_type=MESH
        ).wait_recv()

    def wait_send(view, sem):
        pltpu.make_async_remote_copy(
            src_ref=view, dst_ref=view, send_sem=sem, recv_sem=sem, device_id=(k, r), device_id_type=MESH
        ).wait_send()

    def build_x(j, via_tp):
        m1, m2 = masks(j)
        pick = jnp.where(m1 | m2, 1.0, 0.0).astype(BF)
        for c in range(0, width, 512):
            rows = dot(pick, x_v[:, c:c + 512]).astype(BF)
            xs[j, :, :, c:c + 512] = rows.reshape(ep_size, cap, 512)
        if via_tp:
            send_row(xs, xr, xs_sem, xd_sem, j, diag)
        for q in near if via_tp else far + near:
            send_row(xs, xr, xs_sem, xr_sem, j, q)
        xr[j, my_place] = xs[j, r]

    ins[0].wait()
    ins[2].start()
    ins[1].start()

    @pl.loop(0, n_loc)
    def _(j):
        for c in weight_copies(j):
            c.start()

    pl.semaphore_wait(barrier, n_dev - 1)

    @pl.loop(0, VIA_TP)
    def _(j):
        build_x(j, True)

    @pl.loop(VIA_TP, n_loc)
    def _(j):
        build_x(j, False)

    def column(row):
        return jnp.transpose(jnp.broadcast_to(row, (128, n_tok)))

    s1c[...] = column(s1r[...])
    s2c[...] = column(s2r[...])
    i1c[...] = column(ids1.astype(F32))
    i2c[...] = column(ids2.astype(F32))
    ins[2].wait()
    wr_hi, wr_mid, wr_low = split3(wr_v[...])
    xv = x_v[...]
    logits = dot(xv, wr_hi, NT) + (dot(xv, wr_mid, NT) + dot(xv, wr_low, NT))
    ex = jnp.exp(logits - jnp.max(logits, axis=1, keepdims=True))
    prob = ex / jnp.sum(ex, axis=1, keepdims=True)
    prob_v[...] = prob
    lane = lax.broadcasted_iota(I32, (n_tok, n_exp), 1).astype(F32)
    q1 = jnp.sum(jnp.where(i1c[:, :n_exp] == lane, prob, 0.0), axis=1, keepdims=True)
    q2 = jnp.sum(jnp.where(i2c[:, :n_exp] == lane, prob, 0.0), axis=1, keepdims=True)
    g1 = jnp.broadcast_to(q1 / (q1 + q2), (n_tok, 128))
    g2 = jnp.broadcast_to(q2 / (q1 + q2), (n_tok, 128))
    g1c[...] = g1
    g2c[...] = g2
    q1c[...] = jnp.broadcast_to(q1, (n_tok, 128))
    q2c[...] = jnp.broadcast_to(q2, (n_tok, 128))
    g1r[...] = jnp.transpose(g1)[0:1, :]
    g2r[...] = jnp.transpose(g2)[0:1, :]
    ins[1].wait()

    def build_d(j):
        m1, m2 = masks(j)
        pick = jnp.where(m1 | m2, 1.0, 0.0).astype(BF)
        gate = jnp.sum(jnp.where(m1, g1r[...], 0.0) + jnp.where(m2, g2r[...], 0.0), axis=1, keepdims=True)
        for c in range(0, width, 512):
            rows = (gate * dot(pick, dy_v[:, c:c + 512])).astype(BF)
            ds[j, :, :, c:c + 512] = rows.reshape(ep_size, cap, 512)
        for q in far + near:
            send_row(ds, dr, ds_sem, dr_sem, j, q)
        dr[j, my_place] = ds[j, r]

    def send_half(src, dst, send_sem, recv_sem, j):
        pltpu.make_async_remote_copy(
            src_ref=src.at[j, pl.ds(other * half, half)], dst_ref=dst.at[j],
            send_sem=send_sem, recv_sem=recv_sem.at[j],
            device_id=(other, r), device_id_type=MESH,
        ).start()

    def merge_and_return(src, got, got_sem, dst, send_sem, recv_sem, j):
        wait_recv(got.at[j], got_sem.at[j])
        mine = pl.ds(k * half, half)
        src[j, mine] = (src[j, mine].astype(F32) + got[j].astype(F32)).astype(BF)
        for d in range(half):
            c = (r // tp_size + d) % half
            q = tp_size * c + k

            @pl.when(q != r)
            def _():
                pltpu.make_async_remote_copy(
                    src_ref=src.at[j, k * half + c], dst_ref=dst.at[j, r],
                    send_sem=send_sem, recv_sem=recv_sem.at[j],
                    device_id=(k, q), device_id_type=MESH,
                ).start()

            @pl.when(q == r)
            def _():
                dst[j, r] = src[j, k * half + c]

    n_near = len(near)
    diag_place = place_of(diag)

    def forward_diag(j):
        wait_recv(xr.at[j, 0], xd_sem.at[j])
        pltpu.make_async_remote_copy(
            src_ref=xr.at[j, diag_place], dst_ref=xr.at[j, diag_place],
            send_sem=xfs_sem, recv_sem=xf_sem.at[j],
            device_id=(other, r), device_id_type=MESH,
        ).start()

    for i in range(FORWARD):
        forward_diag(i)

    @pl.loop(0, n_loc)
    def _(j):
        @pl.when(j >= n_loc - AHEAD)
        def _():
            build_d(j + AHEAD - n_loc)

        @pl.when(j + FORWARD < VIA_TP)
        def _():
            forward_diag(j + FORWARD)

        for c in weight_copies(j):
            c.wait()

        @pl.when(j < VIA_TP)
        def _():
            wait_recv(xr.at[j, pl.ds(0, n_near)], xr_sem.at[j])
            wait_recv(xr.at[j, 0], xf_sem.at[j])

        @pl.when(j >= VIA_TP)
        def _():
            wait_recv(xr.at[j, pl.ds(0, ep_size - 1)], xr_sem.at[j])

        rows = xr[j].reshape(blk, width)
        pa = dot(rows, wa_v[j])
        pb = dot(rows, wb_v[j])
        th = jnp.tanh(GELU_COEF * (pa + 0.044715 * pa * pa * pa))
        gv = 0.5 * pa * (1.0 + th)
        slope = 0.5 * (1.0 + th) + 0.5 * pa * (1.0 - th * th) * GELU_COEF * (1.0 + 0.134145 * pa * pa)
        gv_v[j] = gv
        bs_v[j] = pb * slope
        hidden = (gv * pb).astype(BF)
        h_v[j] = hidden
        for c in range(0, width, 512):
            ps[j, :, :, c:c + 512] = dot(hidden, wc_v[j, :, c:c + 512]).astype(BF).reshape(ep_size, cap, 512)
        send_half(ps, pr, ps_sem, pr_sem, j)

        @pl.when(j >= LAG)
        def _():
            merge_and_return(ps, pr, pr_sem, orr, os_sem, or_sem, j - LAG)

    tb = 128
    n_tb = n_tok // tb

    def spots(col, toks):
        lanes = lax.broadcasted_iota(I32, (tb, 128), 1).astype(F32)
        base = col[toks, :]
        return jnp.concatenate([base == lanes + float(u * 128) for u in range(n_exp * cap // 128)], axis=1)

    def ship(buf, t, send_sem, recv_sem):
        toks = pl.ds(pl.multiple_of(t * tb, tb), tb)
        pltpu.make_async_remote_copy(
            src_ref=buf.at[toks], dst_ref=buf.at[toks], send_sem=send_sem, recv_sem=recv_sem.at[t],
            device_id=(other, r), device_id_type=MESH,
        ).start()

    def combine_y(t):
        toks = pl.ds(pl.multiple_of(t * tb, tb), tb)
        pick1 = jnp.where(spots(s1c, toks), 1.0, 0.0).astype(BF)
        pick2 = jnp.where(spots(s2c, toks), 1.0, 0.0).astype(BF)
        dg1 = jnp.zeros((tb, 1), F32)
        dg2 = jnp.zeros((tb, 1), F32)
        ga = g1c[toks, 0:1]
        gb = g2c[toks, 0:1]
        for c in range(0, width, 512):
            rows = orr[:, :, :, c:c + 512].reshape(n_exp * cap, 512)
            o1 = dot(pick1, rows)
            o2 = dot(pick2, rows)
            y_v[toks, c:c + 512] = (ga * o1 + gb * o2).astype(BF)
            dyf = dy_v[toks, c:c + 512].astype(F32)
            dg1 = dg1 + jnp.sum(dyf * o1, axis=1, keepdims=True)
            dg2 = dg2 + jnp.sum(dyf * o2, axis=1, keepdims=True)
        qa = q1c[toks, 0:1]
        qb = q2c[toks, 0:1]
        shared = dg1 * ga + dg2 * gb
        dq1 = (dg1 - shared) / (qa + qb)
        dq2 = (dg2 - shared) / (qa + qb)
        centre = dq1 * qa + dq2 * qb
        lanes = lax.broadcasted_iota(I32, (tb, n_exp), 1).astype(F32)
        pull = jnp.where(i1c[toks, :n_exp] == lanes, dq1, 0.0) + jnp.where(i2c[toks, :n_exp] == lanes, dq2, 0.0)
        dl_v[toks, :] = prob_v[toks, :] * (pull - centre)

    def router_parts():
        d_hi, d_mid, d_low = split3(dl_v[...])
        for c in range(0, width, 512):
            xc = x_v[:, c:c + 512]
            piece = dot(d_hi, xc, TN) + (dot(d_mid, xc, TN) + dot(d_low, xc, TN))
            dwp[:, :, c:c + 512] = piece.reshape(ep_size, n_loc, 512)
        for d in range(1, ep_size):
            q = (r + d) % ep_size
            pltpu.make_async_remote_copy(
                src_ref=dwp.at[q], dst_ref=dwi.at[r], send_sem=rs_sem, recv_sem=rr_sem,
                device_id=(q % tp_size, q), device_id_type=MESH,
            ).start()
        dwi[r] = dwp[r]

    def router_sum():
        wait_recv(dwi.at[pl.ds(0, ep_size - 1)], rr_sem)
        total = dwi[0]
        for q in range(1, ep_size):
            total = total + dwi[q]
        dwf[r] = total
        for d in range(1, ep_size):
            q = (r + d) % ep_size
            pltpu.make_async_remote_copy(
                src_ref=dwf.at[r], dst_ref=dwf.at[r], send_sem=fs_sem, recv_sem=fr_sem,
                device_id=(q % tp_size, q), device_id_type=MESH,
            ).start()

    wait_send(xs.at[pl.ds(0, VIA_TP), pl.ds(0, n_near + 1)], xs_sem)
    wait_send(xs.at[pl.ds(VIA_TP, n_loc - VIA_TP), pl.ds(0, ep_size - 1)], xs_sem)
    @pl.loop(0, n_loc)
    def _(j):
        @pl.when(j + AHEAD < n_loc)
        def _():
            build_d(j + AHEAD)

        wait_recv(dr.at[j, pl.ds(0, ep_size - 1)], dr_sem.at[j])
        rows = dr[j].reshape(blk, width)
        dh = dot(rows, wc_v[j], NT)
        da = (dh * bs_v[j]).astype(BF)
        db = (dh * gv_v[j]).astype(BF)
        da_v[j] = da
        db_v[j] = db
        for c in range(0, width, 512):
            part = dot(da, wa_v[j, c:c + 512, :], NT) + dot(db, wb_v[j, c:c + 512, :], NT)
            xs[j, :, :, c:c + 512] = part.astype(BF).reshape(ep_size, cap, 512)
        send_half(xs, pdr, pds_sem, pdr_sem, j)

        @pl.when(j == 0)
        def _():
            for i in range(LAG):
                merge_and_return(ps, pr, pr_sem, orr, os_sem, or_sem, n_loc - LAG + i)

        @pl.when(j >= LAG)
        def _():
            merge_and_return(xs, pdr, pdr_sem, dxr, dxs_sem, dxr_sem, j - LAG)

        @pl.when(owner & (j == Y_STEP))
        def _():
            @pl.loop(0, n_loc)
            def _(i):
                wait_recv(orr.at[i, pl.ds(0, ep_size - 1)], or_sem.at[i])

        @pl.when(owner & (j >= Y_STEP) & (j < Y_STEP + n_tb // 2))
        def _():
            t0 = 2 * (j - Y_STEP)

            @pl.loop(t0, t0 + 2)
            def _(t):
                combine_y(t)

            ship(y_v, j - Y_STEP, ys_sem, yr_sem)

        @pl.when(owner & (j == Y_STEP + n_tb // 2 - 1))
        def _():
            router_parts()

    outs = [
        pltpu.make_async_copy(xr, xe_out, out_sem.at[0]),
        pltpu.make_async_copy(dr, de_out, out_sem.at[1]),
        pltpu.make_async_copy(h_v, h_out, out_sem.at[2]),
        pltpu.make_async_copy(da_v, da_out, out_sem.at[3]),
        pltpu.make_async_copy(db_v, db_out, out_sem.at[4]),
    ]
    for c in outs[:3]:
        c.start()

    split = n_loc - 2

    def pick_both(t):
        toks = pl.ds(pl.multiple_of(t * tb, tb), tb)
        return toks, jnp.where(spots(s1c, toks) | spots(s2c, toks), 1.0, 0.0).astype(BF)

    def sum_first(t):
        toks, pick = pick_both(t)
        dl = dl_v[toks, :]
        for c in range(0, width, 512):
            rows = dxr[0:split, :, :, c:c + 512].reshape(split * blk, 512)
            router = lax.dot_general(
                dl, wr_v[:, c:c + 512], NN, precision=lax.Precision.HIGHEST, preferred_element_type=F32
            )
            acc_v[toks, c:c + 512] = dot(pick[:, :split * blk], rows) + router

    def sum_last(t):
        toks, pick = pick_both(t)
        for c in range(0, width, 512):
            rows = dxr[split:n_loc, :, :, c:c + 512].reshape((n_loc - split) * blk, 512)
            dx_v[toks, c:c + 512] = (acc_v[toks, c:c + 512] + dot(pick[:, split * blk:], rows)).astype(BF)
        pltpu.make_async_copy(dx_v.at[toks], dx_out.at[toks], in_sem.at[1]).start()

    for c in outs[3:]:
        c.start()

    @pl.when(owner)
    def _():
        ship(y_v, n_tb - 2, ys_sem, yr_sem)

    for i in range(LAG - 1):
        merge_and_return(xs, pdr, pdr_sem, dxr, dxs_sem, dxr_sem, n_loc - LAG + i)

    @pl.when(owner)
    def _():
        router_sum()
        ship(y_v, n_tb - 1, ys_sem, yr_sem)
        pltpu.make_async_copy(y_v, y_out, in_sem.at[0]).start()

    merge_and_return(xs, pdr, pdr_sem, dxr, dxs_sem, dxr_sem, n_loc - 1)

    @pl.when(owner)
    def _():
        @pl.loop(0, split)
        def _(j):
            wait_recv(dxr.at[j, pl.ds(0, ep_size - 1)], dxr_sem.at[j])

        @pl.loop(0, n_tb)
        def _(t):
            sum_first(t)

        wait_recv(dwf.at[pl.ds(0, ep_size - 1)], fr_sem)
        pltpu.make_async_remote_copy(
            src_ref=dwf, dst_ref=dwf, send_sem=gs_sem, recv_sem=gr_sem,
            device_id=(k, 2 * chip + 1 - core), device_id_type=MESH,
        ).start()

        @pl.loop(split, n_loc)
        def _(j):
            wait_recv(dxr.at[j, pl.ds(0, ep_size - 1)], dxr_sem.at[j])

        @pl.loop(0, n_tb)
        def _(t):
            sum_last(t)

        wait_send(dwp.at[pl.ds(0, ep_size - 1)], rs_sem)
        wait_send(dwf.at[pl.ds(0, ep_size - 1)], fs_sem)
        wait_send(dwf, gs_sem)
        wait_send(y_v, ys_sem)
        wait_send(orr.at[:, pl.ds(0, half - 1)], os_sem)
        wait_send(dxr.at[:, pl.ds(0, half - 1)], dxs_sem)

    @pl.when(jnp.logical_not(owner))
    def _():
        dx_v[...] = jnp.zeros_like(dx_v)
        pltpu.make_async_copy(dx_v, dx_out, in_sem.at[1]).start()
        for t in range(n_tb):
            toks = pl.ds(t * tb, tb)
            wait_recv(y_v.at[toks], yr_sem.at[t])
            pltpu.make_async_copy(y_v.at[toks], y_out.at[toks], in_sem.at[0]).start()
        wait_recv(dwf, gr_sem)
        wait_send(orr.at[:, pl.ds(0, half)], os_sem)
        wait_send(dxr.at[:, pl.ds(0, half)], dxs_sem)

    finals = [
        pltpu.make_async_copy(dwf, dwr_out, in_sem.at[2]),
        pltpu.make_async_copy(y_v, y_out, in_sem.at[0]),
        pltpu.make_async_copy(dx_v, dx_out, in_sem.at[1]),
    ]
    finals[0].start()
    wait_send(ds.at[:, pl.ds(0, ep_size - 1)], ds_sem)
    wait_send(xr.at[pl.ds(0, VIA_TP), 0], xfs_sem)
    wait_send(ps.at[:, pl.ds(0, half)], ps_sem)
    wait_send(xs.at[:, pl.ds(0, half)], pds_sem)
    for c in outs + finals:
        c.wait()


def weight_kernel(xe, de, h, da, db, y, dwr, ga_out, gb_out, gc_out, y_out, dwr_out):
    y_out[...] = y[...]
    dwr_out[...] = dwr[...]
    rows = xe[0]
    ga_out[0] = dot(rows, da[0], TN)
    gb_out[0] = dot(rows, db[0], TN)
    gc_out[0] = dot(h[0], de[0], TN)


def solution(mesh):
    tp_size = mesh.shape["tp"]
    ep_size = mesh.shape["ep"]

    def local_step(x_rows, w_router, first_ids, second_ids, w_gelu, w_lin, w_out, dy_rows):
        n_tok, width = x_rows.shape
        n_exp = w_router.shape[1]
        n_loc, _, hid = w_gelu.shape
        cap = 2 * n_tok // n_exp
        blk = ep_size * cap
        half = ep_size // tp_size
        dma = pltpu.SemaphoreType.DMA
        any_spec = pl.BlockSpec(memory_space=pl.ANY)
        sds = jax.ShapeDtypeStruct
        rows_shape = (n_loc, ep_size, cap, width)
        half_shape = (n_loc, half, cap, width)
        hid_shape = (n_loc, blk, hid)
        col = pltpu.VMEM((n_tok, 128), F32)
        row = pltpu.VMEM((1, n_tok), F32)
        outs = pl.pallas_call(
            functools.partial(moe_kernel, tp_size, ep_size, cap),
            name="moe",
            in_specs=[any_spec] * 8,
            out_specs=[any_spec] * 8,
            out_shape=[
                sds((n_tok, width), BF), sds((n_tok, width), BF), sds((ep_size, n_loc, width), F32),
                sds(rows_shape, BF), sds(rows_shape, BF), sds(hid_shape, BF), sds(hid_shape, BF), sds(hid_shape, BF),
            ],
            scratch_shapes=[
                pltpu.VMEM((n_tok, width), BF), pltpu.VMEM((n_tok, width), BF), pltpu.VMEM((n_exp, width), F32),
                pltpu.VMEM((n_loc, width, hid), BF), pltpu.VMEM((n_loc, width, hid), BF), pltpu.VMEM((n_loc, hid, width), BF),
                pltpu.VMEM(rows_shape, BF), pltpu.VMEM(rows_shape, BF), pltpu.VMEM(rows_shape, BF), pltpu.VMEM(rows_shape, BF),
                pltpu.VMEM(hid_shape, BF), pltpu.VMEM(hid_shape, BF), pltpu.VMEM(hid_shape, BF),
                pltpu.VMEM(hid_shape, F32), pltpu.VMEM(hid_shape, F32),
                pltpu.VMEM(rows_shape, BF), pltpu.VMEM(half_shape, BF), pltpu.VMEM(half_shape, BF),
                pltpu.VMEM(rows_shape, BF), pltpu.VMEM(rows_shape, BF),
                pltpu.VMEM((n_tok, width), BF), pltpu.VMEM((n_tok, width), BF),
                row, row, row, row, col, col, col, col, col, col, col, col,
                pltpu.VMEM((n_tok, n_exp), F32), pltpu.VMEM((n_tok, n_exp), F32),
                pltpu.VMEM((ep_size, n_loc, width), F32), pltpu.VMEM((ep_size, n_loc, width), F32),
                pltpu.VMEM((ep_size, n_loc, width), F32), pltpu.VMEM((n_tok, width), F32),
                pltpu.VMEM((1, n_tok), I32), pltpu.VMEM((1, n_tok), I32),
                dma((3,)), dma((3, n_loc)), dma((5,)), dma((2,)),
                dma(()), dma((n_loc,)), dma((n_loc,)), dma((n_loc,)), dma(()), dma(()), dma((n_loc,)),
                dma(()), dma((n_loc,)), dma(()), dma((n_loc,)),
                dma(()), dma((n_loc,)), dma(()), dma((n_loc,)),
                dma(()), dma((n_tok // 128,)),
                dma(()), dma(()), dma(()), dma(()), dma(()), dma(()),
            ],
            compiler_params=pltpu.CompilerParams(
                collective_id=0, has_side_effects=True, vmem_limit_bytes=67043328
            ),
        )(
            first_ids.reshape(1, n_tok), second_ids.reshape(1, n_tok), x_rows, dy_rows, w_router.T,
            w_gelu, w_lin, w_out,
        )
        act_out, grad_in, grad_router, xe, de, h, da, db = outs
        partners = [
            ((q % tp_size) * ep_size + q, (1 - q % tp_size) * ep_size + q) for q in range(ep_size)
        ]
        passed = lax.ppermute(grad_in, ("tp", "ep"), partners)
        owner = lax.axis_index("ep") % tp_size == lax.axis_index("tp")
        grad_in = jnp.where(owner, grad_in, passed)
        xe = xe.reshape(n_loc, blk, width)
        de = de.reshape(n_loc, blk, width)

        y_spec = pl.BlockSpec((n_tok // n_loc, width), lambda e: (e, 0))

        def spec(*shape):
            return pl.BlockSpec((1,) + shape, lambda e: (e, 0, 0))

        grad_wa, grad_wb, grad_wc, act_out, grad_router = pl.pallas_call(
            weight_kernel,
            name="weight_grads",
            grid=(n_loc,),
            in_specs=[spec(blk, width), spec(blk, width), spec(blk, hid), spec(blk, hid), spec(blk, hid), y_spec, spec(n_exp // n_loc, width)],
            out_specs=[spec(width, hid), spec(width, hid), spec(hid, width), y_spec, spec(n_exp // n_loc, width)],
            out_shape=[
                sds((n_loc, width, hid), F32), sds((n_loc, width, hid), F32), sds((n_loc, hid, width), F32),
                sds((n_tok, width), BF), sds((n_loc, n_exp // n_loc, width), F32),
            ],
            compiler_params=pltpu.CompilerParams(
                dimension_semantics=("arbitrary",), vmem_limit_bytes=63743328
            ),
            cost_estimate=pl.CostEstimate(
                flops=6 * n_loc * blk * width * hid, transcendentals=0,
                bytes_accessed=12 * n_loc * width * hid + 4 * n_loc * blk * width + 6 * n_loc * blk * hid,
            ),
        )(xe, de, h, da, db, act_out, grad_router.reshape(n_loc, n_exp // n_loc, width))
        return act_out, grad_in, grad_wa, grad_wb, grad_wc, grad_router.reshape(n_exp, width).T

    return jax.shard_map(
        local_step,
        mesh=mesh,
        in_specs=(P("ep", None), P(), P("ep"), P("ep"), P("ep", None, "tp"), P("ep", None, "tp"), P("ep", "tp", None), P("ep", None)),
        out_specs=(P("ep", None), P("ep", None), P("ep", None, "tp"), P("ep", None, "tp"), P("ep", "tp", None), P()),
        check_vma=False,
    )
```

```python
import functools

import jax
import jax.numpy as jnp
from jax import lax
from jax.experimental import pallas as pl
from jax.experimental.pallas import tpu as pltpu
from jax.sharding import PartitionSpec as P

BF = jnp.bfloat16
F32 = jnp.float32
I32 = jnp.int32
MESH = pl.DeviceIdType.MESH
GELU_COEF = 0.7978845608028654
AHEAD = 4
LAG = 3
Y_STEP = 4
FORWARD = 2
VIA_TP = 8
NN = (((1,), (0,)), ((), ()))
NT = (((1,), (1,)), ((), ()))
TN = (((0,), (0,)), ((), ()))


def dot(a, b, dims=NN):
    return lax.dot_general(a, b, dims, preferred_element_type=F32)


def split3(v):
    hi = v.astype(BF)
    rest = v - hi.astype(F32)
    mid = rest.astype(BF)
    low = (rest - mid.astype(F32)).astype(BF)
    return hi, mid, low


def moe_kernel(
    tp_size, ep_size, cap,
    ids1_hbm, ids2_hbm, x_hbm, dy_hbm, wr_hbm, wa_hbm, wb_hbm, wc_hbm,
    y_out, dx_out, dwr_out, xe_out, de_out, h_out, da_out, db_out,
    x_v, dy_v, wr_v, wa_v, wb_v, wc_v,
    xs, ds, xr, dr, h_v, da_v, db_v, bs_v, gv_v,
    ps, pr, pdr, orr, dxr, y_v, dx_v,
    s1r, s2r, g1r, g2r, s1c, s2c, g1c, g2c, q1c, q2c, i1c, i2c, prob_v, dl_v,
    dwp, dwi, dwf, acc_v, ids1_ref, ids2_ref,
    in_sem, w_sem, out_sem, id_sem,
    xs_sem, xr_sem, xd_sem, xf_sem, xfs_sem, ds_sem, dr_sem,
    ps_sem, pr_sem, pds_sem, pdr_sem,
    os_sem, or_sem, dxs_sem, dxr_sem,
    ys_sem, yr_sem,
    rs_sem, rr_sem, fs_sem, fr_sem, gs_sem, gr_sem,
):
    k = lax.axis_index("tp")
    r = lax.axis_index("ep")
    n_loc = wa_v.shape[0]
    n_tok, width = x_v.shape
    hid = wa_v.shape[2]
    n_exp = n_loc * ep_size
    blk = ep_size * cap
    half = ep_size // tp_size
    my_place = (r % tp_size) * half + r // tp_size
    owner = (r % tp_size) == k
    other = 1 - k

    ins = [
        pltpu.make_async_copy(x_hbm, x_v, in_sem.at[0]),
        pltpu.make_async_copy(dy_hbm, dy_v, in_sem.at[1]),
        pltpu.make_async_copy(wr_hbm, wr_v, in_sem.at[2]),
    ]
    id_loads = [pltpu.make_async_copy(ids1_hbm, ids1_ref, id_sem.at[0]), pltpu.make_async_copy(ids2_hbm, ids2_ref, id_sem.at[1])]
    for c in id_loads:
        c.start()
    ins[0].start()

    def weight_copies(j):
        return [
            pltpu.make_async_copy(wa_hbm.at[j], wa_v.at[j], w_sem.at[0, j]),
            pltpu.make_async_copy(wb_hbm.at[j], wb_v.at[j], w_sem.at[1, j]),
            pltpu.make_async_copy(wc_hbm.at[j], wc_v.at[j], w_sem.at[2, j]),
        ]

    n_dev = tp_size * ep_size
    barrier = pltpu.get_barrier_semaphore()
    for d in range(1, n_dev):
        flat = (k * ep_size + r + d) % n_dev
        pl.semaphore_signal(barrier, inc=1, device_id=(flat // ep_size, flat % ep_size), device_id_type=MESH)

    for c in id_loads:
        c.wait()
    ids1 = ids1_ref[...]
    ids2 = ids2_ref[...]
    e_iota = lax.broadcasted_iota(I32, (n_exp, n_tok), 0)
    hot1 = jnp.where(ids1 == e_iota, 1.0, 0.0).astype(F32)
    hot2 = jnp.where(ids2 == e_iota, 1.0, 0.0).astype(F32)
    before = jnp.where(
        lax.broadcasted_iota(I32, (n_tok, n_tok), 0) < lax.broadcasted_iota(I32, (n_tok, n_tok), 1), 1.0, 0.0
    ).astype(BF)
    cum1 = dot(hot1.astype(BF), before)
    cum2 = dot(hot2.astype(BF), before)
    fill1 = jnp.sum(hot1, axis=1, keepdims=True)
    pos1 = jnp.sum(cum1 * hot1, axis=0, keepdims=True)
    pos2 = jnp.sum((cum2 + fill1) * hot2, axis=0, keepdims=True)

    def place(ids, pos):
        spot = (ids & (n_loc - 1)) * blk + (ids // n_loc) * cap
        return jnp.where(pos < cap, spot.astype(F32) + pos, float(n_exp * cap))

    s1r[...] = place(ids1, pos1)
    s2r[...] = place(ids2, pos2)

    def masks(j):
        spot = (lax.broadcasted_iota(I32, (blk, n_tok), 0) + j * blk).astype(F32)
        return s1r[...] == spot, s2r[...] == spot

    chip = r // 2
    chip_x = chip + 1 - 2 * (chip % 2)
    chip_y = (chip + 2) % 4
    chip_d = 3 - chip
    core = r % 2
    diag = 2 * chip_d + (k + r) % 2
    near = [2 * chip_x + core, 2 * chip_y + core, 2 * chip_x + 1 - core, 2 * chip_y + 1 - core, 2 * chip + 1 - core]
    far = [2 * chip_d + core, 2 * chip_d + 1 - core]

    def place_of(q):
        return (q % tp_size) * half + q // tp_size

    def send_row(src, dst, send_sem, recv_sem, j, q):
        pltpu.make_async_remote_copy(
            src_ref=src.at[j, q], dst_ref=dst.at[j, my_place],
            send_sem=send_sem, recv_sem=recv_sem.at[j],
            device_id=(k, q), device_id_type=MESH,
        ).start()

    def wait_recv(view, sem):
        pltpu.make_async_remote_copy(
            src_ref=view, dst_ref=view, send_sem=sem, recv_sem=sem, device_id=(k, r), device_id_type=MESH
        ).wait_recv()

    def wait_send(view, sem):
        pltpu.make_async_remote_copy(
            src_ref=view, dst_ref=view, send_sem=sem, recv_sem=sem, device_id=(k, r), device_id_type=MESH
        ).wait_send()

    def build_x(j, via_tp):
        m1, m2 = masks(j)
        pick = jnp.where(m1 | m2, 1.0, 0.0).astype(BF)
        for c in range(0, width, 512):
            rows = dot(pick, x_v[:, c:c + 512]).astype(BF)
            xs[j, :, :, c:c + 512] = rows.reshape(ep_size, cap, 512)
        if via_tp:
            send_row(xs, xr, xs_sem, xd_sem, j, diag)
        for q in near if via_tp else far + near:
            send_row(xs, xr, xs_sem, xr_sem, j, q)
        xr[j, my_place] = xs[j, r]

    ins[0].wait()
    ins[2].start()
    ins[1].start()

    @pl.loop(0, n_loc)
    def _(j):
        for c in weight_copies(j):
            c.start()

    pl.semaphore_wait(barrier, n_dev - 1)

    @pl.loop(0, VIA_TP)
    def _(j):
        build_x(j, True)

    if VIA_TP < n_loc:
        @pl.loop(VIA_TP, n_loc)
        def _(j):
            build_x(j, False)

    def column(row):
        return jnp.transpose(jnp.broadcast_to(row, (128, n_tok)))

    s1c[...] = column(s1r[...])
    s2c[...] = column(s2r[...])
    i1c[...] = column(ids1.astype(F32))
    i2c[...] = column(ids2.astype(F32))
    ins[2].wait()
    wr_hi, wr_mid, wr_low = split3(wr_v[...])
    xv = x_v[...]
    logits = dot(xv, wr_hi, NT) + (dot(xv, wr_mid, NT) + dot(xv, wr_low, NT))
    ex = jnp.exp(logits - jnp.max(logits, axis=1, keepdims=True))
    prob = ex / jnp.sum(ex, axis=1, keepdims=True)
    prob_v[...] = prob
    lane = lax.broadcasted_iota(I32, (n_tok, n_exp), 1).astype(F32)
    q1 = jnp.sum(jnp.where(i1c[:, :n_exp] == lane, prob, 0.0), axis=1, keepdims=True)
    q2 = jnp.sum(jnp.where(i2c[:, :n_exp] == lane, prob, 0.0), axis=1, keepdims=True)
    g1 = jnp.broadcast_to(q1 / (q1 + q2), (n_tok, 128))
    g2 = jnp.broadcast_to(q2 / (q1 + q2), (n_tok, 128))
    g1c[...] = g1
    g2c[...] = g2
    q1c[...] = jnp.broadcast_to(q1, (n_tok, 128))
    q2c[...] = jnp.broadcast_to(q2, (n_tok, 128))
    g1r[...] = jnp.transpose(g1)[0:1, :]
    g2r[...] = jnp.transpose(g2)[0:1, :]
    ins[1].wait()

    def build_d(j):
        m1, m2 = masks(j)
        pick = jnp.where(m1 | m2, 1.0, 0.0).astype(BF)
        gate = jnp.sum(jnp.where(m1, g1r[...], 0.0) + jnp.where(m2, g2r[...], 0.0), axis=1, keepdims=True)
        for c in range(0, width, 512):
            rows = (gate * dot(pick, dy_v[:, c:c + 512])).astype(BF)
            ds[j, :, :, c:c + 512] = rows.reshape(ep_size, cap, 512)
        for q in far + near:
            send_row(ds, dr, ds_sem, dr_sem, j, q)
        dr[j, my_place] = ds[j, r]

    def send_half(src, dst, send_sem, recv_sem, j):
        pltpu.make_async_remote_copy(
            src_ref=src.at[j, pl.ds(other * half, half)], dst_ref=dst.at[j],
            send_sem=send_sem, recv_sem=recv_sem.at[j],
            device_id=(other, r), device_id_type=MESH,
        ).start()

    def merge_and_return(src, got, got_sem, dst, send_sem, recv_sem, j):
        wait_recv(got.at[j], got_sem.at[j])
        mine = pl.ds(k * half, half)
        src[j, mine] = (src[j, mine].astype(F32) + got[j].astype(F32)).astype(BF)
        for d in range(half):
            c = (r // tp_size + d) % half
            q = tp_size * c + k

            @pl.when(q != r)
            def _():
                pltpu.make_async_remote_copy(
                    src_ref=src.at[j, k * half + c], dst_ref=dst.at[j, r],
                    send_sem=send_sem, recv_sem=recv_sem.at[j],
                    device_id=(k, q), device_id_type=MESH,
                ).start()

            @pl.when(q == r)
            def _():
                dst[j, r] = src[j, k * half + c]

    n_near = len(near)
    diag_place = place_of(diag)

    def forward_diag(j):
        wait_recv(xr.at[j, 0], xd_sem.at[j])
        pltpu.make_async_remote_copy(
            src_ref=xr.at[j, diag_place], dst_ref=xr.at[j, diag_place],
            send_sem=xfs_sem, recv_sem=xf_sem.at[j],
            device_id=(other, r), device_id_type=MESH,
        ).start()

    for i in range(FORWARD):
        forward_diag(i)

    @pl.loop(0, n_loc)
    def _(j):
        @pl.when(j >= n_loc - AHEAD)
        def _():
            build_d(j + AHEAD - n_loc)

        @pl.when(j + FORWARD < VIA_TP)
        def _():
            forward_diag(j + FORWARD)

        for c in weight_copies(j):
            c.wait()

        @pl.when(j < VIA_TP)
        def _():
            wait_recv(xr.at[j, pl.ds(0, n_near)], xr_sem.at[j])
            wait_recv(xr.at[j, 0], xf_sem.at[j])

        if VIA_TP < n_loc:
            @pl.when(j >= VIA_TP)
            def _():
                wait_recv(xr.at[j, pl.ds(0, ep_size - 1)], xr_sem.at[j])

        rows = xr[j].reshape(blk, width)
        pa = dot(rows, wa_v[j])
        pb = dot(rows, wb_v[j])
        th = jnp.tanh(GELU_COEF * (pa + 0.044715 * pa * pa * pa))
        gv = 0.5 * pa * (1.0 + th)
        slope = 0.5 * (1.0 + th) + 0.5 * pa * (1.0 - th * th) * GELU_COEF * (1.0 + 0.134145 * pa * pa)
        gv_v[j] = gv
        bs_v[j] = pb * slope
        hidden = (gv * pb).astype(BF)
        h_v[j] = hidden
        for c in range(0, width, 512):
            ps[j, :, :, c:c + 512] = dot(hidden, wc_v[j, :, c:c + 512]).astype(BF).reshape(ep_size, cap, 512)
        send_half(ps, pr, ps_sem, pr_sem, j)

        @pl.when(j >= LAG)
        def _():
            merge_and_return(ps, pr, pr_sem, orr, os_sem, or_sem, j - LAG)

    tb = 128
    n_tb = n_tok // tb

    def spots(col, toks):
        lanes = lax.broadcasted_iota(I32, (tb, 128), 1).astype(F32)
        base = col[toks, :]
        return jnp.concatenate([base == lanes + float(u * 128) for u in range(n_exp * cap // 128)], axis=1)

    def ship(buf, t, send_sem, recv_sem):
        toks = pl.ds(pl.multiple_of(t * tb, tb), tb)
        pltpu.make_async_remote_copy(
            src_ref=buf.at[toks], dst_ref=buf.at[toks], send_sem=send_sem, recv_sem=recv_sem.at[t],
            device_id=(other, r), device_id_type=MESH,
        ).start()

    def combine_y(t):
        toks = pl.ds(pl.multiple_of(t * tb, tb), tb)
        pick1 = jnp.where(spots(s1c, toks), 1.0, 0.0).astype(BF)
        pick2 = jnp.where(spots(s2c, toks), 1.0, 0.0).astype(BF)
        dg1 = jnp.zeros((tb, 1), F32)
        dg2 = jnp.zeros((tb, 1), F32)
        ga = g1c[toks, 0:1]
        gb = g2c[toks, 0:1]
        for c in range(0, width, 512):
            rows = orr[:, :, :, c:c + 512].reshape(n_exp * cap, 512)
            o1 = dot(pick1, rows)
            o2 = dot(pick2, rows)
            y_v[toks, c:c + 512] = (ga * o1 + gb * o2).astype(BF)
            dyf = dy_v[toks, c:c + 512].astype(F32)
            dg1 = dg1 + jnp.sum(dyf * o1, axis=1, keepdims=True)
            dg2 = dg2 + jnp.sum(dyf * o2, axis=1, keepdims=True)
        qa = q1c[toks, 0:1]
        qb = q2c[toks, 0:1]
        shared = dg1 * ga + dg2 * gb
        dq1 = (dg1 - shared) / (qa + qb)
        dq2 = (dg2 - shared) / (qa + qb)
        centre = dq1 * qa + dq2 * qb
        lanes = lax.broadcasted_iota(I32, (tb, n_exp), 1).astype(F32)
        pull = jnp.where(i1c[toks, :n_exp] == lanes, dq1, 0.0) + jnp.where(i2c[toks, :n_exp] == lanes, dq2, 0.0)
        dl_v[toks, :] = prob_v[toks, :] * (pull - centre)

    def router_parts():
        d_hi, d_mid, d_low = split3(dl_v[...])
        for c in range(0, width, 512):
            xc = x_v[:, c:c + 512]
            piece = dot(d_hi, xc, TN) + (dot(d_mid, xc, TN) + dot(d_low, xc, TN))
            dwp[:, :, c:c + 512] = piece.reshape(ep_size, n_loc, 512)
        for d in range(1, ep_size):
            q = (r + d) % ep_size
            pltpu.make_async_remote_copy(
                src_ref=dwp.at[q], dst_ref=dwi.at[r], send_sem=rs_sem, recv_sem=rr_sem,
                device_id=(q % tp_size, q), device_id_type=MESH,
            ).start()
        dwi[r] = dwp[r]

    def router_sum():
        wait_recv(dwi.at[pl.ds(0, ep_size - 1)], rr_sem)
        total = dwi[0]
        for q in range(1, ep_size):
            total = total + dwi[q]
        dwf[r] = total
        for d in range(1, ep_size):
            q = (r + d) % ep_size
            pltpu.make_async_remote_copy(
                src_ref=dwf.at[r], dst_ref=dwf.at[r], send_sem=fs_sem, recv_sem=fr_sem,
                device_id=(q % tp_size, q), device_id_type=MESH,
            ).start()

    wait_send(xs.at[pl.ds(0, VIA_TP), pl.ds(0, n_near + 1)], xs_sem)
    if VIA_TP < n_loc:
        wait_send(xs.at[pl.ds(VIA_TP, n_loc - VIA_TP), pl.ds(0, ep_size - 1)], xs_sem)
    @pl.loop(0, n_loc)
    def _(j):
        @pl.when(j + AHEAD < n_loc)
        def _():
            build_d(j + AHEAD)

        wait_recv(dr.at[j, pl.ds(0, ep_size - 1)], dr_sem.at[j])
        rows = dr[j].reshape(blk, width)
        dh = dot(rows, wc_v[j], NT)
        da = (dh * bs_v[j]).astype(BF)
        db = (dh * gv_v[j]).astype(BF)
        da_v[j] = da
        db_v[j] = db
        for c in range(0, width, 512):
            part = dot(da, wa_v[j, c:c + 512, :], NT) + dot(db, wb_v[j, c:c + 512, :], NT)
            xs[j, :, :, c:c + 512] = part.astype(BF).reshape(ep_size, cap, 512)
        send_half(xs, pdr, pds_sem, pdr_sem, j)

        @pl.when(j == 0)
        def _():
            for i in range(LAG):
                merge_and_return(ps, pr, pr_sem, orr, os_sem, or_sem, n_loc - LAG + i)

        @pl.when(j >= LAG)
        def _():
            merge_and_return(xs, pdr, pdr_sem, dxr, dxs_sem, dxr_sem, j - LAG)

        @pl.when(owner & (j == Y_STEP))
        def _():
            @pl.loop(0, n_loc)
            def _(i):
                wait_recv(orr.at[i, pl.ds(0, ep_size - 1)], or_sem.at[i])

        @pl.when(owner & (j >= Y_STEP) & (j < Y_STEP + n_tb // 2))
        def _():
            t0 = 2 * (j - Y_STEP)

            @pl.loop(t0, t0 + 2)
            def _(t):
                combine_y(t)

            ship(y_v, j - Y_STEP, ys_sem, yr_sem)

        @pl.when(owner & (j == Y_STEP + n_tb // 2 - 1))
        def _():
            router_parts()

    outs = [
        pltpu.make_async_copy(xr, xe_out, out_sem.at[0]),
        pltpu.make_async_copy(dr, de_out, out_sem.at[1]),
        pltpu.make_async_copy(h_v, h_out, out_sem.at[2]),
        pltpu.make_async_copy(da_v, da_out, out_sem.at[3]),
        pltpu.make_async_copy(db_v, db_out, out_sem.at[4]),
    ]
    for c in outs[:3]:
        c.start()

    split = n_loc - 2

    def pick_both(t):
        toks = pl.ds(pl.multiple_of(t * tb, tb), tb)
        return toks, jnp.where(spots(s1c, toks) | spots(s2c, toks), 1.0, 0.0).astype(BF)

    def sum_first(t):
        toks, pick = pick_both(t)
        dl = dl_v[toks, :]
        for c in range(0, width, 512):
            rows = dxr[0:split, :, :, c:c + 512].reshape(split * blk, 512)
            router = lax.dot_general(
                dl, wr_v[:, c:c + 512], NN, precision=lax.Precision.HIGHEST, preferred_element_type=F32
            )
            acc_v[toks, c:c + 512] = dot(pick[:, :split * blk], rows) + router

    def sum_last(t):
        toks, pick = pick_both(t)
        for c in range(0, width, 512):
            rows = dxr[split:n_loc, :, :, c:c + 512].reshape((n_loc - split) * blk, 512)
            dx_v[toks, c:c + 512] = (acc_v[toks, c:c + 512] + dot(pick[:, split * blk:], rows)).astype(BF)
        pltpu.make_async_copy(dx_v.at[toks], dx_out.at[toks], in_sem.at[1]).start()

    for c in outs[3:]:
        c.start()

    @pl.when(owner)
    def _():
        ship(y_v, n_tb - 2, ys_sem, yr_sem)

    for i in range(LAG - 1):
        merge_and_return(xs, pdr, pdr_sem, dxr, dxs_sem, dxr_sem, n_loc - LAG + i)

    @pl.when(owner)
    def _():
        router_sum()
        ship(y_v, n_tb - 1, ys_sem, yr_sem)
        pltpu.make_async_copy(y_v, y_out, in_sem.at[0]).start()

    merge_and_return(xs, pdr, pdr_sem, dxr, dxs_sem, dxr_sem, n_loc - 1)

    @pl.when(owner)
    def _():
        @pl.loop(0, split)
        def _(j):
            wait_recv(dxr.at[j, pl.ds(0, ep_size - 1)], dxr_sem.at[j])

        @pl.loop(0, n_tb)
        def _(t):
            sum_first(t)

        wait_recv(dwf.at[pl.ds(0, ep_size - 1)], fr_sem)
        pltpu.make_async_remote_copy(
            src_ref=dwf, dst_ref=dwf, send_sem=gs_sem, recv_sem=gr_sem,
            device_id=(k, 2 * chip + 1 - core), device_id_type=MESH,
        ).start()

        @pl.loop(split, n_loc)
        def _(j):
            wait_recv(dxr.at[j, pl.ds(0, ep_size - 1)], dxr_sem.at[j])

        @pl.loop(0, n_tb)
        def _(t):
            sum_last(t)

        wait_send(dwp.at[pl.ds(0, ep_size - 1)], rs_sem)
        wait_send(dwf.at[pl.ds(0, ep_size - 1)], fs_sem)
        wait_send(dwf, gs_sem)
        wait_send(y_v, ys_sem)
        wait_send(orr.at[:, pl.ds(0, half - 1)], os_sem)
        wait_send(dxr.at[:, pl.ds(0, half - 1)], dxs_sem)

    @pl.when(jnp.logical_not(owner))
    def _():
        dx_v[...] = jnp.zeros_like(dx_v)
        pltpu.make_async_copy(dx_v, dx_out, in_sem.at[1]).start()
        for t in range(n_tb):
            toks = pl.ds(t * tb, tb)
            wait_recv(y_v.at[toks], yr_sem.at[t])
            pltpu.make_async_copy(y_v.at[toks], y_out.at[toks], in_sem.at[0]).start()
        wait_recv(dwf, gr_sem)
        wait_send(orr.at[:, pl.ds(0, half)], os_sem)
        wait_send(dxr.at[:, pl.ds(0, half)], dxs_sem)

    finals = [
        pltpu.make_async_copy(dwf, dwr_out, in_sem.at[2]),
        pltpu.make_async_copy(y_v, y_out, in_sem.at[0]),
        pltpu.make_async_copy(dx_v, dx_out, in_sem.at[1]),
    ]
    finals[0].start()
    wait_send(ds.at[:, pl.ds(0, ep_size - 1)], ds_sem)
    wait_send(xr.at[pl.ds(0, VIA_TP), 0], xfs_sem)
    wait_send(ps.at[:, pl.ds(0, half)], ps_sem)
    wait_send(xs.at[:, pl.ds(0, half)], pds_sem)
    for c in outs + finals:
        c.wait()


def weight_kernel(xe, de, h, da, db, y, dwr, ga_out, gb_out, gc_out, y_out, dwr_out):
    y_out[...] = y[...]
    dwr_out[...] = dwr[...]
    rows = xe[0]
    ga_out[0] = dot(rows, da[0], TN)
    gb_out[0] = dot(rows, db[0], TN)
    gc_out[0] = dot(h[0], de[0], TN)


def solution(mesh):
    tp_size = mesh.shape["tp"]
    ep_size = mesh.shape["ep"]

    def local_step(x_rows, w_router, first_ids, second_ids, w_gelu, w_lin, w_out, dy_rows):
        n_tok, width = x_rows.shape
        n_exp = w_router.shape[1]
        n_loc, _, hid = w_gelu.shape
        cap = 2 * n_tok // n_exp
        blk = ep_size * cap
        half = ep_size // tp_size
        dma = pltpu.SemaphoreType.DMA
        any_spec = pl.BlockSpec(memory_space=pl.ANY)
        sds = jax.ShapeDtypeStruct
        rows_shape = (n_loc, ep_size, cap, width)
        half_shape = (n_loc, half, cap, width)
        hid_shape = (n_loc, blk, hid)
        col = pltpu.VMEM((n_tok, 128), F32)
        row = pltpu.VMEM((1, n_tok), F32)
        outs = pl.pallas_call(
            functools.partial(moe_kernel, tp_size, ep_size, cap),
            name="moe",
            in_specs=[any_spec] * 8,
            out_specs=[any_spec] * 8,
            out_shape=[
                sds((n_tok, width), BF), sds((n_tok, width), BF), sds((ep_size, n_loc, width), F32),
                sds(rows_shape, BF), sds(rows_shape, BF), sds(hid_shape, BF), sds(hid_shape, BF), sds(hid_shape, BF),
            ],
            scratch_shapes=[
                pltpu.VMEM((n_tok, width), BF), pltpu.VMEM((n_tok, width), BF), pltpu.VMEM((n_exp, width), F32),
                pltpu.VMEM((n_loc, width, hid), BF), pltpu.VMEM((n_loc, width, hid), BF), pltpu.VMEM((n_loc, hid, width), BF),
                pltpu.VMEM(rows_shape, BF), pltpu.VMEM(rows_shape, BF), pltpu.VMEM(rows_shape, BF), pltpu.VMEM(rows_shape, BF),
                pltpu.VMEM(hid_shape, BF), pltpu.VMEM(hid_shape, BF), pltpu.VMEM(hid_shape, BF),
                pltpu.VMEM(hid_shape, F32), pltpu.VMEM(hid_shape, F32),
                pltpu.VMEM(rows_shape, BF), pltpu.VMEM(half_shape, BF), pltpu.VMEM(half_shape, BF),
                pltpu.VMEM(rows_shape, BF), pltpu.VMEM(rows_shape, BF),
                pltpu.VMEM((n_tok, width), BF), pltpu.VMEM((n_tok, width), BF),
                row, row, row, row, col, col, col, col, col, col, col, col,
                pltpu.VMEM((n_tok, n_exp), F32), pltpu.VMEM((n_tok, n_exp), F32),
                pltpu.VMEM((ep_size, n_loc, width), F32), pltpu.VMEM((ep_size, n_loc, width), F32),
                pltpu.VMEM((ep_size, n_loc, width), F32), pltpu.VMEM((n_tok, width), F32),
                pltpu.VMEM((1, n_tok), I32), pltpu.VMEM((1, n_tok), I32),
                dma((3,)), dma((3, n_loc)), dma((5,)), dma((2,)),
                dma(()), dma((n_loc,)), dma((n_loc,)), dma((n_loc,)), dma(()), dma(()), dma((n_loc,)),
                dma(()), dma((n_loc,)), dma(()), dma((n_loc,)),
                dma(()), dma((n_loc,)), dma(()), dma((n_loc,)),
                dma(()), dma((n_tok // 128,)),
                dma(()), dma(()), dma(()), dma(()), dma(()), dma(()),
            ],
            compiler_params=pltpu.CompilerParams(
                collective_id=0, has_side_effects=True, vmem_limit_bytes=67043328
            ),
        )(
            first_ids.reshape(1, n_tok), second_ids.reshape(1, n_tok), x_rows, dy_rows, w_router.T,
            w_gelu, w_lin, w_out,
        )
        act_out, grad_in, grad_router, xe, de, h, da, db = outs
        partners = [
            ((q % tp_size) * ep_size + q, (1 - q % tp_size) * ep_size + q) for q in range(ep_size)
        ]
        passed = lax.ppermute(grad_in, ("tp", "ep"), partners)
        owner = lax.axis_index("ep") % tp_size == lax.axis_index("tp")
        grad_in = jnp.where(owner, grad_in, passed)
        xe = xe.reshape(n_loc, blk, width)
        de = de.reshape(n_loc, blk, width)

        y_spec = pl.BlockSpec((n_tok // n_loc, width), lambda e: (e, 0))

        def spec(*shape):
            return pl.BlockSpec((1,) + shape, lambda e: (e, 0, 0))

        grad_wa, grad_wb, grad_wc, act_out, grad_router = pl.pallas_call(
            weight_kernel,
            name="weight_grads",
            grid=(n_loc,),
            in_specs=[spec(blk, width), spec(blk, width), spec(blk, hid), spec(blk, hid), spec(blk, hid), y_spec, spec(n_exp // n_loc, width)],
            out_specs=[spec(width, hid), spec(width, hid), spec(hid, width), y_spec, spec(n_exp // n_loc, width)],
            out_shape=[
                sds((n_loc, width, hid), F32), sds((n_loc, width, hid), F32), sds((n_loc, hid, width), F32),
                sds((n_tok, width), BF), sds((n_loc, n_exp // n_loc, width), F32),
            ],
            compiler_params=pltpu.CompilerParams(
                dimension_semantics=("arbitrary",), vmem_limit_bytes=63743328
            ),
            cost_estimate=pl.CostEstimate(
                flops=6 * n_loc * blk * width * hid, transcendentals=0,
                bytes_accessed=12 * n_loc * width * hid + 4 * n_loc * blk * width + 6 * n_loc * blk * hid,
            ),
        )(xe, de, h, da, db, act_out, grad_router.reshape(n_loc, n_exp // n_loc, width))
        return act_out, grad_in, grad_wa, grad_wb, grad_wc, grad_router.reshape(n_exp, width).T

    return jax.shard_map(
        local_step,
        mesh=mesh,
        in_specs=(P("ep", None), P(), P("ep"), P("ep"), P("ep", None, "tp"), P("ep", None, "tp"), P("ep", "tp", None), P("ep", None)),
        out_specs=(P("ep", None), P("ep", None), P("ep", None, "tp"), P("ep", None, "tp"), P("ep", "tp", None), P()),
        check_vma=False,
    )
```

```python
import functools

import jax
import jax.numpy as jnp
from jax import lax
from jax.experimental import pallas as pl
from jax.experimental.pallas import tpu as pltpu
from jax.sharding import PartitionSpec as P

BF = jnp.bfloat16
F32 = jnp.float32
I32 = jnp.int32
MESH = pl.DeviceIdType.MESH
GELU_COEF = 0.7978845608028654
AHEAD = 4
LAG = 3
Y_STEP = 4
FORWARD = 2
VIA_TP = 8
EARLY = 2
NN = (((1,), (0,)), ((), ()))
NT = (((1,), (1,)), ((), ()))
TN = (((0,), (0,)), ((), ()))


def dot(a, b, dims=NN):
    return lax.dot_general(a, b, dims, preferred_element_type=F32)


def split3(v):
    hi = v.astype(BF)
    rest = v - hi.astype(F32)
    mid = rest.astype(BF)
    low = (rest - mid.astype(F32)).astype(BF)
    return hi, mid, low


def moe_kernel(
    tp_size, ep_size, cap,
    ids1_hbm, ids2_hbm, x_hbm, dy_hbm, wr_hbm, wa_hbm, wb_hbm, wc_hbm,
    y_out, dx_out, dwr_out, xe_out, de_out, h_out, da_out, db_out,
    x_v, dy_v, wr_v, wa_v, wb_v, wc_v,
    xs, ds, xr, dr, h_v, da_v, db_v, bs_v, gv_v,
    ps, pr, pdr, orr, dxr, y_v, dx_v,
    s1r, s2r, g1r, g2r, s1c, s2c, g1c, g2c, q1c, q2c, i1c, i2c, prob_v, dl_v,
    dwp, dwi, dwf, acc_v, ids1_ref, ids2_ref,
    in_sem, w_sem, out_sem, id_sem,
    xs_sem, xr_sem, xd_sem, xf_sem, xfs_sem, ds_sem, dr_sem,
    ps_sem, pr_sem, pds_sem, pdr_sem,
    os_sem, or_sem, dxs_sem, dxr_sem,
    ys_sem, yr_sem,
    rs_sem, rr_sem, fs_sem, fr_sem, gs_sem, gr_sem,
):
    k = lax.axis_index("tp")
    r = lax.axis_index("ep")
    n_loc = wa_v.shape[0]
    n_tok, width = x_v.shape
    hid = wa_v.shape[2]
    n_exp = n_loc * ep_size
    blk = ep_size * cap
    half = ep_size // tp_size
    my_place = (r % tp_size) * half + r // tp_size
    owner = (r % tp_size) == k
    other = 1 - k

    ins = [
        pltpu.make_async_copy(x_hbm, x_v, in_sem.at[0]),
        pltpu.make_async_copy(dy_hbm, dy_v, in_sem.at[1]),
        pltpu.make_async_copy(wr_hbm, wr_v, in_sem.at[2]),
    ]
    id_loads = [pltpu.make_async_copy(ids1_hbm, ids1_ref, id_sem.at[0]), pltpu.make_async_copy(ids2_hbm, ids2_ref, id_sem.at[1])]
    for c in id_loads:
        c.start()
    ins[0].start()

    def weight_copies(j):
        return [
            pltpu.make_async_copy(wa_hbm.at[j], wa_v.at[j], w_sem.at[0, j]),
            pltpu.make_async_copy(wb_hbm.at[j], wb_v.at[j], w_sem.at[1, j]),
            pltpu.make_async_copy(wc_hbm.at[j], wc_v.at[j], w_sem.at[2, j]),
        ]

    n_dev = tp_size * ep_size
    barrier = pltpu.get_barrier_semaphore()
    for d in range(1, n_dev):
        flat = (k * ep_size + r + d) % n_dev
        pl.semaphore_signal(barrier, inc=1, device_id=(flat // ep_size, flat % ep_size), device_id_type=MESH)

    for c in id_loads:
        c.wait()
    ids1 = ids1_ref[...]
    ids2 = ids2_ref[...]
    e_iota = lax.broadcasted_iota(I32, (n_exp, n_tok), 0)
    hot1 = jnp.where(ids1 == e_iota, 1.0, 0.0).astype(F32)
    hot2 = jnp.where(ids2 == e_iota, 1.0, 0.0).astype(F32)
    before = jnp.where(
        lax.broadcasted_iota(I32, (n_tok, n_tok), 0) < lax.broadcasted_iota(I32, (n_tok, n_tok), 1), 1.0, 0.0
    ).astype(BF)
    cum1 = dot(hot1.astype(BF), before)
    cum2 = dot(hot2.astype(BF), before)
    fill1 = jnp.sum(hot1, axis=1, keepdims=True)
    pos1 = jnp.sum(cum1 * hot1, axis=0, keepdims=True)
    pos2 = jnp.sum((cum2 + fill1) * hot2, axis=0, keepdims=True)

    def place(ids, pos):
        spot = (ids & (n_loc - 1)) * blk + (ids // n_loc) * cap
        return jnp.where(pos < cap, spot.astype(F32) + pos, float(n_exp * cap))

    s1r[...] = place(ids1, pos1)
    s2r[...] = place(ids2, pos2)

    def masks(j):
        spot = (lax.broadcasted_iota(I32, (blk, n_tok), 0) + j * blk).astype(F32)
        return s1r[...] == spot, s2r[...] == spot

    chip = r // 2
    chip_x = chip + 1 - 2 * (chip % 2)
    chip_y = (chip + 2) % 4
    chip_d = 3 - chip
    core = r % 2
    diag = 2 * chip_d + (k + r) % 2
    near = [2 * chip_x + core, 2 * chip_y + core, 2 * chip_x + 1 - core, 2 * chip_y + 1 - core, 2 * chip + 1 - core]
    far = [2 * chip_d + core, 2 * chip_d + 1 - core]

    def place_of(q):
        return (q % tp_size) * half + q // tp_size

    def send_row(src, dst, send_sem, recv_sem, j, q):
        pltpu.make_async_remote_copy(
            src_ref=src.at[j, q], dst_ref=dst.at[j, my_place],
            send_sem=send_sem, recv_sem=recv_sem.at[j],
            device_id=(k, q), device_id_type=MESH,
        ).start()

    def wait_recv(view, sem):
        pltpu.make_async_remote_copy(
            src_ref=view, dst_ref=view, send_sem=sem, recv_sem=sem, device_id=(k, r), device_id_type=MESH
        ).wait_recv()

    def wait_send(view, sem):
        pltpu.make_async_remote_copy(
            src_ref=view, dst_ref=view, send_sem=sem, recv_sem=sem, device_id=(k, r), device_id_type=MESH
        ).wait_send()

    def gather_x(j):
        m1, m2 = masks(j)
        pick = jnp.where(m1 | m2, 1.0, 0.0).astype(BF)
        for c in range(0, width, 512):
            rows = dot(pick, x_v[:, c:c + 512]).astype(BF)
            xs[j, :, :, c:c + 512] = rows.reshape(ep_size, cap, 512)

    def send_x(j, via_tp):
        if via_tp:
            send_row(xs, xr, xs_sem, xd_sem, j, diag)
        for q in near if via_tp else far + near:
            send_row(xs, xr, xs_sem, xr_sem, j, q)
        xr[j, my_place] = xs[j, r]

    ins[0].wait()
    ins[2].start()
    ins[1].start()

    @pl.loop(0, n_loc)
    def _(j):
        for c in weight_copies(j):
            c.start()

    @pl.loop(0, EARLY)
    def _(j):
        gather_x(j)

    pl.semaphore_wait(barrier, n_dev - 1)

    @pl.loop(0, EARLY)
    def _(j):
        send_x(j, True)

    @pl.loop(EARLY, VIA_TP)
    def _(j):
        gather_x(j)
        send_x(j, True)

    if VIA_TP < n_loc:
        @pl.loop(VIA_TP, n_loc)
        def _(j):
            gather_x(j)
            send_x(j, False)

    def column(row):
        return jnp.transpose(jnp.broadcast_to(row, (128, n_tok)))

    s1c[...] = column(s1r[...])
    s2c[...] = column(s2r[...])
    i1c[...] = column(ids1.astype(F32))
    i2c[...] = column(ids2.astype(F32))
    ins[2].wait()
    wr_hi, wr_mid, wr_low = split3(wr_v[...])
    xv = x_v[...]
    logits = dot(xv, wr_hi, NT) + (dot(xv, wr_mid, NT) + dot(xv, wr_low, NT))
    ex = jnp.exp(logits - jnp.max(logits, axis=1, keepdims=True))
    prob = ex / jnp.sum(ex, axis=1, keepdims=True)
    prob_v[...] = prob
    lane = lax.broadcasted_iota(I32, (n_tok, n_exp), 1).astype(F32)
    q1 = jnp.sum(jnp.where(i1c[:, :n_exp] == lane, prob, 0.0), axis=1, keepdims=True)
    q2 = jnp.sum(jnp.where(i2c[:, :n_exp] == lane, prob, 0.0), axis=1, keepdims=True)
    g1 = jnp.broadcast_to(q1 / (q1 + q2), (n_tok, 128))
    g2 = jnp.broadcast_to(q2 / (q1 + q2), (n_tok, 128))
    g1c[...] = g1
    g2c[...] = g2
    q1c[...] = jnp.broadcast_to(q1, (n_tok, 128))
    q2c[...] = jnp.broadcast_to(q2, (n_tok, 128))
    g1r[...] = jnp.transpose(g1)[0:1, :]
    g2r[...] = jnp.transpose(g2)[0:1, :]
    ins[1].wait()

    def build_d(j):
        m1, m2 = masks(j)
        pick = jnp.where(m1 | m2, 1.0, 0.0).astype(BF)
        gate = jnp.sum(jnp.where(m1, g1r[...], 0.0) + jnp.where(m2, g2r[...], 0.0), axis=1, keepdims=True)
        for c in range(0, width, 512):
            rows = (gate * dot(pick, dy_v[:, c:c + 512])).astype(BF)
            ds[j, :, :, c:c + 512] = rows.reshape(ep_size, cap, 512)
        for q in far + near:
            send_row(ds, dr, ds_sem, dr_sem, j, q)
        dr[j, my_place] = ds[j, r]

    def send_half(src, dst, send_sem, recv_sem, j):
        pltpu.make_async_remote_copy(
            src_ref=src.at[j, pl.ds(other * half, half)], dst_ref=dst.at[j],
            send_sem=send_sem, recv_sem=recv_sem.at[j],
            device_id=(other, r), device_id_type=MESH,
        ).start()

    def merge_and_return(src, got, got_sem, dst, send_sem, recv_sem, j):
        wait_recv(got.at[j], got_sem.at[j])
        mine = pl.ds(k * half, half)
        src[j, mine] = (src[j, mine].astype(F32) + got[j].astype(F32)).astype(BF)
        for d in range(half):
            c = (r // tp_size + d) % half
            q = tp_size * c + k

            @pl.when(q != r)
            def _():
                pltpu.make_async_remote_copy(
                    src_ref=src.at[j, k * half + c], dst_ref=dst.at[j, r],
                    send_sem=send_sem, recv_sem=recv_sem.at[j],
                    device_id=(k, q), device_id_type=MESH,
                ).start()

            @pl.when(q == r)
            def _():
                dst[j, r] = src[j, k * half + c]

    n_near = len(near)
    diag_place = place_of(diag)

    def forward_diag(j):
        wait_recv(xr.at[j, 0], xd_sem.at[j])
        pltpu.make_async_remote_copy(
            src_ref=xr.at[j, diag_place], dst_ref=xr.at[j, diag_place],
            send_sem=xfs_sem, recv_sem=xf_sem.at[j],
            device_id=(other, r), device_id_type=MESH,
        ).start()

    for i in range(FORWARD):
        forward_diag(i)

    @pl.loop(0, n_loc)
    def _(j):
        @pl.when(j >= n_loc - AHEAD)
        def _():
            build_d(j + AHEAD - n_loc)

        @pl.when(j + FORWARD < VIA_TP)
        def _():
            forward_diag(j + FORWARD)

        for c in weight_copies(j):
            c.wait()

        @pl.when(j < VIA_TP)
        def _():
            wait_recv(xr.at[j, pl.ds(0, n_near)], xr_sem.at[j])
            wait_recv(xr.at[j, 0], xf_sem.at[j])

        if VIA_TP < n_loc:
            @pl.when(j >= VIA_TP)
            def _():
                wait_recv(xr.at[j, pl.ds(0, ep_size - 1)], xr_sem.at[j])

        rows = xr[j].reshape(blk, width)
        pa = dot(rows, wa_v[j])
        pb = dot(rows, wb_v[j])
        th = jnp.tanh(GELU_COEF * (pa + 0.044715 * pa * pa * pa))
        gv = 0.5 * pa * (1.0 + th)
        slope = 0.5 * (1.0 + th) + 0.5 * pa * (1.0 - th * th) * GELU_COEF * (1.0 + 0.134145 * pa * pa)
        gv_v[j] = gv
        bs_v[j] = pb * slope
        hidden = (gv * pb).astype(BF)
        h_v[j] = hidden
        for c in range(0, width, 512):
            ps[j, :, :, c:c + 512] = dot(hidden, wc_v[j, :, c:c + 512]).astype(BF).reshape(ep_size, cap, 512)
        send_half(ps, pr, ps_sem, pr_sem, j)

        @pl.when(j >= LAG)
        def _():
            merge_and_return(ps, pr, pr_sem, orr, os_sem, or_sem, j - LAG)

    tb = 128
    n_tb = n_tok // tb

    def spots(col, toks):
        lanes = lax.broadcasted_iota(I32, (tb, 128), 1).astype(F32)
        base = col[toks, :]
        return jnp.concatenate([base == lanes + float(u * 128) for u in range(n_exp * cap // 128)], axis=1)

    def ship(buf, t, send_sem, recv_sem):
        toks = pl.ds(pl.multiple_of(t * tb, tb), tb)
        pltpu.make_async_remote_copy(
            src_ref=buf.at[toks], dst_ref=buf.at[toks], send_sem=send_sem, recv_sem=recv_sem.at[t],
            device_id=(other, r), device_id_type=MESH,
        ).start()

    def combine_y(t):
        toks = pl.ds(pl.multiple_of(t * tb, tb), tb)
        pick1 = jnp.where(spots(s1c, toks), 1.0, 0.0).astype(BF)
        pick2 = jnp.where(spots(s2c, toks), 1.0, 0.0).astype(BF)
        dg1 = jnp.zeros((tb, 1), F32)
        dg2 = jnp.zeros((tb, 1), F32)
        ga = g1c[toks, 0:1]
        gb = g2c[toks, 0:1]
        for c in range(0, width, 512):
            rows = orr[:, :, :, c:c + 512].reshape(n_exp * cap, 512)
            o1 = dot(pick1, rows)
            o2 = dot(pick2, rows)
            y_v[toks, c:c + 512] = (ga * o1 + gb * o2).astype(BF)
            dyf = dy_v[toks, c:c + 512].astype(F32)
            dg1 = dg1 + jnp.sum(dyf * o1, axis=1, keepdims=True)
            dg2 = dg2 + jnp.sum(dyf * o2, axis=1, keepdims=True)
        qa = q1c[toks, 0:1]
        qb = q2c[toks, 0:1]
        shared = dg1 * ga + dg2 * gb
        dq1 = (dg1 - shared) / (qa + qb)
        dq2 = (dg2 - shared) / (qa + qb)
        centre = dq1 * qa + dq2 * qb
        lanes = lax.broadcasted_iota(I32, (tb, n_exp), 1).astype(F32)
        pull = jnp.where(i1c[toks, :n_exp] == lanes, dq1, 0.0) + jnp.where(i2c[toks, :n_exp] == lanes, dq2, 0.0)
        dl_v[toks, :] = prob_v[toks, :] * (pull - centre)

    def router_parts():
        d_hi, d_mid, d_low = split3(dl_v[...])
        for c in range(0, width, 512):
            xc = x_v[:, c:c + 512]
            piece = dot(d_hi, xc, TN) + (dot(d_mid, xc, TN) + dot(d_low, xc, TN))
            dwp[:, :, c:c + 512] = piece.reshape(ep_size, n_loc, 512)
        for d in range(1, ep_size):
            q = (r + d) % ep_size
            pltpu.make_async_remote_copy(
                src_ref=dwp.at[q], dst_ref=dwi.at[r], send_sem=rs_sem, recv_sem=rr_sem,
                device_id=(q % tp_size, q), device_id_type=MESH,
            ).start()
        dwi[r] = dwp[r]

    def router_sum():
        wait_recv(dwi.at[pl.ds(0, ep_size - 1)], rr_sem)
        total = dwi[0]
        for q in range(1, ep_size):
            total = total + dwi[q]
        dwf[r] = total
        for d in range(1, ep_size):
            q = (r + d) % ep_size
            pltpu.make_async_remote_copy(
                src_ref=dwf.at[r], dst_ref=dwf.at[r], send_sem=fs_sem, recv_sem=fr_sem,
                device_id=(q % tp_size, q), device_id_type=MESH,
            ).start()

    wait_send(xs.at[pl.ds(0, VIA_TP), pl.ds(0, n_near + 1)], xs_sem)
    if VIA_TP < n_loc:
        wait_send(xs.at[pl.ds(VIA_TP, n_loc - VIA_TP), pl.ds(0, ep_size - 1)], xs_sem)
    @pl.loop(0, n_loc)
    def _(j):
        @pl.when(j + AHEAD < n_loc)
        def _():
            build_d(j + AHEAD)

        wait_recv(dr.at[j, pl.ds(0, ep_size - 1)], dr_sem.at[j])
        rows = dr[j].reshape(blk, width)
        dh = dot(rows, wc_v[j], NT)
        da = (dh * bs_v[j]).astype(BF)
        db = (dh * gv_v[j]).astype(BF)
        da_v[j] = da
        db_v[j] = db
        for c in range(0, width, 512):
            part = dot(da, wa_v[j, c:c + 512, :], NT) + dot(db, wb_v[j, c:c + 512, :], NT)
            xs[j, :, :, c:c + 512] = part.astype(BF).reshape(ep_size, cap, 512)
        send_half(xs, pdr, pds_sem, pdr_sem, j)

        @pl.when(j == 0)
        def _():
            for i in range(LAG):
                merge_and_return(ps, pr, pr_sem, orr, os_sem, or_sem, n_loc - LAG + i)

        @pl.when(j >= LAG)
        def _():
            merge_and_return(xs, pdr, pdr_sem, dxr, dxs_sem, dxr_sem, j - LAG)

        @pl.when(owner & (j == Y_STEP))
        def _():
            @pl.loop(0, n_loc)
            def _(i):
                wait_recv(orr.at[i, pl.ds(0, ep_size - 1)], or_sem.at[i])

        @pl.when(owner & (j >= Y_STEP) & (j < Y_STEP + n_tb // 2))
        def _():
            t0 = 2 * (j - Y_STEP)

            @pl.loop(t0, t0 + 2)
            def _(t):
                combine_y(t)

            ship(y_v, j - Y_STEP, ys_sem, yr_sem)

        @pl.when(owner & (j == Y_STEP + n_tb // 2 - 1))
        def _():
            router_parts()

    outs = [
        pltpu.make_async_copy(xr, xe_out, out_sem.at[0]),
        pltpu.make_async_copy(dr, de_out, out_sem.at[1]),
        pltpu.make_async_copy(h_v, h_out, out_sem.at[2]),
        pltpu.make_async_copy(da_v, da_out, out_sem.at[3]),
        pltpu.make_async_copy(db_v, db_out, out_sem.at[4]),
    ]
    for c in outs[:3]:
        c.start()

    split = n_loc - 2

    def pick_both(t):
        toks = pl.ds(pl.multiple_of(t * tb, tb), tb)
        return toks, jnp.where(spots(s1c, toks) | spots(s2c, toks), 1.0, 0.0).astype(BF)

    def sum_first(t):
        toks, pick = pick_both(t)
        dl = dl_v[toks, :]
        for c in range(0, width, 512):
            rows = dxr[0:split, :, :, c:c + 512].reshape(split * blk, 512)
            router = lax.dot_general(
                dl, wr_v[:, c:c + 512], NN, precision=lax.Precision.HIGHEST, preferred_element_type=F32
            )
            acc_v[toks, c:c + 512] = dot(pick[:, :split * blk], rows) + router

    def sum_last(t):
        toks, pick = pick_both(t)
        for c in range(0, width, 512):
            rows = dxr[split:n_loc, :, :, c:c + 512].reshape((n_loc - split) * blk, 512)
            dx_v[toks, c:c + 512] = (acc_v[toks, c:c + 512] + dot(pick[:, split * blk:], rows)).astype(BF)
        pltpu.make_async_copy(dx_v.at[toks], dx_out.at[toks], in_sem.at[1]).start()

    for c in outs[3:]:
        c.start()

    @pl.when(owner)
    def _():
        ship(y_v, n_tb - 2, ys_sem, yr_sem)
        ship(y_v, n_tb - 1, ys_sem, yr_sem)
        pltpu.make_async_copy(y_v, y_out, in_sem.at[0]).start()

    for i in range(LAG - 1):
        merge_and_return(xs, pdr, pdr_sem, dxr, dxs_sem, dxr_sem, n_loc - LAG + i)

    @pl.when(owner)
    def _():
        router_sum()

    merge_and_return(xs, pdr, pdr_sem, dxr, dxs_sem, dxr_sem, n_loc - 1)

    @pl.when(owner)
    def _():
        @pl.loop(0, split)
        def _(j):
            wait_recv(dxr.at[j, pl.ds(0, ep_size - 1)], dxr_sem.at[j])

        @pl.loop(0, n_tb)
        def _(t):
            sum_first(t)

        wait_recv(dwf.at[pl.ds(0, ep_size - 1)], fr_sem)
        pltpu.make_async_remote_copy(
            src_ref=dwf, dst_ref=dwf, send_sem=gs_sem, recv_sem=gr_sem,
            device_id=(k, 2 * chip + 1 - core), device_id_type=MESH,
        ).start()

        @pl.loop(split, n_loc)
        def _(j):
            wait_recv(dxr.at[j, pl.ds(0, ep_size - 1)], dxr_sem.at[j])

        @pl.loop(0, n_tb)
        def _(t):
            sum_last(t)

        wait_send(dwp.at[pl.ds(0, ep_size - 1)], rs_sem)
        wait_send(dwf.at[pl.ds(0, ep_size - 1)], fs_sem)
        wait_send(dwf, gs_sem)
        wait_send(y_v, ys_sem)
        wait_send(orr.at[:, pl.ds(0, half - 1)], os_sem)
        wait_send(dxr.at[:, pl.ds(0, half - 1)], dxs_sem)

    @pl.when(jnp.logical_not(owner))
    def _():
        dx_v[...] = jnp.zeros_like(dx_v)
        pltpu.make_async_copy(dx_v, dx_out, in_sem.at[1]).start()
        for t in range(n_tb):
            toks = pl.ds(t * tb, tb)
            wait_recv(y_v.at[toks], yr_sem.at[t])
            pltpu.make_async_copy(y_v.at[toks], y_out.at[toks], in_sem.at[0]).start()
        wait_recv(dwf, gr_sem)
        wait_send(orr.at[:, pl.ds(0, half)], os_sem)
        wait_send(dxr.at[:, pl.ds(0, half)], dxs_sem)

    finals = [
        pltpu.make_async_copy(dwf, dwr_out, in_sem.at[2]),
        pltpu.make_async_copy(y_v, y_out, in_sem.at[0]),
        pltpu.make_async_copy(dx_v, dx_out, in_sem.at[1]),
    ]
    finals[0].start()
    wait_send(ds.at[:, pl.ds(0, ep_size - 1)], ds_sem)
    wait_send(xr.at[pl.ds(0, VIA_TP), 0], xfs_sem)
    wait_send(ps.at[:, pl.ds(0, half)], ps_sem)
    wait_send(xs.at[:, pl.ds(0, half)], pds_sem)
    for c in outs + finals:
        c.wait()


def weight_kernel(xe, de, h, da, db, y, dwr, ga_out, gb_out, gc_out, y_out, dwr_out):
    y_out[...] = y[...]
    dwr_out[...] = dwr[...]
    rows = xe[0]
    ga_out[0] = dot(rows, da[0], TN)
    gb_out[0] = dot(rows, db[0], TN)
    gc_out[0] = dot(h[0], de[0], TN)


def solution(mesh):
    tp_size = mesh.shape["tp"]
    ep_size = mesh.shape["ep"]

    def local_step(x_rows, w_router, first_ids, second_ids, w_gelu, w_lin, w_out, dy_rows):
        n_tok, width = x_rows.shape
        n_exp = w_router.shape[1]
        n_loc, _, hid = w_gelu.shape
        cap = 2 * n_tok // n_exp
        blk = ep_size * cap
        half = ep_size // tp_size
        dma = pltpu.SemaphoreType.DMA
        any_spec = pl.BlockSpec(memory_space=pl.ANY)
        sds = jax.ShapeDtypeStruct
        rows_shape = (n_loc, ep_size, cap, width)
        half_shape = (n_loc, half, cap, width)
        hid_shape = (n_loc, blk, hid)
        col = pltpu.VMEM((n_tok, 128), F32)
        row = pltpu.VMEM((1, n_tok), F32)
        outs = pl.pallas_call(
            functools.partial(moe_kernel, tp_size, ep_size, cap),
            name="moe",
            in_specs=[any_spec] * 8,
            out_specs=[any_spec] * 8,
            out_shape=[
                sds((n_tok, width), BF), sds((n_tok, width), BF), sds((ep_size, n_loc, width), F32),
                sds(rows_shape, BF), sds(rows_shape, BF), sds(hid_shape, BF), sds(hid_shape, BF), sds(hid_shape, BF),
            ],
            scratch_shapes=[
                pltpu.VMEM((n_tok, width), BF), pltpu.VMEM((n_tok, width), BF), pltpu.VMEM((n_exp, width), F32),
                pltpu.VMEM((n_loc, width, hid), BF), pltpu.VMEM((n_loc, width, hid), BF), pltpu.VMEM((n_loc, hid, width), BF),
                pltpu.VMEM(rows_shape, BF), pltpu.VMEM(rows_shape, BF), pltpu.VMEM(rows_shape, BF), pltpu.VMEM(rows_shape, BF),
                pltpu.VMEM(hid_shape, BF), pltpu.VMEM(hid_shape, BF), pltpu.VMEM(hid_shape, BF),
                pltpu.VMEM(hid_shape, F32), pltpu.VMEM(hid_shape, F32),
                pltpu.VMEM(rows_shape, BF), pltpu.VMEM(half_shape, BF), pltpu.VMEM(half_shape, BF),
                pltpu.VMEM(rows_shape, BF), pltpu.VMEM(rows_shape, BF),
                pltpu.VMEM((n_tok, width), BF), pltpu.VMEM((n_tok, width), BF),
                row, row, row, row, col, col, col, col, col, col, col, col,
                pltpu.VMEM((n_tok, n_exp), F32), pltpu.VMEM((n_tok, n_exp), F32),
                pltpu.VMEM((ep_size, n_loc, width), F32), pltpu.VMEM((ep_size, n_loc, width), F32),
                pltpu.VMEM((ep_size, n_loc, width), F32), pltpu.VMEM((n_tok, width), F32),
                pltpu.VMEM((1, n_tok), I32), pltpu.VMEM((1, n_tok), I32),
                dma((3,)), dma((3, n_loc)), dma((5,)), dma((2,)),
                dma(()), dma((n_loc,)), dma((n_loc,)), dma((n_loc,)), dma(()), dma(()), dma((n_loc,)),
                dma(()), dma((n_loc,)), dma(()), dma((n_loc,)),
                dma(()), dma((n_loc,)), dma(()), dma((n_loc,)),
                dma(()), dma((n_tok // 128,)),
                dma(()), dma(()), dma(()), dma(()), dma(()), dma(()),
            ],
            compiler_params=pltpu.CompilerParams(
                collective_id=0, has_side_effects=True, vmem_limit_bytes=67043328
            ),
        )(
            first_ids.reshape(1, n_tok), second_ids.reshape(1, n_tok), x_rows, dy_rows, w_router.T,
            w_gelu, w_lin, w_out,
        )
        act_out, grad_in, grad_router, xe, de, h, da, db = outs
        partners = [
            ((q % tp_size) * ep_size + q, (1 - q % tp_size) * ep_size + q) for q in range(ep_size)
        ]
        passed = lax.ppermute(grad_in, ("tp", "ep"), partners)
        owner = lax.axis_index("ep") % tp_size == lax.axis_index("tp")
        grad_in = jnp.where(owner, grad_in, passed)
        xe = xe.reshape(n_loc, blk, width)
        de = de.reshape(n_loc, blk, width)

        y_spec = pl.BlockSpec((n_tok // n_loc, width), lambda e: (e, 0))

        def spec(*shape):
            return pl.BlockSpec((1,) + shape, lambda e: (e, 0, 0))

        grad_wa, grad_wb, grad_wc, act_out, grad_router = pl.pallas_call(
            weight_kernel,
            name="weight_grads",
            grid=(n_loc,),
            in_specs=[spec(blk, width), spec(blk, width), spec(blk, hid), spec(blk, hid), spec(blk, hid), y_spec, spec(n_exp // n_loc, width)],
            out_specs=[spec(width, hid), spec(width, hid), spec(hid, width), y_spec, spec(n_exp // n_loc, width)],
            out_shape=[
                sds((n_loc, width, hid), F32), sds((n_loc, width, hid), F32), sds((n_loc, hid, width), F32),
                sds((n_tok, width), BF), sds((n_loc, n_exp // n_loc, width), F32),
            ],
            compiler_params=pltpu.CompilerParams(
                dimension_semantics=("arbitrary",), vmem_limit_bytes=63743328
            ),
            cost_estimate=pl.CostEstimate(
                flops=6 * n_loc * blk * width * hid, transcendentals=0,
                bytes_accessed=12 * n_loc * width * hid + 4 * n_loc * blk * width + 6 * n_loc * blk * hid,
            ),
        )(xe, de, h, da, db, act_out, grad_router.reshape(n_loc, n_exp // n_loc, width))
        return act_out, grad_in, grad_wa, grad_wb, grad_wc, grad_router.reshape(n_exp, width).T

    return jax.shard_map(
        local_step,
        mesh=mesh,
        in_specs=(P("ep", None), P(), P("ep"), P("ep"), P("ep", None, "tp"), P("ep", None, "tp"), P("ep", "tp", None), P("ep", None)),
        out_specs=(P("ep", None), P("ep", None), P("ep", None, "tp"), P("ep", None, "tp"), P("ep", "tp", None), P()),
        check_vma=False,
    )
```

```python
import functools

import jax
import jax.numpy as jnp
from jax import lax
from jax.experimental import pallas as pl
from jax.experimental.pallas import tpu as pltpu
from jax.sharding import PartitionSpec as P

BF = jnp.bfloat16
F32 = jnp.float32
I32 = jnp.int32
MESH = pl.DeviceIdType.MESH
GELU_COEF = 0.7978845608028654
AHEAD = 4
LAG = 3
Y_STEP = 4
FORWARD = 2
VIA_TP = 7
BACK_LAG = 2
EARLY = 2
NN = (((1,), (0,)), ((), ()))
NT = (((1,), (1,)), ((), ()))
TN = (((0,), (0,)), ((), ()))


def dot(a, b, dims=NN):
    return lax.dot_general(a, b, dims, preferred_element_type=F32)


def split3(v):
    hi = v.astype(BF)
    rest = v - hi.astype(F32)
    mid = rest.astype(BF)
    low = (rest - mid.astype(F32)).astype(BF)
    return hi, mid, low


def moe_kernel(
    tp_size, ep_size, cap,
    ids1_hbm, ids2_hbm, x_hbm, dy_hbm, wr_hbm, wa_hbm, wb_hbm, wc_hbm,
    y_out, dx_out, dwr_out, xe_out, de_out, h_out, da_out, db_out,
    x_v, dy_v, wr_v, wa_v, wb_v, wc_v,
    xs, ds, xr, dr, h_v, da_v, db_v, bs_v, gv_v,
    ps, pr, pdr, orr, dxr, y_v, dx_v,
    s1r, s2r, g1r, g2r, s1c, s2c, g1c, g2c, q1c, q2c, i1c, i2c, prob_v, dl_v,
    dwp, dwi, dwf, acc_v, ids1_ref, ids2_ref,
    in_sem, w_sem, out_sem, id_sem,
    xs_sem, xr_sem, xd_sem, xf_sem, xfs_sem, ds_sem, dr_sem,
    ps_sem, pr_sem, pds_sem, pdr_sem,
    os_sem, or_sem, dxs_sem, dxr_sem,
    ys_sem, yr_sem,
    rs_sem, rr_sem, fs_sem, fr_sem, gs_sem, gr_sem,
):
    k = lax.axis_index("tp")
    r = lax.axis_index("ep")
    n_loc = wa_v.shape[0]
    n_tok, width = x_v.shape
    hid = wa_v.shape[2]
    n_exp = n_loc * ep_size
    blk = ep_size * cap
    half = ep_size // tp_size
    my_place = (r % tp_size) * half + r // tp_size
    owner = (r % tp_size) == k
    other = 1 - k

    ins = [
        pltpu.make_async_copy(x_hbm, x_v, in_sem.at[0]),
        pltpu.make_async_copy(dy_hbm, dy_v, in_sem.at[1]),
        pltpu.make_async_copy(wr_hbm, wr_v, in_sem.at[2]),
    ]
    id_loads = [pltpu.make_async_copy(ids1_hbm, ids1_ref, id_sem.at[0]), pltpu.make_async_copy(ids2_hbm, ids2_ref, id_sem.at[1])]
    for c in id_loads:
        c.start()
    ins[0].start()

    def weight_copies(j):
        return [
            pltpu.make_async_copy(wa_hbm.at[j], wa_v.at[j], w_sem.at[0, j]),
            pltpu.make_async_copy(wb_hbm.at[j], wb_v.at[j], w_sem.at[1, j]),
            pltpu.make_async_copy(wc_hbm.at[j], wc_v.at[j], w_sem.at[2, j]),
        ]

    n_dev = tp_size * ep_size
    barrier = pltpu.get_barrier_semaphore()
    for d in range(1, n_dev):
        flat = (k * ep_size + r + d) % n_dev
        pl.semaphore_signal(barrier, inc=1, device_id=(flat // ep_size, flat % ep_size), device_id_type=MESH)

    for c in id_loads:
        c.wait()
    ids1 = ids1_ref[...]
    ids2 = ids2_ref[...]
    e_iota = lax.broadcasted_iota(I32, (n_exp, n_tok), 0)
    hot1 = jnp.where(ids1 == e_iota, 1.0, 0.0).astype(F32)
    hot2 = jnp.where(ids2 == e_iota, 1.0, 0.0).astype(F32)
    before = jnp.where(
        lax.broadcasted_iota(I32, (n_tok, n_tok), 0) < lax.broadcasted_iota(I32, (n_tok, n_tok), 1), 1.0, 0.0
    ).astype(BF)
    cum1 = dot(hot1.astype(BF), before)
    cum2 = dot(hot2.astype(BF), before)
    fill1 = jnp.sum(hot1, axis=1, keepdims=True)
    pos1 = jnp.sum(cum1 * hot1, axis=0, keepdims=True)
    pos2 = jnp.sum((cum2 + fill1) * hot2, axis=0, keepdims=True)

    def place(ids, pos):
        spot = (ids & (n_loc - 1)) * blk + (ids // n_loc) * cap
        return jnp.where(pos < cap, spot.astype(F32) + pos, float(n_exp * cap))

    s1r[...] = place(ids1, pos1)
    s2r[...] = place(ids2, pos2)

    def masks(j):
        spot = (lax.broadcasted_iota(I32, (blk, n_tok), 0) + j * blk).astype(F32)
        return s1r[...] == spot, s2r[...] == spot

    chip = r // 2
    chip_x = chip + 1 - 2 * (chip % 2)
    chip_y = (chip + 2) % 4
    chip_d = 3 - chip
    core = r % 2
    diag = 2 * chip_d + (k + r) % 2
    near = [2 * chip_x + core, 2 * chip_y + core, 2 * chip_x + 1 - core, 2 * chip_y + 1 - core, 2 * chip + 1 - core]
    far = [2 * chip_d + core, 2 * chip_d + 1 - core]

    def place_of(q):
        return (q % tp_size) * half + q // tp_size

    def send_row(src, dst, send_sem, recv_sem, j, q):
        pltpu.make_async_remote_copy(
            src_ref=src.at[j, q], dst_ref=dst.at[j, my_place],
            send_sem=send_sem, recv_sem=recv_sem.at[j],
            device_id=(k, q), device_id_type=MESH,
        ).start()

    def wait_recv(view, sem):
        pltpu.make_async_remote_copy(
            src_ref=view, dst_ref=view, send_sem=sem, recv_sem=sem, device_id=(k, r), device_id_type=MESH
        ).wait_recv()

    def wait_send(view, sem):
        pltpu.make_async_remote_copy(
            src_ref=view, dst_ref=view, send_sem=sem, recv_sem=sem, device_id=(k, r), device_id_type=MESH
        ).wait_send()

    def gather_x(j):
        m1, m2 = masks(j)
        pick = jnp.where(m1 | m2, 1.0, 0.0).astype(BF)
        for c in range(0, width, 512):
            rows = dot(pick, x_v[:, c:c + 512]).astype(BF)
            xs[j, :, :, c:c + 512] = rows.reshape(ep_size, cap, 512)

    def send_x(j, via_tp):
        if via_tp:
            send_row(xs, xr, xs_sem, xd_sem, j, diag)
        for q in near if via_tp else far + near:
            send_row(xs, xr, xs_sem, xr_sem, j, q)
        xr[j, my_place] = xs[j, r]

    ins[0].wait()
    ins[2].start()
    ins[1].start()

    @pl.loop(0, n_loc)
    def _(j):
        for c in weight_copies(j):
            c.start()

    @pl.loop(0, EARLY)
    def _(j):
        gather_x(j)

    pl.semaphore_wait(barrier, n_dev - 1)

    @pl.loop(0, EARLY)
    def _(j):
        send_x(j, True)

    @pl.loop(EARLY, VIA_TP)
    def _(j):
        gather_x(j)
        send_x(j, True)

    if VIA_TP < n_loc:
        @pl.loop(VIA_TP, n_loc)
        def _(j):
            gather_x(j)
            send_x(j, False)

    def column(row):
        return jnp.transpose(jnp.broadcast_to(row, (128, n_tok)))

    s1c[...] = column(s1r[...])
    s2c[...] = column(s2r[...])
    i1c[...] = column(ids1.astype(F32))
    i2c[...] = column(ids2.astype(F32))
    ins[2].wait()
    wr_hi, wr_mid, wr_low = split3(wr_v[...])
    xv = x_v[...]
    logits = dot(xv, wr_hi, NT) + (dot(xv, wr_mid, NT) + dot(xv, wr_low, NT))
    ex = jnp.exp(logits - jnp.max(logits, axis=1, keepdims=True))
    prob = ex / jnp.sum(ex, axis=1, keepdims=True)
    prob_v[...] = prob
    lane = lax.broadcasted_iota(I32, (n_tok, n_exp), 1).astype(F32)
    q1 = jnp.sum(jnp.where(i1c[:, :n_exp] == lane, prob, 0.0), axis=1, keepdims=True)
    q2 = jnp.sum(jnp.where(i2c[:, :n_exp] == lane, prob, 0.0), axis=1, keepdims=True)
    g1 = jnp.broadcast_to(q1 / (q1 + q2), (n_tok, 128))
    g2 = jnp.broadcast_to(q2 / (q1 + q2), (n_tok, 128))
    g1c[...] = g1
    g2c[...] = g2
    q1c[...] = jnp.broadcast_to(q1, (n_tok, 128))
    q2c[...] = jnp.broadcast_to(q2, (n_tok, 128))
    g1r[...] = jnp.transpose(g1)[0:1, :]
    g2r[...] = jnp.transpose(g2)[0:1, :]
    ins[1].wait()

    def build_d(j):
        m1, m2 = masks(j)
        pick = jnp.where(m1 | m2, 1.0, 0.0).astype(BF)
        gate = jnp.sum(jnp.where(m1, g1r[...], 0.0) + jnp.where(m2, g2r[...], 0.0), axis=1, keepdims=True)
        for c in range(0, width, 512):
            rows = (gate * dot(pick, dy_v[:, c:c + 512])).astype(BF)
            ds[j, :, :, c:c + 512] = rows.reshape(ep_size, cap, 512)
        for q in far + near:
            send_row(ds, dr, ds_sem, dr_sem, j, q)
        dr[j, my_place] = ds[j, r]

    def send_half(src, dst, send_sem, recv_sem, j):
        pltpu.make_async_remote_copy(
            src_ref=src.at[j, pl.ds(other * half, half)], dst_ref=dst.at[j],
            send_sem=send_sem, recv_sem=recv_sem.at[j],
            device_id=(other, r), device_id_type=MESH,
        ).start()

    def merge_and_return(src, got, got_sem, dst, send_sem, recv_sem, j):
        wait_recv(got.at[j], got_sem.at[j])
        mine = pl.ds(k * half, half)
        src[j, mine] = (src[j, mine].astype(F32) + got[j].astype(F32)).astype(BF)
        for d in range(half):
            c = (r // tp_size + d) % half
            q = tp_size * c + k

            @pl.when(q != r)
            def _():
                pltpu.make_async_remote_copy(
                    src_ref=src.at[j, k * half + c], dst_ref=dst.at[j, r],
                    send_sem=send_sem, recv_sem=recv_sem.at[j],
                    device_id=(k, q), device_id_type=MESH,
                ).start()

            @pl.when(q == r)
            def _():
                dst[j, r] = src[j, k * half + c]

    n_near = len(near)
    diag_place = place_of(diag)

    def forward_diag(j):
        wait_recv(xr.at[j, 0], xd_sem.at[j])
        pltpu.make_async_remote_copy(
            src_ref=xr.at[j, diag_place], dst_ref=xr.at[j, diag_place],
            send_sem=xfs_sem, recv_sem=xf_sem.at[j],
            device_id=(other, r), device_id_type=MESH,
        ).start()

    for i in range(FORWARD):
        forward_diag(i)

    @pl.loop(0, n_loc)
    def _(j):
        @pl.when(j >= n_loc - AHEAD)
        def _():
            build_d(j + AHEAD - n_loc)

        @pl.when(j + FORWARD < VIA_TP)
        def _():
            forward_diag(j + FORWARD)

        for c in weight_copies(j):
            c.wait()

        @pl.when(j < VIA_TP)
        def _():
            wait_recv(xr.at[j, pl.ds(0, n_near)], xr_sem.at[j])
            wait_recv(xr.at[j, 0], xf_sem.at[j])

        if VIA_TP < n_loc:
            @pl.when(j >= VIA_TP)
            def _():
                wait_recv(xr.at[j, pl.ds(0, ep_size - 1)], xr_sem.at[j])

        rows = xr[j].reshape(blk, width)
        pa = dot(rows, wa_v[j])
        pb = dot(rows, wb_v[j])
        th = jnp.tanh(GELU_COEF * (pa + 0.044715 * pa * pa * pa))
        gv = 0.5 * pa * (1.0 + th)
        slope = 0.5 * (1.0 + th) + 0.5 * pa * (1.0 - th * th) * GELU_COEF * (1.0 + 0.134145 * pa * pa)
        gv_v[j] = gv
        bs_v[j] = pb * slope
        hidden = (gv * pb).astype(BF)
        h_v[j] = hidden
        for c in range(0, width, 512):
            ps[j, :, :, c:c + 512] = dot(hidden, wc_v[j, :, c:c + 512]).astype(BF).reshape(ep_size, cap, 512)
        send_half(ps, pr, ps_sem, pr_sem, j)

        @pl.when(j >= LAG)
        def _():
            merge_and_return(ps, pr, pr_sem, orr, os_sem, or_sem, j - LAG)

    tb = 128
    n_tb = n_tok // tb

    def spots(col, toks):
        lanes = lax.broadcasted_iota(I32, (tb, 128), 1).astype(F32)
        base = col[toks, :]
        return jnp.concatenate([base == lanes + float(u * 128) for u in range(n_exp * cap // 128)], axis=1)

    def ship(buf, t, send_sem, recv_sem):
        toks = pl.ds(pl.multiple_of(t * tb, tb), tb)
        pltpu.make_async_remote_copy(
            src_ref=buf.at[toks], dst_ref=buf.at[toks], send_sem=send_sem, recv_sem=recv_sem.at[t],
            device_id=(other, r), device_id_type=MESH,
        ).start()

    def combine_y(t):
        toks = pl.ds(pl.multiple_of(t * tb, tb), tb)
        pick1 = jnp.where(spots(s1c, toks), 1.0, 0.0).astype(BF)
        pick2 = jnp.where(spots(s2c, toks), 1.0, 0.0).astype(BF)
        dg1 = jnp.zeros((tb, 1), F32)
        dg2 = jnp.zeros((tb, 1), F32)
        ga = g1c[toks, 0:1]
        gb = g2c[toks, 0:1]
        for c in range(0, width, 512):
            rows = orr[:, :, :, c:c + 512].reshape(n_exp * cap, 512)
            o1 = dot(pick1, rows)
            o2 = dot(pick2, rows)
            y_v[toks, c:c + 512] = (ga * o1 + gb * o2).astype(BF)
            dyf = dy_v[toks, c:c + 512].astype(F32)
            dg1 = dg1 + jnp.sum(dyf * o1, axis=1, keepdims=True)
            dg2 = dg2 + jnp.sum(dyf * o2, axis=1, keepdims=True)
        qa = q1c[toks, 0:1]
        qb = q2c[toks, 0:1]
        shared = dg1 * ga + dg2 * gb
        dq1 = (dg1 - shared) / (qa + qb)
        dq2 = (dg2 - shared) / (qa + qb)
        centre = dq1 * qa + dq2 * qb
        lanes = lax.broadcasted_iota(I32, (tb, n_exp), 1).astype(F32)
        pull = jnp.where(i1c[toks, :n_exp] == lanes, dq1, 0.0) + jnp.where(i2c[toks, :n_exp] == lanes, dq2, 0.0)
        dl_v[toks, :] = prob_v[toks, :] * (pull - centre)

    def router_parts():
        d_hi, d_mid, d_low = split3(dl_v[...])
        for c in range(0, width, 512):
            xc = x_v[:, c:c + 512]
            piece = dot(d_hi, xc, TN) + (dot(d_mid, xc, TN) + dot(d_low, xc, TN))
            dwp[:, :, c:c + 512] = piece.reshape(ep_size, n_loc, 512)
        for d in range(1, ep_size):
            q = (r + d) % ep_size
            pltpu.make_async_remote_copy(
                src_ref=dwp.at[q], dst_ref=dwi.at[r], send_sem=rs_sem, recv_sem=rr_sem,
                device_id=(q % tp_size, q), device_id_type=MESH,
            ).start()
        dwi[r] = dwp[r]

    def router_sum():
        wait_recv(dwi.at[pl.ds(0, ep_size - 1)], rr_sem)
        total = dwi[0]
        for q in range(1, ep_size):
            total = total + dwi[q]
        dwf[r] = total
        for d in range(1, ep_size):
            q = (r + d) % ep_size
            pltpu.make_async_remote_copy(
                src_ref=dwf.at[r], dst_ref=dwf.at[r], send_sem=fs_sem, recv_sem=fr_sem,
                device_id=(q % tp_size, q), device_id_type=MESH,
            ).start()

    wait_send(xs.at[pl.ds(0, VIA_TP), pl.ds(0, n_near + 1)], xs_sem)
    if VIA_TP < n_loc:
        wait_send(xs.at[pl.ds(VIA_TP, n_loc - VIA_TP), pl.ds(0, ep_size - 1)], xs_sem)
    @pl.loop(0, n_loc)
    def _(j):
        @pl.when(j + AHEAD < n_loc)
        def _():
            build_d(j + AHEAD)

        wait_recv(dr.at[j, pl.ds(0, ep_size - 1)], dr_sem.at[j])
        rows = dr[j].reshape(blk, width)
        dh = dot(rows, wc_v[j], NT)
        da = (dh * bs_v[j]).astype(BF)
        db = (dh * gv_v[j]).astype(BF)
        da_v[j] = da
        db_v[j] = db
        for c in range(0, width, 512):
            part = dot(da, wa_v[j, c:c + 512, :], NT) + dot(db, wb_v[j, c:c + 512, :], NT)
            xs[j, :, :, c:c + 512] = part.astype(BF).reshape(ep_size, cap, 512)
        send_half(xs, pdr, pds_sem, pdr_sem, j)

        @pl.when(j == 0)
        def _():
            for i in range(LAG):
                merge_and_return(ps, pr, pr_sem, orr, os_sem, or_sem, n_loc - LAG + i)

        @pl.when(j >= BACK_LAG)
        def _():
            merge_and_return(xs, pdr, pdr_sem, dxr, dxs_sem, dxr_sem, j - BACK_LAG)

        @pl.when(owner & (j == Y_STEP))
        def _():
            @pl.loop(0, n_loc)
            def _(i):
                wait_recv(orr.at[i, pl.ds(0, ep_size - 1)], or_sem.at[i])

        @pl.when(owner & (j >= Y_STEP) & (j < Y_STEP + n_tb // 2))
        def _():
            t0 = 2 * (j - Y_STEP)

            @pl.loop(t0, t0 + 2)
            def _(t):
                combine_y(t)

            ship(y_v, j - Y_STEP, ys_sem, yr_sem)

        @pl.when(owner & (j == Y_STEP + n_tb // 2 - 1))
        def _():
            router_parts()

    outs = [
        pltpu.make_async_copy(xr, xe_out, out_sem.at[0]),
        pltpu.make_async_copy(dr, de_out, out_sem.at[1]),
        pltpu.make_async_copy(h_v, h_out, out_sem.at[2]),
        pltpu.make_async_copy(da_v, da_out, out_sem.at[3]),
        pltpu.make_async_copy(db_v, db_out, out_sem.at[4]),
    ]
    for c in outs[:3]:
        c.start()

    split = n_loc - 2

    def pick_both(t):
        toks = pl.ds(pl.multiple_of(t * tb, tb), tb)
        return toks, jnp.where(spots(s1c, toks) | spots(s2c, toks), 1.0, 0.0).astype(BF)

    def sum_first(t):
        toks, pick = pick_both(t)
        dl = dl_v[toks, :]
        for c in range(0, width, 512):
            rows = dxr[0:split, :, :, c:c + 512].reshape(split * blk, 512)
            router = lax.dot_general(
                dl, wr_v[:, c:c + 512], NN, precision=lax.Precision.HIGHEST, preferred_element_type=F32
            )
            acc_v[toks, c:c + 512] = dot(pick[:, :split * blk], rows) + router

    def sum_last(t):
        toks, pick = pick_both(t)
        for c in range(0, width, 512):
            rows = dxr[split:n_loc, :, :, c:c + 512].reshape((n_loc - split) * blk, 512)
            dx_v[toks, c:c + 512] = (acc_v[toks, c:c + 512] + dot(pick[:, split * blk:], rows)).astype(BF)
        pltpu.make_async_copy(dx_v.at[toks], dx_out.at[toks], in_sem.at[1]).start()

    for c in outs[3:]:
        c.start()

    @pl.when(owner)
    def _():
        ship(y_v, n_tb - 2, ys_sem, yr_sem)

    for i in range(BACK_LAG - 1):
        merge_and_return(xs, pdr, pdr_sem, dxr, dxs_sem, dxr_sem, n_loc - BACK_LAG + i)

    @pl.when(owner)
    def _():
        router_sum()
        ship(y_v, n_tb - 1, ys_sem, yr_sem)
        pltpu.make_async_copy(y_v, y_out, in_sem.at[0]).start()

    merge_and_return(xs, pdr, pdr_sem, dxr, dxs_sem, dxr_sem, n_loc - 1)

    @pl.when(owner)
    def _():
        @pl.loop(0, split)
        def _(j):
            wait_recv(dxr.at[j, pl.ds(0, ep_size - 1)], dxr_sem.at[j])

        @pl.loop(0, n_tb)
        def _(t):
            sum_first(t)

        wait_recv(dwf.at[pl.ds(0, ep_size - 1)], fr_sem)
        pltpu.make_async_remote_copy(
            src_ref=dwf, dst_ref=dwf, send_sem=gs_sem, recv_sem=gr_sem,
            device_id=(k, 2 * chip + 1 - core), device_id_type=MESH,
        ).start()

        @pl.loop(split, n_loc)
        def _(j):
            wait_recv(dxr.at[j, pl.ds(0, ep_size - 1)], dxr_sem.at[j])

        @pl.loop(0, n_tb)
        def _(t):
            sum_last(t)

        wait_send(dwp.at[pl.ds(0, ep_size - 1)], rs_sem)
        wait_send(dwf.at[pl.ds(0, ep_size - 1)], fs_sem)
        wait_send(dwf, gs_sem)
        wait_send(y_v, ys_sem)
        wait_send(orr.at[:, pl.ds(0, half - 1)], os_sem)
        wait_send(dxr.at[:, pl.ds(0, half - 1)], dxs_sem)

    @pl.when(jnp.logical_not(owner))
    def _():
        dx_v[...] = jnp.zeros_like(dx_v)
        pltpu.make_async_copy(dx_v, dx_out, in_sem.at[1]).start()
        for t in range(n_tb):
            toks = pl.ds(t * tb, tb)
            wait_recv(y_v.at[toks], yr_sem.at[t])
            pltpu.make_async_copy(y_v.at[toks], y_out.at[toks], in_sem.at[0]).start()
        wait_recv(dwf, gr_sem)
        wait_send(orr.at[:, pl.ds(0, half)], os_sem)
        wait_send(dxr.at[:, pl.ds(0, half)], dxs_sem)

    finals = [
        pltpu.make_async_copy(dwf, dwr_out, in_sem.at[2]),
        pltpu.make_async_copy(y_v, y_out, in_sem.at[0]),
        pltpu.make_async_copy(dx_v, dx_out, in_sem.at[1]),
    ]
    finals[0].start()
    wait_send(ds.at[:, pl.ds(0, ep_size - 1)], ds_sem)
    wait_send(xr.at[pl.ds(0, VIA_TP), 0], xfs_sem)
    wait_send(ps.at[:, pl.ds(0, half)], ps_sem)
    wait_send(xs.at[:, pl.ds(0, half)], pds_sem)
    for c in outs + finals:
        c.wait()


def weight_kernel(xe, de, h, da, db, y, dwr, ga_out, gb_out, gc_out, y_out, dwr_out):
    y_out[...] = y[...]
    dwr_out[...] = dwr[...]
    rows = xe[0]
    ga_out[0] = dot(rows, da[0], TN)
    gb_out[0] = dot(rows, db[0], TN)
    gc_out[0] = dot(h[0], de[0], TN)


def solution(mesh):
    tp_size = mesh.shape["tp"]
    ep_size = mesh.shape["ep"]

    def local_step(x_rows, w_router, first_ids, second_ids, w_gelu, w_lin, w_out, dy_rows):
        n_tok, width = x_rows.shape
        n_exp = w_router.shape[1]
        n_loc, _, hid = w_gelu.shape
        cap = 2 * n_tok // n_exp
        blk = ep_size * cap
        half = ep_size // tp_size
        dma = pltpu.SemaphoreType.DMA
        any_spec = pl.BlockSpec(memory_space=pl.ANY)
        sds = jax.ShapeDtypeStruct
        rows_shape = (n_loc, ep_size, cap, width)
        half_shape = (n_loc, half, cap, width)
        hid_shape = (n_loc, blk, hid)
        col = pltpu.VMEM((n_tok, 128), F32)
        row = pltpu.VMEM((1, n_tok), F32)
        outs = pl.pallas_call(
            functools.partial(moe_kernel, tp_size, ep_size, cap),
            name="moe",
            in_specs=[any_spec] * 8,
            out_specs=[any_spec] * 8,
            out_shape=[
                sds((n_tok, width), BF), sds((n_tok, width), BF), sds((ep_size, n_loc, width), F32),
                sds(rows_shape, BF), sds(rows_shape, BF), sds(hid_shape, BF), sds(hid_shape, BF), sds(hid_shape, BF),
            ],
            scratch_shapes=[
                pltpu.VMEM((n_tok, width), BF), pltpu.VMEM((n_tok, width), BF), pltpu.VMEM((n_exp, width), F32),
                pltpu.VMEM((n_loc, width, hid), BF), pltpu.VMEM((n_loc, width, hid), BF), pltpu.VMEM((n_loc, hid, width), BF),
                pltpu.VMEM(rows_shape, BF), pltpu.VMEM(rows_shape, BF), pltpu.VMEM(rows_shape, BF), pltpu.VMEM(rows_shape, BF),
                pltpu.VMEM(hid_shape, BF), pltpu.VMEM(hid_shape, BF), pltpu.VMEM(hid_shape, BF),
                pltpu.VMEM(hid_shape, F32), pltpu.VMEM(hid_shape, F32),
                pltpu.VMEM(rows_shape, BF), pltpu.VMEM(half_shape, BF), pltpu.VMEM(half_shape, BF),
                pltpu.VMEM(rows_shape, BF), pltpu.VMEM(rows_shape, BF),
                pltpu.VMEM((n_tok, width), BF), pltpu.VMEM((n_tok, width), BF),
                row, row, row, row, col, col, col, col, col, col, col, col,
                pltpu.VMEM((n_tok, n_exp), F32), pltpu.VMEM((n_tok, n_exp), F32),
                pltpu.VMEM((ep_size, n_loc, width), F32), pltpu.VMEM((ep_size, n_loc, width), F32),
                pltpu.VMEM((ep_size, n_loc, width), F32), pltpu.VMEM((n_tok, width), F32),
                pltpu.VMEM((1, n_tok), I32), pltpu.VMEM((1, n_tok), I32),
                dma((3,)), dma((3, n_loc)), dma((5,)), dma((2,)),
                dma(()), dma((n_loc,)), dma((n_loc,)), dma((n_loc,)), dma(()), dma(()), dma((n_loc,)),
                dma(()), dma((n_loc,)), dma(()), dma((n_loc,)),
                dma(()), dma((n_loc,)), dma(()), dma((n_loc,)),
                dma(()), dma((n_tok // 128,)),
                dma(()), dma(()), dma(()), dma(()), dma(()), dma(()),
            ],
            compiler_params=pltpu.CompilerParams(
                collective_id=0, has_side_effects=True, vmem_limit_bytes=67043328
            ),
        )(
            first_ids.reshape(1, n_tok), second_ids.reshape(1, n_tok), x_rows, dy_rows, w_router.T,
            w_gelu, w_lin, w_out,
        )
        act_out, grad_in, grad_router, xe, de, h, da, db = outs
        partners = [
            ((q % tp_size) * ep_size + q, (1 - q % tp_size) * ep_size + q) for q in range(ep_size)
        ]
        passed = lax.ppermute(grad_in, ("tp", "ep"), partners)
        owner = lax.axis_index("ep") % tp_size == lax.axis_index("tp")
        grad_in = jnp.where(owner, grad_in, passed)
        xe = xe.reshape(n_loc, blk, width)
        de = de.reshape(n_loc, blk, width)

        y_spec = pl.BlockSpec((n_tok // n_loc, width), lambda e: (e, 0))

        def spec(*shape):
            return pl.BlockSpec((1,) + shape, lambda e: (e, 0, 0))

        grad_wa, grad_wb, grad_wc, act_out, grad_router = pl.pallas_call(
            weight_kernel,
            name="weight_grads",
            grid=(n_loc,),
            in_specs=[spec(blk, width), spec(blk, width), spec(blk, hid), spec(blk, hid), spec(blk, hid), y_spec, spec(n_exp // n_loc, width)],
            out_specs=[spec(width, hid), spec(width, hid), spec(hid, width), y_spec, spec(n_exp // n_loc, width)],
            out_shape=[
                sds((n_loc, width, hid), F32), sds((n_loc, width, hid), F32), sds((n_loc, hid, width), F32),
                sds((n_tok, width), BF), sds((n_loc, n_exp // n_loc, width), F32),
            ],
            compiler_params=pltpu.CompilerParams(
                dimension_semantics=("arbitrary",), vmem_limit_bytes=63743328
            ),
            cost_estimate=pl.CostEstimate(
                flops=6 * n_loc * blk * width * hid, transcendentals=0,
                bytes_accessed=12 * n_loc * width * hid + 4 * n_loc * blk * width + 6 * n_loc * blk * hid,
            ),
        )(xe, de, h, da, db, act_out, grad_router.reshape(n_loc, n_exp // n_loc, width))
        return act_out, grad_in, grad_wa, grad_wb, grad_wc, grad_router.reshape(n_exp, width).T

    return jax.shard_map(
        local_step,
        mesh=mesh,
        in_specs=(P("ep", None), P(), P("ep"), P("ep"), P("ep", None, "tp"), P("ep", None, "tp"), P("ep", "tp", None), P("ep", None)),
        out_specs=(P("ep", None), P("ep", None), P("ep", None, "tp"), P("ep", None, "tp"), P("ep", "tp", None), P()),
        check_vma=False,
    )
```

```python
import functools

import jax
import jax.numpy as jnp
from jax import lax
from jax.experimental import pallas as pl
from jax.experimental.pallas import tpu as pltpu
from jax.sharding import PartitionSpec as P

BF = jnp.bfloat16
F32 = jnp.float32
I32 = jnp.int32
MESH = pl.DeviceIdType.MESH
GELU_COEF = 0.7978845608028654
AHEAD = 4
LAG = 3
Y_STEP = 4
FORWARD = 2
VIA_TP = 7
BACK_LAG = 2
EARLY = 2
NN = (((1,), (0,)), ((), ()))
NT = (((1,), (1,)), ((), ()))
TN = (((0,), (0,)), ((), ()))


def dot(a, b, dims=NN):
    return lax.dot_general(a, b, dims, preferred_element_type=F32)


def split3(v):
    hi = v.astype(BF)
    rest = v - hi.astype(F32)
    mid = rest.astype(BF)
    low = (rest - mid.astype(F32)).astype(BF)
    return hi, mid, low


def moe_kernel(
    tp_size, ep_size, cap,
    ids1_hbm, ids2_hbm, x_hbm, dy_hbm, wr_hbm, wa_hbm, wb_hbm, wc_hbm,
    y_out, dx_out, dwr_out, xe_out, de_out, h_out, da_out, db_out,
    x_v, dy_v, wr_v, wa_v, wb_v, wc_v,
    xs, ds, xr, dr, h_v, da_v, db_v, bs_v, gv_v,
    ps, pr, pdr, orr, dxr, y_v, dx_v,
    s1r, s2r, g1r, g2r, s1c, s2c, g1c, g2c, q1c, q2c, i1c, i2c, prob_v, dl_v,
    dwp, dwi, dwf, acc_v, ids1_ref, ids2_ref,
    in_sem, w_sem, out_sem, id_sem,
    xs_sem, xr_sem, xd_sem, xf_sem, xfs_sem, ds_sem, dr_sem,
    ps_sem, pr_sem, pds_sem, pdr_sem,
    os_sem, or_sem, dxs_sem, dxr_sem,
    ys_sem, yr_sem,
    rs_sem, rr_sem, fs_sem, fr_sem, gs_sem, gr_sem,
):
    k = lax.axis_index("tp")
    r = lax.axis_index("ep")
    n_loc = wa_v.shape[0]
    n_tok, width = x_v.shape
    hid = wa_v.shape[2]
    n_exp = n_loc * ep_size
    blk = ep_size * cap
    half = ep_size // tp_size
    my_place = (r % tp_size) * half + r // tp_size
    owner = (r % tp_size) == k
    other = 1 - k

    ins = [
        pltpu.make_async_copy(x_hbm, x_v, in_sem.at[0]),
        pltpu.make_async_copy(dy_hbm, dy_v, in_sem.at[1]),
        pltpu.make_async_copy(wr_hbm, wr_v, in_sem.at[2]),
    ]
    id_loads = [pltpu.make_async_copy(ids1_hbm, ids1_ref, id_sem.at[0]), pltpu.make_async_copy(ids2_hbm, ids2_ref, id_sem.at[1])]
    for c in id_loads:
        c.start()
    ins[0].start()

    def weight_copies(j):
        return [
            pltpu.make_async_copy(wa_hbm.at[j], wa_v.at[j], w_sem.at[0, j]),
            pltpu.make_async_copy(wb_hbm.at[j], wb_v.at[j], w_sem.at[1, j]),
            pltpu.make_async_copy(wc_hbm.at[j], wc_v.at[j], w_sem.at[2, j]),
        ]

    n_dev = tp_size * ep_size
    barrier = pltpu.get_barrier_semaphore()
    for d in range(1, n_dev):
        flat = (k * ep_size + r + d) % n_dev
        pl.semaphore_signal(barrier, inc=1, device_id=(flat // ep_size, flat % ep_size), device_id_type=MESH)

    for c in id_loads:
        c.wait()
    ids1 = ids1_ref[...]
    ids2 = ids2_ref[...]
    e_iota = lax.broadcasted_iota(I32, (n_exp, n_tok), 0)
    hot1 = jnp.where(ids1 == e_iota, 1.0, 0.0).astype(F32)
    hot2 = jnp.where(ids2 == e_iota, 1.0, 0.0).astype(F32)
    before = jnp.where(
        lax.broadcasted_iota(I32, (n_tok, n_tok), 0) < lax.broadcasted_iota(I32, (n_tok, n_tok), 1), 1.0, 0.0
    ).astype(BF)
    cum1 = dot(hot1.astype(BF), before)
    cum2 = dot(hot2.astype(BF), before)
    fill1 = jnp.sum(hot1, axis=1, keepdims=True)
    pos1 = jnp.sum(cum1 * hot1, axis=0, keepdims=True)
    pos2 = jnp.sum((cum2 + fill1) * hot2, axis=0, keepdims=True)

    def place(ids, pos):
        spot = (ids & (n_loc - 1)) * blk + (ids // n_loc) * cap
        return jnp.where(pos < cap, spot.astype(F32) + pos, float(n_exp * cap))

    s1r[...] = place(ids1, pos1)
    s2r[...] = place(ids2, pos2)

    def masks(j):
        spot = (lax.broadcasted_iota(I32, (blk, n_tok), 0) + j * blk).astype(F32)
        return s1r[...] == spot, s2r[...] == spot

    chip = r // 2
    chip_x = chip + 1 - 2 * (chip % 2)
    chip_y = (chip + 2) % 4
    chip_d = 3 - chip
    core = r % 2
    diag = 2 * chip_d + (k + r) % 2
    near = [2 * chip_x + core, 2 * chip_y + core, 2 * chip_x + 1 - core, 2 * chip_y + 1 - core, 2 * chip + 1 - core]
    far = [2 * chip_d + core, 2 * chip_d + 1 - core]

    def place_of(q):
        return (q % tp_size) * half + q // tp_size

    def send_row(src, dst, send_sem, recv_sem, j, q):
        pltpu.make_async_remote_copy(
            src_ref=src.at[j, q], dst_ref=dst.at[j, my_place],
            send_sem=send_sem, recv_sem=recv_sem.at[j],
            device_id=(k, q), device_id_type=MESH,
        ).start()

    def wait_recv(view, sem):
        pltpu.make_async_remote_copy(
            src_ref=view, dst_ref=view, send_sem=sem, recv_sem=sem, device_id=(k, r), device_id_type=MESH
        ).wait_recv()

    def wait_send(view, sem):
        pltpu.make_async_remote_copy(
            src_ref=view, dst_ref=view, send_sem=sem, recv_sem=sem, device_id=(k, r), device_id_type=MESH
        ).wait_send()

    def gather_x(j):
        m1, m2 = masks(j)
        pick = jnp.where(m1 | m2, 1.0, 0.0).astype(BF)
        for c in range(0, width, 512):
            rows = dot(pick, x_v[:, c:c + 512]).astype(BF)
            xs[j, :, :, c:c + 512] = rows.reshape(ep_size, cap, 512)

    def send_x(j, via_tp):
        if via_tp:
            send_row(xs, xr, xs_sem, xd_sem, j, diag)
        for q in near if via_tp else far + near:
            send_row(xs, xr, xs_sem, xr_sem, j, q)
        xr[j, my_place] = xs[j, r]

    ins[0].wait()
    ins[2].start()
    ins[1].start()

    @pl.loop(0, n_loc)
    def _(j):
        for c in weight_copies(j):
            c.start()

    @pl.loop(0, EARLY)
    def _(j):
        gather_x(j)

    pl.semaphore_wait(barrier, n_dev - 1)

    @pl.loop(0, EARLY)
    def _(j):
        send_x(j, True)

    @pl.loop(EARLY, VIA_TP)
    def _(j):
        gather_x(j)
        send_x(j, True)

    if VIA_TP < n_loc:
        @pl.loop(VIA_TP, n_loc)
        def _(j):
            gather_x(j)
            send_x(j, False)

    def column(row):
        return jnp.transpose(jnp.broadcast_to(row, (128, n_tok)))

    s1c[...] = column(s1r[...])
    s2c[...] = column(s2r[...])
    i1c[...] = column(ids1.astype(F32))
    i2c[...] = column(ids2.astype(F32))
    ins[2].wait()
    wr_hi, wr_mid, wr_low = split3(wr_v[...])
    xv = x_v[...]
    logits = dot(xv, wr_hi, NT) + (dot(xv, wr_mid, NT) + dot(xv, wr_low, NT))
    ex = jnp.exp(logits - jnp.max(logits, axis=1, keepdims=True))
    prob = ex / jnp.sum(ex, axis=1, keepdims=True)
    prob_v[...] = prob
    lane = lax.broadcasted_iota(I32, (n_tok, n_exp), 1).astype(F32)
    q1 = jnp.sum(jnp.where(i1c[:, :n_exp] == lane, prob, 0.0), axis=1, keepdims=True)
    q2 = jnp.sum(jnp.where(i2c[:, :n_exp] == lane, prob, 0.0), axis=1, keepdims=True)
    g1 = jnp.broadcast_to(q1 / (q1 + q2), (n_tok, 128))
    g2 = jnp.broadcast_to(q2 / (q1 + q2), (n_tok, 128))
    g1c[...] = g1
    g2c[...] = g2
    q1c[...] = jnp.broadcast_to(q1, (n_tok, 128))
    q2c[...] = jnp.broadcast_to(q2, (n_tok, 128))
    g1r[...] = jnp.transpose(g1)[0:1, :]
    g2r[...] = jnp.transpose(g2)[0:1, :]
    ins[1].wait()

    def build_d(j):
        m1, m2 = masks(j)
        pick = jnp.where(m1 | m2, 1.0, 0.0).astype(BF)
        gate = jnp.sum(jnp.where(m1, g1r[...], 0.0) + jnp.where(m2, g2r[...], 0.0), axis=1, keepdims=True)
        for c in range(0, width, 512):
            rows = (gate * dot(pick, dy_v[:, c:c + 512])).astype(BF)
            ds[j, :, :, c:c + 512] = rows.reshape(ep_size, cap, 512)
        for q in far + near:
            send_row(ds, dr, ds_sem, dr_sem, j, q)
        dr[j, my_place] = ds[j, r]

    def send_half(src, dst, send_sem, recv_sem, j):
        pltpu.make_async_remote_copy(
            src_ref=src.at[j, pl.ds(other * half, half)], dst_ref=dst.at[j],
            send_sem=send_sem, recv_sem=recv_sem.at[j],
            device_id=(other, r), device_id_type=MESH,
        ).start()

    def merge_and_return(src, got, got_sem, dst, send_sem, recv_sem, j):
        wait_recv(got.at[j], got_sem.at[j])
        mine = pl.ds(k * half, half)
        src[j, mine] = (src[j, mine].astype(F32) + got[j].astype(F32)).astype(BF)
        for d in range(half):
            c = (r // tp_size + d) % half
            q = tp_size * c + k

            @pl.when(q != r)
            def _():
                pltpu.make_async_remote_copy(
                    src_ref=src.at[j, k * half + c], dst_ref=dst.at[j, r],
                    send_sem=send_sem, recv_sem=recv_sem.at[j],
                    device_id=(k, q), device_id_type=MESH,
                ).start()

            @pl.when(q == r)
            def _():
                dst[j, r] = src[j, k * half + c]

    n_near = len(near)
    diag_place = place_of(diag)

    def forward_diag(j):
        wait_recv(xr.at[j, 0], xd_sem.at[j])
        pltpu.make_async_remote_copy(
            src_ref=xr.at[j, diag_place], dst_ref=xr.at[j, diag_place],
            send_sem=xfs_sem, recv_sem=xf_sem.at[j],
            device_id=(other, r), device_id_type=MESH,
        ).start()

    for i in range(FORWARD):
        forward_diag(i)

    @pl.loop(0, n_loc)
    def _(j):
        @pl.when(j >= n_loc - AHEAD)
        def _():
            build_d(j + AHEAD - n_loc)

        @pl.when(j + FORWARD < VIA_TP)
        def _():
            forward_diag(j + FORWARD)

        for c in weight_copies(j):
            c.wait()

        @pl.when(j < VIA_TP)
        def _():
            wait_recv(xr.at[j, pl.ds(0, n_near)], xr_sem.at[j])
            wait_recv(xr.at[j, 0], xf_sem.at[j])

        if VIA_TP < n_loc:
            @pl.when(j >= VIA_TP)
            def _():
                wait_recv(xr.at[j, pl.ds(0, ep_size - 1)], xr_sem.at[j])

        rows = xr[j].reshape(blk, width)
        pa = dot(rows, wa_v[j])
        pb = dot(rows, wb_v[j])
        th = jnp.tanh(GELU_COEF * (pa + 0.044715 * pa * pa * pa))
        gv = 0.5 * pa * (1.0 + th)
        slope = 0.5 * (1.0 + th) + 0.5 * pa * (1.0 - th * th) * GELU_COEF * (1.0 + 0.134145 * pa * pa)
        gv_v[j] = gv
        bs_v[j] = pb * slope
        hidden = (gv * pb).astype(BF)
        h_v[j] = hidden
        for c in range(0, width, 512):
            ps[j, :, :, c:c + 512] = dot(hidden, wc_v[j, :, c:c + 512]).astype(BF).reshape(ep_size, cap, 512)
        send_half(ps, pr, ps_sem, pr_sem, j)

        @pl.when(j >= LAG)
        def _():
            merge_and_return(ps, pr, pr_sem, orr, os_sem, or_sem, j - LAG)

    tb = 128
    n_tb = n_tok // tb

    def spots(col, toks):
        lanes = lax.broadcasted_iota(I32, (tb, 128), 1).astype(F32)
        base = col[toks, :]
        return jnp.concatenate([base == lanes + float(u * 128) for u in range(n_exp * cap // 128)], axis=1)

    def ship(buf, t, send_sem, recv_sem):
        toks = pl.ds(pl.multiple_of(t * tb, tb), tb)
        pltpu.make_async_remote_copy(
            src_ref=buf.at[toks], dst_ref=buf.at[toks], send_sem=send_sem, recv_sem=recv_sem.at[t],
            device_id=(other, r), device_id_type=MESH,
        ).start()

    def combine_y(t):
        toks = pl.ds(pl.multiple_of(t * tb, tb), tb)
        pick1 = jnp.where(spots(s1c, toks), 1.0, 0.0).astype(BF)
        pick2 = jnp.where(spots(s2c, toks), 1.0, 0.0).astype(BF)
        dg1 = jnp.zeros((tb, 1), F32)
        dg2 = jnp.zeros((tb, 1), F32)
        ga = g1c[toks, 0:1]
        gb = g2c[toks, 0:1]
        for c in range(0, width, 512):
            rows = orr[:, :, :, c:c + 512].reshape(n_exp * cap, 512)
            o1 = dot(pick1, rows)
            o2 = dot(pick2, rows)
            y_v[toks, c:c + 512] = (ga * o1 + gb * o2).astype(BF)
            dyf = dy_v[toks, c:c + 512].astype(F32)
            dg1 = dg1 + jnp.sum(dyf * o1, axis=1, keepdims=True)
            dg2 = dg2 + jnp.sum(dyf * o2, axis=1, keepdims=True)
        qa = q1c[toks, 0:1]
        qb = q2c[toks, 0:1]
        shared = dg1 * ga + dg2 * gb
        dq1 = (dg1 - shared) / (qa + qb)
        dq2 = (dg2 - shared) / (qa + qb)
        centre = dq1 * qa + dq2 * qb
        lanes = lax.broadcasted_iota(I32, (tb, n_exp), 1).astype(F32)
        pull = jnp.where(i1c[toks, :n_exp] == lanes, dq1, 0.0) + jnp.where(i2c[toks, :n_exp] == lanes, dq2, 0.0)
        dl_v[toks, :] = prob_v[toks, :] * (pull - centre)

    def router_parts():
        d_hi, d_mid, d_low = split3(dl_v[...])
        for c in range(0, width, 512):
            xc = x_v[:, c:c + 512]
            piece = dot(d_hi, xc, TN) + (dot(d_mid, xc, TN) + dot(d_low, xc, TN))
            dwp[:, :, c:c + 512] = piece.reshape(ep_size, n_loc, 512)
        for d in range(1, ep_size):
            q = (r + d) % ep_size
            pltpu.make_async_remote_copy(
                src_ref=dwp.at[q], dst_ref=dwi.at[r], send_sem=rs_sem, recv_sem=rr_sem,
                device_id=(q % tp_size, q), device_id_type=MESH,
            ).start()
        dwi[r] = dwp[r]

    def router_sum():
        wait_recv(dwi.at[pl.ds(0, ep_size - 1)], rr_sem)
        total = dwi[0]
        for q in range(1, ep_size):
            total = total + dwi[q]
        dwf[r] = total
        for d in range(1, ep_size):
            q = (r + d) % ep_size
            pltpu.make_async_remote_copy(
                src_ref=dwf.at[r], dst_ref=dwf.at[r], send_sem=fs_sem, recv_sem=fr_sem,
                device_id=(q % tp_size, q), device_id_type=MESH,
            ).start()

    wait_send(xs.at[pl.ds(0, VIA_TP), pl.ds(0, n_near + 1)], xs_sem)
    if VIA_TP < n_loc:
        wait_send(xs.at[pl.ds(VIA_TP, n_loc - VIA_TP), pl.ds(0, ep_size - 1)], xs_sem)
    @pl.loop(0, n_loc)
    def _(j):
        @pl.when(j + AHEAD < n_loc)
        def _():
            build_d(j + AHEAD)

        wait_recv(dr.at[j, pl.ds(0, ep_size - 1)], dr_sem.at[j])
        rows = dr[j].reshape(blk, width)
        dh = dot(rows, wc_v[j], NT)
        da = (dh * bs_v[j]).astype(BF)
        db = (dh * gv_v[j]).astype(BF)
        da_v[j] = da
        db_v[j] = db
        for c in range(0, width, 512):
            part = dot(da, wa_v[j, c:c + 512, :], NT) + dot(db, wb_v[j, c:c + 512, :], NT)
            xs[j, :, :, c:c + 512] = part.astype(BF).reshape(ep_size, cap, 512)
        send_half(xs, pdr, pds_sem, pdr_sem, j)

        @pl.when(j == 0)
        def _():
            for i in range(LAG):
                merge_and_return(ps, pr, pr_sem, orr, os_sem, or_sem, n_loc - LAG + i)

        @pl.when(j >= BACK_LAG)
        def _():
            merge_and_return(xs, pdr, pdr_sem, dxr, dxs_sem, dxr_sem, j - BACK_LAG)

        @pl.when(owner & (j == Y_STEP))
        def _():
            @pl.loop(0, n_loc)
            def _(i):
                wait_recv(orr.at[i, pl.ds(0, ep_size - 1)], or_sem.at[i])

        @pl.when(owner & (j >= Y_STEP) & (j < Y_STEP + n_tb // 2))
        def _():
            t0 = 2 * (j - Y_STEP)

            @pl.loop(t0, t0 + 2)
            def _(t):
                combine_y(t)

            ship(y_v, j - Y_STEP, ys_sem, yr_sem)

        @pl.when(owner & (j == Y_STEP + n_tb // 2))
        def _():
            ship(y_v, n_tb // 2, ys_sem, yr_sem)

        @pl.when(owner & (j == Y_STEP + n_tb // 2 - 1))
        def _():
            router_parts()

    outs = [
        pltpu.make_async_copy(xr, xe_out, out_sem.at[0]),
        pltpu.make_async_copy(dr, de_out, out_sem.at[1]),
        pltpu.make_async_copy(h_v, h_out, out_sem.at[2]),
        pltpu.make_async_copy(da_v, da_out, out_sem.at[3]),
        pltpu.make_async_copy(db_v, db_out, out_sem.at[4]),
    ]
    for c in outs[:3]:
        c.start()

    split = n_loc - 2

    def pick_both(t):
        toks = pl.ds(pl.multiple_of(t * tb, tb), tb)
        return toks, jnp.where(spots(s1c, toks) | spots(s2c, toks), 1.0, 0.0).astype(BF)

    def sum_first(t):
        toks, pick = pick_both(t)
        dl = dl_v[toks, :]
        for c in range(0, width, 512):
            rows = dxr[0:split, :, :, c:c + 512].reshape(split * blk, 512)
            router = lax.dot_general(
                dl, wr_v[:, c:c + 512], NN, precision=lax.Precision.HIGHEST, preferred_element_type=F32
            )
            acc_v[toks, c:c + 512] = dot(pick[:, :split * blk], rows) + router

    def sum_last(t):
        toks, pick = pick_both(t)
        for c in range(0, width, 512):
            rows = dxr[split:n_loc, :, :, c:c + 512].reshape((n_loc - split) * blk, 512)
            dx_v[toks, c:c + 512] = (acc_v[toks, c:c + 512] + dot(pick[:, split * blk:], rows)).astype(BF)
        pltpu.make_async_copy(dx_v.at[toks], dx_out.at[toks], in_sem.at[1]).start()

    for c in outs[3:]:
        c.start()

    for i in range(BACK_LAG - 1):
        merge_and_return(xs, pdr, pdr_sem, dxr, dxs_sem, dxr_sem, n_loc - BACK_LAG + i)

    @pl.when(owner)
    def _():
        router_sum()
        ship(y_v, n_tb - 1, ys_sem, yr_sem)
        pltpu.make_async_copy(y_v, y_out, in_sem.at[0]).start()

    merge_and_return(xs, pdr, pdr_sem, dxr, dxs_sem, dxr_sem, n_loc - 1)

    @pl.when(owner)
    def _():
        @pl.loop(0, split)
        def _(j):
            wait_recv(dxr.at[j, pl.ds(0, ep_size - 1)], dxr_sem.at[j])

        @pl.loop(0, n_tb)
        def _(t):
            sum_first(t)

        wait_recv(dwf.at[pl.ds(0, ep_size - 1)], fr_sem)
        pltpu.make_async_remote_copy(
            src_ref=dwf, dst_ref=dwf, send_sem=gs_sem, recv_sem=gr_sem,
            device_id=(k, 2 * chip + 1 - core), device_id_type=MESH,
        ).start()

        @pl.loop(split, n_loc)
        def _(j):
            wait_recv(dxr.at[j, pl.ds(0, ep_size - 1)], dxr_sem.at[j])

        @pl.loop(0, n_tb)
        def _(t):
            sum_last(t)

        wait_send(dwp.at[pl.ds(0, ep_size - 1)], rs_sem)
        wait_send(dwf.at[pl.ds(0, ep_size - 1)], fs_sem)
        wait_send(dwf, gs_sem)
        wait_send(y_v, ys_sem)
        wait_send(orr.at[:, pl.ds(0, half - 1)], os_sem)
        wait_send(dxr.at[:, pl.ds(0, half - 1)], dxs_sem)

    @pl.when(jnp.logical_not(owner))
    def _():
        dx_v[...] = jnp.zeros_like(dx_v)
        pltpu.make_async_copy(dx_v, dx_out, in_sem.at[1]).start()
        for t in range(n_tb):
            toks = pl.ds(t * tb, tb)
            wait_recv(y_v.at[toks], yr_sem.at[t])
            pltpu.make_async_copy(y_v.at[toks], y_out.at[toks], in_sem.at[0]).start()
        wait_recv(dwf, gr_sem)
        wait_send(orr.at[:, pl.ds(0, half)], os_sem)
        wait_send(dxr.at[:, pl.ds(0, half)], dxs_sem)

    finals = [
        pltpu.make_async_copy(dwf, dwr_out, in_sem.at[2]),
        pltpu.make_async_copy(y_v, y_out, in_sem.at[0]),
        pltpu.make_async_copy(dx_v, dx_out, in_sem.at[1]),
    ]
    finals[0].start()
    wait_send(ds.at[:, pl.ds(0, ep_size - 1)], ds_sem)
    wait_send(xr.at[pl.ds(0, VIA_TP), 0], xfs_sem)
    wait_send(ps.at[:, pl.ds(0, half)], ps_sem)
    wait_send(xs.at[:, pl.ds(0, half)], pds_sem)
    for c in outs + finals:
        c.wait()


def weight_kernel(xe, de, h, da, db, y, dwr, ga_out, gb_out, gc_out, y_out, dwr_out):
    y_out[...] = y[...]
    dwr_out[...] = dwr[...]
    rows = xe[0]
    ga_out[0] = dot(rows, da[0], TN)
    gb_out[0] = dot(rows, db[0], TN)
    gc_out[0] = dot(h[0], de[0], TN)


def solution(mesh):
    tp_size = mesh.shape["tp"]
    ep_size = mesh.shape["ep"]

    def local_step(x_rows, w_router, first_ids, second_ids, w_gelu, w_lin, w_out, dy_rows):
        n_tok, width = x_rows.shape
        n_exp = w_router.shape[1]
        n_loc, _, hid = w_gelu.shape
        cap = 2 * n_tok // n_exp
        blk = ep_size * cap
        half = ep_size // tp_size
        dma = pltpu.SemaphoreType.DMA
        any_spec = pl.BlockSpec(memory_space=pl.ANY)
        sds = jax.ShapeDtypeStruct
        rows_shape = (n_loc, ep_size, cap, width)
        half_shape = (n_loc, half, cap, width)
        hid_shape = (n_loc, blk, hid)
        col = pltpu.VMEM((n_tok, 128), F32)
        row = pltpu.VMEM((1, n_tok), F32)
        outs = pl.pallas_call(
            functools.partial(moe_kernel, tp_size, ep_size, cap),
            name="moe",
            in_specs=[any_spec] * 8,
            out_specs=[any_spec] * 8,
            out_shape=[
                sds((n_tok, width), BF), sds((n_tok, width), BF), sds((ep_size, n_loc, width), F32),
                sds(rows_shape, BF), sds(rows_shape, BF), sds(hid_shape, BF), sds(hid_shape, BF), sds(hid_shape, BF),
            ],
            scratch_shapes=[
                pltpu.VMEM((n_tok, width), BF), pltpu.VMEM((n_tok, width), BF), pltpu.VMEM((n_exp, width), F32),
                pltpu.VMEM((n_loc, width, hid), BF), pltpu.VMEM((n_loc, width, hid), BF), pltpu.VMEM((n_loc, hid, width), BF),
                pltpu.VMEM(rows_shape, BF), pltpu.VMEM(rows_shape, BF), pltpu.VMEM(rows_shape, BF), pltpu.VMEM(rows_shape, BF),
                pltpu.VMEM(hid_shape, BF), pltpu.VMEM(hid_shape, BF), pltpu.VMEM(hid_shape, BF),
                pltpu.VMEM(hid_shape, F32), pltpu.VMEM(hid_shape, F32),
                pltpu.VMEM(rows_shape, BF), pltpu.VMEM(half_shape, BF), pltpu.VMEM(half_shape, BF),
                pltpu.VMEM(rows_shape, BF), pltpu.VMEM(rows_shape, BF),
                pltpu.VMEM((n_tok, width), BF), pltpu.VMEM((n_tok, width), BF),
                row, row, row, row, col, col, col, col, col, col, col, col,
                pltpu.VMEM((n_tok, n_exp), F32), pltpu.VMEM((n_tok, n_exp), F32),
                pltpu.VMEM((ep_size, n_loc, width), F32), pltpu.VMEM((ep_size, n_loc, width), F32),
                pltpu.VMEM((ep_size, n_loc, width), F32), pltpu.VMEM((n_tok, width), F32),
                pltpu.VMEM((1, n_tok), I32), pltpu.VMEM((1, n_tok), I32),
                dma((3,)), dma((3, n_loc)), dma((5,)), dma((2,)),
                dma(()), dma((n_loc,)), dma((n_loc,)), dma((n_loc,)), dma(()), dma(()), dma((n_loc,)),
                dma(()), dma((n_loc,)), dma(()), dma((n_loc,)),
                dma(()), dma((n_loc,)), dma(()), dma((n_loc,)),
                dma(()), dma((n_tok // 128,)),
                dma(()), dma(()), dma(()), dma(()), dma(()), dma(()),
            ],
            compiler_params=pltpu.CompilerParams(
                collective_id=0, has_side_effects=True, vmem_limit_bytes=67043328
            ),
        )(
            first_ids.reshape(1, n_tok), second_ids.reshape(1, n_tok), x_rows, dy_rows, w_router.T,
            w_gelu, w_lin, w_out,
        )
        act_out, grad_in, grad_router, xe, de, h, da, db = outs
        partners = [
            ((q % tp_size) * ep_size + q, (1 - q % tp_size) * ep_size + q) for q in range(ep_size)
        ]
        passed = lax.ppermute(grad_in, ("tp", "ep"), partners)
        owner = lax.axis_index("ep") % tp_size == lax.axis_index("tp")
        grad_in = jnp.where(owner, grad_in, passed)
        xe = xe.reshape(n_loc, blk, width)
        de = de.reshape(n_loc, blk, width)

        y_spec = pl.BlockSpec((n_tok // n_loc, width), lambda e: (e, 0))

        def spec(*shape):
            return pl.BlockSpec((1,) + shape, lambda e: (e, 0, 0))

        grad_wa, grad_wb, grad_wc, act_out, grad_router = pl.pallas_call(
            weight_kernel,
            name="weight_grads",
            grid=(n_loc,),
            in_specs=[spec(blk, width), spec(blk, width), spec(blk, hid), spec(blk, hid), spec(blk, hid), y_spec, spec(n_exp // n_loc, width)],
            out_specs=[spec(width, hid), spec(width, hid), spec(hid, width), y_spec, spec(n_exp // n_loc, width)],
            out_shape=[
                sds((n_loc, width, hid), F32), sds((n_loc, width, hid), F32), sds((n_loc, hid, width), F32),
                sds((n_tok, width), BF), sds((n_loc, n_exp // n_loc, width), F32),
            ],
            compiler_params=pltpu.CompilerParams(
                dimension_semantics=("arbitrary",), vmem_limit_bytes=63743328
            ),
            cost_estimate=pl.CostEstimate(
                flops=6 * n_loc * blk * width * hid, transcendentals=0,
                bytes_accessed=12 * n_loc * width * hid + 4 * n_loc * blk * width + 6 * n_loc * blk * hid,
            ),
        )(xe, de, h, da, db, act_out, grad_router.reshape(n_loc, n_exp // n_loc, width))
        return act_out, grad_in, grad_wa, grad_wb, grad_wc, grad_router.reshape(n_exp, width).T

    return jax.shard_map(
        local_step,
        mesh=mesh,
        in_specs=(P("ep", None), P(), P("ep"), P("ep"), P("ep", None, "tp"), P("ep", None, "tp"), P("ep", "tp", None), P("ep", None)),
        out_specs=(P("ep", None), P("ep", None), P("ep", None, "tp"), P("ep", None, "tp"), P("ep", "tp", None), P()),
        check_vma=False,
    )
```

```python
import functools

import jax
import jax.numpy as jnp
from jax import lax
from jax.experimental import pallas as pl
from jax.experimental.pallas import tpu as pltpu
from jax.sharding import PartitionSpec as P

BF = jnp.bfloat16
F32 = jnp.float32
I32 = jnp.int32
MESH = pl.DeviceIdType.MESH
GELU_COEF = 0.7978845608028654
AHEAD = 4
LAG = 3
Y_STEP = 4
FORWARD = 2
VIA_TP = 6
BACK_LAG = 2
EARLY = 2
NN = (((1,), (0,)), ((), ()))
NT = (((1,), (1,)), ((), ()))
TN = (((0,), (0,)), ((), ()))


def dot(a, b, dims=NN):
    return lax.dot_general(a, b, dims, preferred_element_type=F32)


def split3(v):
    hi = v.astype(BF)
    rest = v - hi.astype(F32)
    mid = rest.astype(BF)
    low = (rest - mid.astype(F32)).astype(BF)
    return hi, mid, low


def moe_kernel(
    tp_size, ep_size, cap,
    ids1_hbm, ids2_hbm, x_hbm, dy_hbm, wr_hbm, wa_hbm, wb_hbm, wc_hbm,
    y_out, dx_out, dwr_out, xe_out, de_out, h_out, da_out, db_out,
    x_v, dy_v, wr_v, wa_v, wb_v, wc_v,
    xs, ds, xr, dr, h_v, da_v, db_v, bs_v, gv_v,
    ps, pr, pdr, orr, dxr, y_v, dx_v,
    s1r, s2r, g1r, g2r, s1c, s2c, g1c, g2c, q1c, q2c, i1c, i2c, prob_v, dl_v,
    dwp, dwi, dwf, acc_v, ids1_ref, ids2_ref,
    in_sem, w_sem, out_sem, id_sem,
    xs_sem, xr_sem, xd_sem, xf_sem, xfs_sem, ds_sem, dr_sem,
    ps_sem, pr_sem, pds_sem, pdr_sem,
    os_sem, or_sem, dxs_sem, dxr_sem,
    ys_sem, yr_sem,
    rs_sem, rr_sem, fs_sem, fr_sem, gs_sem, gr_sem,
):
    k = lax.axis_index("tp")
    r = lax.axis_index("ep")
    n_loc = wa_v.shape[0]
    n_tok, width = x_v.shape
    hid = wa_v.shape[2]
    n_exp = n_loc * ep_size
    blk = ep_size * cap
    half = ep_size // tp_size
    my_place = (r % tp_size) * half + r // tp_size
    owner = (r % tp_size) == k
    other = 1 - k

    ins = [
        pltpu.make_async_copy(x_hbm, x_v, in_sem.at[0]),
        pltpu.make_async_copy(dy_hbm, dy_v, in_sem.at[1]),
        pltpu.make_async_copy(wr_hbm, wr_v, in_sem.at[2]),
    ]
    id_loads = [pltpu.make_async_copy(ids1_hbm, ids1_ref, id_sem.at[0]), pltpu.make_async_copy(ids2_hbm, ids2_ref, id_sem.at[1])]
    for c in id_loads:
        c.start()
    ins[0].start()

    def weight_copies(j):
        return [
            pltpu.make_async_copy(wa_hbm.at[j], wa_v.at[j], w_sem.at[0, j]),
            pltpu.make_async_copy(wb_hbm.at[j], wb_v.at[j], w_sem.at[1, j]),
            pltpu.make_async_copy(wc_hbm.at[j], wc_v.at[j], w_sem.at[2, j]),
        ]

    n_dev = tp_size * ep_size
    barrier = pltpu.get_barrier_semaphore()
    for d in range(1, n_dev):
        flat = (k * ep_size + r + d) % n_dev
        pl.semaphore_signal(barrier, inc=1, device_id=(flat // ep_size, flat % ep_size), device_id_type=MESH)

    for c in id_loads:
        c.wait()
    ids1 = ids1_ref[...]
    ids2 = ids2_ref[...]
    e_iota = lax.broadcasted_iota(I32, (n_exp, n_tok), 0)
    hot1 = jnp.where(ids1 == e_iota, 1.0, 0.0).astype(F32)
    hot2 = jnp.where(ids2 == e_iota, 1.0, 0.0).astype(F32)
    before = jnp.where(
        lax.broadcasted_iota(I32, (n_tok, n_tok), 0) < lax.broadcasted_iota(I32, (n_tok, n_tok), 1), 1.0, 0.0
    ).astype(BF)
    cum1 = dot(hot1.astype(BF), before)
    cum2 = dot(hot2.astype(BF), before)
    fill1 = jnp.sum(hot1, axis=1, keepdims=True)
    pos1 = jnp.sum(cum1 * hot1, axis=0, keepdims=True)
    pos2 = jnp.sum((cum2 + fill1) * hot2, axis=0, keepdims=True)

    def place(ids, pos):
        spot = (ids & (n_loc - 1)) * blk + (ids // n_loc) * cap
        return jnp.where(pos < cap, spot.astype(F32) + pos, float(n_exp * cap))

    s1r[...] = place(ids1, pos1)
    s2r[...] = place(ids2, pos2)

    def masks(j):
        spot = (lax.broadcasted_iota(I32, (blk, n_tok), 0) + j * blk).astype(F32)
        return s1r[...] == spot, s2r[...] == spot

    chip = r // 2
    chip_x = chip + 1 - 2 * (chip % 2)
    chip_y = (chip + 2) % 4
    chip_d = 3 - chip
    core = r % 2
    diag = 2 * chip_d + (k + r) % 2
    near = [2 * chip_x + core, 2 * chip_y + core, 2 * chip_x + 1 - core, 2 * chip_y + 1 - core, 2 * chip + 1 - core]
    far = [2 * chip_d + core, 2 * chip_d + 1 - core]

    def place_of(q):
        return (q % tp_size) * half + q // tp_size

    def send_row(src, dst, send_sem, recv_sem, j, q):
        pltpu.make_async_remote_copy(
            src_ref=src.at[j, q], dst_ref=dst.at[j, my_place],
            send_sem=send_sem, recv_sem=recv_sem.at[j],
            device_id=(k, q), device_id_type=MESH,
        ).start()

    def wait_recv(view, sem):
        pltpu.make_async_remote_copy(
            src_ref=view, dst_ref=view, send_sem=sem, recv_sem=sem, device_id=(k, r), device_id_type=MESH
        ).wait_recv()

    def wait_send(view, sem):
        pltpu.make_async_remote_copy(
            src_ref=view, dst_ref=view, send_sem=sem, recv_sem=sem, device_id=(k, r), device_id_type=MESH
        ).wait_send()

    def gather_x(j):
        m1, m2 = masks(j)
        pick = jnp.where(m1 | m2, 1.0, 0.0).astype(BF)
        for c in range(0, width, 512):
            rows = dot(pick, x_v[:, c:c + 512]).astype(BF)
            xs[j, :, :, c:c + 512] = rows.reshape(ep_size, cap, 512)

    def send_x(j, via_tp):
        if via_tp:
            send_row(xs, xr, xs_sem, xd_sem, j, diag)
        for q in near if via_tp else far + near:
            send_row(xs, xr, xs_sem, xr_sem, j, q)
        xr[j, my_place] = xs[j, r]

    ins[0].wait()
    ins[2].start()
    ins[1].start()

    @pl.loop(0, n_loc)
    def _(j):
        for c in weight_copies(j):
            c.start()

    @pl.loop(0, EARLY)
    def _(j):
        gather_x(j)

    pl.semaphore_wait(barrier, n_dev - 1)

    @pl.loop(0, EARLY)
    def _(j):
        send_x(j, True)

    @pl.loop(EARLY, VIA_TP)
    def _(j):
        gather_x(j)
        send_x(j, True)

    if VIA_TP < n_loc:
        @pl.loop(VIA_TP, n_loc)
        def _(j):
            gather_x(j)
            send_x(j, False)

    def column(row):
        return jnp.transpose(jnp.broadcast_to(row, (128, n_tok)))

    s1c[...] = column(s1r[...])
    s2c[...] = column(s2r[...])
    i1c[...] = column(ids1.astype(F32))
    i2c[...] = column(ids2.astype(F32))
    ins[2].wait()
    wr_hi, wr_mid, wr_low = split3(wr_v[...])
    xv = x_v[...]
    logits = dot(xv, wr_hi, NT) + (dot(xv, wr_mid, NT) + dot(xv, wr_low, NT))
    ex = jnp.exp(logits - jnp.max(logits, axis=1, keepdims=True))
    prob = ex / jnp.sum(ex, axis=1, keepdims=True)
    prob_v[...] = prob
    lane = lax.broadcasted_iota(I32, (n_tok, n_exp), 1).astype(F32)
    q1 = jnp.sum(jnp.where(i1c[:, :n_exp] == lane, prob, 0.0), axis=1, keepdims=True)
    q2 = jnp.sum(jnp.where(i2c[:, :n_exp] == lane, prob, 0.0), axis=1, keepdims=True)
    g1 = jnp.broadcast_to(q1 / (q1 + q2), (n_tok, 128))
    g2 = jnp.broadcast_to(q2 / (q1 + q2), (n_tok, 128))
    g1c[...] = g1
    g2c[...] = g2
    q1c[...] = jnp.broadcast_to(q1, (n_tok, 128))
    q2c[...] = jnp.broadcast_to(q2, (n_tok, 128))
    g1r[...] = jnp.transpose(g1)[0:1, :]
    g2r[...] = jnp.transpose(g2)[0:1, :]
    ins[1].wait()

    def build_d(j):
        m1, m2 = masks(j)
        pick = jnp.where(m1 | m2, 1.0, 0.0).astype(BF)
        gate = jnp.sum(jnp.where(m1, g1r[...], 0.0) + jnp.where(m2, g2r[...], 0.0), axis=1, keepdims=True)
        for c in range(0, width, 512):
            rows = (gate * dot(pick, dy_v[:, c:c + 512])).astype(BF)
            ds[j, :, :, c:c + 512] = rows.reshape(ep_size, cap, 512)
        for q in far + near:
            send_row(ds, dr, ds_sem, dr_sem, j, q)
        dr[j, my_place] = ds[j, r]

    def send_half(src, dst, send_sem, recv_sem, j):
        pltpu.make_async_remote_copy(
            src_ref=src.at[j, pl.ds(other * half, half)], dst_ref=dst.at[j],
            send_sem=send_sem, recv_sem=recv_sem.at[j],
            device_id=(other, r), device_id_type=MESH,
        ).start()

    def merge_and_return(src, got, got_sem, dst, send_sem, recv_sem, j):
        wait_recv(got.at[j], got_sem.at[j])
        mine = pl.ds(k * half, half)
        src[j, mine] = (src[j, mine].astype(F32) + got[j].astype(F32)).astype(BF)
        for d in range(half):
            c = (r // tp_size + d) % half
            q = tp_size * c + k

            @pl.when(q != r)
            def _():
                pltpu.make_async_remote_copy(
                    src_ref=src.at[j, k * half + c], dst_ref=dst.at[j, r],
                    send_sem=send_sem, recv_sem=recv_sem.at[j],
                    device_id=(k, q), device_id_type=MESH,
                ).start()

            @pl.when(q == r)
            def _():
                dst[j, r] = src[j, k * half + c]

    n_near = len(near)
    diag_place = place_of(diag)

    def forward_diag(j):
        wait_recv(xr.at[j, 0], xd_sem.at[j])
        pltpu.make_async_remote_copy(
            src_ref=xr.at[j, diag_place], dst_ref=xr.at[j, diag_place],
            send_sem=xfs_sem, recv_sem=xf_sem.at[j],
            device_id=(other, r), device_id_type=MESH,
        ).start()

    for i in range(FORWARD):
        forward_diag(i)

    @pl.loop(0, n_loc)
    def _(j):
        @pl.when(j >= n_loc - AHEAD)
        def _():
            build_d(j + AHEAD - n_loc)

        @pl.when(j + FORWARD < VIA_TP)
        def _():
            forward_diag(j + FORWARD)

        for c in weight_copies(j):
            c.wait()

        @pl.when(j < VIA_TP)
        def _():
            wait_recv(xr.at[j, pl.ds(0, n_near)], xr_sem.at[j])
            wait_recv(xr.at[j, 0], xf_sem.at[j])

        if VIA_TP < n_loc:
            @pl.when(j >= VIA_TP)
            def _():
                wait_recv(xr.at[j, pl.ds(0, ep_size - 1)], xr_sem.at[j])

        rows = xr[j].reshape(blk, width)
        pa = dot(rows, wa_v[j])
        pb = dot(rows, wb_v[j])
        th = jnp.tanh(GELU_COEF * (pa + 0.044715 * pa * pa * pa))
        gv = 0.5 * pa * (1.0 + th)
        slope = 0.5 * (1.0 + th) + 0.5 * pa * (1.0 - th * th) * GELU_COEF * (1.0 + 0.134145 * pa * pa)
        gv_v[j] = gv
        bs_v[j] = pb * slope
        hidden = (gv * pb).astype(BF)
        h_v[j] = hidden
        for c in range(0, width, 512):
            ps[j, :, :, c:c + 512] = dot(hidden, wc_v[j, :, c:c + 512]).astype(BF).reshape(ep_size, cap, 512)
        send_half(ps, pr, ps_sem, pr_sem, j)

        @pl.when(j >= LAG)
        def _():
            merge_and_return(ps, pr, pr_sem, orr, os_sem, or_sem, j - LAG)

    tb = 128
    n_tb = n_tok // tb

    def spots(col, toks):
        lanes = lax.broadcasted_iota(I32, (tb, 128), 1).astype(F32)
        base = col[toks, :]
        return jnp.concatenate([base == lanes + float(u * 128) for u in range(n_exp * cap // 128)], axis=1)

    def ship(buf, t, send_sem, recv_sem):
        toks = pl.ds(pl.multiple_of(t * tb, tb), tb)
        pltpu.make_async_remote_copy(
            src_ref=buf.at[toks], dst_ref=buf.at[toks], send_sem=send_sem, recv_sem=recv_sem.at[t],
            device_id=(other, r), device_id_type=MESH,
        ).start()

    def combine_y(t):
        toks = pl.ds(pl.multiple_of(t * tb, tb), tb)
        pick1 = jnp.where(spots(s1c, toks), 1.0, 0.0).astype(BF)
        pick2 = jnp.where(spots(s2c, toks), 1.0, 0.0).astype(BF)
        dg1 = jnp.zeros((tb, 1), F32)
        dg2 = jnp.zeros((tb, 1), F32)
        ga = g1c[toks, 0:1]
        gb = g2c[toks, 0:1]
        for c in range(0, width, 512):
            rows = orr[:, :, :, c:c + 512].reshape(n_exp * cap, 512)
            o1 = dot(pick1, rows)
            o2 = dot(pick2, rows)
            y_v[toks, c:c + 512] = (ga * o1 + gb * o2).astype(BF)
            dyf = dy_v[toks, c:c + 512].astype(F32)
            dg1 = dg1 + jnp.sum(dyf * o1, axis=1, keepdims=True)
            dg2 = dg2 + jnp.sum(dyf * o2, axis=1, keepdims=True)
        qa = q1c[toks, 0:1]
        qb = q2c[toks, 0:1]
        shared = dg1 * ga + dg2 * gb
        dq1 = (dg1 - shared) / (qa + qb)
        dq2 = (dg2 - shared) / (qa + qb)
        centre = dq1 * qa + dq2 * qb
        lanes = lax.broadcasted_iota(I32, (tb, n_exp), 1).astype(F32)
        pull = jnp.where(i1c[toks, :n_exp] == lanes, dq1, 0.0) + jnp.where(i2c[toks, :n_exp] == lanes, dq2, 0.0)
        dl_v[toks, :] = prob_v[toks, :] * (pull - centre)

    def router_parts():
        d_hi, d_mid, d_low = split3(dl_v[...])
        for c in range(0, width, 512):
            xc = x_v[:, c:c + 512]
            piece = dot(d_hi, xc, TN) + (dot(d_mid, xc, TN) + dot(d_low, xc, TN))
            dwp[:, :, c:c + 512] = piece.reshape(ep_size, n_loc, 512)
        for d in range(1, ep_size):
            q = (r + d) % ep_size
            pltpu.make_async_remote_copy(
                src_ref=dwp.at[q], dst_ref=dwi.at[r], send_sem=rs_sem, recv_sem=rr_sem,
                device_id=(q % tp_size, q), device_id_type=MESH,
            ).start()
        dwi[r] = dwp[r]

    def router_sum():
        wait_recv(dwi.at[pl.ds(0, ep_size - 1)], rr_sem)
        total = dwi[0]
        for q in range(1, ep_size):
            total = total + dwi[q]
        dwf[r] = total
        for d in range(1, ep_size):
            q = (r + d) % ep_size
            pltpu.make_async_remote_copy(
                src_ref=dwf.at[r], dst_ref=dwf.at[r], send_sem=fs_sem, recv_sem=fr_sem,
                device_id=(q % tp_size, q), device_id_type=MESH,
            ).start()

    wait_send(xs.at[pl.ds(0, VIA_TP), pl.ds(0, n_near + 1)], xs_sem)
    if VIA_TP < n_loc:
        wait_send(xs.at[pl.ds(VIA_TP, n_loc - VIA_TP), pl.ds(0, ep_size - 1)], xs_sem)
    @pl.loop(0, n_loc)
    def _(j):
        @pl.when(j + AHEAD < n_loc)
        def _():
            build_d(j + AHEAD)

        wait_recv(dr.at[j, pl.ds(0, ep_size - 1)], dr_sem.at[j])
        rows = dr[j].reshape(blk, width)
        dh = dot(rows, wc_v[j], NT)
        da = (dh * bs_v[j]).astype(BF)
        db = (dh * gv_v[j]).astype(BF)
        da_v[j] = da
        db_v[j] = db
        for c in range(0, width, 512):
            part = dot(da, wa_v[j, c:c + 512, :], NT) + dot(db, wb_v[j, c:c + 512, :], NT)
            xs[j, :, :, c:c + 512] = part.astype(BF).reshape(ep_size, cap, 512)
        send_half(xs, pdr, pds_sem, pdr_sem, j)

        @pl.when(j == 0)
        def _():
            for i in range(LAG):
                merge_and_return(ps, pr, pr_sem, orr, os_sem, or_sem, n_loc - LAG + i)

        @pl.when(j >= BACK_LAG)
        def _():
            merge_and_return(xs, pdr, pdr_sem, dxr, dxs_sem, dxr_sem, j - BACK_LAG)

        @pl.when(owner & (j == Y_STEP))
        def _():
            @pl.loop(0, n_loc)
            def _(i):
                wait_recv(orr.at[i, pl.ds(0, ep_size - 1)], or_sem.at[i])

        @pl.when(owner & (j >= Y_STEP) & (j < Y_STEP + n_tb // 2))
        def _():
            t0 = 2 * (j - Y_STEP)

            @pl.loop(t0, t0 + 2)
            def _(t):
                combine_y(t)

            ship(y_v, j - Y_STEP, ys_sem, yr_sem)

        @pl.when(owner & (j == Y_STEP + n_tb // 2))
        def _():
            ship(y_v, n_tb // 2, ys_sem, yr_sem)

        @pl.when(owner & (j == Y_STEP + n_tb // 2 - 1))
        def _():
            router_parts()

    outs = [
        pltpu.make_async_copy(xr, xe_out, out_sem.at[0]),
        pltpu.make_async_copy(dr, de_out, out_sem.at[1]),
        pltpu.make_async_copy(h_v, h_out, out_sem.at[2]),
        pltpu.make_async_copy(da_v, da_out, out_sem.at[3]),
        pltpu.make_async_copy(db_v, db_out, out_sem.at[4]),
    ]
    for c in outs[:3]:
        c.start()

    split = n_loc - 2

    def pick_both(t):
        toks = pl.ds(pl.multiple_of(t * tb, tb), tb)
        return toks, jnp.where(spots(s1c, toks) | spots(s2c, toks), 1.0, 0.0).astype(BF)

    def sum_first(t):
        toks, pick = pick_both(t)
        dl = dl_v[toks, :]
        for c in range(0, width, 512):
            rows = dxr[0:split, :, :, c:c + 512].reshape(split * blk, 512)
            router = lax.dot_general(
                dl, wr_v[:, c:c + 512], NN, precision=lax.Precision.HIGHEST, preferred_element_type=F32
            )
            acc_v[toks, c:c + 512] = dot(pick[:, :split * blk], rows) + router

    def sum_last(t):
        toks, pick = pick_both(t)
        for c in range(0, width, 512):
            rows = dxr[split:n_loc, :, :, c:c + 512].reshape((n_loc - split) * blk, 512)
            dx_v[toks, c:c + 512] = (acc_v[toks, c:c + 512] + dot(pick[:, split * blk:], rows)).astype(BF)
        pltpu.make_async_copy(dx_v.at[toks], dx_out.at[toks], in_sem.at[1]).start()

    for c in outs[3:]:
        c.start()

    for i in range(BACK_LAG - 1):
        merge_and_return(xs, pdr, pdr_sem, dxr, dxs_sem, dxr_sem, n_loc - BACK_LAG + i)

    @pl.when(owner)
    def _():
        router_sum()
        ship(y_v, n_tb - 1, ys_sem, yr_sem)
        pltpu.make_async_copy(y_v, y_out, in_sem.at[0]).start()

    merge_and_return(xs, pdr, pdr_sem, dxr, dxs_sem, dxr_sem, n_loc - 1)

    @pl.when(owner)
    def _():
        @pl.loop(0, split)
        def _(j):
            wait_recv(dxr.at[j, pl.ds(0, ep_size - 1)], dxr_sem.at[j])

        @pl.loop(0, n_tb)
        def _(t):
            sum_first(t)

        wait_recv(dwf.at[pl.ds(0, ep_size - 1)], fr_sem)
        pltpu.make_async_remote_copy(
            src_ref=dwf, dst_ref=dwf, send_sem=gs_sem, recv_sem=gr_sem,
            device_id=(k, 2 * chip + 1 - core), device_id_type=MESH,
        ).start()

        @pl.loop(split, n_loc)
        def _(j):
            wait_recv(dxr.at[j, pl.ds(0, ep_size - 1)], dxr_sem.at[j])

        @pl.loop(0, n_tb)
        def _(t):
            sum_last(t)

        wait_send(dwp.at[pl.ds(0, ep_size - 1)], rs_sem)
        wait_send(dwf.at[pl.ds(0, ep_size - 1)], fs_sem)
        wait_send(dwf, gs_sem)
        wait_send(y_v, ys_sem)
        wait_send(orr.at[:, pl.ds(0, half - 1)], os_sem)
        wait_send(dxr.at[:, pl.ds(0, half - 1)], dxs_sem)

    @pl.when(jnp.logical_not(owner))
    def _():
        dx_v[...] = jnp.zeros_like(dx_v)
        pltpu.make_async_copy(dx_v, dx_out, in_sem.at[1]).start()
        for t in range(n_tb):
            toks = pl.ds(t * tb, tb)
            wait_recv(y_v.at[toks], yr_sem.at[t])
            pltpu.make_async_copy(y_v.at[toks], y_out.at[toks], in_sem.at[0]).start()
        wait_recv(dwf, gr_sem)
        wait_send(orr.at[:, pl.ds(0, half)], os_sem)
        wait_send(dxr.at[:, pl.ds(0, half)], dxs_sem)

    finals = [
        pltpu.make_async_copy(dwf, dwr_out, in_sem.at[2]),
        pltpu.make_async_copy(y_v, y_out, in_sem.at[0]),
        pltpu.make_async_copy(dx_v, dx_out, in_sem.at[1]),
    ]
    finals[0].start()
    wait_send(ds.at[:, pl.ds(0, ep_size - 1)], ds_sem)
    wait_send(xr.at[pl.ds(0, VIA_TP), 0], xfs_sem)
    wait_send(ps.at[:, pl.ds(0, half)], ps_sem)
    wait_send(xs.at[:, pl.ds(0, half)], pds_sem)
    for c in outs + finals:
        c.wait()


def weight_kernel(xe, de, h, da, db, y, dwr, ga_out, gb_out, gc_out, y_out, dwr_out):
    y_out[...] = y[...]
    dwr_out[...] = dwr[...]
    rows = xe[0]
    ga_out[0] = dot(rows, da[0], TN)
    gb_out[0] = dot(rows, db[0], TN)
    gc_out[0] = dot(h[0], de[0], TN)


def solution(mesh):
    tp_size = mesh.shape["tp"]
    ep_size = mesh.shape["ep"]

    def local_step(x_rows, w_router, first_ids, second_ids, w_gelu, w_lin, w_out, dy_rows):
        n_tok, width = x_rows.shape
        n_exp = w_router.shape[1]
        n_loc, _, hid = w_gelu.shape
        cap = 2 * n_tok // n_exp
        blk = ep_size * cap
        half = ep_size // tp_size
        dma = pltpu.SemaphoreType.DMA
        any_spec = pl.BlockSpec(memory_space=pl.ANY)
        sds = jax.ShapeDtypeStruct
        rows_shape = (n_loc, ep_size, cap, width)
        half_shape = (n_loc, half, cap, width)
        hid_shape = (n_loc, blk, hid)
        col = pltpu.VMEM((n_tok, 128), F32)
        row = pltpu.VMEM((1, n_tok), F32)
        outs = pl.pallas_call(
            functools.partial(moe_kernel, tp_size, ep_size, cap),
            name="moe",
            in_specs=[any_spec] * 8,
            out_specs=[any_spec] * 8,
            out_shape=[
                sds((n_tok, width), BF), sds((n_tok, width), BF), sds((ep_size, n_loc, width), F32),
                sds(rows_shape, BF), sds(rows_shape, BF), sds(hid_shape, BF), sds(hid_shape, BF), sds(hid_shape, BF),
            ],
            scratch_shapes=[
                pltpu.VMEM((n_tok, width), BF), pltpu.VMEM((n_tok, width), BF), pltpu.VMEM((n_exp, width), F32),
                pltpu.VMEM((n_loc, width, hid), BF), pltpu.VMEM((n_loc, width, hid), BF), pltpu.VMEM((n_loc, hid, width), BF),
                pltpu.VMEM(rows_shape, BF), pltpu.VMEM(rows_shape, BF), pltpu.VMEM(rows_shape, BF), pltpu.VMEM(rows_shape, BF),
                pltpu.VMEM(hid_shape, BF), pltpu.VMEM(hid_shape, BF), pltpu.VMEM(hid_shape, BF),
                pltpu.VMEM(hid_shape, F32), pltpu.VMEM(hid_shape, F32),
                pltpu.VMEM(rows_shape, BF), pltpu.VMEM(half_shape, BF), pltpu.VMEM(half_shape, BF),
                pltpu.VMEM(rows_shape, BF), pltpu.VMEM(rows_shape, BF),
                pltpu.VMEM((n_tok, width), BF), pltpu.VMEM((n_tok, width), BF),
                row, row, row, row, col, col, col, col, col, col, col, col,
                pltpu.VMEM((n_tok, n_exp), F32), pltpu.VMEM((n_tok, n_exp), F32),
                pltpu.VMEM((ep_size, n_loc, width), F32), pltpu.VMEM((ep_size, n_loc, width), F32),
                pltpu.VMEM((ep_size, n_loc, width), F32), pltpu.VMEM((n_tok, width), F32),
                pltpu.VMEM((1, n_tok), I32), pltpu.VMEM((1, n_tok), I32),
                dma((3,)), dma((3, n_loc)), dma((5,)), dma((2,)),
                dma(()), dma((n_loc,)), dma((n_loc,)), dma((n_loc,)), dma(()), dma(()), dma((n_loc,)),
                dma(()), dma((n_loc,)), dma(()), dma((n_loc,)),
                dma(()), dma((n_loc,)), dma(()), dma((n_loc,)),
                dma(()), dma((n_tok // 128,)),
                dma(()), dma(()), dma(()), dma(()), dma(()), dma(()),
            ],
            compiler_params=pltpu.CompilerParams(
                collective_id=0, has_side_effects=True, vmem_limit_bytes=67043328
            ),
        )(
            first_ids.reshape(1, n_tok), second_ids.reshape(1, n_tok), x_rows, dy_rows, w_router.T,
            w_gelu, w_lin, w_out,
        )
        act_out, grad_in, grad_router, xe, de, h, da, db = outs
        partners = [
            ((q % tp_size) * ep_size + q, (1 - q % tp_size) * ep_size + q) for q in range(ep_size)
        ]
        passed = lax.ppermute(grad_in, ("tp", "ep"), partners)
        owner = lax.axis_index("ep") % tp_size == lax.axis_index("tp")
        grad_in = jnp.where(owner, grad_in, passed)
        xe = xe.reshape(n_loc, blk, width)
        de = de.reshape(n_loc, blk, width)

        y_spec = pl.BlockSpec((n_tok // n_loc, width), lambda e: (e, 0))

        def spec(*shape):
            return pl.BlockSpec((1,) + shape, lambda e: (e, 0, 0))

        grad_wa, grad_wb, grad_wc, act_out, grad_router = pl.pallas_call(
            weight_kernel,
            name="weight_grads",
            grid=(n_loc,),
            in_specs=[spec(blk, width), spec(blk, width), spec(blk, hid), spec(blk, hid), spec(blk, hid), y_spec, spec(n_exp // n_loc, width)],
            out_specs=[spec(width, hid), spec(width, hid), spec(hid, width), y_spec, spec(n_exp // n_loc, width)],
            out_shape=[
                sds((n_loc, width, hid), F32), sds((n_loc, width, hid), F32), sds((n_loc, hid, width), F32),
                sds((n_tok, width), BF), sds((n_loc, n_exp // n_loc, width), F32),
            ],
            compiler_params=pltpu.CompilerParams(
                dimension_semantics=("arbitrary",), vmem_limit_bytes=63743328
            ),
            cost_estimate=pl.CostEstimate(
                flops=6 * n_loc * blk * width * hid, transcendentals=0,
                bytes_accessed=12 * n_loc * width * hid + 4 * n_loc * blk * width + 6 * n_loc * blk * hid,
            ),
        )(xe, de, h, da, db, act_out, grad_router.reshape(n_loc, n_exp // n_loc, width))
        return act_out, grad_in, grad_wa, grad_wb, grad_wc, grad_router.reshape(n_exp, width).T

    return jax.shard_map(
        local_step,
        mesh=mesh,
        in_specs=(P("ep", None), P(), P("ep"), P("ep"), P("ep", None, "tp"), P("ep", None, "tp"), P("ep", "tp", None), P("ep", None)),
        out_specs=(P("ep", None), P("ep", None), P("ep", None, "tp"), P("ep", None, "tp"), P("ep", "tp", None), P()),
        check_vma=False,
    )
```

```python
import functools

import jax
import jax.numpy as jnp
from jax import lax
from jax.experimental import pallas as pl
from jax.experimental.pallas import tpu as pltpu
from jax.sharding import PartitionSpec as P

BF = jnp.bfloat16
F32 = jnp.float32
I32 = jnp.int32
MESH = pl.DeviceIdType.MESH
GELU_COEF = 0.7978845608028654
AHEAD = 4
LAG = 3
Y_STEP = 4
FORWARD = 2
VIA_TP = 8
BACK_LAG = 2
EARLY = 2
NN = (((1,), (0,)), ((), ()))
NT = (((1,), (1,)), ((), ()))
TN = (((0,), (0,)), ((), ()))


def dot(a, b, dims=NN):
    return lax.dot_general(a, b, dims, preferred_element_type=F32)


def split3(v):
    hi = v.astype(BF)
    rest = v - hi.astype(F32)
    mid = rest.astype(BF)
    low = (rest - mid.astype(F32)).astype(BF)
    return hi, mid, low


def moe_kernel(
    tp_size, ep_size, cap,
    ids1_hbm, ids2_hbm, x_hbm, dy_hbm, wr_hbm, wa_hbm, wb_hbm, wc_hbm,
    y_out, dx_out, dwr_out, xe_out, de_out, h_out, da_out, db_out,
    x_v, dy_v, wr_v, wa_v, wb_v, wc_v,
    xs, ds, xr, dr, h_v, da_v, db_v, bs_v, gv_v,
    ps, pr, pdr, orr, dxr, y_v, dx_v,
    s1r, s2r, g1r, g2r, s1c, s2c, g1c, g2c, q1c, q2c, i1c, i2c, prob_v, dl_v,
    dwp, dwi, dwf, acc_v, ids1_ref, ids2_ref,
    in_sem, w_sem, out_sem, id_sem,
    xs_sem, xr_sem, xd_sem, xf_sem, xfs_sem, ds_sem, dr_sem,
    ps_sem, pr_sem, pds_sem, pdr_sem,
    os_sem, or_sem, dxs_sem, dxr_sem,
    ys_sem, yr_sem,
    rs_sem, rr_sem, fs_sem, fr_sem, gs_sem, gr_sem,
):
    k = lax.axis_index("tp")
    r = lax.axis_index("ep")
    n_loc = wa_v.shape[0]
    n_tok, width = x_v.shape
    hid = wa_v.shape[2]
    n_exp = n_loc * ep_size
    blk = ep_size * cap
    half = ep_size // tp_size
    my_place = (r % tp_size) * half + r // tp_size
    owner = (r % tp_size) == k
    other = 1 - k

    ins = [
        pltpu.make_async_copy(x_hbm, x_v, in_sem.at[0]),
        pltpu.make_async_copy(dy_hbm, dy_v, in_sem.at[1]),
        pltpu.make_async_copy(wr_hbm, wr_v, in_sem.at[2]),
    ]
    id_loads = [pltpu.make_async_copy(ids1_hbm, ids1_ref, id_sem.at[0]), pltpu.make_async_copy(ids2_hbm, ids2_ref, id_sem.at[1])]
    for c in id_loads:
        c.start()
    ins[0].start()

    def weight_copies(j):
        return [
            pltpu.make_async_copy(wa_hbm.at[j], wa_v.at[j], w_sem.at[0, j]),
            pltpu.make_async_copy(wb_hbm.at[j], wb_v.at[j], w_sem.at[1, j]),
            pltpu.make_async_copy(wc_hbm.at[j], wc_v.at[j], w_sem.at[2, j]),
        ]

    n_dev = tp_size * ep_size
    barrier = pltpu.get_barrier_semaphore()
    for d in range(1, n_dev):
        flat = (k * ep_size + r + d) % n_dev
        pl.semaphore_signal(barrier, inc=1, device_id=(flat // ep_size, flat % ep_size), device_id_type=MESH)

    for c in id_loads:
        c.wait()
    ids1 = ids1_ref[...]
    ids2 = ids2_ref[...]
    e_iota = lax.broadcasted_iota(I32, (n_exp, n_tok), 0)
    hot1 = jnp.where(ids1 == e_iota, 1.0, 0.0).astype(F32)
    hot2 = jnp.where(ids2 == e_iota, 1.0, 0.0).astype(F32)
    before = jnp.where(
        lax.broadcasted_iota(I32, (n_tok, n_tok), 0) < lax.broadcasted_iota(I32, (n_tok, n_tok), 1), 1.0, 0.0
    ).astype(BF)
    cum1 = dot(hot1.astype(BF), before)
    cum2 = dot(hot2.astype(BF), before)
    fill1 = jnp.sum(hot1, axis=1, keepdims=True)
    pos1 = jnp.sum(cum1 * hot1, axis=0, keepdims=True)
    pos2 = jnp.sum((cum2 + fill1) * hot2, axis=0, keepdims=True)

    def place(ids, pos):
        spot = (ids & (n_loc - 1)) * blk + (ids // n_loc) * cap
        return jnp.where(pos < cap, spot.astype(F32) + pos, float(n_exp * cap))

    s1r[...] = place(ids1, pos1)
    s2r[...] = place(ids2, pos2)

    def masks(j):
        spot = (lax.broadcasted_iota(I32, (blk, n_tok), 0) + j * blk).astype(F32)
        return s1r[...] == spot, s2r[...] == spot

    chip = r // 2
    chip_x = chip + 1 - 2 * (chip % 2)
    chip_y = (chip + 2) % 4
    chip_d = 3 - chip
    core = r % 2
    diag = 2 * chip_d + (k + r) % 2
    near = [2 * chip_x + core, 2 * chip_y + core, 2 * chip_x + 1 - core, 2 * chip_y + 1 - core, 2 * chip + 1 - core]
    far = [2 * chip_d + core, 2 * chip_d + 1 - core]

    def place_of(q):
        return (q % tp_size) * half + q // tp_size

    def send_row(src, dst, send_sem, recv_sem, j, q):
        pltpu.make_async_remote_copy(
            src_ref=src.at[j, q], dst_ref=dst.at[j, my_place],
            send_sem=send_sem, recv_sem=recv_sem.at[j],
            device_id=(k, q), device_id_type=MESH,
        ).start()

    def wait_recv(view, sem):
        pltpu.make_async_remote_copy(
            src_ref=view, dst_ref=view, send_sem=sem, recv_sem=sem, device_id=(k, r), device_id_type=MESH
        ).wait_recv()

    def wait_send(view, sem):
        pltpu.make_async_remote_copy(
            src_ref=view, dst_ref=view, send_sem=sem, recv_sem=sem, device_id=(k, r), device_id_type=MESH
        ).wait_send()

    def gather_x(j):
        m1, m2 = masks(j)
        pick = jnp.where(m1 | m2, 1.0, 0.0).astype(BF)
        for c in range(0, width, 512):
            rows = dot(pick, x_v[:, c:c + 512]).astype(BF)
            xs[j, :, :, c:c + 512] = rows.reshape(ep_size, cap, 512)

    def send_x(j, via_tp):
        if via_tp:
            send_row(xs, xr, xs_sem, xd_sem, j, diag)
        for q in near if via_tp else far + near:
            send_row(xs, xr, xs_sem, xr_sem, j, q)
        xr[j, my_place] = xs[j, r]

    ins[0].wait()
    ins[2].start()
    ins[1].start()

    @pl.loop(0, n_loc)
    def _(j):
        for c in weight_copies(j):
            c.start()

    @pl.loop(0, EARLY)
    def _(j):
        gather_x(j)

    pl.semaphore_wait(barrier, n_dev - 1)

    @pl.loop(0, EARLY)
    def _(j):
        send_x(j, True)

    @pl.loop(EARLY, VIA_TP)
    def _(j):
        gather_x(j)
        send_x(j, True)

    if VIA_TP < n_loc:
        @pl.loop(VIA_TP, n_loc)
        def _(j):
            gather_x(j)
            send_x(j, False)

    def column(row):
        return jnp.transpose(jnp.broadcast_to(row, (128, n_tok)))

    s1c[...] = column(s1r[...])
    s2c[...] = column(s2r[...])
    i1c[...] = column(ids1.astype(F32))
    i2c[...] = column(ids2.astype(F32))
    ins[2].wait()
    wr_hi, wr_mid, wr_low = split3(wr_v[...])
    xv = x_v[...]
    logits = dot(xv, wr_hi, NT) + (dot(xv, wr_mid, NT) + dot(xv, wr_low, NT))
    ex = jnp.exp(logits - jnp.max(logits, axis=1, keepdims=True))
    prob = ex / jnp.sum(ex, axis=1, keepdims=True)
    prob_v[...] = prob
    lane = lax.broadcasted_iota(I32, (n_tok, n_exp), 1).astype(F32)
    q1 = jnp.sum(jnp.where(i1c[:, :n_exp] == lane, prob, 0.0), axis=1, keepdims=True)
    q2 = jnp.sum(jnp.where(i2c[:, :n_exp] == lane, prob, 0.0), axis=1, keepdims=True)
    g1 = jnp.broadcast_to(q1 / (q1 + q2), (n_tok, 128))
    g2 = jnp.broadcast_to(q2 / (q1 + q2), (n_tok, 128))
    g1c[...] = g1
    g2c[...] = g2
    q1c[...] = jnp.broadcast_to(q1, (n_tok, 128))
    q2c[...] = jnp.broadcast_to(q2, (n_tok, 128))
    g1r[...] = jnp.transpose(g1)[0:1, :]
    g2r[...] = jnp.transpose(g2)[0:1, :]
    ins[1].wait()

    def build_d(j):
        m1, m2 = masks(j)
        pick = jnp.where(m1 | m2, 1.0, 0.0).astype(BF)
        gate = jnp.sum(jnp.where(m1, g1r[...], 0.0) + jnp.where(m2, g2r[...], 0.0), axis=1, keepdims=True)
        for c in range(0, width, 512):
            rows = (gate * dot(pick, dy_v[:, c:c + 512])).astype(BF)
            ds[j, :, :, c:c + 512] = rows.reshape(ep_size, cap, 512)
        for q in far + near:
            send_row(ds, dr, ds_sem, dr_sem, j, q)
        dr[j, my_place] = ds[j, r]

    def send_half(src, dst, send_sem, recv_sem, j):
        pltpu.make_async_remote_copy(
            src_ref=src.at[j, pl.ds(other * half, half)], dst_ref=dst.at[j],
            send_sem=send_sem, recv_sem=recv_sem.at[j],
            device_id=(other, r), device_id_type=MESH,
        ).start()

    def merge_and_return(src, got, got_sem, dst, send_sem, recv_sem, j):
        wait_recv(got.at[j], got_sem.at[j])
        mine = pl.ds(k * half, half)
        src[j, mine] = (src[j, mine].astype(F32) + got[j].astype(F32)).astype(BF)
        for d in range(half):
            c = (r // tp_size + d) % half
            q = tp_size * c + k

            @pl.when(q != r)
            def _():
                pltpu.make_async_remote_copy(
                    src_ref=src.at[j, k * half + c], dst_ref=dst.at[j, r],
                    send_sem=send_sem, recv_sem=recv_sem.at[j],
                    device_id=(k, q), device_id_type=MESH,
                ).start()

            @pl.when(q == r)
            def _():
                dst[j, r] = src[j, k * half + c]

    n_near = len(near)
    diag_place = place_of(diag)

    def forward_diag(j):
        wait_recv(xr.at[j, 0], xd_sem.at[j])
        pltpu.make_async_remote_copy(
            src_ref=xr.at[j, diag_place], dst_ref=xr.at[j, diag_place],
            send_sem=xfs_sem, recv_sem=xf_sem.at[j],
            device_id=(other, r), device_id_type=MESH,
        ).start()

    for i in range(FORWARD):
        forward_diag(i)

    @pl.loop(0, n_loc)
    def _(j):
        @pl.when(j >= n_loc - AHEAD)
        def _():
            build_d(j + AHEAD - n_loc)

        @pl.when(j + FORWARD < VIA_TP)
        def _():
            forward_diag(j + FORWARD)

        for c in weight_copies(j):
            c.wait()

        @pl.when(j < VIA_TP)
        def _():
            wait_recv(xr.at[j, pl.ds(0, n_near)], xr_sem.at[j])
            wait_recv(xr.at[j, 0], xf_sem.at[j])

        if VIA_TP < n_loc:
            @pl.when(j >= VIA_TP)
            def _():
                wait_recv(xr.at[j, pl.ds(0, ep_size - 1)], xr_sem.at[j])

        rows = xr[j].reshape(blk, width)
        pa = dot(rows, wa_v[j])
        pb = dot(rows, wb_v[j])
        th = jnp.tanh(GELU_COEF * (pa + 0.044715 * pa * pa * pa))
        gv = 0.5 * pa * (1.0 + th)
        slope = 0.5 * (1.0 + th) + 0.5 * pa * (1.0 - th * th) * GELU_COEF * (1.0 + 0.134145 * pa * pa)
        gv_v[j] = gv
        bs_v[j] = pb * slope
        hidden = (gv * pb).astype(BF)
        h_v[j] = hidden
        for c in range(0, width, 512):
            ps[j, :, :, c:c + 512] = dot(hidden, wc_v[j, :, c:c + 512]).astype(BF).reshape(ep_size, cap, 512)
        send_half(ps, pr, ps_sem, pr_sem, j)

        @pl.when(j >= LAG)
        def _():
            merge_and_return(ps, pr, pr_sem, orr, os_sem, or_sem, j - LAG)

    tb = 128
    n_tb = n_tok // tb

    def spots(col, toks):
        lanes = lax.broadcasted_iota(I32, (tb, 128), 1).astype(F32)
        base = col[toks, :]
        return jnp.concatenate([base == lanes + float(u * 128) for u in range(n_exp * cap // 128)], axis=1)

    def ship(buf, t, send_sem, recv_sem):
        toks = pl.ds(pl.multiple_of(t * tb, tb), tb)
        pltpu.make_async_remote_copy(
            src_ref=buf.at[toks], dst_ref=buf.at[toks], send_sem=send_sem, recv_sem=recv_sem.at[t],
            device_id=(other, r), device_id_type=MESH,
        ).start()

    def combine_y(t):
        toks = pl.ds(pl.multiple_of(t * tb, tb), tb)
        pick1 = jnp.where(spots(s1c, toks), 1.0, 0.0).astype(BF)
        pick2 = jnp.where(spots(s2c, toks), 1.0, 0.0).astype(BF)
        dg1 = jnp.zeros((tb, 1), F32)
        dg2 = jnp.zeros((tb, 1), F32)
        ga = g1c[toks, 0:1]
        gb = g2c[toks, 0:1]
        for c in range(0, width, 512):
            rows = orr[:, :, :, c:c + 512].reshape(n_exp * cap, 512)
            o1 = dot(pick1, rows)
            o2 = dot(pick2, rows)
            y_v[toks, c:c + 512] = (ga * o1 + gb * o2).astype(BF)
            dyf = dy_v[toks, c:c + 512].astype(F32)
            dg1 = dg1 + jnp.sum(dyf * o1, axis=1, keepdims=True)
            dg2 = dg2 + jnp.sum(dyf * o2, axis=1, keepdims=True)
        qa = q1c[toks, 0:1]
        qb = q2c[toks, 0:1]
        shared = dg1 * ga + dg2 * gb
        dq1 = (dg1 - shared) / (qa + qb)
        dq2 = (dg2 - shared) / (qa + qb)
        centre = dq1 * qa + dq2 * qb
        lanes = lax.broadcasted_iota(I32, (tb, n_exp), 1).astype(F32)
        pull = jnp.where(i1c[toks, :n_exp] == lanes, dq1, 0.0) + jnp.where(i2c[toks, :n_exp] == lanes, dq2, 0.0)
        dl_v[toks, :] = prob_v[toks, :] * (pull - centre)

    def router_parts():
        d_hi, d_mid, d_low = split3(dl_v[...])
        for c in range(0, width, 512):
            xc = x_v[:, c:c + 512]
            piece = dot(d_hi, xc, TN) + (dot(d_mid, xc, TN) + dot(d_low, xc, TN))
            dwp[:, :, c:c + 512] = piece.reshape(ep_size, n_loc, 512)
        for d in range(1, ep_size):
            q = (r + d) % ep_size
            pltpu.make_async_remote_copy(
                src_ref=dwp.at[q], dst_ref=dwi.at[r], send_sem=rs_sem, recv_sem=rr_sem,
                device_id=(q % tp_size, q), device_id_type=MESH,
            ).start()
        dwi[r] = dwp[r]

    def router_sum():
        wait_recv(dwi.at[pl.ds(0, ep_size - 1)], rr_sem)
        total = dwi[0]
        for q in range(1, ep_size):
            total = total + dwi[q]
        dwf[r] = total
        for d in range(1, ep_size):
            q = (r + d) % ep_size
            pltpu.make_async_remote_copy(
                src_ref=dwf.at[r], dst_ref=dwf.at[r], send_sem=fs_sem, recv_sem=fr_sem,
                device_id=(q % tp_size, q), device_id_type=MESH,
            ).start()

    wait_send(xs.at[pl.ds(0, VIA_TP), pl.ds(0, n_near + 1)], xs_sem)
    if VIA_TP < n_loc:
        wait_send(xs.at[pl.ds(VIA_TP, n_loc - VIA_TP), pl.ds(0, ep_size - 1)], xs_sem)
    @pl.loop(0, n_loc)
    def _(j):
        @pl.when(j + AHEAD < n_loc)
        def _():
            build_d(j + AHEAD)

        wait_recv(dr.at[j, pl.ds(0, ep_size - 1)], dr_sem.at[j])
        rows = dr[j].reshape(blk, width)
        dh = dot(rows, wc_v[j], NT)
        da = (dh * bs_v[j]).astype(BF)
        db = (dh * gv_v[j]).astype(BF)
        da_v[j] = da
        db_v[j] = db
        for c in range(0, width, 512):
            part = dot(da, wa_v[j, c:c + 512, :], NT) + dot(db, wb_v[j, c:c + 512, :], NT)
            xs[j, :, :, c:c + 512] = part.astype(BF).reshape(ep_size, cap, 512)
        send_half(xs, pdr, pds_sem, pdr_sem, j)

        @pl.when(j == 0)
        def _():
            for i in range(LAG):
                merge_and_return(ps, pr, pr_sem, orr, os_sem, or_sem, n_loc - LAG + i)

        @pl.when(j >= BACK_LAG)
        def _():
            merge_and_return(xs, pdr, pdr_sem, dxr, dxs_sem, dxr_sem, j - BACK_LAG)

        @pl.when(owner & (j == Y_STEP))
        def _():
            @pl.loop(0, n_loc)
            def _(i):
                wait_recv(orr.at[i, pl.ds(0, ep_size - 1)], or_sem.at[i])

        @pl.when(owner & (j >= Y_STEP) & (j < Y_STEP + n_tb // 2))
        def _():
            t0 = 2 * (j - Y_STEP)

            @pl.loop(t0, t0 + 2)
            def _(t):
                combine_y(t)

            ship(y_v, j - Y_STEP, ys_sem, yr_sem)

        @pl.when(owner & (j == Y_STEP + n_tb // 2))
        def _():
            ship(y_v, n_tb // 2, ys_sem, yr_sem)

        @pl.when(owner & (j == Y_STEP + n_tb // 2 - 1))
        def _():
            router_parts()

    outs = [
        pltpu.make_async_copy(xr, xe_out, out_sem.at[0]),
        pltpu.make_async_copy(dr, de_out, out_sem.at[1]),
        pltpu.make_async_copy(h_v, h_out, out_sem.at[2]),
        pltpu.make_async_copy(da_v, da_out, out_sem.at[3]),
        pltpu.make_async_copy(db_v, db_out, out_sem.at[4]),
    ]
    for c in outs[:3]:
        c.start()

    split = n_loc - 2

    def pick_both(t):
        toks = pl.ds(pl.multiple_of(t * tb, tb), tb)
        return toks, jnp.where(spots(s1c, toks) | spots(s2c, toks), 1.0, 0.0).astype(BF)

    def sum_first(t):
        toks, pick = pick_both(t)
        dl = dl_v[toks, :]
        for c in range(0, width, 512):
            rows = dxr[0:split, :, :, c:c + 512].reshape(split * blk, 512)
            router = lax.dot_general(
                dl, wr_v[:, c:c + 512], NN, precision=lax.Precision.HIGHEST, preferred_element_type=F32
            )
            acc_v[toks, c:c + 512] = dot(pick[:, :split * blk], rows) + router

    def sum_last(t):
        toks, pick = pick_both(t)
        for c in range(0, width, 512):
            rows = dxr[split:n_loc, :, :, c:c + 512].reshape((n_loc - split) * blk, 512)
            dx_v[toks, c:c + 512] = (acc_v[toks, c:c + 512] + dot(pick[:, split * blk:], rows)).astype(BF)
        pltpu.make_async_copy(dx_v.at[toks], dx_out.at[toks], in_sem.at[1]).start()

    for c in outs[3:]:
        c.start()

    for i in range(BACK_LAG - 1):
        merge_and_return(xs, pdr, pdr_sem, dxr, dxs_sem, dxr_sem, n_loc - BACK_LAG + i)

    @pl.when(owner)
    def _():
        router_sum()
        ship(y_v, n_tb - 1, ys_sem, yr_sem)
        pltpu.make_async_copy(y_v, y_out, in_sem.at[0]).start()

    merge_and_return(xs, pdr, pdr_sem, dxr, dxs_sem, dxr_sem, n_loc - 1)

    @pl.when(owner)
    def _():
        @pl.loop(0, split)
        def _(j):
            wait_recv(dxr.at[j, pl.ds(0, ep_size - 1)], dxr_sem.at[j])

        @pl.loop(0, n_tb)
        def _(t):
            sum_first(t)

        wait_recv(dwf.at[pl.ds(0, ep_size - 1)], fr_sem)
        pltpu.make_async_remote_copy(
            src_ref=dwf, dst_ref=dwf, send_sem=gs_sem, recv_sem=gr_sem,
            device_id=(k, 2 * chip + 1 - core), device_id_type=MESH,
        ).start()

        @pl.loop(split, n_loc)
        def _(j):
            wait_recv(dxr.at[j, pl.ds(0, ep_size - 1)], dxr_sem.at[j])

        @pl.loop(0, n_tb)
        def _(t):
            sum_last(t)

        wait_send(dwp.at[pl.ds(0, ep_size - 1)], rs_sem)
        wait_send(dwf.at[pl.ds(0, ep_size - 1)], fs_sem)
        wait_send(dwf, gs_sem)
        wait_send(y_v, ys_sem)
        wait_send(orr.at[:, pl.ds(0, half - 1)], os_sem)
        wait_send(dxr.at[:, pl.ds(0, half - 1)], dxs_sem)

    @pl.when(jnp.logical_not(owner))
    def _():
        dx_v[...] = jnp.zeros_like(dx_v)
        pltpu.make_async_copy(dx_v, dx_out, in_sem.at[1]).start()
        for t in range(n_tb):
            toks = pl.ds(t * tb, tb)
            wait_recv(y_v.at[toks], yr_sem.at[t])
            pltpu.make_async_copy(y_v.at[toks], y_out.at[toks], in_sem.at[0]).start()
        wait_recv(dwf, gr_sem)
        wait_send(orr.at[:, pl.ds(0, half)], os_sem)
        wait_send(dxr.at[:, pl.ds(0, half)], dxs_sem)

    finals = [
        pltpu.make_async_copy(dwf, dwr_out, in_sem.at[2]),
        pltpu.make_async_copy(y_v, y_out, in_sem.at[0]),
        pltpu.make_async_copy(dx_v, dx_out, in_sem.at[1]),
    ]
    finals[0].start()
    wait_send(ds.at[:, pl.ds(0, ep_size - 1)], ds_sem)
    wait_send(xr.at[pl.ds(0, VIA_TP), 0], xfs_sem)
    wait_send(ps.at[:, pl.ds(0, half)], ps_sem)
    wait_send(xs.at[:, pl.ds(0, half)], pds_sem)
    for c in outs + finals:
        c.wait()


def weight_kernel(xe, de, h, da, db, y, dwr, ga_out, gb_out, gc_out, y_out, dwr_out):
    y_out[...] = y[...]
    dwr_out[...] = dwr[...]
    rows = xe[0]
    ga_out[0] = dot(rows, da[0], TN)
    gb_out[0] = dot(rows, db[0], TN)
    gc_out[0] = dot(h[0], de[0], TN)


def solution(mesh):
    tp_size = mesh.shape["tp"]
    ep_size = mesh.shape["ep"]

    def local_step(x_rows, w_router, first_ids, second_ids, w_gelu, w_lin, w_out, dy_rows):
        n_tok, width = x_rows.shape
        n_exp = w_router.shape[1]
        n_loc, _, hid = w_gelu.shape
        cap = 2 * n_tok // n_exp
        blk = ep_size * cap
        half = ep_size // tp_size
        dma = pltpu.SemaphoreType.DMA
        any_spec = pl.BlockSpec(memory_space=pl.ANY)
        sds = jax.ShapeDtypeStruct
        rows_shape = (n_loc, ep_size, cap, width)
        half_shape = (n_loc, half, cap, width)
        hid_shape = (n_loc, blk, hid)
        col = pltpu.VMEM((n_tok, 128), F32)
        row = pltpu.VMEM((1, n_tok), F32)
        outs = pl.pallas_call(
            functools.partial(moe_kernel, tp_size, ep_size, cap),
            name="moe",
            in_specs=[any_spec] * 8,
            out_specs=[any_spec] * 8,
            out_shape=[
                sds((n_tok, width), BF), sds((n_tok, width), BF), sds((ep_size, n_loc, width), F32),
                sds(rows_shape, BF), sds(rows_shape, BF), sds(hid_shape, BF), sds(hid_shape, BF), sds(hid_shape, BF),
            ],
            scratch_shapes=[
                pltpu.VMEM((n_tok, width), BF), pltpu.VMEM((n_tok, width), BF), pltpu.VMEM((n_exp, width), F32),
                pltpu.VMEM((n_loc, width, hid), BF), pltpu.VMEM((n_loc, width, hid), BF), pltpu.VMEM((n_loc, hid, width), BF),
                pltpu.VMEM(rows_shape, BF), pltpu.VMEM(rows_shape, BF), pltpu.VMEM(rows_shape, BF), pltpu.VMEM(rows_shape, BF),
                pltpu.VMEM(hid_shape, BF), pltpu.VMEM(hid_shape, BF), pltpu.VMEM(hid_shape, BF),
                pltpu.VMEM(hid_shape, F32), pltpu.VMEM(hid_shape, F32),
                pltpu.VMEM(rows_shape, BF), pltpu.VMEM(half_shape, BF), pltpu.VMEM(half_shape, BF),
                pltpu.VMEM(rows_shape, BF), pltpu.VMEM(rows_shape, BF),
                pltpu.VMEM((n_tok, width), BF), pltpu.VMEM((n_tok, width), BF),
                row, row, row, row, col, col, col, col, col, col, col, col,
                pltpu.VMEM((n_tok, n_exp), F32), pltpu.VMEM((n_tok, n_exp), F32),
                pltpu.VMEM((ep_size, n_loc, width), F32), pltpu.VMEM((ep_size, n_loc, width), F32),
                pltpu.VMEM((ep_size, n_loc, width), F32), pltpu.VMEM((n_tok, width), F32),
                pltpu.VMEM((1, n_tok), I32), pltpu.VMEM((1, n_tok), I32),
                dma((3,)), dma((3, n_loc)), dma((5,)), dma((2,)),
                dma(()), dma((n_loc,)), dma((n_loc,)), dma((n_loc,)), dma(()), dma(()), dma((n_loc,)),
                dma(()), dma((n_loc,)), dma(()), dma((n_loc,)),
                dma(()), dma((n_loc,)), dma(()), dma((n_loc,)),
                dma(()), dma((n_tok // 128,)),
                dma(()), dma(()), dma(()), dma(()), dma(()), dma(()),
            ],
            compiler_params=pltpu.CompilerParams(
                collective_id=0, has_side_effects=True, vmem_limit_bytes=67043328
            ),
        )(
            first_ids.reshape(1, n_tok), second_ids.reshape(1, n_tok), x_rows, dy_rows, w_router.T,
            w_gelu, w_lin, w_out,
        )
        act_out, grad_in, grad_router, xe, de, h, da, db = outs
        partners = [
            ((q % tp_size) * ep_size + q, (1 - q % tp_size) * ep_size + q) for q in range(ep_size)
        ]
        passed = lax.ppermute(grad_in, ("tp", "ep"), partners)
        owner = lax.axis_index("ep") % tp_size == lax.axis_index("tp")
        grad_in = jnp.where(owner, grad_in, passed)
        xe = xe.reshape(n_loc, blk, width)
        de = de.reshape(n_loc, blk, width)

        y_spec = pl.BlockSpec((n_tok // n_loc, width), lambda e: (e, 0))

        def spec(*shape):
            return pl.BlockSpec((1,) + shape, lambda e: (e, 0, 0))

        grad_wa, grad_wb, grad_wc, act_out, grad_router = pl.pallas_call(
            weight_kernel,
            name="weight_grads",
            grid=(n_loc,),
            in_specs=[spec(blk, width), spec(blk, width), spec(blk, hid), spec(blk, hid), spec(blk, hid), y_spec, spec(n_exp // n_loc, width)],
            out_specs=[spec(width, hid), spec(width, hid), spec(hid, width), y_spec, spec(n_exp // n_loc, width)],
            out_shape=[
                sds((n_loc, width, hid), F32), sds((n_loc, width, hid), F32), sds((n_loc, hid, width), F32),
                sds((n_tok, width), BF), sds((n_loc, n_exp // n_loc, width), F32),
            ],
            compiler_params=pltpu.CompilerParams(
                dimension_semantics=("arbitrary",), vmem_limit_bytes=63743328
            ),
            cost_estimate=pl.CostEstimate(
                flops=6 * n_loc * blk * width * hid, transcendentals=0,
                bytes_accessed=12 * n_loc * width * hid + 4 * n_loc * blk * width + 6 * n_loc * blk * hid,
            ),
        )(xe, de, h, da, db, act_out, grad_router.reshape(n_loc, n_exp // n_loc, width))
        return act_out, grad_in, grad_wa, grad_wb, grad_wc, grad_router.reshape(n_exp, width).T

    return jax.shard_map(
        local_step,
        mesh=mesh,
        in_specs=(P("ep", None), P(), P("ep"), P("ep"), P("ep", None, "tp"), P("ep", None, "tp"), P("ep", "tp", None), P("ep", None)),
        out_specs=(P("ep", None), P("ep", None), P("ep", None, "tp"), P("ep", None, "tp"), P("ep", "tp", None), P()),
        check_vma=False,
    )
```

```python
import functools

import jax
import jax.numpy as jnp
from jax import lax
from jax.experimental import pallas as pl
from jax.experimental.pallas import tpu as pltpu
from jax.sharding import PartitionSpec as P

BF = jnp.bfloat16
F32 = jnp.float32
I32 = jnp.int32
MESH = pl.DeviceIdType.MESH
GELU_COEF = 0.7978845608028654
AHEAD = 3
LAG = 3
Y_STEP = 3
FORWARD = 2
VIA_TP = 8
BACK_LAG = 2
EARLY = 2
NN = (((1,), (0,)), ((), ()))
NT = (((1,), (1,)), ((), ()))
TN = (((0,), (0,)), ((), ()))


def dot(a, b, dims=NN):
    return lax.dot_general(a, b, dims, preferred_element_type=F32)


def split3(v):
    hi = v.astype(BF)
    rest = v - hi.astype(F32)
    mid = rest.astype(BF)
    low = (rest - mid.astype(F32)).astype(BF)
    return hi, mid, low


def moe_kernel(
    tp_size, ep_size, cap,
    ids1_hbm, ids2_hbm, x_hbm, dy_hbm, wr_hbm, wa_hbm, wb_hbm, wc_hbm,
    y_out, dx_out, dwr_out, xe_out, de_out, h_out, da_out, db_out,
    x_v, dy_v, wr_v, wa_v, wb_v, wc_v,
    xs, ds, xr, dr, h_v, da_v, db_v, bs_v, gv_v,
    ps, pr, pdr, orr, dxr, y_v, dx_v,
    s1r, s2r, g1r, g2r, s1c, s2c, g1c, g2c, q1c, q2c, i1c, i2c, prob_v, dl_v,
    dwp, dwi, dwf, acc_v, ids1_ref, ids2_ref,
    in_sem, w_sem, out_sem, id_sem,
    xs_sem, xr_sem, xd_sem, xf_sem, xfs_sem, ds_sem, dr_sem,
    ps_sem, pr_sem, pds_sem, pdr_sem,
    os_sem, or_sem, dxs_sem, dxr_sem,
    ys_sem, yr_sem,
    rs_sem, rr_sem, fs_sem, fr_sem, gs_sem, gr_sem,
):
    k = lax.axis_index("tp")
    r = lax.axis_index("ep")
    n_loc = wa_v.shape[0]
    n_tok, width = x_v.shape
    hid = wa_v.shape[2]
    n_exp = n_loc * ep_size
    blk = ep_size * cap
    half = ep_size // tp_size
    my_place = (r % tp_size) * half + r // tp_size
    owner = (r % tp_size) == k
    other = 1 - k

    ins = [
        pltpu.make_async_copy(x_hbm, x_v, in_sem.at[0]),
        pltpu.make_async_copy(dy_hbm, dy_v, in_sem.at[1]),
        pltpu.make_async_copy(wr_hbm, wr_v, in_sem.at[2]),
    ]
    id_loads = [pltpu.make_async_copy(ids1_hbm, ids1_ref, id_sem.at[0]), pltpu.make_async_copy(ids2_hbm, ids2_ref, id_sem.at[1])]
    for c in id_loads:
        c.start()
    ins[0].start()

    def weight_copies(j):
        return [
            pltpu.make_async_copy(wa_hbm.at[j], wa_v.at[j], w_sem.at[0, j]),
            pltpu.make_async_copy(wb_hbm.at[j], wb_v.at[j], w_sem.at[1, j]),
            pltpu.make_async_copy(wc_hbm.at[j], wc_v.at[j], w_sem.at[2, j]),
        ]

    n_dev = tp_size * ep_size
    barrier = pltpu.get_barrier_semaphore()
    for d in range(1, n_dev):
        flat = (k * ep_size + r + d) % n_dev
        pl.semaphore_signal(barrier, inc=1, device_id=(flat // ep_size, flat % ep_size), device_id_type=MESH)

    for c in id_loads:
        c.wait()
    ids1 = ids1_ref[...]
    ids2 = ids2_ref[...]
    e_iota = lax.broadcasted_iota(I32, (n_exp, n_tok), 0)
    hot1 = jnp.where(ids1 == e_iota, 1.0, 0.0).astype(F32)
    hot2 = jnp.where(ids2 == e_iota, 1.0, 0.0).astype(F32)
    before = jnp.where(
        lax.broadcasted_iota(I32, (n_tok, n_tok), 0) < lax.broadcasted_iota(I32, (n_tok, n_tok), 1), 1.0, 0.0
    ).astype(BF)
    cum1 = dot(hot1.astype(BF), before)
    cum2 = dot(hot2.astype(BF), before)
    fill1 = jnp.sum(hot1, axis=1, keepdims=True)
    pos1 = jnp.sum(cum1 * hot1, axis=0, keepdims=True)
    pos2 = jnp.sum((cum2 + fill1) * hot2, axis=0, keepdims=True)

    def place(ids, pos):
        spot = (ids & (n_loc - 1)) * blk + (ids // n_loc) * cap
        return jnp.where(pos < cap, spot.astype(F32) + pos, float(n_exp * cap))

    s1r[...] = place(ids1, pos1)
    s2r[...] = place(ids2, pos2)

    def masks(j):
        spot = (lax.broadcasted_iota(I32, (blk, n_tok), 0) + j * blk).astype(F32)
        return s1r[...] == spot, s2r[...] == spot

    chip = r // 2
    chip_x = chip + 1 - 2 * (chip % 2)
    chip_y = (chip + 2) % 4
    chip_d = 3 - chip
    core = r % 2
    diag = 2 * chip_d + (k + r) % 2
    near = [2 * chip_x + core, 2 * chip_y + core, 2 * chip_x + 1 - core, 2 * chip_y + 1 - core, 2 * chip + 1 - core]
    far = [2 * chip_d + core, 2 * chip_d + 1 - core]

    def place_of(q):
        return (q % tp_size) * half + q // tp_size

    def send_row(src, dst, send_sem, recv_sem, j, q):
        pltpu.make_async_remote_copy(
            src_ref=src.at[j, q], dst_ref=dst.at[j, my_place],
            send_sem=send_sem, recv_sem=recv_sem.at[j],
            device_id=(k, q), device_id_type=MESH,
        ).start()

    def wait_recv(view, sem):
        pltpu.make_async_remote_copy(
            src_ref=view, dst_ref=view, send_sem=sem, recv_sem=sem, device_id=(k, r), device_id_type=MESH
        ).wait_recv()

    def wait_send(view, sem):
        pltpu.make_async_remote_copy(
            src_ref=view, dst_ref=view, send_sem=sem, recv_sem=sem, device_id=(k, r), device_id_type=MESH
        ).wait_send()

    def gather_x(j):
        m1, m2 = masks(j)
        pick = jnp.where(m1 | m2, 1.0, 0.0).astype(BF)
        for c in range(0, width, 512):
            rows = dot(pick, x_v[:, c:c + 512]).astype(BF)
            xs[j, :, :, c:c + 512] = rows.reshape(ep_size, cap, 512)

    def send_x(j, via_tp):
        if via_tp:
            send_row(xs, xr, xs_sem, xd_sem, j, diag)
        for q in near if via_tp else far + near:
            send_row(xs, xr, xs_sem, xr_sem, j, q)
        xr[j, my_place] = xs[j, r]

    ins[0].wait()
    ins[2].start()
    ins[1].start()

    @pl.loop(0, n_loc)
    def _(j):
        for c in weight_copies(j):
            c.start()

    @pl.loop(0, EARLY)
    def _(j):
        gather_x(j)

    pl.semaphore_wait(barrier, n_dev - 1)

    @pl.loop(0, EARLY)
    def _(j):
        send_x(j, True)

    @pl.loop(EARLY, VIA_TP)
    def _(j):
        gather_x(j)
        send_x(j, True)

    if VIA_TP < n_loc:
        @pl.loop(VIA_TP, n_loc)
        def _(j):
            gather_x(j)
            send_x(j, False)

    def column(row):
        return jnp.transpose(jnp.broadcast_to(row, (128, n_tok)))

    s1c[...] = column(s1r[...])
    s2c[...] = column(s2r[...])
    i1c[...] = column(ids1.astype(F32))
    i2c[...] = column(ids2.astype(F32))
    ins[2].wait()
    wr_hi, wr_mid, wr_low = split3(wr_v[...])
    xv = x_v[...]
    logits = dot(xv, wr_hi, NT) + (dot(xv, wr_mid, NT) + dot(xv, wr_low, NT))
    ex = jnp.exp(logits - jnp.max(logits, axis=1, keepdims=True))
    prob = ex / jnp.sum(ex, axis=1, keepdims=True)
    prob_v[...] = prob
    lane = lax.broadcasted_iota(I32, (n_tok, n_exp), 1).astype(F32)
    q1 = jnp.sum(jnp.where(i1c[:, :n_exp] == lane, prob, 0.0), axis=1, keepdims=True)
    q2 = jnp.sum(jnp.where(i2c[:, :n_exp] == lane, prob, 0.0), axis=1, keepdims=True)
    g1 = jnp.broadcast_to(q1 / (q1 + q2), (n_tok, 128))
    g2 = jnp.broadcast_to(q2 / (q1 + q2), (n_tok, 128))
    g1c[...] = g1
    g2c[...] = g2
    q1c[...] = jnp.broadcast_to(q1, (n_tok, 128))
    q2c[...] = jnp.broadcast_to(q2, (n_tok, 128))
    g1r[...] = jnp.transpose(g1)[0:1, :]
    g2r[...] = jnp.transpose(g2)[0:1, :]
    ins[1].wait()

    def build_d(j):
        m1, m2 = masks(j)
        pick = jnp.where(m1 | m2, 1.0, 0.0).astype(BF)
        gate = jnp.sum(jnp.where(m1, g1r[...], 0.0) + jnp.where(m2, g2r[...], 0.0), axis=1, keepdims=True)
        for c in range(0, width, 512):
            rows = (gate * dot(pick, dy_v[:, c:c + 512])).astype(BF)
            ds[j, :, :, c:c + 512] = rows.reshape(ep_size, cap, 512)
        for q in far + near:
            send_row(ds, dr, ds_sem, dr_sem, j, q)
        dr[j, my_place] = ds[j, r]

    def send_half(src, dst, send_sem, recv_sem, j):
        pltpu.make_async_remote_copy(
            src_ref=src.at[j, pl.ds(other * half, half)], dst_ref=dst.at[j],
            send_sem=send_sem, recv_sem=recv_sem.at[j],
            device_id=(other, r), device_id_type=MESH,
        ).start()

    def merge_and_return(src, got, got_sem, dst, send_sem, recv_sem, j):
        wait_recv(got.at[j], got_sem.at[j])
        mine = pl.ds(k * half, half)
        src[j, mine] = (src[j, mine].astype(F32) + got[j].astype(F32)).astype(BF)
        for d in range(half):
            c = (r // tp_size + d) % half
            q = tp_size * c + k

            @pl.when(q != r)
            def _():
                pltpu.make_async_remote_copy(
                    src_ref=src.at[j, k * half + c], dst_ref=dst.at[j, r],
                    send_sem=send_sem, recv_sem=recv_sem.at[j],
                    device_id=(k, q), device_id_type=MESH,
                ).start()

            @pl.when(q == r)
            def _():
                dst[j, r] = src[j, k * half + c]

    n_near = len(near)
    diag_place = place_of(diag)

    def forward_diag(j):
        wait_recv(xr.at[j, 0], xd_sem.at[j])
        pltpu.make_async_remote_copy(
            src_ref=xr.at[j, diag_place], dst_ref=xr.at[j, diag_place],
            send_sem=xfs_sem, recv_sem=xf_sem.at[j],
            device_id=(other, r), device_id_type=MESH,
        ).start()

    for i in range(FORWARD):
        forward_diag(i)

    @pl.loop(0, n_loc)
    def _(j):
        @pl.when(j >= n_loc - AHEAD)
        def _():
            build_d(j + AHEAD - n_loc)

        @pl.when(j + FORWARD < VIA_TP)
        def _():
            forward_diag(j + FORWARD)

        for c in weight_copies(j):
            c.wait()

        @pl.when(j < VIA_TP)
        def _():
            wait_recv(xr.at[j, pl.ds(0, n_near)], xr_sem.at[j])
            wait_recv(xr.at[j, 0], xf_sem.at[j])

        if VIA_TP < n_loc:
            @pl.when(j >= VIA_TP)
            def _():
                wait_recv(xr.at[j, pl.ds(0, ep_size - 1)], xr_sem.at[j])

        rows = xr[j].reshape(blk, width)
        pa = dot(rows, wa_v[j])
        pb = dot(rows, wb_v[j])
        th = jnp.tanh(GELU_COEF * (pa + 0.044715 * pa * pa * pa))
        gv = 0.5 * pa * (1.0 + th)
        slope = 0.5 * (1.0 + th) + 0.5 * pa * (1.0 - th * th) * GELU_COEF * (1.0 + 0.134145 * pa * pa)
        gv_v[j] = gv
        bs_v[j] = pb * slope
        hidden = (gv * pb).astype(BF)
        h_v[j] = hidden
        for c in range(0, width, 512):
            ps[j, :, :, c:c + 512] = dot(hidden, wc_v[j, :, c:c + 512]).astype(BF).reshape(ep_size, cap, 512)
        send_half(ps, pr, ps_sem, pr_sem, j)

        @pl.when(j >= LAG)
        def _():
            merge_and_return(ps, pr, pr_sem, orr, os_sem, or_sem, j - LAG)

    tb = 128
    n_tb = n_tok // tb

    def spots(col, toks):
        lanes = lax.broadcasted_iota(I32, (tb, 128), 1).astype(F32)
        base = col[toks, :]
        return jnp.concatenate([base == lanes + float(u * 128) for u in range(n_exp * cap // 128)], axis=1)

    def ship(buf, t, send_sem, recv_sem):
        toks = pl.ds(pl.multiple_of(t * tb, tb), tb)
        pltpu.make_async_remote_copy(
            src_ref=buf.at[toks], dst_ref=buf.at[toks], send_sem=send_sem, recv_sem=recv_sem.at[t],
            device_id=(other, r), device_id_type=MESH,
        ).start()

    def combine_y(t):
        toks = pl.ds(pl.multiple_of(t * tb, tb), tb)
        pick1 = jnp.where(spots(s1c, toks), 1.0, 0.0).astype(BF)
        pick2 = jnp.where(spots(s2c, toks), 1.0, 0.0).astype(BF)
        dg1 = jnp.zeros((tb, 1), F32)
        dg2 = jnp.zeros((tb, 1), F32)
        ga = g1c[toks, 0:1]
        gb = g2c[toks, 0:1]
        for c in range(0, width, 512):
            rows = orr[:, :, :, c:c + 512].reshape(n_exp * cap, 512)
            o1 = dot(pick1, rows)
            o2 = dot(pick2, rows)
            y_v[toks, c:c + 512] = (ga * o1 + gb * o2).astype(BF)
            dyf = dy_v[toks, c:c + 512].astype(F32)
            dg1 = dg1 + jnp.sum(dyf * o1, axis=1, keepdims=True)
            dg2 = dg2 + jnp.sum(dyf * o2, axis=1, keepdims=True)
        qa = q1c[toks, 0:1]
        qb = q2c[toks, 0:1]
        shared = dg1 * ga + dg2 * gb
        dq1 = (dg1 - shared) / (qa + qb)
        dq2 = (dg2 - shared) / (qa + qb)
        centre = dq1 * qa + dq2 * qb
        lanes = lax.broadcasted_iota(I32, (tb, n_exp), 1).astype(F32)
        pull = jnp.where(i1c[toks, :n_exp] == lanes, dq1, 0.0) + jnp.where(i2c[toks, :n_exp] == lanes, dq2, 0.0)
        dl_v[toks, :] = prob_v[toks, :] * (pull - centre)

    def router_parts():
        d_hi, d_mid, d_low = split3(dl_v[...])
        for c in range(0, width, 512):
            xc = x_v[:, c:c + 512]
            piece = dot(d_hi, xc, TN) + (dot(d_mid, xc, TN) + dot(d_low, xc, TN))
            dwp[:, :, c:c + 512] = piece.reshape(ep_size, n_loc, 512)
        for d in range(1, ep_size):
            q = (r + d) % ep_size
            pltpu.make_async_remote_copy(
                src_ref=dwp.at[q], dst_ref=dwi.at[r], send_sem=rs_sem, recv_sem=rr_sem,
                device_id=(q % tp_size, q), device_id_type=MESH,
            ).start()
        dwi[r] = dwp[r]

    def router_sum():
        wait_recv(dwi.at[pl.ds(0, ep_size - 1)], rr_sem)
        total = dwi[0]
        for q in range(1, ep_size):
            total = total + dwi[q]
        dwf[r] = total
        for d in range(1, ep_size):
            q = (r + d) % ep_size
            pltpu.make_async_remote_copy(
                src_ref=dwf.at[r], dst_ref=dwf.at[r], send_sem=fs_sem, recv_sem=fr_sem,
                device_id=(q % tp_size, q), device_id_type=MESH,
            ).start()

    wait_send(xs.at[pl.ds(0, VIA_TP), pl.ds(0, n_near + 1)], xs_sem)
    if VIA_TP < n_loc:
        wait_send(xs.at[pl.ds(VIA_TP, n_loc - VIA_TP), pl.ds(0, ep_size - 1)], xs_sem)
    @pl.loop(0, n_loc)
    def _(j):
        @pl.when(j + AHEAD < n_loc)
        def _():
            build_d(j + AHEAD)

        wait_recv(dr.at[j, pl.ds(0, ep_size - 1)], dr_sem.at[j])
        rows = dr[j].reshape(blk, width)
        dh = dot(rows, wc_v[j], NT)
        da = (dh * bs_v[j]).astype(BF)
        db = (dh * gv_v[j]).astype(BF)
        da_v[j] = da
        db_v[j] = db
        for c in range(0, width, 512):
            part = dot(da, wa_v[j, c:c + 512, :], NT) + dot(db, wb_v[j, c:c + 512, :], NT)
            xs[j, :, :, c:c + 512] = part.astype(BF).reshape(ep_size, cap, 512)
        send_half(xs, pdr, pds_sem, pdr_sem, j)

        @pl.when(j == 0)
        def _():
            for i in range(LAG):
                merge_and_return(ps, pr, pr_sem, orr, os_sem, or_sem, n_loc - LAG + i)

        @pl.when(j >= BACK_LAG)
        def _():
            merge_and_return(xs, pdr, pdr_sem, dxr, dxs_sem, dxr_sem, j - BACK_LAG)

        @pl.when(owner & (j == Y_STEP))
        def _():
            @pl.loop(0, n_loc)
            def _(i):
                wait_recv(orr.at[i, pl.ds(0, ep_size - 1)], or_sem.at[i])

        @pl.when(owner & (j >= Y_STEP) & (j < Y_STEP + n_tb // 2))
        def _():
            t0 = 2 * (j - Y_STEP)

            @pl.loop(t0, t0 + 2)
            def _(t):
                combine_y(t)

            ship(y_v, j - Y_STEP, ys_sem, yr_sem)

        @pl.when(owner & (j == Y_STEP + n_tb // 2))
        def _():
            ship(y_v, n_tb // 2, ys_sem, yr_sem)

        @pl.when(owner & (j == Y_STEP + n_tb // 2 - 1))
        def _():
            router_parts()

    outs = [
        pltpu.make_async_copy(xr, xe_out, out_sem.at[0]),
        pltpu.make_async_copy(dr, de_out, out_sem.at[1]),
        pltpu.make_async_copy(h_v, h_out, out_sem.at[2]),
        pltpu.make_async_copy(da_v, da_out, out_sem.at[3]),
        pltpu.make_async_copy(db_v, db_out, out_sem.at[4]),
    ]
    for c in outs[:3]:
        c.start()

    split = n_loc - 2

    def pick_both(t):
        toks = pl.ds(pl.multiple_of(t * tb, tb), tb)
        return toks, jnp.where(spots(s1c, toks) | spots(s2c, toks), 1.0, 0.0).astype(BF)

    def sum_first(t):
        toks, pick = pick_both(t)
        dl = dl_v[toks, :]
        for c in range(0, width, 512):
            rows = dxr[0:split, :, :, c:c + 512].reshape(split * blk, 512)
            router = lax.dot_general(
                dl, wr_v[:, c:c + 512], NN, precision=lax.Precision.HIGHEST, preferred_element_type=F32
            )
            acc_v[toks, c:c + 512] = dot(pick[:, :split * blk], rows) + router

    def sum_last(t):
        toks, pick = pick_both(t)
        for c in range(0, width, 512):
            rows = dxr[split:n_loc, :, :, c:c + 512].reshape((n_loc - split) * blk, 512)
            dx_v[toks, c:c + 512] = (acc_v[toks, c:c + 512] + dot(pick[:, split * blk:], rows)).astype(BF)
        pltpu.make_async_copy(dx_v.at[toks], dx_out.at[toks], in_sem.at[1]).start()

    for c in outs[3:]:
        c.start()

    for i in range(BACK_LAG - 1):
        merge_and_return(xs, pdr, pdr_sem, dxr, dxs_sem, dxr_sem, n_loc - BACK_LAG + i)

    @pl.when(owner)
    def _():
        router_sum()
        ship(y_v, n_tb - 1, ys_sem, yr_sem)
        pltpu.make_async_copy(y_v, y_out, in_sem.at[0]).start()

    merge_and_return(xs, pdr, pdr_sem, dxr, dxs_sem, dxr_sem, n_loc - 1)

    @pl.when(owner)
    def _():
        @pl.loop(0, split)
        def _(j):
            wait_recv(dxr.at[j, pl.ds(0, ep_size - 1)], dxr_sem.at[j])

        @pl.loop(0, n_tb)
        def _(t):
            sum_first(t)

        wait_recv(dwf.at[pl.ds(0, ep_size - 1)], fr_sem)
        pltpu.make_async_remote_copy(
            src_ref=dwf, dst_ref=dwf, send_sem=gs_sem, recv_sem=gr_sem,
            device_id=(k, 2 * chip + 1 - core), device_id_type=MESH,
        ).start()

        @pl.loop(split, n_loc)
        def _(j):
            wait_recv(dxr.at[j, pl.ds(0, ep_size - 1)], dxr_sem.at[j])

        @pl.loop(0, n_tb)
        def _(t):
            sum_last(t)

        wait_send(dwp.at[pl.ds(0, ep_size - 1)], rs_sem)
        wait_send(dwf.at[pl.ds(0, ep_size - 1)], fs_sem)
        wait_send(dwf, gs_sem)
        wait_send(y_v, ys_sem)
        wait_send(orr.at[:, pl.ds(0, half - 1)], os_sem)
        wait_send(dxr.at[:, pl.ds(0, half - 1)], dxs_sem)

    @pl.when(jnp.logical_not(owner))
    def _():
        dx_v[...] = jnp.zeros_like(dx_v)
        pltpu.make_async_copy(dx_v, dx_out, in_sem.at[1]).start()
        for t in range(n_tb):
            toks = pl.ds(t * tb, tb)
            wait_recv(y_v.at[toks], yr_sem.at[t])
            pltpu.make_async_copy(y_v.at[toks], y_out.at[toks], in_sem.at[0]).start()
        wait_recv(dwf, gr_sem)
        wait_send(orr.at[:, pl.ds(0, half)], os_sem)
        wait_send(dxr.at[:, pl.ds(0, half)], dxs_sem)

    finals = [
        pltpu.make_async_copy(dwf, dwr_out, in_sem.at[2]),
        pltpu.make_async_copy(y_v, y_out, in_sem.at[0]),
        pltpu.make_async_copy(dx_v, dx_out, in_sem.at[1]),
    ]
    finals[0].start()
    wait_send(ds.at[:, pl.ds(0, ep_size - 1)], ds_sem)
    wait_send(xr.at[pl.ds(0, VIA_TP), 0], xfs_sem)
    wait_send(ps.at[:, pl.ds(0, half)], ps_sem)
    wait_send(xs.at[:, pl.ds(0, half)], pds_sem)
    for c in outs + finals:
        c.wait()


def weight_kernel(xe, de, h, da, db, y, dwr, ga_out, gb_out, gc_out, y_out, dwr_out):
    y_out[...] = y[...]
    dwr_out[...] = dwr[...]
    rows = xe[0]
    ga_out[0] = dot(rows, da[0], TN)
    gb_out[0] = dot(rows, db[0], TN)
    gc_out[0] = dot(h[0], de[0], TN)


def solution(mesh):
    tp_size = mesh.shape["tp"]
    ep_size = mesh.shape["ep"]

    def local_step(x_rows, w_router, first_ids, second_ids, w_gelu, w_lin, w_out, dy_rows):
        n_tok, width = x_rows.shape
        n_exp = w_router.shape[1]
        n_loc, _, hid = w_gelu.shape
        cap = 2 * n_tok // n_exp
        blk = ep_size * cap
        half = ep_size // tp_size
        dma = pltpu.SemaphoreType.DMA
        any_spec = pl.BlockSpec(memory_space=pl.ANY)
        sds = jax.ShapeDtypeStruct
        rows_shape = (n_loc, ep_size, cap, width)
        half_shape = (n_loc, half, cap, width)
        hid_shape = (n_loc, blk, hid)
        col = pltpu.VMEM((n_tok, 128), F32)
        row = pltpu.VMEM((1, n_tok), F32)
        outs = pl.pallas_call(
            functools.partial(moe_kernel, tp_size, ep_size, cap),
            name="moe",
            in_specs=[any_spec] * 8,
            out_specs=[any_spec] * 8,
            out_shape=[
                sds((n_tok, width), BF), sds((n_tok, width), BF), sds((ep_size, n_loc, width), F32),
                sds(rows_shape, BF), sds(rows_shape, BF), sds(hid_shape, BF), sds(hid_shape, BF), sds(hid_shape, BF),
            ],
            scratch_shapes=[
                pltpu.VMEM((n_tok, width), BF), pltpu.VMEM((n_tok, width), BF), pltpu.VMEM((n_exp, width), F32),
                pltpu.VMEM((n_loc, width, hid), BF), pltpu.VMEM((n_loc, width, hid), BF), pltpu.VMEM((n_loc, hid, width), BF),
                pltpu.VMEM(rows_shape, BF), pltpu.VMEM(rows_shape, BF), pltpu.VMEM(rows_shape, BF), pltpu.VMEM(rows_shape, BF),
                pltpu.VMEM(hid_shape, BF), pltpu.VMEM(hid_shape, BF), pltpu.VMEM(hid_shape, BF),
                pltpu.VMEM(hid_shape, F32), pltpu.VMEM(hid_shape, F32),
                pltpu.VMEM(rows_shape, BF), pltpu.VMEM(half_shape, BF), pltpu.VMEM(half_shape, BF),
                pltpu.VMEM(rows_shape, BF), pltpu.VMEM(rows_shape, BF),
                pltpu.VMEM((n_tok, width), BF), pltpu.VMEM((n_tok, width), BF),
                row, row, row, row, col, col, col, col, col, col, col, col,
                pltpu.VMEM((n_tok, n_exp), F32), pltpu.VMEM((n_tok, n_exp), F32),
                pltpu.VMEM((ep_size, n_loc, width), F32), pltpu.VMEM((ep_size, n_loc, width), F32),
                pltpu.VMEM((ep_size, n_loc, width), F32), pltpu.VMEM((n_tok, width), F32),
                pltpu.VMEM((1, n_tok), I32), pltpu.VMEM((1, n_tok), I32),
                dma((3,)), dma((3, n_loc)), dma((5,)), dma((2,)),
                dma(()), dma((n_loc,)), dma((n_loc,)), dma((n_loc,)), dma(()), dma(()), dma((n_loc,)),
                dma(()), dma((n_loc,)), dma(()), dma((n_loc,)),
                dma(()), dma((n_loc,)), dma(()), dma((n_loc,)),
                dma(()), dma((n_tok // 128,)),
                dma(()), dma(()), dma(()), dma(()), dma(()), dma(()),
            ],
            compiler_params=pltpu.CompilerParams(
                collective_id=0, has_side_effects=True, vmem_limit_bytes=67043328
            ),
        )(
            first_ids.reshape(1, n_tok), second_ids.reshape(1, n_tok), x_rows, dy_rows, w_router.T,
            w_gelu, w_lin, w_out,
        )
        act_out, grad_in, grad_router, xe, de, h, da, db = outs
        partners = [
            ((q % tp_size) * ep_size + q, (1 - q % tp_size) * ep_size + q) for q in range(ep_size)
        ]
        passed = lax.ppermute(grad_in, ("tp", "ep"), partners)
        owner = lax.axis_index("ep") % tp_size == lax.axis_index("tp")
        grad_in = jnp.where(owner, grad_in, passed)
        xe = xe.reshape(n_loc, blk, width)
        de = de.reshape(n_loc, blk, width)

        y_spec = pl.BlockSpec((n_tok // n_loc, width), lambda e: (e, 0))

        def spec(*shape):
            return pl.BlockSpec((1,) + shape, lambda e: (e, 0, 0))

        grad_wa, grad_wb, grad_wc, act_out, grad_router = pl.pallas_call(
            weight_kernel,
            name="weight_grads",
            grid=(n_loc,),
            in_specs=[spec(blk, width), spec(blk, width), spec(blk, hid), spec(blk, hid), spec(blk, hid), y_spec, spec(n_exp // n_loc, width)],
            out_specs=[spec(width, hid), spec(width, hid), spec(hid, width), y_spec, spec(n_exp // n_loc, width)],
            out_shape=[
                sds((n_loc, width, hid), F32), sds((n_loc, width, hid), F32), sds((n_loc, hid, width), F32),
                sds((n_tok, width), BF), sds((n_loc, n_exp // n_loc, width), F32),
            ],
            compiler_params=pltpu.CompilerParams(
                dimension_semantics=("arbitrary",), vmem_limit_bytes=63743328
            ),
            cost_estimate=pl.CostEstimate(
                flops=6 * n_loc * blk * width * hid, transcendentals=0,
                bytes_accessed=12 * n_loc * width * hid + 4 * n_loc * blk * width + 6 * n_loc * blk * hid,
            ),
        )(xe, de, h, da, db, act_out, grad_router.reshape(n_loc, n_exp // n_loc, width))
        return act_out, grad_in, grad_wa, grad_wb, grad_wc, grad_router.reshape(n_exp, width).T

    return jax.shard_map(
        local_step,
        mesh=mesh,
        in_specs=(P("ep", None), P(), P("ep"), P("ep"), P("ep", None, "tp"), P("ep", None, "tp"), P("ep", "tp", None), P("ep", None)),
        out_specs=(P("ep", None), P("ep", None), P("ep", None, "tp"), P("ep", None, "tp"), P("ep", "tp", None), P()),
        check_vma=False,
    )
```
